32 devices in a mesh: px: 4 (over x, core), py: 8 (over z, y).
Axes of the slice: x: 2, y: 2, z: 4, core: 2. Of those that a mesh axis runs over, the one named last changes fastest.
Arguments:
- root_density: float32 [384, 384, 384], P('px', 'py'), may hold values from -6 to 6
- subgrid_density: float32 [256, 32, 1024], P(('px', 'py')), may hold values from -24 to 24
- velocity: float32 [3, 256, 32, 1024], P(None, ('px', 'py')), may hold values from -6 to 6
- slot_anchor: int32 [3, 256], replicated, may hold values from 0 to 376, as said below
- slot_count: int32 [32], replicated, may hold values from 1 to 8, as said below
- neighbour: int32 [2, 256], replicated, may hold values from -1 to 255, as said below
Outputs:
- coarse_potential: float32 [384, 384, 384], P('px', 'py')
- subgrid_potential: float32 [256, 32, 1024], P(('px', 'py'))
- kicked_velocity: float32 [3, 256, 32, 1024], P(None, ('px', 'py'))
The draws below stay inside these ranges and needn't reach their ends.
Inputs may be any that keep to these rules, and one draw needn't show every extreme that they name: Slot j of device d is slot d * 8 + j, devices numbered in the order of px+py; it is live when j < slot_count[d]. Some device has every slot live. `slot_anchor`: entries are multiples of 8; live slots cover distinct regions of 8^3 root cells; empty slots hold 0. The region of live slot j of the device at px = p, py = q has its lower corner among the root cells that the device at px = p, py = (q + j) mod 8 holds of root_density. neighbour[0, s] is s - 8 or -1 and neighbour[1, s] is s + 8 or -1, the same slot of the device one index lower or higher along py with the same px; where set, both slots are live and the two regions lie next to each other along the second dimension, the lower one below. Empty slots hold -1.
All inputs are finite; a program needn't handle non-finite values.
Results may differ from the reference program's by a relative error of at most 0.000094.
Values sent between devices are 32-bit elements; how exact they have to be, the bound alone decides.
A program may use at most 192 MiB of HBM per device.

```python
import jax
import jax.numpy as jnp
from jax import lax

NR = 384
REG = 8
REF = 4
SWEEPS = 4
SUBGRID_CELLS = 32
DEVICE_SLOTS = 8
TOTAL_SLOTS = 256
DEVICES = 32


def slot_layout(key):
    base_key = jax.random.fold_in(key, 4021)
    count_key, busy_key, place_key, shift_random_key, border_key, face_side_key = jax.random.split(base_key, 6)
    rows_px = DEVICES // DEVICE_SLOTS
    wave_band = NR // DEVICE_SLOTS // REG
    first_band = NR // rows_px // REG
    third_band = NR // REG
    counts = jax.random.randint(count_key, (DEVICES,), 1, DEVICE_SLOTS + 1, dtype=jnp.int32)
    busiest = jax.random.permutation(busy_key, DEVICES)[:2]
    counts = counts.at[busiest].set(DEVICE_SLOTS)
    row_keys = jax.random.split(place_key, rows_px)
    picks = jax.vmap(lambda row_key: jax.random.permutation(row_key, first_band * third_band)[:DEVICE_SLOTS])(row_keys)
    picks = picks.astype(jnp.int32)
    slot_numbers = jnp.arange(TOTAL_SLOTS, dtype=jnp.int32)
    owners = slot_numbers // DEVICE_SLOTS
    within = slot_numbers % DEVICE_SLOTS
    row_place = owners // DEVICE_SLOTS
    column_place = owners % DEVICE_SLOTS
    live_mask = within < counts[owners]
    pair = picks[row_place, within]
    first = row_place * first_band + pair // third_band
    third = pair % third_band
    source_column = (column_place + within) % DEVICE_SLOTS
    constant_shift = jax.random.randint(shift_random_key, (TOTAL_SLOTS,), 0, wave_band, dtype=jnp.int32)
    border_face = jax.random.randint(border_key, (TOTAL_SLOTS,), 0, 2, dtype=jnp.int32)
    face_side = jax.random.randint(face_side_key, (TOTAL_SLOTS,), 0, 2, dtype=jnp.int32)
    offset = jnp.where(border_face == 1, face_side * (wave_band - 1), constant_shift)
    second = source_column * wave_band + offset
    anchor = jnp.stack([first * REG, second * REG, third * REG]).astype(jnp.int32)
    anchor = jnp.where(live_mask[None, :], anchor, 0)
    upper_neighbour_slot = jnp.minimum(slot_numbers + DEVICE_SLOTS, TOTAL_SLOTS - 1)
    has_upper = live_mask & (column_place < DEVICE_SLOTS - 1) & live_mask[upper_neighbour_slot] & (offset == wave_band - 1) & (offset[upper_neighbour_slot] == 0) & (source_column < DEVICE_SLOTS - 1)
    lower_id = jnp.maximum(slot_numbers - DEVICE_SLOTS, 0)
    has_lower = live_mask & (column_place > 0) & live_mask[lower_id] & (offset[lower_id] == wave_band - 1) & (offset == 0) & (source_column[lower_id] < DEVICE_SLOTS - 1)
    upper_slot = jnp.where(has_upper, slot_numbers + DEVICE_SLOTS, -1)
    lower_slot = jnp.where(has_lower, slot_numbers - DEVICE_SLOTS, -1)
    return (anchor, counts.astype(jnp.int32), jnp.stack([lower_slot, upper_slot]).astype(jnp.int32))


def draw_slot_anchor(key, part):
    return slot_layout(key)[0]


def draw_slot_count(key, part):
    return slot_layout(key)[1]


def draw_neighbour(key, part):
    return slot_layout(key)[2]


def draw_root_density(key, part):
    density = jnp.clip(jax.random.normal(jax.random.fold_in(key, 77), (NR, NR, NR), jnp.float32), -6.0, 6.0)
    return density


def steps_of(stream_key, shape, shards, least, high):
    gain = 1.0
    for position, parts in shards:
        steps = jax.random.uniform(jax.random.fold_in(jax.random.fold_in(stream_key, 6), position), (parts,), jnp.float32, least / len(shards), high / len(shards))
        gain = gain * jnp.repeat(jnp.exp(steps), shape[position] // parts).reshape((-1,) + (1,) * (len(shape) - 1 - position))
    return gain


def noise(own_key, extent, spread, most, cuts=(), kind=jnp.bfloat16):
    entries = spread * jax.random.normal(own_key, extent, jnp.float32)
    if cuts:
        entries = entries * steps_of(own_key, extent, cuts, -0.22, 0.18)
    return jnp.clip(entries, -most, most).astype(kind)


def setup_inputs(seed: int = 0) -> dict:
    key_of = jax.random.split(jax.random.key(seed), 7)
    root_density = draw_root_density(jax.random.fold_in(key_of[6], 71), 0)
    subgrid_density = noise(key_of[1], (TOTAL_SLOTS, SUBGRID_CELLS, SUBGRID_CELLS * SUBGRID_CELLS), 4.0, 24.0, ((0, 32),), jnp.float32)
    velocity = noise(key_of[2], (3, TOTAL_SLOTS, SUBGRID_CELLS, SUBGRID_CELLS * SUBGRID_CELLS), 1.0, 6.0, ((1, 32),), jnp.float32)
    slot_anchor = draw_slot_anchor(jax.random.fold_in(key_of[6], 71), 0)
    slot_count = draw_slot_count(jax.random.fold_in(key_of[6], 71), 0)
    neighbour = draw_neighbour(jax.random.fold_in(key_of[6], 71), 0)
    return {"root_density": root_density, "subgrid_density": subgrid_density, "velocity": velocity, "slot_anchor": slot_anchor, "slot_count": slot_count, "neighbour": neighbour}


HIGHEST_PRECISION = lax.Precision.HIGHEST
RELAXATION = 6.0 / 7.0


def eigenvalue(wavenumber):
    return -4.0 * jnp.sin((jnp.pi / NR) * wavenumber.astype(jnp.float32)) ** 2


def green_block(wave_first, wave_second, wave_third):
    total = eigenvalue(wave_first)[:, None, None] + eigenvalue(wave_second)[None, :, None] + eigenvalue(wave_third)[None, None, :]
    zero_mode = (wave_first[:, None, None] == 0) & (wave_second[None, :, None] == 0) & (wave_third[None, None, :] == 0)
    safe_total = jnp.where(zero_mode, -1.0, total)
    return jnp.where(zero_mode, 0.0, 1.0 / safe_total)


def weights_table():
    cells = jnp.arange(REG * REF + 2, dtype=jnp.int32)
    marks = 2 * cells - 1 + REF
    lower_cell = jnp.minimum(marks // (2 * REF), REG)
    fraction = (marks - 2 * REF * lower_cell).astype(jnp.float32) / (2 * REF)
    columns = jnp.arange(REG + 2, dtype=jnp.int32)
    return (jnp.where(columns[None, :] == lower_cell[:, None], 1.0 - fraction[:, None], 0.0)
            + jnp.where(columns[None, :] == lower_cell[:, None] + 1, fraction[:, None], 0.0))


def interpolate(patch, matrix):
    step_one = jnp.einsum("sabc,kc->sabk", patch, matrix, precision=HIGHEST_PRECISION)
    step_two = jnp.einsum("sabk,jb->sajk", step_one, matrix, precision=HIGHEST_PRECISION)
    return jnp.einsum("sajk,ia->sijk", step_two, matrix, precision=HIGHEST_PRECISION)


def extend(coarse, interior, below_face, above_face, use_below, use_above):
    grown = coarse.at[:, 1:-1, 1:-1, 1:-1].set(interior)
    grown = grown.at[:, 1:-1, 0, 1:-1].set(jnp.where(use_below[:, None, None], below_face, grown[:, 1:-1, 0, 1:-1]))
    grown = grown.at[:, 1:-1, -1, 1:-1].set(jnp.where(use_above[:, None, None], above_face, grown[:, 1:-1, -1, 1:-1]))
    return grown


def relax(grown, interior, density):
    beside_all = (grown[:, 2:, 1:-1, 1:-1] + grown[:, :-2, 1:-1, 1:-1]
              + grown[:, 1:-1, 2:, 1:-1] + grown[:, 1:-1, :-2, 1:-1]
              + grown[:, 1:-1, 1:-1, 2:] + grown[:, 1:-1, 1:-1, :-2])
    return (1.0 - RELAXATION) * interior + RELAXATION * (beside_all - density * (1.0 / (REF * REF))) / 6.0


def kick(grown, velocity, live_mask):
    scale_factor = REF / 2.0
    slope_first = (grown[:, 2:, 1:-1, 1:-1] - grown[:, :-2, 1:-1, 1:-1]) * scale_factor
    slope_second = (grown[:, 1:-1, 2:, 1:-1] - grown[:, 1:-1, :-2, 1:-1]) * scale_factor
    slope_third = (grown[:, 1:-1, 1:-1, 2:] - grown[:, 1:-1, 1:-1, :-2]) * scale_factor
    velocity_after_kick = velocity - jnp.stack([slope_first, slope_second, slope_third])
    return jnp.where(live_mask[None, :, None, None, None], velocity_after_kick, 0.0)


def reference(root_density, subgrid_density, velocity, slot_anchor, slot_count, neighbour):
    subgrid_cells = subgrid_density.reshape(TOTAL_SLOTS, SUBGRID_CELLS, SUBGRID_CELLS, SUBGRID_CELLS)
    cell_velocity = velocity.reshape(3, TOTAL_SLOTS, SUBGRID_CELLS, SUBGRID_CELLS, SUBGRID_CELLS)
    every_wave = jnp.arange(NR, dtype=jnp.int32)
    factor = green_block(every_wave, every_wave, every_wave)
    coarse_potential = jnp.real(jnp.fft.ifftn(jnp.fft.fftn(root_density) * factor)).astype(jnp.float32)
    slot_numbers = jnp.arange(TOTAL_SLOTS, dtype=jnp.int32)
    live_mask = (slot_numbers % DEVICE_SLOTS) < slot_count[slot_numbers // DEVICE_SLOTS]
    offsets = jnp.arange(REG + 2, dtype=jnp.int32)
    index_first = (slot_anchor[0][:, None] - 1 + offsets[None, :]) % NR
    index_second = (slot_anchor[1][:, None] - 1 + offsets[None, :]) % NR
    index_third = (slot_anchor[2][:, None] - 1 + offsets[None, :]) % NR
    patch = coarse_potential[index_first[:, :, None, None], index_second[:, None, :, None], index_third[:, None, None, :]]
    coarse = interpolate(patch, weights_table())
    interior = coarse[:, 1:-1, 1:-1, 1:-1]
    below_slot = jnp.maximum(neighbour[0], 0)
    above_slot = jnp.maximum(neighbour[1], 0)
    grown = coarse
    for sweep_index in range(SWEEPS + 1):
        grown = extend(coarse, interior, interior[below_slot, :, -1, :], interior[above_slot, :, 0, :],
                       neighbour[0] >= 0, neighbour[1] >= 0)
        if sweep_index < SWEEPS:
            interior = relax(grown, interior, subgrid_cells)
    subgrid_potential = jnp.where(live_mask[:, None, None, None], interior, 0.0)
    velocity_after_kick = kick(grown, cell_velocity, live_mask)
    return (coarse_potential, subgrid_potential.reshape(TOTAL_SLOTS, SUBGRID_CELLS, SUBGRID_CELLS * SUBGRID_CELLS),
            velocity_after_kick.reshape(3, TOTAL_SLOTS, SUBGRID_CELLS, SUBGRID_CELLS * SUBGRID_CELLS))
```

```python
import jax
import jax.numpy as jnp
import numpy as np
from jax import lax
from jax.experimental import pallas as pl
from jax.experimental.pallas import tpu as pltpu
from jax.sharding import PartitionSpec as P

NR = 384
REG = 8
REF = 4
SWEEPS = 4
CELLS = REG * REF
EDGE = SWEEPS
LAYERS = CELLS + 2 * EDGE
WIDE = LAYERS * CELLS
RELAXATION = 6.0 / 7.0
HIGHEST = lax.Precision.HIGHEST
HIGH = lax.Precision.HIGH
F32 = jnp.float32


def fourier_basis(length):
    cell = np.arange(length)
    rows = []
    for k in range(length):
        if k in (0, length // 2):
            rows.append(np.cos(2 * np.pi * (k * cell % length) / length) / np.sqrt(length))
        elif k < length // 2:
            rows.append(np.cos(2 * np.pi * (k * cell % length) / length) * np.sqrt(2 / length))
        else:
            rows.append(
                np.sin(2 * np.pi * ((length - k) * cell % length) / length) * np.sqrt(2 / length)
            )
    return np.stack(rows)


def strip_basis(cells):
    place = np.arange(cells) - (cells - 1) / 2
    mode = 2 * np.arange(cells // 2) + 1
    angle = np.pi * mode[:, None] * place[None, :] / cells
    basis = np.concatenate([np.cos(angle), np.sin(angle)]) * np.sqrt(2 / cells)
    eig = 4 * np.sin(np.pi * mode / (2 * cells)) ** 2
    return basis, np.concatenate([eig, eig])


def strip_coupling(count, rows):
    basis = fourier_basis(count)
    turn = np.zeros((count, count))
    theta = 2 * np.pi * np.arange(count) / count
    for k in range(1, (count + 1) // 2):
        turn[k, count - k] = np.sin(theta[k])
        turn[count - k, k] = -np.sin(theta[k])
    wide = lambda matrix: np.kron(matrix, np.eye(rows))
    mixes = np.stack([wide(basis), wide(turn @ basis), wide(basis.T)])
    half_sine = np.sin(theta / 2) ** 2
    factors = np.stack([half_sine, 4 * (1 - half_sine)])
    return mixes, np.repeat(factors, rows, axis=1)[:, :, None]


def axis_weights(cells, first, count):
    table = np.zeros((len(cells), count))
    for row, cell in enumerate(cells):
        mark = 2 * cell - 1 + REF
        low = mark // (2 * REF)
        frac = (mark - 2 * REF * low) / (2 * REF)
        table[row, low - first] += 1 - frac
        if frac:
            table[row, low + 1 - first] += frac
    return table


PATCH_X = REG + 2
PATCH_Y = REG + 4
PATCH_Z = REG + 2


def patch_tables():
    inner = np.arange(1, CELLS + 1)
    x_side = axis_weights(np.concatenate([inner, [0, CELLS + 1]]), 0, PATCH_X)
    x_table = np.zeros((CELLS + 8, 16))
    x_table[: CELLS + 2, :PATCH_X] = x_side
    y_cells = np.arange(1 - EDGE, CELLS + EDGE + 1)
    y_side = axis_weights(y_cells, -1, PATCH_Y)
    y_out = axis_weights(np.array([-EDGE, CELLS + EDGE + 1]), -1, PATCH_Y)
    z_side = axis_weights(np.arange(CELLS + 2), 0, PATCH_Z)
    z_edge = np.zeros((CELLS, PATCH_Z))
    z_edge[0] = z_side[0]
    z_edge[-1] = z_side[-1]
    y_edge = np.zeros((LAYERS, PATCH_Y))
    y_edge[0] = y_out[0]
    y_edge[-1] = y_out[1]

    def both(ys, zs):
        return np.einsum("jb,kc->bcjk", ys, zs).reshape(PATCH_Y * PATCH_Z, WIDE)

    table = np.zeros((128, 3 * WIDE))
    table[: PATCH_Y * PATCH_Z] = np.concatenate(
        [both(y_side, z_side[1:-1]), both(y_side, z_edge), both(y_edge, z_side[1:-1])], axis=1
    )
    return x_table.astype(np.float32), table.astype(np.float32)


def from_behind(value, axis, steps):
    count = lax.axis_size(axis)
    initial, last = (max(0, -steps), min(count, count - steps))
    return lax.ppermute(value, axis, [(source, source + steps) for source in range(initial, last)])


def extended(block, axis, dim, width):
    count = lax.axis_size(axis)
    forward = [(i, (i + 1) % count) for i in range(count)]
    backward = [(target, source) for source, target in forward]
    low = lax.ppermute(
        lax.slice_in_dim(block, block.shape[dim] - width, None, axis=dim), axis, forward
    )
    high = lax.ppermute(lax.slice_in_dim(block, 0, width, axis=dim), axis, backward)
    return jnp.concatenate([low, block, high], axis=dim)


def decay(delta):
    return 1.0 / (1.0 + 0.5 * delta + jnp.sqrt(delta + 0.25 * delta * delta))


def power(value, exponent):
    result = None
    while exponent:
        if exponent & 1:
            result = value if result is None else result * value
        exponent >>= 1
        if exponent:
            value = value * value
    return result


def grid_kernel(
    sizes,
    f_ref,
    eig_b_ref,
    eig_ref,
    own_ref,
    vec_ref,
    basis_ref,
    mix_ref,
    angle_ref,
    out_ref,
    held,
    lines,
    sent,
    got,
    answer,
    back,
    mom_one,
    mom_two,
    part,
    table,
    weight,
    send_one,
    recv_one,
    send_two,
    recv_two,
    send_line,
    recv_line,
    send_back,
    recv_back,
    self_sem,
):
    count_first, count_second, owners = sizes
    devices = count_first * count_second
    rows, strip, wave = f_ref.shape
    groups = strip // 8
    half = strip // 2
    chunk = sent.shape[0] // owners
    width = lines.shape[0]
    mesh = pl.DeviceIdType.MESH
    place_first = lax.axis_index("px")
    place_second = lax.axis_index("py")
    me = place_first * count_second + place_second
    barrier = pltpu.get_barrier_semaphore()

    def greet(step, carry):
        other = lax.rem(me + step, devices)
        pl.semaphore_signal(
            barrier,
            inc=1,
            device_id=(other // count_second, lax.rem(other, count_second)),
            device_id_type=mesh,
        )
        return carry

    lax.fori_loop(1, devices, greet, 0)

    def split(value):
        return tuple(value[8 * g : 8 * g + 8] for g in range(groups))

    r_all = decay(eig_b_ref[...] + eig_ref[...])
    scale_all = -r_all / ((1.0 - r_all) * (1.0 + r_all))
    ratio = power(r_all, rows)
    norm = 1.0 / (1.0 - power(ratio, count_first))
    weight[0] = r_all
    weight[1] = scale_all
    weight[2] = 2.0 * vec_ref[0] * scale_all
    weight[3] = -2.0 * vec_ref[1] * scale_all
    r = split(r_all)
    zeros = tuple(jnp.zeros((8, wave), F32) for _ in range(groups))
    even_groups = [g for g in range(groups) if 8 * g < half]
    odd_groups = [g for g in range(groups) if 8 * g + 8 > half]

    table[...] = jnp.zeros_like(table)
    for i in range(count_first):
        block = basis_ref[i * rows : (i + 1) * rows, :]
        table[i, :rows, :wave] = block
        table[i, rows : 2 * rows, wave:] = block

    def row_of(ref, i):
        return tuple(ref[i, 8 * g : 8 * g + 8, :] for g in range(groups))

    def up_first(i, carry):
        up, total = carry
        f = row_of(f_ref, i)
        up = tuple(r[g] * up[g] + f[g] for g in range(groups))
        return up, tuple(total[g] + f[g] for g in range(groups))

    def down_first(i, down):
        f = row_of(f_ref, rows - 1 - i)
        return tuple(r[g] * down[g] + f[g] for g in range(groups))

    up, total = lax.fori_loop(0, rows, up_first, (zeros, zeros))
    down = lax.fori_loop(0, rows, down_first, zeros)
    for g in range(groups):
        mom_one[0, 0, 8 * g : 8 * g + 8, :] = up[g]
        mom_one[0, 1, 8 * g : 8 * g + 8, :] = down[g]
    whole = jnp.concatenate(total, axis=0)

    def shares(buffer, send, recv):
        return [
            pltpu.make_async_remote_copy(
                src_ref=buffer.at[0],
                dst_ref=buffer.at[d],
                send_sem=send.at[d],
                recv_sem=recv.at[d],
                device_id=(lax.rem(place_first + d, count_first), place_second),
                device_id_type=mesh,
            )
            for d in range(1, count_first)
        ]

    def carries(buffer):
        up = jnp.zeros((strip, wave), F32)
        down = jnp.zeros((strip, wave), F32)
        for d in [0] + list(range(count_first - 1, 0, -1)):
            up = ratio * up + buffer[d, 0]
        for d in range(count_first):
            down = ratio * down + buffer[d, 1]
        return split(up * norm), split(down * norm)

    pl.semaphore_wait(barrier, devices - 1)
    first = shares(mom_one, send_one, recv_one)
    for copy in first:
        copy.start()
    lines[2 * rows :, :] = jnp.zeros((width - 2 * rows, wave), F32)
    lines[2 * rows : 2 * rows + 1, :] = jnp.sum(vec_ref[2] * whole, axis=0, keepdims=True)
    lines[2 * rows + 1 : 2 * rows + 2, :] = jnp.sum(vec_ref[3] * whole, axis=0, keepdims=True)
    for copy in first:
        copy.wait()
    carry_up, carry_down = carries(mom_one)

    def weighed(which, members, value):
        total = None
        for g in members:
            term = weight[which, 8 * g : 8 * g + 8, :] * value[g]
            total = term if total is None else total + term
        return total

    def up_lines(i, up):
        f = row_of(f_ref, i)
        up = tuple(r[g] * up[g] + f[g] for g in range(groups))
        part[0, i] = weighed(2, even_groups, up)
        part[1, i] = weighed(3, odd_groups, up)
        return up

    def down_lines(step, down):
        i = rows - 1 - step
        f = row_of(f_ref, i)
        down = tuple(r[g] * down[g] for g in range(groups))
        part[0, i] += weighed(2, even_groups, down)
        part[1, i] += weighed(3, odd_groups, down)
        return tuple(down[g] + f[g] for g in range(groups))

    lax.fori_loop(0, rows, up_lines, carry_up)
    lax.fori_loop(0, rows, down_lines, carry_down)
    lines[:rows, :] = jnp.sum(part[0], axis=1)
    lines[rows : 2 * rows, :] = jnp.sum(part[1], axis=1)
    sent[...] = lines[...].T

    def line_copy(o):
        return pltpu.make_async_remote_copy(
            src_ref=sent.at[pl.ds(o * chunk, chunk)],
            dst_ref=got.at[me],
            send_sem=send_line.at[o],
            recv_sem=recv_line.at[me],
            device_id=(o // count_second, lax.rem(o, count_second)),
            device_id_type=mesh,
        )

    def line_from(d):
        return pltpu.make_async_remote_copy(
            src_ref=sent.at[pl.ds(0, chunk)],
            dst_ref=got.at[d],
            send_sem=self_sem.at[1],
            recv_sem=recv_line.at[d],
            device_id=(d // count_second, lax.rem(d, count_second)),
            device_id_type=mesh,
        )

    def back_copy(d):
        return pltpu.make_async_remote_copy(
            src_ref=answer.at[d],
            dst_ref=back.at[pl.ds(me * chunk, chunk)],
            send_sem=send_back.at[d],
            recv_sem=recv_back.at[me],
            device_id=(d // count_second, lax.rem(d, count_second)),
            device_id_type=mesh,
        )

    def back_from(o):
        return pltpu.make_async_remote_copy(
            src_ref=answer.at[0],
            dst_ref=back.at[pl.ds(o * chunk, chunk)],
            send_sem=self_sem.at[1],
            recv_sem=recv_back.at[o],
            device_id=(o // count_second, lax.rem(o, count_second)),
            device_id_type=mesh,
        )

    def over(count, action):
        def body(k, carry):
            @pl.when(k != me)
            def _():
                action(k)

            return carry

        lax.fori_loop(0, count, body, 0)

    over(owners, lambda o: line_copy(o).start())

    @pl.when(me < owners)
    def _():
        own = pltpu.make_async_copy(
            sent.at[pl.ds(me * chunk, chunk)], got.at[me], self_sem.at[0]
        )
        own.start()
        over(devices, lambda d: line_from(d).wait_recv())
        own.wait()
        modes = None
        for i in range(count_first):
            piece = got[i * count_second : (i + 1) * count_second]
            piece = piece.reshape(count_second * chunk, width)
            term = jnp.dot(piece, table[i], precision=HIGHEST, preferred_element_type=F32)
            modes = term if modes is None else modes + term
        straight = jnp.dot(mix_ref[0], modes, precision=HIGHEST, preferred_element_type=F32)
        turned = jnp.dot(mix_ref[1], modes, precision=HIGHEST, preferred_element_type=F32)
        s, t = straight[:, :wave], straight[:, wave:]
        s_turned, t_turned = turned[:, :wave], turned[:, wave:]
        own_eig = own_ref[...]
        lam = own_eig + eig_ref[...]
        sinh = jnp.sqrt(lam + 0.25 * lam * lam)
        flat = lam <= 0.0
        far = power(decay(lam), strip)
        tanh = (1.0 - far) / (1.0 + far)
        green = jnp.where(flat, strip / 4.0, tanh / jnp.where(flat, 1.0, 2.0 * sinh))
        square = tanh * tanh
        half_sine = angle_ref[0]
        det = half_sine * (1.0 - square) + square
        zero = flat & (half_sine <= 0.0)
        inverse = 1.0 / jnp.where(zero, 1.0, det)
        gain = angle_ref[1] * green * inverse
        sums = jnp.sum(got[...], axis=0)
        lane = lax.broadcasted_iota(jnp.int32, sums.shape, 1)
        sigma = jnp.sum(jnp.where(lane == 2 * rows, sums, 0.0), axis=1, keepdims=True)
        lever = jnp.sum(jnp.where(lane == 2 * rows + 1, sums, 0.0), axis=1, keepdims=True)
        k = np.arange(strip)
        bow = 0.5 * (k * k - (strip - 1) * k) - strip / 4
        mean = jnp.where(own_eig[:chunk] <= 0.0, sigma, 0.0) * (1.0 / (wave * wave))
        gauge = lever - mean * float(wave * count_second * bow.sum())
        gauge = gauge * float(1.0 / (bow[0] * np.sqrt(wave * count_second)))
        tall = lambda value: jnp.concatenate([value] * count_second, axis=0)
        mean, gauge = tall(mean), tall(gauge)
        new_s = gain * (2.0 + 0.5 * lam) * s - t_turned * inverse
        new_t = gain * (0.5 * lam) * t - s_turned * inverse
        new_s = jnp.where(zero, gauge, new_s)
        new_t = jnp.where(zero, (2.0 / strip) * t, new_t)
        solved = jnp.concatenate([new_s, new_t], axis=1)
        solved = jnp.dot(mix_ref[2], solved, precision=HIGHEST, preferred_element_type=F32)
        wide = lax.broadcasted_iota(jnp.int32, (count_second * chunk, width), 1)
        for i in range(count_first):
            piece = lax.dot_general(
                solved,
                table[i],
                (((1,), (1,)), ((), ())),
                precision=HIGHEST,
                preferred_element_type=F32,
            )
            piece = jnp.where(wide == 2 * rows, mean, piece)
            answer[i * count_second : (i + 1) * count_second] = piece.reshape(
                count_second, chunk, width
            )
        over(devices, lambda d: back_copy(d).start())
        kept = pltpu.make_async_copy(
            answer.at[me], back.at[pl.ds(me * chunk, chunk)], self_sem.at[0]
        )
        kept.start()
        kept.wait()

    over(owners, lambda o: back_from(o).wait_recv())
    lines[...] = back[...].T
    mean_term = vec_ref[2] * lines[2 * rows : 2 * rows + 1, :]
    weight[2] = mean_term

    def up_second(i, up):
        f = row_of(f_ref, i)
        line_s = lines[pl.ds(i, 1), :]
        line_t = lines[pl.ds(rows + i, 1), :]
        fresh = []
        for g in range(groups):
            window = slice(8 * g, 8 * g + 8)
            value = f[g] - weight[2, window, :]
            if g in even_groups:
                value = value - vec_ref[0, window, :] * line_s
            if g in odd_groups:
                value = value - vec_ref[1, window, :] * line_t
            held[i, window, :] = value
            fresh.append(value)
        return tuple(r[g] * up[g] + fresh[g] for g in range(groups))

    def down_second(i, down):
        f = row_of(held, rows - 1 - i)
        return tuple(r[g] * down[g] + f[g] for g in range(groups))

    up = lax.fori_loop(0, rows, up_second, zeros)
    down = lax.fori_loop(0, rows, down_second, zeros)
    for g in range(groups):
        mom_two[0, 0, 8 * g : 8 * g + 8, :] = up[g]
        mom_two[0, 1, 8 * g : 8 * g + 8, :] = down[g]
    second = shares(mom_two, send_two, recv_two)
    for copy in second:
        copy.start()
    over(owners, lambda o: line_copy(o).wait_send())

    @pl.when(me < owners)
    def _():
        over(devices, lambda d: back_copy(d).wait_send())

    for copy in second:
        copy.wait()
    carry_up, carry_down = carries(mom_two)

    def up_last(i, up):
        f = row_of(held, i)
        up = tuple(r[g] * up[g] + f[g] for g in range(groups))
        for g in range(groups):
            out_ref[i, 8 * g : 8 * g + 8, :] = up[g]
        return up

    def down_last(step, down):
        i = rows - 1 - step
        f = row_of(held, i)
        down = tuple(r[g] * down[g] for g in range(groups))
        for g in range(groups):
            window = slice(8 * g, 8 * g + 8)
            out_ref[i, window, :] = (out_ref[i, window, :] + down[g]) * weight[1, window, :]
        return tuple(down[g] + f[g] for g in range(groups))

    lax.fori_loop(0, rows, up_last, carry_up)
    lax.fori_loop(0, rows, down_last, carry_down)


def subgrid_kernel(
    flag_ref, patch_ref, xt_ref, yz_ref, mid_ref, low_ref, high_ref, vel_ref, pot_ref, kick_ref
):
    slot = pl.program_id(0)
    live = flag_ref[0, slot] > 0
    has_below = flag_ref[1, slot] > 0
    has_above = flag_ref[2, slot] > 0
    back_below = flag_ref[3, slot] > 0
    back_above = flag_ref[4, slot] > 0
    planes = jnp.dot(patch_ref[0], yz_ref[...], precision=HIGHEST, preferred_element_type=F32)
    coarse = jnp.dot(xt_ref[...], planes, precision=HIGHEST, preferred_element_type=F32)
    start = coarse[:CELLS, :WIDE]
    x_low = coarse[CELLS : CELLS + 1, :WIDE]
    x_high = coarse[CELLS + 1 : CELLS + 2, :WIDE]
    z_edge = coarse[:CELLS, WIDE : 2 * WIDE]
    y_edge = coarse[:CELLS, 2 * WIDE :]
    shape = (CELLS, WIDE)
    row = lax.broadcasted_iota(jnp.int32, shape, 0)
    lane = lax.broadcasted_iota(jnp.int32, shape, 1)
    third = lane % CELLS
    side = EDGE * CELLS
    end = WIDE - side
    y_above = jnp.where(lane >= WIDE - CELLS, y_edge, pltpu.roll(start, WIDE - CELLS, 1))
    y_below = jnp.where(lane < CELLS, y_edge, pltpu.roll(start, CELLS, 1))
    cut_above = (lane >= WIDE - CELLS) | (
        (lane >= side - CELLS) & (lane < side) & jnp.logical_not(back_below)
    )
    cut_below = (lane < CELLS) | (
        (lane >= end) & (lane < end + CELLS) & jnp.logical_not(back_above)
    )
    fixed = ((lane < side) & jnp.logical_not(has_below)) | (
        (lane >= end) & jnp.logical_not(has_above)
    )
    rho = jnp.concatenate([low_ref[0], mid_ref[0], high_ref[0]], axis=1) * (1.0 / (REF * REF))

    def beside(v):
        return (
            (
                jnp.where(row == 0, x_low, pltpu.roll(v, 1, 0)),
                jnp.where(row == CELLS - 1, x_high, pltpu.roll(v, CELLS - 1, 0)),
            ),
            (
                jnp.where(cut_below, y_below, pltpu.roll(v, CELLS, 1)),
                jnp.where(cut_above, y_above, pltpu.roll(v, WIDE - CELLS, 1)),
            ),
            (
                jnp.where(third == 0, z_edge, pltpu.roll(v, 1, 1)),
                jnp.where(third == CELLS - 1, z_edge, pltpu.roll(v, WIDE - 1, 1)),
            ),
        )

    v = start
    for _ in range(SWEEPS):
        first, second, last = beside(v)
        total = first[1] + first[0] + second[1] + second[0] + last[1] + last[0]
        new = (1.0 - RELAXATION) * v + RELAXATION * (total - rho) / 6.0
        v = jnp.where(fixed, v, new)
    pot_ref[0] = jnp.where(live, v[:, side:end], 0.0)
    for q, (below, above) in enumerate(beside(v)):
        slope = (above[:, side:end] - below[:, side:end]) * (REF / 2.0)
        kick_ref[q, 0] = jnp.where(live, vel_ref[q, 0] - slope, 0.0)


def poisson(root_density):
    count_first = lax.axis_size("px")
    count_second = lax.axis_size("py")
    devices = count_first * count_second
    device = lax.axis_index("px") * count_second + lax.axis_index("py")
    rows, strip, wave = root_density.shape
    chunk = next(q for q in range(8, wave + 1, 8) if wave % q == 0 and wave // q <= devices)
    owners = wave // chunk
    width = -(-(2 * rows + 2) // 128) * 128
    basis = fourier_basis(wave)
    strip_table, strip_eig = strip_basis(strip)
    eig = 4.0 * np.sin(np.pi / wave * np.arange(wave)) ** 2
    mixes, angles = strip_coupling(count_second, chunk)
    cell = np.arange(strip)
    bow = 0.5 * (cell * cell - (strip - 1) * cell) - strip / 4
    lower = cell < strip // 2
    edge = strip_table[:, 0]
    vectors = np.stack(
        [
            np.where(lower, edge, 0.0),
            np.where(lower, 0.0, edge),
            strip_table.sum(1),
            strip_table @ bow,
        ]
    )[:, :, None]
    own = lax.rem(device, owners) * chunk
    own_eig = lax.dynamic_slice_in_dim(jnp.asarray(eig, F32), own, chunk)
    own_eig = jnp.tile(own_eig, count_second)[:, None]
    z_basis = jnp.asarray(basis, F32)
    y_basis = jnp.asarray(strip_table, F32)
    f = jnp.einsum("xyz,cz->xyc", root_density, z_basis, precision=HIGH)
    f = jnp.einsum("xyc,by->xbc", f, y_basis, precision=HIGH)
    moment = pltpu.VMEM((count_first, 2, strip, wave), F32)
    dma = pltpu.SemaphoreType.DMA
    u = pl.pallas_call(
        lambda *refs: grid_kernel((count_first, count_second, owners), *refs),
        in_specs=[pl.BlockSpec(memory_space=pltpu.VMEM)] * 8,
        out_specs=pl.BlockSpec(memory_space=pltpu.VMEM),
        out_shape=jax.ShapeDtypeStruct((rows, strip, wave), F32),
        scratch_shapes=[
            pltpu.VMEM((rows, strip, wave), F32),
            pltpu.VMEM((width, wave), F32),
            pltpu.VMEM((wave, width), F32),
            pltpu.VMEM((devices, chunk, width), F32),
            pltpu.VMEM((devices, chunk, width), F32),
            pltpu.VMEM((wave, width), F32),
            moment,
            moment,
            pltpu.VMEM((2, rows, 8, wave), F32),
            pltpu.VMEM((count_first, width, 2 * wave), F32),
            pltpu.VMEM((4, strip, wave), F32),
            dma((count_first,)),
            dma((count_first,)),
            dma((count_first,)),
            dma((count_first,)),
            dma((owners,)),
            dma((devices,)),
            dma((devices,)),
            dma((owners,)),
            dma((2,)),
        ],
        compiler_params=pltpu.CompilerParams(
            collective_id=1, has_side_effects=True, vmem_limit_bytes=60 * 1024 * 1024
        ),
    )(
        f,
        jnp.asarray(strip_eig[:, None], F32),
        jnp.asarray(eig[None, :], F32),
        own_eig,
        jnp.asarray(vectors, F32),
        jnp.asarray(basis.T, F32),
        jnp.asarray(mixes, F32),
        jnp.asarray(angles, F32),
    )
    u = jnp.einsum("xbc,by->xyc", u, y_basis, precision=HIGH)
    return jnp.einsum("xyc,cz->xyz", u, z_basis, precision=HIGH)


def local(root_density, subgrid_density, velocity, slot_anchor, slot_count, neighbour):
    first_rows, second_rows = root_density.shape[:2]
    size_second = lax.axis_size("py")
    place_first = lax.axis_index("px")
    place_second = lax.axis_index("py")
    device = place_first * size_second + place_second
    per_device = subgrid_density.shape[0]
    side = EDGE * CELLS
    inner = CELLS * CELLS
    positions = jnp.arange(per_device, dtype=jnp.int32)

    def early(density, anchors, counts, near):
        low_density = from_behind(density[:, :, inner - side :], "py", 1)
        high_density = from_behind(density[:, :, :side], "py", -1)
        owner = place_first * size_second + jnp.arange(size_second, dtype=jnp.int32)
        wanted = (place_second - jnp.arange(size_second, dtype=jnp.int32)) % size_second
        anchor = anchors[:, owner * per_device + wanted]
        x = jnp.clip(anchor[0] - place_first * first_rows, 0, first_rows - REG)
        y = jnp.clip(anchor[1] - place_second * second_rows, 0, second_rows - REG)
        columns = (anchor[2][:, None] - 1 + jnp.arange(PATCH_Z, dtype=jnp.int32)) % NR
        pick = (jnp.arange(NR, dtype=jnp.int32)[None, :, None] == columns[:, None, :]).astype(F32)
        slots = device * per_device + positions
        below, above = near[0][slots], near[1][slots]
        flags = jnp.stack(
            [
                positions < counts[device],
                below >= 0,
                above >= 0,
                near[1][jnp.maximum(below, 0)] >= 0,
                near[0][jnp.maximum(above, 0)] >= 0,
            ]
        ).astype(jnp.int32)
        return low_density, high_density, x, y, pick, flags

    low_density, high_density, x, y, pick, flags = early(
        subgrid_density, slot_anchor, slot_count, neighbour
    )
    coarse_potential = poisson(root_density)
    padded = extended(extended(coarse_potential, "px", 0, 1), "py", 1, 2)
    cuts = jnp.stack(
        [
            lax.dynamic_slice(padded, (x[t], y[t], 0), (PATCH_X, PATCH_Y, NR))
            for t in range(size_second)
        ]
    )
    patches = jnp.einsum("txyn,tnz->txyz", cuts, pick, precision=HIGHEST)
    patches = patches.reshape(size_second, -1)
    arrived = lax.all_to_all(
        patches, "py", split_axis=0, concat_axis=0, tiled=True
    )
    patch = arrived[(place_second + positions) % size_second]
    patch = patch.reshape(per_device, PATCH_X, PATCH_Y * PATCH_Z)
    patch = jnp.pad(
        patch, ((0, 0), (0, 16 - PATCH_X), (0, 128 - PATCH_Y * PATCH_Z))
    )
    x_table, yz_table = patch_tables()
    slot_spec = lambda width: pl.BlockSpec((1, CELLS, width), lambda s: (s, 0, 0))
    vel_spec = pl.BlockSpec((3, 1, CELLS, inner), lambda s: (0, s, 0, 0))
    potential, kicked = pl.pallas_call(
        subgrid_kernel,
        grid=(per_device,),
        in_specs=[
            pl.BlockSpec(memory_space=pltpu.SMEM),
            pl.BlockSpec((1, 16, 128), lambda s: (s, 0, 0)),
            pl.BlockSpec(x_table.shape, lambda s: (0, 0)),
            pl.BlockSpec(yz_table.shape, lambda s: (0, 0)),
            slot_spec(inner),
            slot_spec(side),
            slot_spec(side),
            vel_spec,
        ],
        out_specs=[slot_spec(inner), vel_spec],
        out_shape=[
            jax.ShapeDtypeStruct(subgrid_density.shape, F32),
            jax.ShapeDtypeStruct(velocity.shape, F32),
        ],
        compiler_params=pltpu.CompilerParams(
            dimension_semantics=("arbitrary",), vmem_limit_bytes=60 * 1024 * 1024
        ),
    )(
        flags,
        patch,
        jnp.asarray(x_table),
        jnp.asarray(yz_table),
        subgrid_density,
        low_density,
        high_density,
        velocity,
    )
    return (coarse_potential, potential, kicked)


def solution(mesh):
    return jax.shard_map(
        local,
        mesh=mesh,
        in_specs=(
            P("px", "py", None),
            P(("px", "py"), None, None),
            P(None, ("px", "py"), None, None),
            P(),
            P(),
            P(),
        ),
        out_specs=(
            P("px", "py", None),
            P(("px", "py"), None, None),
            P(None, ("px", "py"), None, None),
        ),
        check_vma=False,
    )
```

```python
import jax
import jax.numpy as jnp
import numpy as np
from jax import lax
from jax.experimental import pallas as pl
from jax.experimental.pallas import tpu as pltpu
from jax.sharding import PartitionSpec as P

NR = 384
REG = 8
REF = 4
SWEEPS = 4
CELLS = REG * REF
EDGE = SWEEPS
LAYERS = CELLS + 2 * EDGE
WIDE = LAYERS * CELLS
RELAXATION = 6.0 / 7.0
HIGHEST = lax.Precision.HIGHEST
HIGH = lax.Precision.HIGH
F32 = jnp.float32


def fourier_basis(length):
    cell = np.arange(length)
    rows = []
    for k in range(length):
        if k in (0, length // 2):
            rows.append(np.cos(2 * np.pi * (k * cell % length) / length) / np.sqrt(length))
        elif k < length // 2:
            rows.append(np.cos(2 * np.pi * (k * cell % length) / length) * np.sqrt(2 / length))
        else:
            rows.append(
                np.sin(2 * np.pi * ((length - k) * cell % length) / length) * np.sqrt(2 / length)
            )
    return np.stack(rows)


def strip_basis(cells):
    place = np.arange(cells) - (cells - 1) / 2
    mode = 2 * np.arange(cells // 2) + 1
    angle = np.pi * mode[:, None] * place[None, :] / cells
    basis = np.concatenate([np.cos(angle), np.sin(angle)]) * np.sqrt(2 / cells)
    eig = 4 * np.sin(np.pi * mode / (2 * cells)) ** 2
    return basis, np.concatenate([eig, eig])


def strip_coupling(count, rows):
    basis = fourier_basis(count)
    turn = np.zeros((count, count))
    theta = 2 * np.pi * np.arange(count) / count
    for k in range(1, (count + 1) // 2):
        turn[k, count - k] = np.sin(theta[k])
        turn[count - k, k] = -np.sin(theta[k])
    wide = lambda matrix: np.kron(matrix, np.eye(rows))
    mixes = np.stack([wide(basis), wide(turn @ basis), wide(basis.T)])
    half_sine = np.sin(theta / 2) ** 2
    factors = np.stack([half_sine, 4 * (1 - half_sine)])
    return mixes, np.repeat(factors, rows, axis=1)[:, :, None]


def axis_weights(cells, first, count):
    table = np.zeros((len(cells), count))
    for row, cell in enumerate(cells):
        mark = 2 * cell - 1 + REF
        low = mark // (2 * REF)
        frac = (mark - 2 * REF * low) / (2 * REF)
        table[row, low - first] += 1 - frac
        if frac:
            table[row, low + 1 - first] += frac
    return table


PATCH = REG + 2
PATCH_X = REG + 2
PATCH_Y = REG + 4
PATCH_Z = REG + 2


def patch_tables():
    inner = np.arange(1, CELLS + 1)
    x_side = axis_weights(np.concatenate([inner, [0, CELLS + 1]]), 0, PATCH_X)
    x_table = np.zeros((CELLS + 8, 16))
    x_table[: CELLS + 2, :PATCH_X] = x_side
    y_cells = np.arange(1 - EDGE, CELLS + EDGE + 1)
    y_side = axis_weights(y_cells, -1, PATCH_Y)
    y_out = axis_weights(np.array([-EDGE, CELLS + EDGE + 1]), -1, PATCH_Y)
    z_side = axis_weights(np.arange(CELLS + 2), 0, PATCH_Z)
    z_edge = np.zeros((CELLS, PATCH_Z))
    z_edge[0] = z_side[0]
    z_edge[-1] = z_side[-1]
    y_edge = np.zeros((LAYERS, PATCH_Y))
    y_edge[0] = y_out[0]
    y_edge[-1] = y_out[1]

    def both(ys, zs):
        return np.einsum("jb,kc->bcjk", ys, zs).reshape(PATCH_Y * PATCH_Z, WIDE)

    table = np.zeros((128, 3 * WIDE))
    table[: PATCH_Y * PATCH_Z] = np.concatenate(
        [both(y_side, z_side[1:-1]), both(y_side, z_edge), both(y_edge, z_side[1:-1])], axis=1
    )
    return x_table.astype(np.float32), table.astype(np.float32)


def decay(delta):
    return 1.0 / (1.0 + 0.5 * delta + jnp.sqrt(delta + 0.25 * delta * delta))


def power(value, exponent):
    result = None
    while exponent:
        if exponent & 1:
            result = value if result is None else result * value
        exponent >>= 1
        if exponent:
            value = value * value
    return result


def grid_kernel(
    sizes,
    f_ref,
    eig_b_ref,
    eig_ref,
    own_ref,
    vec_ref,
    basis_ref,
    mix_ref,
    angle_ref,
    density_ref,
    out_ref,
    edge_ref,
    low_ref,
    high_ref,
    held,
    lines,
    sent,
    got,
    answer,
    back,
    mom_one,
    mom_two,
    part,
    table,
    weight,
    send_one,
    recv_one,
    send_two,
    recv_two,
    send_line,
    recv_line,
    send_back,
    recv_back,
    self_sem,
    send_face,
    recv_face,
):
    count_first, count_second, owners = sizes
    devices = count_first * count_second
    rows, strip, wave = f_ref.shape
    groups = strip // 8
    half = strip // 2
    chunk = sent.shape[0] // owners
    width = lines.shape[0]
    mesh = pl.DeviceIdType.MESH
    place_first = lax.axis_index("px")
    place_second = lax.axis_index("py")
    me = place_first * count_second + place_second
    barrier = pltpu.get_barrier_semaphore()

    def greet(step, carry):
        other = lax.rem(me + step, devices)
        pl.semaphore_signal(
            barrier,
            inc=1,
            device_id=(other // count_second, lax.rem(other, count_second)),
            device_id_type=mesh,
        )
        return carry

    lax.fori_loop(1, devices, greet, 0)

    def split(value):
        return tuple(value[8 * g : 8 * g + 8] for g in range(groups))

    r_all = decay(eig_b_ref[...] + eig_ref[...])
    scale_all = -r_all / ((1.0 - r_all) * (1.0 + r_all))
    ratio = power(r_all, rows)
    norm = 1.0 / (1.0 - power(ratio, count_first))
    weight[0] = r_all
    weight[1] = scale_all
    weight[2] = 2.0 * vec_ref[0] * scale_all
    weight[3] = -2.0 * vec_ref[1] * scale_all
    r = split(r_all)
    zeros = tuple(jnp.zeros((8, wave), F32) for _ in range(groups))
    even_groups = [g for g in range(groups) if 8 * g < half]
    odd_groups = [g for g in range(groups) if 8 * g + 8 > half]

    table[...] = jnp.zeros_like(table)
    for i in range(count_first):
        block = basis_ref[i * rows : (i + 1) * rows, :]
        table[i, :rows, :wave] = block
        table[i, rows : 2 * rows, wave:] = block
        for place, row in enumerate((rows * (i + 1) % wave, (rows * i - 1) % wave)):
            line = basis_ref[row : row + 1, :]
            table[i, 2 * rows + 2 + place : 2 * rows + 3 + place, :wave] = line
            table[i, 2 * rows + 4 + place : 2 * rows + 5 + place, wave:] = line

    def row_of(ref, i):
        return tuple(ref[i, 8 * g : 8 * g + 8, :] for g in range(groups))

    def up_first(i, carry):
        up, total = carry
        f = row_of(f_ref, i)
        up = tuple(r[g] * up[g] + f[g] for g in range(groups))
        return up, tuple(total[g] + f[g] for g in range(groups))

    def down_first(i, down):
        f = row_of(f_ref, rows - 1 - i)
        return tuple(r[g] * down[g] + f[g] for g in range(groups))

    up, total = lax.fori_loop(0, rows, up_first, (zeros, zeros))
    down = lax.fori_loop(0, rows, down_first, zeros)
    for g in range(groups):
        mom_one[0, 0, 8 * g : 8 * g + 8, :] = up[g]
        mom_one[0, 1, 8 * g : 8 * g + 8, :] = down[g]
    whole = jnp.concatenate(total, axis=0)

    def shares(buffer, send, recv):
        return [
            pltpu.make_async_remote_copy(
                src_ref=buffer.at[0],
                dst_ref=buffer.at[d],
                send_sem=send.at[d],
                recv_sem=recv.at[d],
                device_id=(lax.rem(place_first + d, count_first), place_second),
                device_id_type=mesh,
            )
            for d in range(1, count_first)
        ]

    def carries(buffer):
        up = jnp.zeros((strip, wave), F32)
        down = jnp.zeros((strip, wave), F32)
        for d in [0] + list(range(count_first - 1, 0, -1)):
            up = ratio * up + buffer[d, 0]
        for d in range(count_first):
            down = ratio * down + buffer[d, 1]
        return split(up * norm), split(down * norm)

    pl.semaphore_wait(barrier, devices - 1)
    face = low_ref.shape[2]
    inner = density_ref.shape[2]
    faces = [
        pltpu.make_async_remote_copy(
            src_ref=density_ref.at[:, :, pl.ds(start, face)],
            dst_ref=target,
            send_sem=send_face.at[n],
            recv_sem=recv_face.at[n],
            device_id=(place_first, lax.rem(place_second + step, count_second)),
            device_id_type=mesh,
        )
        for n, (start, target, step) in enumerate(
            ((inner - face, low_ref, 1), (0, high_ref, count_second - 1))
        )
    ]
    first = shares(mom_one, send_one, recv_one)
    for copy in first + faces:
        copy.start()
    lines[2 * rows :, :] = jnp.zeros((width - 2 * rows, wave), F32)
    lines[2 * rows : 2 * rows + 1, :] = jnp.sum(vec_ref[2] * whole, axis=0, keepdims=True)
    lines[2 * rows + 1 : 2 * rows + 2, :] = jnp.sum(vec_ref[3] * whole, axis=0, keepdims=True)
    for copy in first:
        copy.wait()
    carry_up, carry_down = carries(mom_one)

    def weighed(which, members, value):
        total = None
        for g in members:
            term = weight[which, 8 * g : 8 * g + 8, :] * value[g]
            total = term if total is None else total + term
        return total

    def up_lines(i, up):
        f = row_of(f_ref, i)
        up = tuple(r[g] * up[g] + f[g] for g in range(groups))
        part[0, i] = weighed(2, even_groups, up)
        part[1, i] = weighed(3, odd_groups, up)
        return up

    def down_lines(step, down):
        i = rows - 1 - step
        f = row_of(f_ref, i)
        down = tuple(r[g] * down[g] for g in range(groups))
        part[0, i] += weighed(2, even_groups, down)
        part[1, i] += weighed(3, odd_groups, down)
        return tuple(down[g] + f[g] for g in range(groups))

    lax.fori_loop(0, rows, up_lines, carry_up)
    lax.fori_loop(0, rows, down_lines, carry_down)
    lines[:rows, :] = jnp.sum(part[0], axis=1)
    lines[rows : 2 * rows, :] = jnp.sum(part[1], axis=1)
    sent[...] = lines[...].T

    def line_copy(o):
        return pltpu.make_async_remote_copy(
            src_ref=sent.at[pl.ds(o * chunk, chunk)],
            dst_ref=got.at[me],
            send_sem=send_line.at[o],
            recv_sem=recv_line.at[me],
            device_id=(o // count_second, lax.rem(o, count_second)),
            device_id_type=mesh,
        )

    def line_from(d):
        return pltpu.make_async_remote_copy(
            src_ref=sent.at[pl.ds(0, chunk)],
            dst_ref=got.at[d],
            send_sem=self_sem.at[1],
            recv_sem=recv_line.at[d],
            device_id=(d // count_second, lax.rem(d, count_second)),
            device_id_type=mesh,
        )

    def back_copy(d):
        return pltpu.make_async_remote_copy(
            src_ref=answer.at[d],
            dst_ref=back.at[pl.ds(me * chunk, chunk)],
            send_sem=send_back.at[d],
            recv_sem=recv_back.at[me],
            device_id=(d // count_second, lax.rem(d, count_second)),
            device_id_type=mesh,
        )

    def back_from(o):
        return pltpu.make_async_remote_copy(
            src_ref=answer.at[0],
            dst_ref=back.at[pl.ds(o * chunk, chunk)],
            send_sem=self_sem.at[1],
            recv_sem=recv_back.at[o],
            device_id=(o // count_second, lax.rem(o, count_second)),
            device_id_type=mesh,
        )

    def over(count, action):
        def body(k, carry):
            @pl.when(k != me)
            def _():
                action(k)

            return carry

        lax.fori_loop(0, count, body, 0)

    over(owners, lambda o: line_copy(o).start())

    @pl.when(me < owners)
    def _():
        own = pltpu.make_async_copy(
            sent.at[pl.ds(me * chunk, chunk)], got.at[me], self_sem.at[0]
        )
        own.start()
        over(devices, lambda d: line_from(d).wait_recv())
        own.wait()
        modes = None
        for i in range(count_first):
            piece = got[i * count_second : (i + 1) * count_second]
            piece = piece.reshape(count_second * chunk, width)
            term = jnp.dot(piece, table[i], precision=HIGHEST, preferred_element_type=F32)
            modes = term if modes is None else modes + term
        straight = jnp.dot(mix_ref[0], modes, precision=HIGHEST, preferred_element_type=F32)
        turned = jnp.dot(mix_ref[1], modes, precision=HIGHEST, preferred_element_type=F32)
        s, t = straight[:, :wave], straight[:, wave:]
        s_turned, t_turned = turned[:, :wave], turned[:, wave:]
        own_eig = own_ref[...]
        lam = own_eig + eig_ref[...]
        sinh = jnp.sqrt(lam + 0.25 * lam * lam)
        flat = lam <= 0.0
        far = power(decay(lam), strip)
        tanh = (1.0 - far) / (1.0 + far)
        green = jnp.where(flat, strip / 4.0, tanh / jnp.where(flat, 1.0, 2.0 * sinh))
        square = tanh * tanh
        half_sine = angle_ref[0]
        det = half_sine * (1.0 - square) + square
        zero = flat & (half_sine <= 0.0)
        inverse = 1.0 / jnp.where(zero, 1.0, det)
        gain = angle_ref[1] * green * inverse
        sums = jnp.sum(got[...], axis=0)
        lane = lax.broadcasted_iota(jnp.int32, sums.shape, 1)
        sigma = jnp.sum(jnp.where(lane == 2 * rows, sums, 0.0), axis=1, keepdims=True)
        lever = jnp.sum(jnp.where(lane == 2 * rows + 1, sums, 0.0), axis=1, keepdims=True)
        k = np.arange(strip)
        bow = 0.5 * (k * k - (strip - 1) * k) - strip / 4
        mean = jnp.where(own_eig[:chunk] <= 0.0, sigma, 0.0) * (1.0 / (wave * wave))
        gauge = lever - mean * float(wave * count_second * bow.sum())
        gauge = gauge * float(1.0 / (bow[0] * np.sqrt(wave * count_second)))
        tall = lambda value: jnp.concatenate([value] * count_second, axis=0)
        mean, gauge = tall(mean), tall(gauge)
        new_s = gain * (2.0 + 0.5 * lam) * s - t_turned * inverse
        new_t = gain * (0.5 * lam) * t - s_turned * inverse
        new_s = jnp.where(zero, gauge, new_s)
        new_t = jnp.where(zero, (2.0 / strip) * t, new_t)
        solved = jnp.concatenate([new_s, new_t], axis=1)
        solved = jnp.dot(mix_ref[2], solved, precision=HIGHEST, preferred_element_type=F32)
        wide = lax.broadcasted_iota(jnp.int32, (count_second * chunk, width), 1)
        for i in range(count_first):
            piece = lax.dot_general(
                solved,
                table[i],
                (((1,), (1,)), ((), ())),
                precision=HIGHEST,
                preferred_element_type=F32,
            )
            piece = jnp.where(wide == 2 * rows, mean, piece)
            answer[i * count_second : (i + 1) * count_second] = piece.reshape(
                count_second, chunk, width
            )
        over(devices, lambda d: back_copy(d).start())
        kept = pltpu.make_async_copy(
            answer.at[me], back.at[pl.ds(me * chunk, chunk)], self_sem.at[0]
        )
        kept.start()
        kept.wait()

    over(owners, lambda o: back_from(o).wait_recv())
    lines[...] = back[...].T
    for n, (start, halo) in enumerate(((0, 2 * rows + 2), (rows, 2 * rows + 4))):
        edge_ref[n, :rows, :] = lines[start : start + rows, :]
        edge_ref[n, rows : rows + 2, :] = lines[halo : halo + 2, :]
    mean_term = vec_ref[2] * lines[2 * rows : 2 * rows + 1, :]
    weight[2] = mean_term

    def up_second(i, up):
        f = row_of(f_ref, i)
        line_s = lines[pl.ds(i, 1), :]
        line_t = lines[pl.ds(rows + i, 1), :]
        fresh = []
        for g in range(groups):
            window = slice(8 * g, 8 * g + 8)
            value = f[g] - weight[2, window, :]
            if g in even_groups:
                value = value - vec_ref[0, window, :] * line_s
            if g in odd_groups:
                value = value - vec_ref[1, window, :] * line_t
            held[i, window, :] = value
            fresh.append(value)
        return tuple(r[g] * up[g] + fresh[g] for g in range(groups))

    def down_second(i, down):
        f = row_of(held, rows - 1 - i)
        return tuple(r[g] * down[g] + f[g] for g in range(groups))

    up = lax.fori_loop(0, rows, up_second, zeros)
    down = lax.fori_loop(0, rows, down_second, zeros)
    for g in range(groups):
        mom_two[0, 0, 8 * g : 8 * g + 8, :] = up[g]
        mom_two[0, 1, 8 * g : 8 * g + 8, :] = down[g]
    second = shares(mom_two, send_two, recv_two)
    for copy in second:
        copy.start()
    over(owners, lambda o: line_copy(o).wait_send())

    @pl.when(me < owners)
    def _():
        over(devices, lambda d: back_copy(d).wait_send())

    for copy in second:
        copy.wait()
    carry_up, carry_down = carries(mom_two)

    def up_last(i, up):
        f = row_of(held, i)
        up = tuple(r[g] * up[g] + f[g] for g in range(groups))
        for g in range(groups):
            out_ref[i, 8 * g : 8 * g + 8, :] = up[g]
        return up

    def down_last(step, down):
        i = rows - 1 - step
        f = row_of(held, i)
        down = tuple(r[g] * down[g] for g in range(groups))
        for g in range(groups):
            window = slice(8 * g, 8 * g + 8)
            out_ref[i, window, :] = (out_ref[i, window, :] + down[g]) * weight[1, window, :]
        return tuple(down[g] + f[g] for g in range(groups))

    up = lax.fori_loop(0, rows, up_last, carry_up)
    down = lax.fori_loop(0, rows, down_last, carry_down)
    for g in range(groups):
        window = slice(8 * g, 8 * g + 8)
        scale = weight[1, window, :]
        out_ref[rows, window, :] = (r[g] * up[g] + carry_down[g]) * scale
        out_ref[rows + 1, window, :] = (carry_up[g] + r[g] * down[g]) * scale
    for copy in faces:
        copy.wait()


def halves(value):
    high = value.astype(jnp.bfloat16)
    return high, (value - high.astype(F32)).astype(jnp.bfloat16)


def grid_values_kernel(
    step, anchor_ref, u_ref, edge_ref, strip_ref, wave_ref, out_ref, patch_ref, ext, cut, sems
):
    planes, strip, wave = u_ref.shape
    rows = planes - 2
    tall = ext.shape[1]
    tiles = tall // 8
    chunks = planes // step
    tail = rows - (chunks - 1) * step
    second = strip_ref.shape[0]
    place_first = lax.axis_index("px")
    place_second = lax.axis_index("py")
    count = lax.axis_size("py")
    sub = lax.broadcasted_iota(jnp.int32, (8, wave), 0)

    def out_copy(c, size):
        start = c * step
        return pltpu.make_async_copy(
            ext.at[pl.ds(start, size), :strip, :], out_ref.at[pl.ds(start, size)], sems.at[c]
        )

    def chunk(c, carry):
        values = []
        for i in range(step):
            k = c * step + i
            high, low = halves(u_ref[k])
            stack = jnp.concatenate([high, high, low], axis=0)
            value = jnp.dot(strip_ref[...], stack, preferred_element_type=F32)
            s, t = edge_ref[0, pl.ds(k, 1), :], edge_ref[1, pl.ds(k, 1), :]
            halo = jnp.where(sub == 0, 0.5 * (s - t), jnp.where(sub == 7, 0.5 * (s + t), 0.0))
            values += [value[:strip], value[strip:] + halo]
        high, low = halves(jnp.concatenate(values, axis=0))
        wide = jnp.concatenate([high, low, high], axis=1)
        result = jnp.dot(wide, wave_ref[...], preferred_element_type=F32)
        ext[pl.ds(c * step, step)] = result.reshape(step, tall, wave)

        @pl.when(c < chunks - 1)
        def _():
            out_copy(c, step).start()

        return carry

    lax.fori_loop(0, chunks, chunk, 0)
    out_copy(chunks - 1, tail).start()
    lane = lax.broadcasted_iota(jnp.int32, cut.shape[::2], 1)
    cut[...] = jnp.zeros_like(cut)

    def patch(t, carry):
        slot = (place_first * count + t) * count + lax.rem(place_second - t + count, count)
        x = jnp.clip(anchor_ref[0, slot] - place_first * rows, 0, rows - REG)
        y = jnp.clip(anchor_ref[1, slot] - place_second * strip, 0, strip - REG) // 8
        shift = lax.rem(wave + 1 - jnp.clip(anchor_ref[2, slot], 0, wave - REG), wave)
        for i in range(REG + 2):
            row = x - 1 + i
            row = jnp.where(row < 0, rows + 1, row)
            for d in range(3):
                tile = lax.rem(y + d - 1 + tiles, tiles)
                value = ext[row, pl.ds(pl.multiple_of(tile * 8, 8), 8), :]
                cut[i, 8 * d : 8 * d + 8, :] = pltpu.roll(value, shift, 1)[:, :128]
        total = jnp.zeros(lane.shape, F32)
        for b in range(PATCH):
            line = jnp.where(lane < PATCH, cut[:, 7 + b, :], 0.0)
            total = total + (pltpu.roll(line, PATCH * b, 1) if b else line)
        patch_ref[t + 1] = total
        return carry

    lax.fori_loop(0, count, patch, 0)
    patch_ref[0] = patch_ref[count]
    patch_ref[count + 1] = patch_ref[1]

    def finish(c, carry):
        out_copy(c, step).wait()
        return carry

    lax.fori_loop(0, chunks - 1, finish, 0)
    out_copy(chunks - 1, tail).wait()


def patch_exchange_kernel(patch_ref, out_ref, send_sems, recv_sems, own_sem):
    count = out_ref.shape[0]
    place_first = lax.axis_index("px")
    place_second = lax.axis_index("py")
    barrier = pltpu.get_barrier_semaphore()
    mesh = pl.DeviceIdType.MESH
    for d in range(1, count):
        pl.semaphore_signal(
            barrier,
            inc=1,
            device_id=(place_first, lax.rem(place_second + d, count)),
            device_id_type=mesh,
        )
    own = pltpu.make_async_copy(
        patch_ref.at[pl.ds(place_second, 3)], out_ref.at[0], own_sem
    )
    own.start()
    pl.semaphore_wait(barrier, count - 1)
    copies = []
    for d in range(1, count):
        target = lax.rem(place_second + d, count)
        copies.append(
            pltpu.make_async_remote_copy(
                src_ref=patch_ref.at[pl.ds(target, 3)],
                dst_ref=out_ref.at[count - d],
                send_sem=send_sems.at[d],
                recv_sem=recv_sems.at[d],
                device_id=(place_first, target),
                device_id_type=mesh,
            )
        )
    for copy in copies:
        copy.start()
    own.wait()
    for copy in copies:
        copy.wait()


def subgrid_kernel(
    count_ref,
    near_ref,
    own_ref,
    under_ref,
    over_ref,
    xt_ref,
    yz_ref,
    mid_ref,
    low_ref,
    high_ref,
    vel_ref,
    pot_ref,
    kick_ref,
):
    device = lax.axis_index("px") * lax.axis_size("py") + lax.axis_index("py")
    place = pl.program_id(0)
    slot = device * pl.num_programs(0) + place
    below = near_ref[0, slot]
    above = near_ref[1, slot]
    live = place < count_ref[device]
    has_below = below >= 0
    has_above = above >= 0
    back_below = near_ref[1, jnp.maximum(below, 0)] >= 0
    back_above = near_ref[0, jnp.maximum(above, 0)] >= 0
    column = lax.broadcasted_iota(jnp.int32, (16, 128), 1)
    patch = jnp.where(
        column < PATCH,
        pltpu.roll(under_ref[0, 0], 128 - (REG - 1) * PATCH, 1),
        jnp.where(
            column < (PATCH + 1) * PATCH,
            pltpu.roll(own_ref[0, 0], PATCH, 1),
            pltpu.roll(over_ref[0, 0], (PATCH - 1) * PATCH, 1),
        ),
    )
    patch = jnp.where(column < (PATCH + 2) * PATCH, patch, 0.0)
    planes = jnp.dot(patch, yz_ref[...], precision=HIGHEST, preferred_element_type=F32)
    coarse = jnp.dot(xt_ref[...], planes, precision=HIGHEST, preferred_element_type=F32)
    start = coarse[:CELLS, :WIDE]
    x_low = coarse[CELLS : CELLS + 1, :WIDE]
    x_high = coarse[CELLS + 1 : CELLS + 2, :WIDE]
    z_edge = coarse[:CELLS, WIDE : 2 * WIDE]
    y_edge = coarse[:CELLS, 2 * WIDE :]
    shape = (CELLS, WIDE)
    row = lax.broadcasted_iota(jnp.int32, shape, 0)
    lane = lax.broadcasted_iota(jnp.int32, shape, 1)
    third = lane % CELLS
    side = EDGE * CELLS
    end = WIDE - side
    y_above = jnp.where(lane >= WIDE - CELLS, y_edge, pltpu.roll(start, WIDE - CELLS, 1))
    y_below = jnp.where(lane < CELLS, y_edge, pltpu.roll(start, CELLS, 1))
    cut_above = (lane >= WIDE - CELLS) | (
        (lane >= side - CELLS) & (lane < side) & jnp.logical_not(back_below)
    )
    cut_below = (lane < CELLS) | (
        (lane >= end) & (lane < end + CELLS) & jnp.logical_not(back_above)
    )
    fixed = ((lane < side) & jnp.logical_not(has_below)) | (
        (lane >= end) & jnp.logical_not(has_above)
    )
    rho = jnp.concatenate([low_ref[0], mid_ref[0], high_ref[0]], axis=1) * (1.0 / (REF * REF))

    def beside(v):
        return (
            (
                jnp.where(row == 0, x_low, pltpu.roll(v, 1, 0)),
                jnp.where(row == CELLS - 1, x_high, pltpu.roll(v, CELLS - 1, 0)),
            ),
            (
                jnp.where(cut_below, y_below, pltpu.roll(v, CELLS, 1)),
                jnp.where(cut_above, y_above, pltpu.roll(v, WIDE - CELLS, 1)),
            ),
            (
                jnp.where(third == 0, z_edge, pltpu.roll(v, 1, 1)),
                jnp.where(third == CELLS - 1, z_edge, pltpu.roll(v, WIDE - 1, 1)),
            ),
        )

    v = start
    for _ in range(SWEEPS):
        first, second, last = beside(v)
        total = first[1] + first[0] + second[1] + second[0] + last[1] + last[0]
        new = (1.0 - RELAXATION) * v + RELAXATION * (total - rho) / 6.0
        v = jnp.where(fixed, v, new)
    pot_ref[0] = jnp.where(live, v[:, side:end], 0.0)
    for q, (below, above) in enumerate(beside(v)):
        slope = (above[:, side:end] - below[:, side:end]) * (REF / 2.0)
        kick_ref[q, 0] = jnp.where(live, vel_ref[q, 0] - slope, 0.0)


def poisson(root_density, density, slot_anchor):
    count_first = lax.axis_size("px")
    count_second = lax.axis_size("py")
    devices = count_first * count_second
    device = lax.axis_index("px") * count_second + lax.axis_index("py")
    rows, strip, wave = root_density.shape
    chunk = next(q for q in range(8, wave + 1, 8) if wave % q == 0 and wave // q <= devices)
    owners = wave // chunk
    width = -(-(2 * rows + 6) // 128) * 128
    basis = fourier_basis(wave)
    strip_table, strip_eig = strip_basis(strip)
    eig = 4.0 * np.sin(np.pi / wave * np.arange(wave)) ** 2
    mixes, angles = strip_coupling(count_second, chunk)
    cell = np.arange(strip)
    bow = 0.5 * (cell * cell - (strip - 1) * cell) - strip / 4
    lower = cell < strip // 2
    edge = strip_table[:, 0]
    vectors = np.stack(
        [
            np.where(lower, edge, 0.0),
            np.where(lower, 0.0, edge),
            strip_table.sum(1),
            strip_table @ bow,
        ]
    )[:, :, None]
    own = lax.rem(device, owners) * chunk
    own_eig = lax.dynamic_slice_in_dim(jnp.asarray(eig, F32), own, chunk)
    own_eig = jnp.tile(own_eig, count_second)[:, None]
    z_basis = jnp.asarray(basis, F32)
    y_basis = jnp.asarray(strip_table, F32)
    f = jnp.einsum("xyz,cz->xyc", root_density, z_basis, precision=HIGH)
    f = jnp.einsum("xyc,by->xbc", f, y_basis, precision=HIGH)
    moment = pltpu.VMEM((count_first, 2, strip, wave), F32)
    dma = pltpu.SemaphoreType.DMA
    face = jax.ShapeDtypeStruct(density.shape[:2] + (EDGE * CELLS,), F32)
    vmem = pl.BlockSpec(memory_space=pltpu.VMEM)
    hbm = pl.BlockSpec(memory_space=pl.ANY)
    u, edges, low_density, high_density = pl.pallas_call(
        lambda *refs: grid_kernel((count_first, count_second, owners), *refs),
        in_specs=[vmem] * 8 + [hbm],
        out_specs=[vmem, vmem, hbm, hbm],
        out_shape=[
            jax.ShapeDtypeStruct((rows + 2, strip, wave), F32),
            jax.ShapeDtypeStruct((2, rows + 2, wave), F32),
            face,
            face,
        ],
        scratch_shapes=[
            pltpu.VMEM((rows, strip, wave), F32),
            pltpu.VMEM((width, wave), F32),
            pltpu.VMEM((wave, width), F32),
            pltpu.VMEM((devices, chunk, width), F32),
            pltpu.VMEM((devices, chunk, width), F32),
            pltpu.VMEM((wave, width), F32),
            moment,
            moment,
            pltpu.VMEM((2, rows, 8, wave), F32),
            pltpu.VMEM((count_first, width, 2 * wave), F32),
            pltpu.VMEM((4, strip, wave), F32),
            dma((count_first,)),
            dma((count_first,)),
            dma((count_first,)),
            dma((count_first,)),
            dma((owners,)),
            dma((devices,)),
            dma((devices,)),
            dma((owners,)),
            dma((2,)),
            dma((2,)),
            dma((2,)),
        ],
        compiler_params=pltpu.CompilerParams(
            collective_id=1, has_side_effects=True, vmem_limit_bytes=60 * 1024 * 1024
        ),
    )(
        f,
        jnp.asarray(strip_eig[:, None], F32),
        jnp.asarray(eig[None, :], F32),
        own_eig,
        jnp.asarray(vectors, F32),
        jnp.asarray(basis.T, F32),
        jnp.asarray(mixes, F32),
        jnp.asarray(angles, F32),
        density,
    )
    tall = strip + 8
    step = max(n for n in range(1, 15) if (rows + 2) % n == 0)
    extended = np.zeros((tall, strip))
    extended[:strip] = strip_table.T
    extended[strip] = -strip_table[:, 0]
    extended[-1] = -strip_table[:, -1]
    high, low = halves(jnp.asarray(extended, F32))
    strip_wide = jnp.concatenate([high, low, high], axis=1)
    high, low = halves(z_basis)
    wave_tall = jnp.concatenate([high, high, low], axis=0)
    chunks = (rows + 2) // step
    coarse, patches = pl.pallas_call(
        lambda *refs: grid_values_kernel(step, *refs),
        in_specs=[pl.BlockSpec(memory_space=pltpu.SMEM)] + [vmem] * 4,
        out_specs=[hbm, vmem],
        out_shape=[
            jax.ShapeDtypeStruct((rows, strip, wave), F32),
            jax.ShapeDtypeStruct((count_second + 2, 16, 128), F32),
        ],
        scratch_shapes=[
            pltpu.VMEM((rows + 2, tall, wave), F32),
            pltpu.VMEM((16, 24, 128), F32),
            dma((chunks,)),
        ],
        compiler_params=pltpu.CompilerParams(vmem_limit_bytes=60 * 1024 * 1024),
    )(slot_anchor, u, edges, strip_wide, wave_tall)
    arrived = pl.pallas_call(
        patch_exchange_kernel,
        in_specs=[vmem],
        out_specs=vmem,
        out_shape=jax.ShapeDtypeStruct((count_second, 3, 16, 128), F32),
        scratch_shapes=[dma((count_second,)), dma((count_second,)), dma(())],
        compiler_params=pltpu.CompilerParams(collective_id=2, has_side_effects=True),
    )(patches)
    return coarse, arrived, low_density, high_density


def local(root_density, subgrid_density, velocity, slot_anchor, slot_count, neighbour):
    per_device = subgrid_density.shape[0]
    side = EDGE * CELLS
    inner = CELLS * CELLS
    coarse_potential, patches, low_density, high_density = poisson(
        root_density, subgrid_density, slot_anchor
    )
    x_table, yz_table = patch_tables()
    count = lax.axis_size("py")
    smem = pl.BlockSpec(memory_space=pltpu.SMEM)
    slot_spec = lambda width: pl.BlockSpec((1, CELLS, width), lambda s: (s, 0, 0))
    vel_spec = pl.BlockSpec((3, 1, CELLS, inner), lambda s: (0, s, 0, 0))
    patch_spec = lambda step: pl.BlockSpec(
        (1, 1, 16, 128), lambda s: (lax.rem(s + step + count, count), step + 1, 0, 0)
    )
    potential, kicked = pl.pallas_call(
        subgrid_kernel,
        grid=(per_device,),
        in_specs=[
            smem,
            smem,
            patch_spec(0),
            patch_spec(-1),
            patch_spec(1),
            pl.BlockSpec(x_table.shape, lambda s: (0, 0)),
            pl.BlockSpec(yz_table.shape, lambda s: (0, 0)),
            slot_spec(inner),
            slot_spec(side),
            slot_spec(side),
            vel_spec,
        ],
        out_specs=[slot_spec(inner), vel_spec],
        out_shape=[
            jax.ShapeDtypeStruct(subgrid_density.shape, F32),
            jax.ShapeDtypeStruct(velocity.shape, F32),
        ],
        compiler_params=pltpu.CompilerParams(
            dimension_semantics=("arbitrary",), vmem_limit_bytes=60 * 1024 * 1024
        ),
    )(
        slot_count,
        neighbour,
        patches,
        patches,
        patches,
        jnp.asarray(x_table),
        jnp.asarray(yz_table),
        subgrid_density,
        low_density,
        high_density,
        velocity,
    )
    return (coarse_potential, potential, kicked)


def solution(mesh):
    return jax.shard_map(
        local,
        mesh=mesh,
        in_specs=(
            P("px", "py", None),
            P(("px", "py"), None, None),
            P(None, ("px", "py"), None, None),
            P(),
            P(),
            P(),
        ),
        out_specs=(
            P("px", "py", None),
            P(("px", "py"), None, None),
            P(None, ("px", "py"), None, None),
        ),
        check_vma=False,
    )
```

```python
import jax
import jax.numpy as jnp
import numpy as np
from jax import lax
from jax.experimental import pallas as pl
from jax.experimental.pallas import tpu as pltpu
from jax.sharding import PartitionSpec as P

NR = 384
REG = 8
REF = 4
SWEEPS = 4
CELLS = REG * REF
EDGE = SWEEPS
LAYERS = CELLS + 2 * EDGE
WIDE = LAYERS * CELLS
RELAXATION = 6.0 / 7.0
HIGHEST = lax.Precision.HIGHEST
HIGH = lax.Precision.HIGH
F32 = jnp.float32


def fourier_basis(length):
    cell = np.arange(length)
    rows = []
    for k in range(length):
        if k in (0, length // 2):
            rows.append(np.cos(2 * np.pi * (k * cell % length) / length) / np.sqrt(length))
        elif k < length // 2:
            rows.append(np.cos(2 * np.pi * (k * cell % length) / length) * np.sqrt(2 / length))
        else:
            rows.append(
                np.sin(2 * np.pi * ((length - k) * cell % length) / length) * np.sqrt(2 / length)
            )
    return np.stack(rows)


def strip_basis(cells):
    place = np.arange(cells) - (cells - 1) / 2
    mode = 2 * np.arange(cells // 2) + 1
    angle = np.pi * mode[:, None] * place[None, :] / cells
    basis = np.concatenate([np.cos(angle), np.sin(angle)]) * np.sqrt(2 / cells)
    eig = 4 * np.sin(np.pi * mode / (2 * cells)) ** 2
    return basis, np.concatenate([eig, eig])


def strip_coupling(count, rows):
    basis = fourier_basis(count)
    turn = np.zeros((count, count))
    theta = 2 * np.pi * np.arange(count) / count
    for k in range(1, (count + 1) // 2):
        turn[k, count - k] = np.sin(theta[k])
        turn[count - k, k] = -np.sin(theta[k])
    wide = lambda matrix: np.kron(matrix, np.eye(rows))
    mixes = np.stack([wide(basis), wide(turn @ basis), wide(basis.T)])
    half_sine = np.sin(theta / 2) ** 2
    factors = np.stack([half_sine, 4 * (1 - half_sine)])
    return mixes, np.repeat(factors, rows, axis=1)[:, :, None]


def axis_weights(cells, first, count):
    table = np.zeros((len(cells), count))
    for row, cell in enumerate(cells):
        mark = 2 * cell - 1 + REF
        low = mark // (2 * REF)
        frac = (mark - 2 * REF * low) / (2 * REF)
        table[row, low - first] += 1 - frac
        if frac:
            table[row, low + 1 - first] += frac
    return table


PATCH = REG + 2
PATCH_X = REG + 2
PATCH_Y = REG + 4
PATCH_Z = REG + 2


def patch_tables():
    inner = np.arange(1, CELLS + 1)
    x_side = axis_weights(np.concatenate([inner, [0, CELLS + 1]]), 0, PATCH_X)
    x_table = np.zeros((CELLS + 8, 16))
    x_table[: CELLS + 2, :PATCH_X] = x_side
    y_cells = np.arange(1 - EDGE, CELLS + EDGE + 1)
    y_side = axis_weights(y_cells, -1, PATCH_Y)
    y_out = axis_weights(np.array([-EDGE, CELLS + EDGE + 1]), -1, PATCH_Y)
    z_side = axis_weights(np.arange(CELLS + 2), 0, PATCH_Z)
    z_edge = np.zeros((CELLS, PATCH_Z))
    z_edge[0] = z_side[0]
    z_edge[-1] = z_side[-1]
    y_edge = np.zeros((LAYERS, PATCH_Y))
    y_edge[0] = y_out[0]
    y_edge[-1] = y_out[1]

    def both(ys, zs):
        return np.einsum("jb,kc->bcjk", ys, zs).reshape(PATCH_Y * PATCH_Z, WIDE)

    table = np.zeros((128, 3 * WIDE))
    table[: PATCH_Y * PATCH_Z] = np.concatenate(
        [both(y_side, z_side[1:-1]), both(y_side, z_edge), both(y_edge, z_side[1:-1])], axis=1
    )
    return x_table.astype(np.float32), table.astype(np.float32)


def decay(delta):
    return 1.0 / (1.0 + 0.5 * delta + jnp.sqrt(delta + 0.25 * delta * delta))


def power(value, exponent):
    result = None
    while exponent:
        if exponent & 1:
            result = value if result is None else result * value
        exponent >>= 1
        if exponent:
            value = value * value
    return result


def halves(value):
    high = value.astype(jnp.bfloat16)
    return high, (value - high.astype(F32)).astype(jnp.bfloat16)


def owner_shift(place_second):
    return place_second // 2 * 2 + 2


LANES = 128


def grid_kernel(
    sizes,
    f_hbm,
    eig_b_ref,
    eig_ref,
    own_ref,
    vec_ref,
    basis_ref,
    mix_ref,
    angle_ref,
    density_ref,
    out_hbm,
    edge_ref,
    low_ref,
    high_ref,
    f_ref,
    out_ref,
    lines,
    sent,
    got,
    answer,
    back,
    mom_one,
    mom_two,
    part,
    table,
    factor,
    weight,
    in_sem,
    out_sem,
    send_one,
    recv_one,
    send_two,
    recv_two,
    send_line,
    recv_line,
    send_back,
    recv_back,
    self_sem,
    send_face,
    recv_face,
):
    count_first, count_second = sizes
    devices = count_first * count_second
    rows, strip, wave = f_ref.shape
    tiles = wave // LANES
    groups = strip // 8
    half = strip // 2
    middle = rows // 2
    fold = 4
    chunk = got.shape[1]
    width = lines.shape[0]
    mesh = pl.DeviceIdType.MESH
    place_first = lax.axis_index("px")
    place_second = lax.axis_index("py")
    me = place_first * count_second + place_second
    own_tile = lax.rem(
        place_first + 2 * count_second * count_first - owner_shift(place_second), count_first
    )
    is_owner = own_tile < tiles
    barrier = pltpu.get_barrier_semaphore()

    def greet(step, carry):
        other = lax.rem(me + step, devices)
        pl.semaphore_signal(
            barrier,
            inc=1,
            device_id=(other // count_second, lax.rem(other, count_second)),
            device_id_type=mesh,
        )
        return carry

    lax.fori_loop(1, devices, greet, 0)
    lane_of = lambda t: slice(t * LANES, (t + 1) * LANES)
    loads = [
        pltpu.make_async_copy(
            f_hbm.at[:, :, lane_of(t)], f_ref.at[:, :, lane_of(t)], in_sem.at[t]
        )
        for t in range(tiles)
    ]
    for copy in loads:
        copy.start()

    window = [slice(8 * g, 8 * g + 8) for g in range(groups)]
    even_groups = [g for g in range(groups) if 8 * g < half]
    odd_groups = [g for g in range(groups) if 8 * g + 8 > half]
    zeros = tuple(jnp.zeros((8, LANES), F32) for _ in range(groups))

    r_all = decay(eig_b_ref[...] + eig_ref[...])
    scale_all = -r_all / ((1.0 - r_all) * (1.0 + r_all))
    ratio_all = power(r_all, rows)
    weight[0] = r_all
    weight[1] = scale_all
    weight[2] = 2.0 * vec_ref[0] * scale_all
    weight[3] = -2.0 * vec_ref[1] * scale_all
    weight[4] = ratio_all
    weight[5] = 1.0 / (1.0 - power(ratio_all, count_first))

    def weights(which, t):
        return tuple(weight[which, window[g], lane_of(t)] for g in range(groups))

    def row_of(ref, i, t):
        return tuple(ref[i, window[g], lane_of(t)] for g in range(groups))

    def step_on(r, state, f):
        return tuple(r[g] * state[g] + f[g] for g in range(groups))

    def both_ways(start, stop, body, carry):
        def folded(n, carry):
            for k in range(fold):
                i = start + n * fold + k
                carry = body(i, rows - 1 - i, carry)
            return carry

        return lax.fori_loop(0, (stop - start) // fold, folded, carry)

    def store_moments(buffer, t, up, down):
        for g in range(groups):
            buffer[t, 0, 0, window[g], :] = up[g]
            buffer[t, 0, 1, window[g], :] = down[g]

    def shares(buffer, send, recv, t):
        return [
            pltpu.make_async_remote_copy(
                src_ref=buffer.at[t, 0],
                dst_ref=buffer.at[t, d],
                send_sem=send.at[t, d],
                recv_sem=recv.at[t, d],
                device_id=(lax.rem(place_first + d, count_first), place_second),
                device_id_type=mesh,
            )
            for d in range(1, count_first)
        ]

    def carries(buffer, t):
        ratio, norm = weights(4, t), weights(5, t)
        up, down = [], []
        for g in range(groups):
            total = buffer[t, 0, 0, window[g], :]
            for d in range(count_first - 1, 0, -1):
                total = ratio[g] * total + buffer[t, d, 0, window[g], :]
            up.append(total * norm[g])
            total = buffer[t, 0, 1, window[g], :]
            for d in range(1, count_first):
                total = ratio[g] * total + buffer[t, d, 1, window[g], :]
            down.append(total * norm[g])
        return tuple(up), tuple(down)

    first = []
    for t in range(tiles):
        r = weights(0, t)
        loads[t].wait()

        def moments(i, j, carry):
            up, down, total = carry
            f = row_of(f_ref, i, t)
            up = step_on(r, up, f)
            down = step_on(r, down, row_of(f_ref, j, t))
            if t == 0:
                total = tuple(total[g] + f[g] for g in range(groups))
            return up, down, total

        up, down, total = both_ways(0, rows, moments, (zeros, zeros, zeros if t == 0 else ()))
        store_moments(mom_one, t, up, down)
        if t == 0:
            whole = jnp.concatenate(total, axis=0)
            pl.semaphore_wait(barrier, devices - 1)
        first.append(shares(mom_one, send_one, recv_one, t))
        for copy in first[t]:
            copy.start()

    face = low_ref.shape[2]
    inner = density_ref.shape[2]
    faces = [
        pltpu.make_async_remote_copy(
            src_ref=density_ref.at[:, :, pl.ds(start, face)],
            dst_ref=target,
            send_sem=send_face.at[n],
            recv_sem=recv_face.at[n],
            device_id=(place_first, lax.rem(place_second + step, count_second)),
            device_id_type=mesh,
        )
        for n, (start, target, step) in enumerate(
            ((inner - face, low_ref, 1), (0, high_ref, count_second - 1))
        )
    ]

    def line_copy(t, k):
        return pltpu.make_async_remote_copy(
            src_ref=sent.at[t, pl.ds(k * chunk, chunk)],
            dst_ref=got.at[me],
            send_sem=send_line.at[t, k],
            recv_sem=recv_line.at[me],
            device_id=(lax.rem(owner_shift(k) + t, count_first), k),
            device_id_type=mesh,
        )

    def line_from(d):
        return pltpu.make_async_remote_copy(
            src_ref=sent.at[0, pl.ds(0, chunk)],
            dst_ref=got.at[d],
            send_sem=self_sem.at[1],
            recv_sem=recv_line.at[d],
            device_id=(d // count_second, lax.rem(d, count_second)),
            device_id_type=mesh,
        )

    def back_copy(d):
        return pltpu.make_async_remote_copy(
            src_ref=answer.at[d],
            dst_ref=back.at[own_tile, pl.ds(place_second * chunk, chunk)],
            send_sem=send_back.at[d],
            recv_sem=recv_back.at[own_tile, place_second],
            device_id=(d // count_second, lax.rem(d, count_second)),
            device_id_type=mesh,
        )

    def back_from(t, k):
        return pltpu.make_async_remote_copy(
            src_ref=answer.at[0],
            dst_ref=back.at[t, pl.ds(k * chunk, chunk)],
            send_sem=self_sem.at[1],
            recv_sem=recv_back.at[t, k],
            device_id=(lax.rem(owner_shift(k) + t, count_first), k),
            device_id_type=mesh,
        )

    def over_devices(action):
        def body(d, carry):
            @pl.when(d != me)
            def _():
                action(d)

            return carry

        lax.fori_loop(0, devices, body, 0)

    def over_owners(t, action):
        def body(k, carry):
            @pl.when((k != place_second) | (own_tile != t))
            def _():
                action(t, k)

            return carry

        lax.fori_loop(0, count_second, body, 0)

    def weighed(values, members, state):
        total = None
        for g in members:
            term = values[g] * state[g]
            total = term if total is None else total + term
        return total

    for t in range(tiles):
        r, even, odd = weights(0, t), weights(2, t), weights(3, t)
        for copy in first[t]:
            copy.wait()
        state = carries(mom_one, t)

        def lines_of(add):
            def body(i, j, carry):
                up, down = carry
                up = step_on(r, up, row_of(f_ref, i, t))
                down = tuple(r[g] * down[g] for g in range(groups))
                for n, (values, members) in enumerate(((even, even_groups), (odd, odd_groups))):
                    one = weighed(values, members, up)
                    two = weighed(values, members, down)
                    part[n, i] = part[n, i] + one if add else one
                    part[n, j] = part[n, j] + two if add else two
                f = row_of(f_ref, j, t)
                return up, tuple(down[g] + f[g] for g in range(groups))

            return body

        state = both_ways(0, middle, lines_of(False), state)
        both_ways(middle, rows, lines_of(True), state)
        lines[:rows, :] = jnp.sum(part[0], axis=1)
        lines[rows : 2 * rows, :] = jnp.sum(part[1], axis=1)
        lines[2 * rows :, :] = jnp.zeros((width - 2 * rows, LANES), F32)
        if t == 0:
            for n in range(2):
                lines[2 * rows + n : 2 * rows + n + 1, :] = jnp.sum(
                    vec_ref[2 + n] * whole, axis=0, keepdims=True
                )
        sent[t] = lines[...].T
        over_owners(t, lambda t, k: line_copy(t, k).start())
    for copy in faces:
        copy.start()

    @pl.when(is_owner)
    def _():
        own = pltpu.make_async_copy(
            sent.at[own_tile, pl.ds(place_second * chunk, chunk)], got.at[me], self_sem.at[0]
        )
        own.start()
        table[...] = jnp.zeros_like(table)
        for i in range(count_first):
            for n in range(2):
                block = basis_ref[n, i * rows : (i + 1) * rows, :]
                table[n, i, :rows, :wave] = block
                table[n, i, rows : 2 * rows, wave:] = block
                for place, row in enumerate((rows * (i + 1) % wave, (rows * i - 1) % wave)):
                    line = basis_ref[n, row : row + 1, :]
                    table[n, i, 2 * rows + 2 + place : 2 * rows + 3 + place, :wave] = line
                    table[n, i, 2 * rows + 4 + place : 2 * rows + 5 + place, wave:] = line
        own_eig = own_ref[...]
        lam = own_eig + eig_ref[...]
        sinh = jnp.sqrt(lam + 0.25 * lam * lam)
        flat = lam <= 0.0
        far = power(decay(lam), strip)
        tanh = (1.0 - far) / (1.0 + far)
        green = jnp.where(flat, strip / 4.0, tanh / jnp.where(flat, 1.0, 2.0 * sinh))
        square = tanh * tanh
        half_sine = angle_ref[0]
        det = half_sine * (1.0 - square) + square
        zero = flat & (half_sine <= 0.0)
        inverse = jnp.where(zero, 0.0, 1.0 / jnp.where(zero, 1.0, det))
        gain = angle_ref[1] * green * inverse
        factor[0] = gain * (2.0 + 0.5 * lam)
        factor[1] = jnp.where(zero, 2.0 / strip, gain * (0.5 * lam))
        factor[2] = inverse
        factor[3] = jnp.where(zero, 1.0, 0.0)
        over_devices(lambda d: line_from(d).wait_recv())
        own.wait()
        dot = lambda a, b: jnp.dot(a, b, preferred_element_type=F32)
        modes = None
        for i in range(count_first):
            piece = got[i * count_second : (i + 1) * count_second]
            high, low = halves(piece.reshape(count_second * chunk, width))
            term = dot(high, table[0, i]) + dot(high, table[1, i]) + dot(low, table[0, i])
            modes = term if modes is None else modes + term

        def mixed(which, value):
            high, low = halves(value)
            stack = jnp.concatenate([high, high, low], axis=0)
            return dot(mix_ref[which], stack)

        straight = mixed(0, modes)
        turned = mixed(1, modes)
        s, t = straight[:, :wave], straight[:, wave:]
        s_turned, t_turned = turned[:, :wave], turned[:, wave:]
        sums = jnp.sum(got[...], axis=0)
        lane = lax.broadcasted_iota(jnp.int32, sums.shape, 1)
        sigma = jnp.sum(jnp.where(lane == 2 * rows, sums, 0.0), axis=1, keepdims=True)
        lever = jnp.sum(jnp.where(lane == 2 * rows + 1, sums, 0.0), axis=1, keepdims=True)
        k = np.arange(strip)
        bow = 0.5 * (k * k - (strip - 1) * k) - strip / 4
        mean = jnp.where(own_eig[:chunk] <= 0.0, sigma, 0.0) * (1.0 / (wave * wave))
        gauge = lever - mean * float(wave * count_second * bow.sum())
        gauge = gauge * float(1.0 / (bow[0] * np.sqrt(wave * count_second)))
        tall = lambda value: jnp.concatenate([value] * count_second, axis=0)
        mean, gauge = tall(mean), tall(gauge)
        new_s = factor[0] * s - t_turned * factor[2] + factor[3] * gauge
        new_t = factor[1] * t - s_turned * factor[2]
        solved = mixed(2, jnp.concatenate([new_s, new_t], axis=1))
        high, low = halves(solved)
        wide = lax.broadcasted_iota(jnp.int32, (count_second * chunk, width), 1)
        across = lambda a, b: lax.dot_general(
            a, b, (((1,), (1,)), ((), ())), preferred_element_type=F32
        )
        for i in range(count_first):
            piece = across(high, table[0, i]) + across(high, table[1, i]) + across(low, table[0, i])
            piece = jnp.where(wide == 2 * rows, mean, piece)
            answer[i * count_second : (i + 1) * count_second] = piece.reshape(
                count_second, chunk, width
            )
        over_devices(lambda d: back_copy(d).start())
        kept = pltpu.make_async_copy(
            answer.at[me], back.at[own_tile, pl.ds(place_second * chunk, chunk)], self_sem.at[0]
        )
        kept.start()
        kept.wait()

    second = []
    for t in range(tiles):
        over_owners(t, lambda t, k: back_from(t, k).wait_recv())
        lines[...] = back[t].T
        for n, (start, halo) in enumerate(((0, 2 * rows + 2), (rows, 2 * rows + 4))):
            edge_ref[n, :rows, lane_of(t)] = lines[start : start + rows, :]
            edge_ref[n, rows : rows + 2, lane_of(t)] = lines[halo : halo + 2, :]
        r = weights(0, t)
        if t == 0:
            mean_term = vec_ref[2] * lines[2 * rows : 2 * rows + 1, :]
            mean_term = tuple(mean_term[window[g]] for g in range(groups))
        wide_vec = [
            jnp.broadcast_to(vec_ref[n], (strip, LANES)) for n in range(2)
        ]

        def fresh(i):
            f = list(row_of(f_ref, i, t))
            line_s = lines[pl.ds(i, 1), :]
            line_t = lines[pl.ds(rows + i, 1), :]
            for g in range(groups):
                if t == 0:
                    f[g] = f[g] - mean_term[g]
                if g in even_groups:
                    f[g] = f[g] - wide_vec[0][window[g]] * line_s
                if g in odd_groups:
                    f[g] = f[g] - wide_vec[1][window[g]] * line_t
                f_ref[i, window[g], lane_of(t)] = f[g]
            return tuple(f)

        def renewed(make):
            def body(i, j, carry):
                up, down = carry
                one = fresh(i) if make else row_of(f_ref, i, t)
                two = fresh(j) if make else row_of(f_ref, j, t)
                return step_on(r, up, one), step_on(r, down, two)

            return body

        state = both_ways(0, middle, renewed(True), (zeros, zeros))
        up, down = both_ways(middle, rows, renewed(False), state)
        store_moments(mom_two, t, up, down)
        second.append(shares(mom_two, send_two, recv_two, t))
        for copy in second[t]:
            copy.start()

    stores = []
    for t in range(tiles):
        r, scale = weights(0, t), weights(1, t)
        for copy in second[t]:
            copy.wait()
        carry_up, carry_down = carries(mom_two, t)

        def put(i, value, add):
            for g in range(groups):
                if add:
                    out_ref[i, window[g], lane_of(t)] = (
                        out_ref[i, window[g], lane_of(t)] + value[g]
                    ) * scale[g]
                else:
                    out_ref[i, window[g], lane_of(t)] = value[g]

        def last(add):
            def body(i, j, carry):
                up, down = carry
                up = step_on(r, up, row_of(f_ref, i, t))
                down = tuple(r[g] * down[g] for g in range(groups))
                put(i, up, add)
                put(j, down, add)
                f = row_of(f_ref, j, t)
                return up, tuple(down[g] + f[g] for g in range(groups))

            return body

        state = both_ways(0, middle, last(False), (carry_up, carry_down))
        up, down = both_ways(middle, rows, last(True), state)
        for g in range(groups):
            out_ref[rows, window[g], lane_of(t)] = (r[g] * up[g] + carry_down[g]) * scale[g]
            out_ref[rows + 1, window[g], lane_of(t)] = (carry_up[g] + r[g] * down[g]) * scale[g]
        stores.append(
            pltpu.make_async_copy(
                out_ref.at[:, :, lane_of(t)], out_hbm.at[:, :, lane_of(t)], out_sem.at[t]
            )
        )
        stores[t].start()

    for t in range(tiles):
        over_owners(t, lambda t, k: line_copy(t, k).wait_send())

    @pl.when(is_owner)
    def _():
        over_devices(lambda d: back_copy(d).wait_send())

    for copy in faces + stores:
        copy.wait()


def grid_values_kernel(
    step, anchor_ref, u_ref, edge_ref, strip_ref, wave_ref, out_ref, patch_ref, ext, cut, sems
):
    planes, strip, wave = u_ref.shape
    rows = planes - 2
    tall = ext.shape[1]
    tiles = tall // 8
    chunks = planes // step
    tail = rows - (chunks - 1) * step
    second = strip_ref.shape[0]
    place_first = lax.axis_index("px")
    place_second = lax.axis_index("py")
    count = lax.axis_size("py")
    sub = lax.broadcasted_iota(jnp.int32, (8, wave), 0)

    def out_copy(c, size):
        start = c * step
        return pltpu.make_async_copy(
            ext.at[pl.ds(start, size), :strip, :], out_ref.at[pl.ds(start, size)], sems.at[c]
        )

    def chunk(c, carry):
        values = []
        for i in range(step):
            k = c * step + i
            high, low = halves(u_ref[k])
            stack = jnp.concatenate([high, high, low], axis=0)
            value = jnp.dot(strip_ref[...], stack, preferred_element_type=F32)
            s, t = edge_ref[0, pl.ds(k, 1), :], edge_ref[1, pl.ds(k, 1), :]
            halo = jnp.where(sub == 0, 0.5 * (s - t), jnp.where(sub == 7, 0.5 * (s + t), 0.0))
            values += [value[:strip], value[strip:] + halo]
        high, low = halves(jnp.concatenate(values, axis=0))
        wide = jnp.concatenate([high, low, high], axis=1)
        result = jnp.dot(wide, wave_ref[...], preferred_element_type=F32)
        ext[pl.ds(c * step, step)] = result.reshape(step, tall, wave)

        @pl.when(c < chunks - 1)
        def _():
            out_copy(c, step).start()

        return carry

    lax.fori_loop(0, chunks, chunk, 0)
    out_copy(chunks - 1, tail).start()
    lane = lax.broadcasted_iota(jnp.int32, cut.shape[::2], 1)
    cut[...] = jnp.zeros_like(cut)

    def patch(t, carry):
        slot = (place_first * count + t) * count + lax.rem(place_second - t + count, count)
        x = jnp.clip(anchor_ref[0, slot] - place_first * rows, 0, rows - REG)
        y = jnp.clip(anchor_ref[1, slot] - place_second * strip, 0, strip - REG) // 8
        shift = lax.rem(wave + 1 - jnp.clip(anchor_ref[2, slot], 0, wave - REG), wave)
        for i in range(REG + 2):
            row = x - 1 + i
            row = jnp.where(row < 0, rows + 1, row)
            for d in range(3):
                tile = lax.rem(y + d - 1 + tiles, tiles)
                value = ext[row, pl.ds(pl.multiple_of(tile * 8, 8), 8), :]
                cut[i, 8 * d : 8 * d + 8, :] = pltpu.roll(value, shift, 1)[:, :128]
        total = jnp.zeros(lane.shape, F32)
        for b in range(PATCH):
            line = jnp.where(lane < PATCH, cut[:, 7 + b, :], 0.0)
            total = total + (pltpu.roll(line, PATCH * b, 1) if b else line)
        patch_ref[t + 1] = total
        return carry

    lax.fori_loop(0, count, patch, 0)
    patch_ref[0] = patch_ref[count]
    patch_ref[count + 1] = patch_ref[1]

    def finish(c, carry):
        out_copy(c, step).wait()
        return carry

    lax.fori_loop(0, chunks - 1, finish, 0)
    out_copy(chunks - 1, tail).wait()


def patch_exchange_kernel(patch_ref, out_ref, send_sems, recv_sems, own_sem):
    count = out_ref.shape[0]
    place_first = lax.axis_index("px")
    place_second = lax.axis_index("py")
    barrier = pltpu.get_barrier_semaphore()
    mesh = pl.DeviceIdType.MESH
    for d in range(1, count):
        pl.semaphore_signal(
            barrier,
            inc=1,
            device_id=(place_first, lax.rem(place_second + d, count)),
            device_id_type=mesh,
        )
    own = pltpu.make_async_copy(
        patch_ref.at[pl.ds(place_second, 3)], out_ref.at[0], own_sem
    )
    own.start()
    pl.semaphore_wait(barrier, count - 1)
    copies = []
    for d in range(1, count):
        target = lax.rem(place_second + d, count)
        copies.append(
            pltpu.make_async_remote_copy(
                src_ref=patch_ref.at[pl.ds(target, 3)],
                dst_ref=out_ref.at[count - d],
                send_sem=send_sems.at[d],
                recv_sem=recv_sems.at[d],
                device_id=(place_first, target),
                device_id_type=mesh,
            )
        )
    for copy in copies:
        copy.start()
    own.wait()
    for copy in copies:
        copy.wait()


def subgrid_kernel(
    count_ref,
    near_ref,
    own_ref,
    under_ref,
    over_ref,
    xt_ref,
    yz_ref,
    mid_ref,
    low_ref,
    high_ref,
    vel_ref,
    pot_ref,
    kick_ref,
):
    device = lax.axis_index("px") * lax.axis_size("py") + lax.axis_index("py")
    place = pl.program_id(0)
    slot = device * pl.num_programs(0) + place
    below = near_ref[0, slot]
    above = near_ref[1, slot]
    live = place < count_ref[device]
    has_below = below >= 0
    has_above = above >= 0
    back_below = near_ref[1, jnp.maximum(below, 0)] >= 0
    back_above = near_ref[0, jnp.maximum(above, 0)] >= 0
    column = lax.broadcasted_iota(jnp.int32, (16, 128), 1)
    patch = jnp.where(
        column < PATCH,
        pltpu.roll(under_ref[0, 0], 128 - (REG - 1) * PATCH, 1),
        jnp.where(
            column < (PATCH + 1) * PATCH,
            pltpu.roll(own_ref[0, 0], PATCH, 1),
            pltpu.roll(over_ref[0, 0], (PATCH - 1) * PATCH, 1),
        ),
    )
    patch = jnp.where(column < (PATCH + 2) * PATCH, patch, 0.0)
    planes = jnp.dot(patch, yz_ref[...], precision=HIGHEST, preferred_element_type=F32)
    coarse = jnp.dot(xt_ref[...], planes, precision=HIGHEST, preferred_element_type=F32)
    start = coarse[:CELLS, :WIDE]
    x_low = coarse[CELLS : CELLS + 1, :WIDE]
    x_high = coarse[CELLS + 1 : CELLS + 2, :WIDE]
    z_edge = coarse[:CELLS, WIDE : 2 * WIDE]
    y_edge = coarse[:CELLS, 2 * WIDE :]
    shape = (CELLS, WIDE)
    row = lax.broadcasted_iota(jnp.int32, shape, 0)
    lane = lax.broadcasted_iota(jnp.int32, shape, 1)
    third = lane % CELLS
    side = EDGE * CELLS
    end = WIDE - side
    y_above = jnp.where(lane >= WIDE - CELLS, y_edge, pltpu.roll(start, WIDE - CELLS, 1))
    y_below = jnp.where(lane < CELLS, y_edge, pltpu.roll(start, CELLS, 1))
    cut_above = (lane >= WIDE - CELLS) | (
        (lane >= side - CELLS) & (lane < side) & jnp.logical_not(back_below)
    )
    cut_below = (lane < CELLS) | (
        (lane >= end) & (lane < end + CELLS) & jnp.logical_not(back_above)
    )
    fixed = ((lane < side) & jnp.logical_not(has_below)) | (
        (lane >= end) & jnp.logical_not(has_above)
    )
    rho = jnp.concatenate([low_ref[0], mid_ref[0], high_ref[0]], axis=1) * (1.0 / (REF * REF))

    def beside(v):
        return (
            (
                jnp.where(row == 0, x_low, pltpu.roll(v, 1, 0)),
                jnp.where(row == CELLS - 1, x_high, pltpu.roll(v, CELLS - 1, 0)),
            ),
            (
                jnp.where(cut_below, y_below, pltpu.roll(v, CELLS, 1)),
                jnp.where(cut_above, y_above, pltpu.roll(v, WIDE - CELLS, 1)),
            ),
            (
                jnp.where(third == 0, z_edge, pltpu.roll(v, 1, 1)),
                jnp.where(third == CELLS - 1, z_edge, pltpu.roll(v, WIDE - 1, 1)),
            ),
        )

    v = start
    for _ in range(SWEEPS):
        first, second, last = beside(v)
        total = first[1] + first[0] + second[1] + second[0] + last[1] + last[0]
        new = (1.0 - RELAXATION) * v + RELAXATION * (total - rho) / 6.0
        v = jnp.where(fixed, v, new)
    pot_ref[0] = jnp.where(live, v[:, side:end], 0.0)
    for q, (below, above) in enumerate(beside(v)):
        slope = (above[:, side:end] - below[:, side:end]) * (REF / 2.0)
        kick_ref[q, 0] = jnp.where(live, vel_ref[q, 0] - slope, 0.0)


def poisson(root_density, density, slot_anchor):
    count_first = lax.axis_size("px")
    count_second = lax.axis_size("py")
    devices = count_first * count_second
    place_second = lax.axis_index("py")
    rows, strip, wave = root_density.shape
    tiles = wave // LANES
    chunk = LANES // count_second
    width = -(-(2 * rows + 6) // 128) * 128
    basis = fourier_basis(wave)
    strip_table, strip_eig = strip_basis(strip)
    eig = 4.0 * np.sin(np.pi / wave * np.arange(wave)) ** 2
    mixes, angles = strip_coupling(count_second, chunk)
    cell = np.arange(strip)
    bow = 0.5 * (cell * cell - (strip - 1) * cell) - strip / 4
    lower = cell < strip // 2
    edge = strip_table[:, 0]
    vectors = np.stack(
        [
            np.where(lower, edge, 0.0),
            np.where(lower, 0.0, edge),
            strip_table.sum(1),
            strip_table @ bow,
        ]
    )[:, :, None]
    own_tile = lax.rem(
        lax.axis_index("px") + 2 * devices - owner_shift(place_second), count_first
    )
    mix_high, mix_low = halves(jnp.asarray(mixes, F32))
    own = jnp.minimum(own_tile, tiles - 1) * LANES + place_second * chunk
    own_eig = lax.dynamic_slice_in_dim(jnp.asarray(eig, F32), own, chunk)
    own_eig = jnp.tile(own_eig, count_second)[:, None]
    z_basis = jnp.asarray(basis, F32)
    y_basis = jnp.asarray(strip_table, F32)
    f = jnp.einsum("xyz,cz->xyc", root_density, z_basis, precision=HIGH)
    f = jnp.einsum("xyc,by->xbc", f, y_basis, precision=HIGH)
    moment = pltpu.VMEM((tiles, count_first, 2, strip, LANES), F32)
    dma = pltpu.SemaphoreType.DMA
    face = jax.ShapeDtypeStruct(density.shape[:2] + (EDGE * CELLS,), F32)
    vmem = pl.BlockSpec(memory_space=pltpu.VMEM)
    hbm = pl.BlockSpec(memory_space=pl.ANY)
    u, edges, low_density, high_density = pl.pallas_call(
        lambda *refs: grid_kernel((count_first, count_second), *refs),
        in_specs=[hbm] + [vmem] * 7 + [hbm],
        out_specs=[hbm, vmem, hbm, hbm],
        out_shape=[
            jax.ShapeDtypeStruct((rows + 2, strip, wave), F32),
            jax.ShapeDtypeStruct((2, rows + 2, wave), F32),
            face,
            face,
        ],
        scratch_shapes=[
            pltpu.VMEM((rows, strip, wave), F32),
            pltpu.VMEM((rows + 2, strip, wave), F32),
            pltpu.VMEM((width, LANES), F32),
            pltpu.VMEM((tiles, LANES, width), F32),
            pltpu.VMEM((devices, chunk, width), F32),
            pltpu.VMEM((devices, chunk, width), F32),
            pltpu.VMEM((tiles, LANES, width), F32),
            moment,
            moment,
            pltpu.VMEM((2, rows, 8, LANES), F32),
            pltpu.VMEM((2, count_first, width, 2 * wave), jnp.bfloat16),
            pltpu.VMEM((4, count_second * chunk, wave), F32),
            pltpu.VMEM((6, strip, wave), F32),
            dma((tiles,)),
            dma((tiles,)),
            dma((tiles, count_first)),
            dma((tiles, count_first)),
            dma((tiles, count_first)),
            dma((tiles, count_first)),
            dma((tiles, count_second)),
            dma((devices,)),
            dma((devices,)),
            dma((tiles, count_second)),
            dma((2,)),
            dma((2,)),
            dma((2,)),
        ],
        compiler_params=pltpu.CompilerParams(
            collective_id=1, has_side_effects=True, vmem_limit_bytes=60 * 1024 * 1024
        ),
    )(
        f,
        jnp.asarray(strip_eig[:, None], F32),
        jnp.asarray(eig[None, :], F32),
        own_eig,
        jnp.asarray(vectors, F32),
        jnp.stack(halves(jnp.asarray(basis.T, F32))),
        jnp.concatenate([mix_high, mix_low, mix_high], axis=2),
        jnp.asarray(angles, F32),
        density,
    )
    tall = strip + 8
    step = max(n for n in range(1, 15) if (rows + 2) % n == 0)
    extended = np.zeros((tall, strip))
    extended[:strip] = strip_table.T
    extended[strip] = -strip_table[:, 0]
    extended[-1] = -strip_table[:, -1]
    high, low = halves(jnp.asarray(extended, F32))
    strip_wide = jnp.concatenate([high, low, high], axis=1)
    high, low = halves(z_basis)
    wave_tall = jnp.concatenate([high, high, low], axis=0)
    chunks = (rows + 2) // step
    coarse, patches = pl.pallas_call(
        lambda *refs: grid_values_kernel(step, *refs),
        in_specs=[pl.BlockSpec(memory_space=pltpu.SMEM)] + [vmem] * 4,
        out_specs=[hbm, vmem],
        out_shape=[
            jax.ShapeDtypeStruct((rows, strip, wave), F32),
            jax.ShapeDtypeStruct((count_second + 2, 16, 128), F32),
        ],
        scratch_shapes=[
            pltpu.VMEM((rows + 2, tall, wave), F32),
            pltpu.VMEM((16, 24, 128), F32),
            dma((chunks,)),
        ],
        compiler_params=pltpu.CompilerParams(vmem_limit_bytes=60 * 1024 * 1024),
    )(slot_anchor, u, edges, strip_wide, wave_tall)
    arrived = pl.pallas_call(
        patch_exchange_kernel,
        in_specs=[vmem],
        out_specs=vmem,
        out_shape=jax.ShapeDtypeStruct((count_second, 3, 16, 128), F32),
        scratch_shapes=[dma((count_second,)), dma((count_second,)), dma(())],
        compiler_params=pltpu.CompilerParams(collective_id=2, has_side_effects=True),
    )(patches)
    return coarse, arrived, low_density, high_density


def local(root_density, subgrid_density, velocity, slot_anchor, slot_count, neighbour):
    per_device = subgrid_density.shape[0]
    side = EDGE * CELLS
    inner = CELLS * CELLS
    coarse_potential, patches, low_density, high_density = poisson(
        root_density, subgrid_density, slot_anchor
    )
    x_table, yz_table = patch_tables()
    count = lax.axis_size("py")
    smem = pl.BlockSpec(memory_space=pltpu.SMEM)
    slot_spec = lambda width: pl.BlockSpec((1, CELLS, width), lambda s: (s, 0, 0))
    vel_spec = pl.BlockSpec((3, 1, CELLS, inner), lambda s: (0, s, 0, 0))
    patch_spec = lambda step: pl.BlockSpec(
        (1, 1, 16, 128), lambda s: (lax.rem(s + step + count, count), step + 1, 0, 0)
    )
    potential, kicked = pl.pallas_call(
        subgrid_kernel,
        grid=(per_device,),
        in_specs=[
            smem,
            smem,
            patch_spec(0),
            patch_spec(-1),
            patch_spec(1),
            pl.BlockSpec(x_table.shape, lambda s: (0, 0)),
            pl.BlockSpec(yz_table.shape, lambda s: (0, 0)),
            slot_spec(inner),
            slot_spec(side),
            slot_spec(side),
            vel_spec,
        ],
        out_specs=[slot_spec(inner), vel_spec],
        out_shape=[
            jax.ShapeDtypeStruct(subgrid_density.shape, F32),
            jax.ShapeDtypeStruct(velocity.shape, F32),
        ],
        compiler_params=pltpu.CompilerParams(
            dimension_semantics=("arbitrary",), vmem_limit_bytes=60 * 1024 * 1024
        ),
    )(
        slot_count,
        neighbour,
        patches,
        patches,
        patches,
        jnp.asarray(x_table),
        jnp.asarray(yz_table),
        subgrid_density,
        low_density,
        high_density,
        velocity,
    )
    return (coarse_potential, potential, kicked)


def solution(mesh):
    return jax.shard_map(
        local,
        mesh=mesh,
        in_specs=(
            P("px", "py", None),
            P(("px", "py"), None, None),
            P(None, ("px", "py"), None, None),
            P(),
            P(),
            P(),
        ),
        out_specs=(
            P("px", "py", None),
            P(("px", "py"), None, None),
            P(None, ("px", "py"), None, None),
        ),
        check_vma=False,
    )
```

```python
import jax
import jax.numpy as jnp
import numpy as np
from jax import lax
from jax.experimental import pallas as pl
from jax.experimental.pallas import tpu as pltpu
from jax.sharding import PartitionSpec as P

NR = 384
REG = 8
REF = 4
SWEEPS = 4
CELLS = REG * REF
EDGE = SWEEPS
LAYERS = CELLS + 2 * EDGE
WIDE = LAYERS * CELLS
RELAXATION = 6.0 / 7.0
HIGHEST = lax.Precision.HIGHEST
HIGH = lax.Precision.HIGH
F32 = jnp.float32


def fourier_basis(length):
    cell = np.arange(length)
    rows = []
    for k in range(length):
        if k in (0, length // 2):
            rows.append(np.cos(2 * np.pi * (k * cell % length) / length) / np.sqrt(length))
        elif k < length // 2:
            rows.append(np.cos(2 * np.pi * (k * cell % length) / length) * np.sqrt(2 / length))
        else:
            rows.append(
                np.sin(2 * np.pi * ((length - k) * cell % length) / length) * np.sqrt(2 / length)
            )
    return np.stack(rows)


def strip_basis(cells):
    place = np.arange(cells) - (cells - 1) / 2
    mode = 2 * np.arange(cells // 2) + 1
    angle = np.pi * mode[:, None] * place[None, :] / cells
    basis = np.concatenate([np.cos(angle), np.sin(angle)]) * np.sqrt(2 / cells)
    eig = 4 * np.sin(np.pi * mode / (2 * cells)) ** 2
    return basis, np.concatenate([eig, eig])


def strip_coupling(count, rows):
    basis = fourier_basis(count)
    turn = np.zeros((count, count))
    theta = 2 * np.pi * np.arange(count) / count
    for k in range(1, (count + 1) // 2):
        turn[k, count - k] = np.sin(theta[k])
        turn[count - k, k] = -np.sin(theta[k])
    wide = lambda matrix: np.kron(matrix, np.eye(rows))
    mixes = np.stack([wide(basis), wide(turn @ basis), wide(basis.T)])
    half_sine = np.sin(theta / 2) ** 2
    factors = np.stack([half_sine, 4 * (1 - half_sine)])
    return mixes, np.repeat(factors, rows, axis=1)[:, :, None]


def axis_weights(cells, first, count):
    table = np.zeros((len(cells), count))
    for row, cell in enumerate(cells):
        mark = 2 * cell - 1 + REF
        low = mark // (2 * REF)
        frac = (mark - 2 * REF * low) / (2 * REF)
        table[row, low - first] += 1 - frac
        if frac:
            table[row, low + 1 - first] += frac
    return table


PATCH = REG + 2
PATCH_X = REG + 2
PATCH_Y = REG + 4
PATCH_Z = REG + 2


def patch_tables():
    inner = np.arange(1, CELLS + 1)
    x_side = axis_weights(np.concatenate([inner, [0, CELLS + 1]]), 0, PATCH_X)
    x_table = np.zeros((CELLS + 8, 16))
    x_table[: CELLS + 2, :PATCH_X] = x_side
    y_cells = np.arange(1 - EDGE, CELLS + EDGE + 1)
    y_side = axis_weights(y_cells, -1, PATCH_Y)
    y_out = axis_weights(np.array([-EDGE, CELLS + EDGE + 1]), -1, PATCH_Y)
    z_side = axis_weights(np.arange(CELLS + 2), 0, PATCH_Z)
    z_edge = np.zeros((CELLS, PATCH_Z))
    z_edge[0] = z_side[0]
    z_edge[-1] = z_side[-1]
    y_edge = np.zeros((LAYERS, PATCH_Y))
    y_edge[0] = y_out[0]
    y_edge[-1] = y_out[1]

    def both(ys, zs):
        return np.einsum("jb,kc->bcjk", ys, zs).reshape(PATCH_Y * PATCH_Z, WIDE)

    table = np.zeros((128, 3 * WIDE))
    table[: PATCH_Y * PATCH_Z] = np.concatenate(
        [both(y_side, z_side[1:-1]), both(y_side, z_edge), both(y_edge, z_side[1:-1])], axis=1
    )
    return x_table.astype(np.float32), table.astype(np.float32)


def decay(delta):
    return 1.0 / (1.0 + 0.5 * delta + jnp.sqrt(delta + 0.25 * delta * delta))


def power(value, exponent):
    result = None
    while exponent:
        if exponent & 1:
            result = value if result is None else result * value
        exponent >>= 1
        if exponent:
            value = value * value
    return result


def halves(value):
    high = value.astype(jnp.bfloat16)
    return high, (value - high.astype(F32)).astype(jnp.bfloat16)


def thirds(value):
    high = value.astype(jnp.bfloat16)
    rest = value - high.astype(F32)
    middle = rest.astype(jnp.bfloat16)
    return high, middle, (rest - middle.astype(F32)).astype(jnp.bfloat16)


def owner_shift(place_second):
    return place_second // 2 * 2 + 2


LANES = 128


def grid_kernel(
    sizes,
    f_hbm,
    eig_b_ref,
    eig_ref,
    own_ref,
    vec_ref,
    basis_ref,
    mix_ref,
    angle_ref,
    density_ref,
    out_hbm,
    edge_ref,
    low_ref,
    high_ref,
    f_ref,
    out_ref,
    lines,
    sent,
    got,
    answer,
    back,
    mom_one,
    mom_two,
    part,
    table,
    factor,
    weight,
    in_sem,
    out_sem,
    send_one,
    recv_one,
    send_two,
    recv_two,
    send_line,
    recv_line,
    send_back,
    recv_back,
    self_sem,
    send_face,
    recv_face,
):
    count_first, count_second = sizes
    devices = count_first * count_second
    rows, strip, wave = f_ref.shape
    tiles = wave // LANES
    groups = strip // 8
    half = strip // 2
    middle = rows // 2
    fold = 4
    chunk = got.shape[1]
    width = lines.shape[0]
    mesh = pl.DeviceIdType.MESH
    place_first = lax.axis_index("px")
    place_second = lax.axis_index("py")
    me = place_first * count_second + place_second
    own_tile = lax.rem(
        place_first + 2 * count_second * count_first - owner_shift(place_second), count_first
    )
    is_owner = own_tile < tiles
    barrier = pltpu.get_barrier_semaphore()

    def greet(step, carry):
        other = lax.rem(me + step, devices)
        pl.semaphore_signal(
            barrier,
            inc=1,
            device_id=(other // count_second, lax.rem(other, count_second)),
            device_id_type=mesh,
        )
        return carry

    lax.fori_loop(1, devices, greet, 0)
    lane_of = lambda t: slice(t * LANES, (t + 1) * LANES)
    loads = [
        pltpu.make_async_copy(
            f_hbm.at[:, :, lane_of(t)], f_ref.at[:, :, lane_of(t)], in_sem.at[t]
        )
        for t in range(tiles)
    ]
    for copy in loads:
        copy.start()

    window = [slice(8 * g, 8 * g + 8) for g in range(groups)]
    even_groups = [g for g in range(groups) if 8 * g < half]
    odd_groups = [g for g in range(groups) if 8 * g + 8 > half]
    zeros = tuple(jnp.zeros((8, LANES), F32) for _ in range(groups))

    r_all = decay(eig_b_ref[...] + eig_ref[...])
    scale_all = -r_all / ((1.0 - r_all) * (1.0 + r_all))
    ratio_all = power(r_all, rows)
    weight[0] = r_all
    weight[1] = scale_all
    weight[2] = 2.0 * vec_ref[0] * scale_all
    weight[3] = -2.0 * vec_ref[1] * scale_all
    weight[4] = ratio_all
    weight[5] = 1.0 / (1.0 - power(ratio_all, count_first))

    def weights(which, t):
        return tuple(weight[which, window[g], lane_of(t)] for g in range(groups))

    def row_of(ref, i, t):
        return tuple(ref[i, window[g], lane_of(t)] for g in range(groups))

    def step_on(r, state, f):
        return tuple(r[g] * state[g] + f[g] for g in range(groups))

    def both_ways(start, stop, body, carry):
        def folded(n, carry):
            for k in range(fold):
                i = start + n * fold + k
                carry = body(i, rows - 1 - i, carry)
            return carry

        return lax.fori_loop(0, (stop - start) // fold, folded, carry)

    def store_moments(buffer, t, up, down):
        for g in range(groups):
            buffer[t, 0, 0, window[g], :] = up[g]
            buffer[t, 0, 1, window[g], :] = down[g]

    def shares(buffer, send, recv, t):
        return [
            pltpu.make_async_remote_copy(
                src_ref=buffer.at[t, 0],
                dst_ref=buffer.at[t, d],
                send_sem=send.at[t, d],
                recv_sem=recv.at[t, d],
                device_id=(lax.rem(place_first + d, count_first), place_second),
                device_id_type=mesh,
            )
            for d in range(1, count_first)
        ]

    def carries(buffer, t):
        ratio, norm = weights(4, t), weights(5, t)
        up, down = [], []
        for g in range(groups):
            total = buffer[t, 0, 0, window[g], :]
            for d in range(count_first - 1, 0, -1):
                total = ratio[g] * total + buffer[t, d, 0, window[g], :]
            up.append(total * norm[g])
            total = buffer[t, 0, 1, window[g], :]
            for d in range(1, count_first):
                total = ratio[g] * total + buffer[t, d, 1, window[g], :]
            down.append(total * norm[g])
        return tuple(up), tuple(down)

    first = []
    for t in range(tiles):
        r = weights(0, t)
        loads[t].wait()

        def moments(i, j, carry):
            up, down, total = carry
            f = row_of(f_ref, i, t)
            up = step_on(r, up, f)
            down = step_on(r, down, row_of(f_ref, j, t))
            if t == 0:
                total = tuple(total[g] + f[g] for g in range(groups))
            return up, down, total

        up, down, total = both_ways(0, rows, moments, (zeros, zeros, zeros if t == 0 else ()))
        store_moments(mom_one, t, up, down)
        if t == 0:
            whole = jnp.concatenate(total, axis=0)
            pl.semaphore_wait(barrier, devices - 1)
        first.append(shares(mom_one, send_one, recv_one, t))
        for copy in first[t]:
            copy.start()

    face = low_ref.shape[2]
    inner = density_ref.shape[2]
    faces = [
        pltpu.make_async_remote_copy(
            src_ref=density_ref.at[:, :, pl.ds(start, face)],
            dst_ref=target,
            send_sem=send_face.at[n],
            recv_sem=recv_face.at[n],
            device_id=(place_first, lax.rem(place_second + step, count_second)),
            device_id_type=mesh,
        )
        for n, (start, target, step) in enumerate(
            ((inner - face, low_ref, 1), (0, high_ref, count_second - 1))
        )
    ]

    def line_copy(t, k):
        return pltpu.make_async_remote_copy(
            src_ref=sent.at[t, pl.ds(k * chunk, chunk)],
            dst_ref=got.at[me],
            send_sem=send_line.at[t, k],
            recv_sem=recv_line.at[me],
            device_id=(lax.rem(owner_shift(k) + t, count_first), k),
            device_id_type=mesh,
        )

    def line_from(d):
        return pltpu.make_async_remote_copy(
            src_ref=sent.at[0, pl.ds(0, chunk)],
            dst_ref=got.at[d],
            send_sem=self_sem.at[1],
            recv_sem=recv_line.at[d],
            device_id=(d // count_second, lax.rem(d, count_second)),
            device_id_type=mesh,
        )

    def back_copy(d):
        return pltpu.make_async_remote_copy(
            src_ref=answer.at[d],
            dst_ref=back.at[own_tile, pl.ds(place_second * chunk, chunk)],
            send_sem=send_back.at[d],
            recv_sem=recv_back.at[own_tile, place_second],
            device_id=(d // count_second, lax.rem(d, count_second)),
            device_id_type=mesh,
        )

    def back_from(t, k):
        return pltpu.make_async_remote_copy(
            src_ref=answer.at[0],
            dst_ref=back.at[t, pl.ds(k * chunk, chunk)],
            send_sem=self_sem.at[1],
            recv_sem=recv_back.at[t, k],
            device_id=(lax.rem(owner_shift(k) + t, count_first), k),
            device_id_type=mesh,
        )

    def over_devices(action):
        def body(d, carry):
            @pl.when(d != me)
            def _():
                action(d)

            return carry

        lax.fori_loop(0, devices, body, 0)

    def over_owners(t, action):
        def body(k, carry):
            @pl.when((k != place_second) | (own_tile != t))
            def _():
                action(t, k)

            return carry

        lax.fori_loop(0, count_second, body, 0)

    def weighed(values, members, state):
        total = None
        for g in members:
            term = values[g] * state[g]
            total = term if total is None else total + term
        return total

    for t in range(tiles):
        r, even, odd = weights(0, t), weights(2, t), weights(3, t)
        for copy in first[t]:
            copy.wait()
        state = carries(mom_one, t)

        def lines_of(add):
            def body(i, j, carry):
                up, down = carry
                up = step_on(r, up, row_of(f_ref, i, t))
                down = tuple(r[g] * down[g] for g in range(groups))
                for n, (values, members) in enumerate(((even, even_groups), (odd, odd_groups))):
                    one = weighed(values, members, up)
                    two = weighed(values, members, down)
                    part[n, i] = part[n, i] + one if add else one
                    part[n, j] = part[n, j] + two if add else two
                f = row_of(f_ref, j, t)
                return up, tuple(down[g] + f[g] for g in range(groups))

            return body

        state = both_ways(0, middle, lines_of(False), state)
        both_ways(middle, rows, lines_of(True), state)
        lines[:rows, :] = jnp.sum(part[0], axis=1)
        lines[rows : 2 * rows, :] = jnp.sum(part[1], axis=1)
        lines[2 * rows :, :] = jnp.zeros((width - 2 * rows, LANES), F32)
        if t == 0:
            for n in range(2):
                lines[2 * rows + n : 2 * rows + n + 1, :] = jnp.sum(
                    vec_ref[2 + n] * whole, axis=0, keepdims=True
                )
        sent[t] = lines[...].T
        over_owners(t, lambda t, k: line_copy(t, k).start())
    for copy in faces:
        copy.start()

    @pl.when(is_owner)
    def _():
        own = pltpu.make_async_copy(
            sent.at[own_tile, pl.ds(place_second * chunk, chunk)], got.at[me], self_sem.at[0]
        )
        own.start()
        table[...] = jnp.zeros_like(table)
        for i in range(count_first):
            for n in range(2):
                block = basis_ref[n, i * rows : (i + 1) * rows, :]
                table[n, i, :rows, :wave] = block
                table[n, i, rows : 2 * rows, wave:] = block
                for place, row in enumerate((rows * (i + 1) % wave, (rows * i - 1) % wave)):
                    line = basis_ref[n, row : row + 1, :]
                    table[n, i, 2 * rows + 2 + place : 2 * rows + 3 + place, :wave] = line
                    table[n, i, 2 * rows + 4 + place : 2 * rows + 5 + place, wave:] = line
        start = own_tile * LANES + place_second * chunk
        own_eig = jnp.concatenate([own_ref[pl.ds(start, chunk), :]] * count_second, axis=0)
        lam = own_eig + eig_ref[...]
        sinh = jnp.sqrt(lam + 0.25 * lam * lam)
        flat = lam <= 0.0
        far = power(decay(lam), strip)
        tanh = (1.0 - far) / (1.0 + far)
        green = jnp.where(flat, strip / 4.0, tanh / jnp.where(flat, 1.0, 2.0 * sinh))
        square = tanh * tanh
        half_sine = angle_ref[0]
        det = half_sine * (1.0 - square) + square
        zero = flat & (half_sine <= 0.0)
        inverse = jnp.where(zero, 0.0, 1.0 / jnp.where(zero, 1.0, det))
        gain = angle_ref[1] * green * inverse
        factor[0] = gain * (2.0 + 0.5 * lam)
        factor[1] = jnp.where(zero, 2.0 / strip, gain * (0.5 * lam))
        factor[2] = inverse
        factor[3] = jnp.where(zero, 1.0, 0.0)
        over_devices(lambda d: line_from(d).wait_recv())
        own.wait()
        dot = lambda a, b: jnp.dot(a, b, preferred_element_type=F32)
        modes = None
        for i in range(count_first):
            piece = got[i * count_second : (i + 1) * count_second]
            high, low = halves(piece.reshape(count_second * chunk, width))
            term = dot(high, table[0, i]) + dot(high, table[1, i]) + dot(low, table[0, i])
            modes = term if modes is None else modes + term

        def mixed(which, value):
            high, low = halves(value)
            stack = jnp.concatenate([high, high, low], axis=0)
            return dot(mix_ref[which], stack)

        straight = mixed(0, modes)
        turned = mixed(1, modes)
        s, t = straight[:, :wave], straight[:, wave:]
        s_turned, t_turned = turned[:, :wave], turned[:, wave:]
        sums = jnp.sum(got[...], axis=0)
        lane = lax.broadcasted_iota(jnp.int32, sums.shape, 1)
        sigma = jnp.sum(jnp.where(lane == 2 * rows, sums, 0.0), axis=1, keepdims=True)
        lever = jnp.sum(jnp.where(lane == 2 * rows + 1, sums, 0.0), axis=1, keepdims=True)
        k = np.arange(strip)
        bow = 0.5 * (k * k - (strip - 1) * k) - strip / 4
        mean = jnp.where(own_eig[:chunk] <= 0.0, sigma, 0.0) * (1.0 / (wave * wave))
        gauge = lever - mean * float(wave * count_second * bow.sum())
        gauge = gauge * float(1.0 / (bow[0] * np.sqrt(wave * count_second)))
        tall = lambda value: jnp.concatenate([value] * count_second, axis=0)
        mean, gauge = tall(mean), tall(gauge)
        new_s = factor[0] * s - t_turned * factor[2] + factor[3] * gauge
        new_t = factor[1] * t - s_turned * factor[2]
        solved = mixed(2, jnp.concatenate([new_s, new_t], axis=1))
        high, low = halves(solved)
        wide = lax.broadcasted_iota(jnp.int32, (count_second * chunk, width), 1)
        across = lambda a, b: lax.dot_general(
            a, b, (((1,), (1,)), ((), ())), preferred_element_type=F32
        )
        for i in range(count_first):
            piece = across(high, table[0, i]) + across(high, table[1, i]) + across(low, table[0, i])
            piece = jnp.where(wide == 2 * rows, mean, piece)
            answer[i * count_second : (i + 1) * count_second] = piece.reshape(
                count_second, chunk, width
            )
        over_devices(lambda d: back_copy(d).start())
        kept = pltpu.make_async_copy(
            answer.at[me], back.at[own_tile, pl.ds(place_second * chunk, chunk)], self_sem.at[0]
        )
        kept.start()
        kept.wait()

    second = []
    for t in range(tiles):
        over_owners(t, lambda t, k: back_from(t, k).wait_recv())
        lines[...] = back[t].T
        for n, (start, halo) in enumerate(((0, 2 * rows + 2), (rows, 2 * rows + 4))):
            edge_ref[n, :rows, lane_of(t)] = lines[start : start + rows, :]
            edge_ref[n, rows : rows + 2, lane_of(t)] = lines[halo : halo + 2, :]
        r = weights(0, t)
        if t == 0:
            mean_term = vec_ref[2] * lines[2 * rows : 2 * rows + 1, :]
            mean_term = tuple(mean_term[window[g]] for g in range(groups))
        wide_vec = [
            jnp.broadcast_to(vec_ref[n], (strip, LANES)) for n in range(2)
        ]

        def fresh(i):
            f = list(row_of(f_ref, i, t))
            line_s = lines[pl.ds(i, 1), :]
            line_t = lines[pl.ds(rows + i, 1), :]
            for g in range(groups):
                if t == 0:
                    f[g] = f[g] - mean_term[g]
                if g in even_groups:
                    f[g] = f[g] - wide_vec[0][window[g]] * line_s
                if g in odd_groups:
                    f[g] = f[g] - wide_vec[1][window[g]] * line_t
                f_ref[i, window[g], lane_of(t)] = f[g]
            return tuple(f)

        def renewed(make):
            def body(i, j, carry):
                up, down = carry
                one = fresh(i) if make else row_of(f_ref, i, t)
                two = fresh(j) if make else row_of(f_ref, j, t)
                return step_on(r, up, one), step_on(r, down, two)

            return body

        state = both_ways(0, middle, renewed(True), (zeros, zeros))
        up, down = both_ways(middle, rows, renewed(False), state)
        store_moments(mom_two, t, up, down)
        second.append(shares(mom_two, send_two, recv_two, t))
        for copy in second[t]:
            copy.start()

    stores = []
    for t in range(tiles):
        r, scale = weights(0, t), weights(1, t)
        for copy in second[t]:
            copy.wait()
        carry_up, carry_down = carries(mom_two, t)

        def put(i, value, add):
            for g in range(groups):
                if add:
                    out_ref[i, window[g], lane_of(t)] = (
                        out_ref[i, window[g], lane_of(t)] + value[g]
                    ) * scale[g]
                else:
                    out_ref[i, window[g], lane_of(t)] = value[g]

        def last(add):
            def body(i, j, carry):
                up, down = carry
                up = step_on(r, up, row_of(f_ref, i, t))
                down = tuple(r[g] * down[g] for g in range(groups))
                put(i, up, add)
                put(j, down, add)
                f = row_of(f_ref, j, t)
                return up, tuple(down[g] + f[g] for g in range(groups))

            return body

        state = both_ways(0, middle, last(False), (carry_up, carry_down))
        up, down = both_ways(middle, rows, last(True), state)
        for g in range(groups):
            out_ref[rows, window[g], lane_of(t)] = (r[g] * up[g] + carry_down[g]) * scale[g]
            out_ref[rows + 1, window[g], lane_of(t)] = (carry_up[g] + r[g] * down[g]) * scale[g]
        stores.append(
            pltpu.make_async_copy(
                out_ref.at[:, :, lane_of(t)], out_hbm.at[:, :, lane_of(t)], out_sem.at[t]
            )
        )
        stores[t].start()

    for t in range(tiles):
        over_owners(t, lambda t, k: line_copy(t, k).wait_send())

    @pl.when(is_owner)
    def _():
        over_devices(lambda d: back_copy(d).wait_send())

    for copy in faces + stores:
        copy.wait()


def grid_values_kernel(
    step, anchor_ref, u_ref, edge_ref, strip_ref, wave_ref, out_ref, patch_ref, ext, cut, sems
):
    planes, strip, wave = u_ref.shape
    rows = planes - 2
    tall = ext.shape[1]
    tiles = tall // 8
    chunks = planes // step
    tail = rows - (chunks - 1) * step
    second = strip_ref.shape[0]
    place_first = lax.axis_index("px")
    place_second = lax.axis_index("py")
    count = lax.axis_size("py")
    sub = lax.broadcasted_iota(jnp.int32, (8, wave), 0)

    def out_copy(c, size):
        start = c * step
        return pltpu.make_async_copy(
            ext.at[pl.ds(start, size), :strip, :], out_ref.at[pl.ds(start, size)], sems.at[c]
        )

    def chunk(c, carry):
        values = []
        for i in range(step):
            k = c * step + i
            high, low = halves(u_ref[k])
            stack = jnp.concatenate([high, high, low], axis=0)
            value = jnp.dot(strip_ref[...], stack, preferred_element_type=F32)
            s, t = edge_ref[0, pl.ds(k, 1), :], edge_ref[1, pl.ds(k, 1), :]
            halo = jnp.where(sub == 0, 0.5 * (s - t), jnp.where(sub == 7, 0.5 * (s + t), 0.0))
            values += [value[:strip], value[strip:] + halo]
        high, low = halves(jnp.concatenate(values, axis=0))
        wide = jnp.concatenate([high, low, high], axis=1)
        result = jnp.dot(wide, wave_ref[...], preferred_element_type=F32)
        ext[pl.ds(c * step, step)] = result.reshape(step, tall, wave)

        @pl.when(c < chunks - 1)
        def _():
            out_copy(c, step).start()

        return carry

    lax.fori_loop(0, chunks, chunk, 0)
    out_copy(chunks - 1, tail).start()
    lane = lax.broadcasted_iota(jnp.int32, cut.shape[::2], 1)
    cut[...] = jnp.zeros_like(cut)

    def patch(t, carry):
        slot = (place_first * count + t) * count + lax.rem(place_second - t + count, count)
        x = jnp.clip(anchor_ref[0, slot] - place_first * rows, 0, rows - REG)
        y = jnp.clip(anchor_ref[1, slot] - place_second * strip, 0, strip - REG) // 8
        shift = lax.rem(wave + 1 - jnp.clip(anchor_ref[2, slot], 0, wave - REG), wave)
        for i in range(REG + 2):
            row = x - 1 + i
            row = jnp.where(row < 0, rows + 1, row)
            for d in range(3):
                tile = lax.rem(y + d - 1 + tiles, tiles)
                value = ext[row, pl.ds(pl.multiple_of(tile * 8, 8), 8), :]
                cut[i, 8 * d : 8 * d + 8, :] = pltpu.roll(value, shift, 1)[:, :128]
        total = jnp.zeros(lane.shape, F32)
        for b in range(PATCH):
            line = jnp.where(lane < PATCH, cut[:, 7 + b, :], 0.0)
            total = total + (pltpu.roll(line, PATCH * b, 1) if b else line)
        patch_ref[t + 1] = total
        return carry

    lax.fori_loop(0, count, patch, 0)
    patch_ref[0] = patch_ref[count]
    patch_ref[count + 1] = patch_ref[1]

    def finish(c, carry):
        out_copy(c, step).wait()
        return carry

    lax.fori_loop(0, chunks - 1, finish, 0)
    out_copy(chunks - 1, tail).wait()


def patch_exchange_kernel(patch_ref, out_ref, send_sems, recv_sems, own_sem):
    count = out_ref.shape[0]
    place_first = lax.axis_index("px")
    place_second = lax.axis_index("py")
    barrier = pltpu.get_barrier_semaphore()
    mesh = pl.DeviceIdType.MESH
    for d in range(1, count):
        pl.semaphore_signal(
            barrier,
            inc=1,
            device_id=(place_first, lax.rem(place_second + d, count)),
            device_id_type=mesh,
        )
    own = pltpu.make_async_copy(
        patch_ref.at[pl.ds(place_second, 3)], out_ref.at[0], own_sem
    )
    own.start()
    pl.semaphore_wait(barrier, count - 1)
    copies = []
    for d in range(1, count):
        target = lax.rem(place_second + d, count)
        copies.append(
            pltpu.make_async_remote_copy(
                src_ref=patch_ref.at[pl.ds(target, 3)],
                dst_ref=out_ref.at[count - d],
                send_sem=send_sems.at[d],
                recv_sem=recv_sems.at[d],
                device_id=(place_first, target),
                device_id_type=mesh,
            )
        )
    for copy in copies:
        copy.start()
    own.wait()
    for copy in copies:
        copy.wait()


def subgrid_kernel(
    count_ref,
    near_ref,
    patch_ref,
    xt_ref,
    yz_ref,
    mid_ref,
    low_ref,
    high_ref,
    vel_ref,
    pot_ref,
    kick_ref,
    plane_ref,
):
    device = lax.axis_index("px") * lax.axis_size("py") + lax.axis_index("py")
    place = pl.program_id(0)
    slot = device * pl.num_programs(0) + place
    below = near_ref[0, slot]
    above = near_ref[1, slot]
    live = place < count_ref[device]
    has_below = below >= 0
    has_above = above >= 0
    back_below = near_ref[1, jnp.maximum(below, 0)] >= 0
    back_above = near_ref[0, jnp.maximum(above, 0)] >= 0

    @pl.when(place == 0)
    def _():
        column = lax.broadcasted_iota(jnp.int32, (16, LANES), 1)
        count = patch_ref.shape[0]
        stack = []
        for s in range(count):
            own = pltpu.roll(patch_ref[s, 1], PATCH, 1)
            under = pltpu.roll(patch_ref[(s - 1) % count, 0], LANES - (REG - 1) * PATCH, 1)
            over = pltpu.roll(patch_ref[(s + 1) % count, 2], (PATCH - 1) * PATCH, 1)
            patch = jnp.where(
                column < PATCH, under, jnp.where(column < (PATCH + 1) * PATCH, own, over)
            )
            stack.append(jnp.where(column < (PATCH + 2) * PATCH, patch, 0.0))
        total = None
        for piece in thirds(jnp.concatenate(stack, axis=0)):
            term = jnp.dot(piece, yz_ref[...], preferred_element_type=F32)
            total = term if total is None else total + term
        plane_ref[...] = total.reshape(plane_ref.shape)

    pieces = jnp.concatenate(thirds(plane_ref[place]), axis=0)
    coarse = jnp.dot(xt_ref[...], pieces, preferred_element_type=F32)
    start = coarse[:CELLS, :WIDE]
    x_low = coarse[CELLS : CELLS + 1, :WIDE]
    x_high = coarse[CELLS + 1 : CELLS + 2, :WIDE]
    z_edge = coarse[:CELLS, WIDE : 2 * WIDE]
    y_edge = coarse[:CELLS, 2 * WIDE :]
    shape = (CELLS, WIDE)
    row = lax.broadcasted_iota(jnp.int32, shape, 0)
    lane = lax.broadcasted_iota(jnp.int32, shape, 1)
    third = lane % CELLS
    side = EDGE * CELLS
    end = WIDE - side
    y_above = jnp.where(lane >= WIDE - CELLS, y_edge, pltpu.roll(start, WIDE - CELLS, 1))
    y_below = jnp.where(lane < CELLS, y_edge, pltpu.roll(start, CELLS, 1))
    cut_above = (lane >= WIDE - CELLS) | (
        (lane >= side - CELLS) & (lane < side) & jnp.logical_not(back_below)
    )
    cut_below = (lane < CELLS) | (
        (lane >= end) & (lane < end + CELLS) & jnp.logical_not(back_above)
    )
    fixed = ((lane < side) & jnp.logical_not(has_below)) | (
        (lane >= end) & jnp.logical_not(has_above)
    )
    rho = jnp.concatenate([low_ref[0], mid_ref[0], high_ref[0]], axis=1) * (1.0 / (REF * REF))

    def beside(v):
        return (
            (
                jnp.where(row == 0, x_low, pltpu.roll(v, 1, 0)),
                jnp.where(row == CELLS - 1, x_high, pltpu.roll(v, CELLS - 1, 0)),
            ),
            (
                jnp.where(cut_below, y_below, pltpu.roll(v, CELLS, 1)),
                jnp.where(cut_above, y_above, pltpu.roll(v, WIDE - CELLS, 1)),
            ),
            (
                jnp.where(third == 0, z_edge, pltpu.roll(v, 1, 1)),
                jnp.where(third == CELLS - 1, z_edge, pltpu.roll(v, WIDE - 1, 1)),
            ),
        )

    v = start
    for _ in range(SWEEPS):
        first, second, last = beside(v)
        total = first[1] + first[0] + second[1] + second[0] + last[1] + last[0]
        new = (total + (v - rho)) * (RELAXATION / 6.0)
        v = jnp.where(fixed, v, new)
    pot_ref[0] = jnp.where(live, v[:, side:end], 0.0)
    for q, (below, above) in enumerate(beside(v)):
        slope = (above[:, side:end] - below[:, side:end]) * (REF / 2.0)
        kick_ref[q, 0] = jnp.where(live, vel_ref[q, 0] - slope, 0.0)


def poisson(root_density, density, slot_anchor):
    count_first = lax.axis_size("px")
    count_second = lax.axis_size("py")
    devices = count_first * count_second
    rows, strip, wave = root_density.shape
    tiles = wave // LANES
    chunk = LANES // count_second
    width = -(-(2 * rows + 6) // 128) * 128
    basis = fourier_basis(wave)
    strip_table, strip_eig = strip_basis(strip)
    eig = 4.0 * np.sin(np.pi / wave * np.arange(wave)) ** 2
    mixes, angles = strip_coupling(count_second, chunk)
    cell = np.arange(strip)
    bow = 0.5 * (cell * cell - (strip - 1) * cell) - strip / 4
    lower = cell < strip // 2
    edge = strip_table[:, 0]
    vectors = np.stack(
        [
            np.where(lower, edge, 0.0),
            np.where(lower, 0.0, edge),
            strip_table.sum(1),
            strip_table @ bow,
        ]
    )[:, :, None]
    mix_high, mix_low = halves(jnp.asarray(mixes, F32))
    z_basis = jnp.asarray(basis, F32)
    y_basis = jnp.asarray(strip_table, F32)
    f = jnp.einsum("xyz,cz->xyc", root_density, z_basis, precision=HIGH)
    f = jnp.einsum("xyc,by->xbc", f, y_basis, precision=HIGH)
    moment = pltpu.VMEM((tiles, count_first, 2, strip, LANES), F32)
    dma = pltpu.SemaphoreType.DMA
    face = jax.ShapeDtypeStruct(density.shape[:2] + (EDGE * CELLS,), F32)
    vmem = pl.BlockSpec(memory_space=pltpu.VMEM)
    hbm = pl.BlockSpec(memory_space=pl.ANY)
    u, edges, low_density, high_density = pl.pallas_call(
        lambda *refs: grid_kernel((count_first, count_second), *refs),
        in_specs=[hbm] + [vmem] * 7 + [hbm],
        out_specs=[hbm, vmem, hbm, hbm],
        out_shape=[
            jax.ShapeDtypeStruct((rows + 2, strip, wave), F32),
            jax.ShapeDtypeStruct((2, rows + 2, wave), F32),
            face,
            face,
        ],
        scratch_shapes=[
            pltpu.VMEM((rows, strip, wave), F32),
            pltpu.VMEM((rows + 2, strip, wave), F32),
            pltpu.VMEM((width, LANES), F32),
            pltpu.VMEM((tiles, LANES, width), F32),
            pltpu.VMEM((devices, chunk, width), F32),
            pltpu.VMEM((devices, chunk, width), F32),
            pltpu.VMEM((tiles, LANES, width), F32),
            moment,
            moment,
            pltpu.VMEM((2, rows, 8, LANES), F32),
            pltpu.VMEM((2, count_first, width, 2 * wave), jnp.bfloat16),
            pltpu.VMEM((4, count_second * chunk, wave), F32),
            pltpu.VMEM((6, strip, wave), F32),
            dma((tiles,)),
            dma((tiles,)),
            dma((tiles, count_first)),
            dma((tiles, count_first)),
            dma((tiles, count_first)),
            dma((tiles, count_first)),
            dma((tiles, count_second)),
            dma((devices,)),
            dma((devices,)),
            dma((tiles, count_second)),
            dma((2,)),
            dma((2,)),
            dma((2,)),
        ],
        compiler_params=pltpu.CompilerParams(
            collective_id=1, has_side_effects=True, vmem_limit_bytes=60 * 1024 * 1024
        ),
    )(
        f,
        jnp.asarray(strip_eig[:, None], F32),
        jnp.asarray(eig[None, :], F32),
        jnp.asarray(eig[:, None], F32),
        jnp.asarray(vectors, F32),
        jnp.stack(halves(jnp.asarray(basis.T, F32))),
        jnp.concatenate([mix_high, mix_low, mix_high], axis=2),
        jnp.asarray(angles, F32),
        density,
    )
    tall = strip + 8
    step = max(n for n in range(1, 15) if (rows + 2) % n == 0)
    extended = np.zeros((tall, strip))
    extended[:strip] = strip_table.T
    extended[strip] = -strip_table[:, 0]
    extended[-1] = -strip_table[:, -1]
    high, low = halves(jnp.asarray(extended, F32))
    strip_wide = jnp.concatenate([high, low, high], axis=1)
    high, low = halves(z_basis)
    wave_tall = jnp.concatenate([high, high, low], axis=0)
    chunks = (rows + 2) // step
    coarse, patches = pl.pallas_call(
        lambda *refs: grid_values_kernel(step, *refs),
        in_specs=[pl.BlockSpec(memory_space=pltpu.SMEM)] + [vmem] * 4,
        out_specs=[hbm, vmem],
        out_shape=[
            jax.ShapeDtypeStruct((rows, strip, wave), F32),
            jax.ShapeDtypeStruct((count_second + 2, 16, 128), F32),
        ],
        scratch_shapes=[
            pltpu.VMEM((rows + 2, tall, wave), F32),
            pltpu.VMEM((16, 24, 128), F32),
            dma((chunks,)),
        ],
        compiler_params=pltpu.CompilerParams(vmem_limit_bytes=60 * 1024 * 1024),
    )(slot_anchor, u, edges, strip_wide, wave_tall)
    arrived = pl.pallas_call(
        patch_exchange_kernel,
        in_specs=[vmem],
        out_specs=vmem,
        out_shape=jax.ShapeDtypeStruct((count_second, 3, 16, 128), F32),
        scratch_shapes=[dma((count_second,)), dma((count_second,)), dma(())],
        compiler_params=pltpu.CompilerParams(collective_id=2, has_side_effects=True),
    )(patches)
    return coarse, arrived, low_density, high_density


def local(root_density, subgrid_density, velocity, slot_anchor, slot_count, neighbour):
    per_device = subgrid_density.shape[0]
    side = EDGE * CELLS
    inner = CELLS * CELLS
    coarse_potential, patches, low_density, high_density = poisson(
        root_density, subgrid_density, slot_anchor
    )
    x_table, yz_table = patch_tables()
    smem = pl.BlockSpec(memory_space=pltpu.SMEM)
    slot_spec = lambda width: pl.BlockSpec((1, CELLS, width), lambda s: (s, 0, 0))
    vel_spec = pl.BlockSpec((3, 1, CELLS, inner), lambda s: (0, s, 0, 0))
    x_table = jnp.asarray(np.tile(x_table, (1, 3)), jnp.bfloat16)
    yz_table = jnp.asarray(yz_table, jnp.bfloat16)
    potential, kicked = pl.pallas_call(
        subgrid_kernel,
        grid=(per_device,),
        in_specs=[
            smem,
            smem,
            pl.BlockSpec(patches.shape, lambda s: (0, 0, 0, 0)),
            pl.BlockSpec(x_table.shape, lambda s: (0, 0)),
            pl.BlockSpec(yz_table.shape, lambda s: (0, 0)),
            slot_spec(inner),
            slot_spec(side),
            slot_spec(side),
            vel_spec,
        ],
        out_specs=[slot_spec(inner), vel_spec],
        out_shape=[
            jax.ShapeDtypeStruct(subgrid_density.shape, F32),
            jax.ShapeDtypeStruct(velocity.shape, F32),
        ],
        scratch_shapes=[pltpu.VMEM((per_device, 16, 3 * WIDE), F32)],
        compiler_params=pltpu.CompilerParams(
            dimension_semantics=("arbitrary",), vmem_limit_bytes=60 * 1024 * 1024
        ),
    )(
        slot_count,
        neighbour,
        patches,
        x_table,
        yz_table,
        subgrid_density,
        low_density,
        high_density,
        velocity,
    )
    return (coarse_potential, potential, kicked)


def solution(mesh):
    return jax.shard_map(
        local,
        mesh=mesh,
        in_specs=(
            P("px", "py", None),
            P(("px", "py"), None, None),
            P(None, ("px", "py"), None, None),
            P(),
            P(),
            P(),
        ),
        out_specs=(
            P("px", "py", None),
            P(("px", "py"), None, None),
            P(None, ("px", "py"), None, None),
        ),
        check_vma=False,
    )
```

```python
import jax
import jax.numpy as jnp
import numpy as np
from jax import lax
from jax.experimental import pallas as pl
from jax.experimental.pallas import tpu as pltpu
from jax.sharding import PartitionSpec as P

NR = 384
REG = 8
REF = 4
SWEEPS = 4
CELLS = REG * REF
EDGE = SWEEPS
LAYERS = CELLS + 2 * EDGE
WIDE = LAYERS * CELLS
RELAXATION = 6.0 / 7.0
HIGHEST = lax.Precision.HIGHEST
HIGH = lax.Precision.HIGH
F32 = jnp.float32


def fourier_basis(length):
    cell = np.arange(length)
    rows = []
    for k in range(length):
        if k in (0, length // 2):
            rows.append(np.cos(2 * np.pi * (k * cell % length) / length) / np.sqrt(length))
        elif k < length // 2:
            rows.append(np.cos(2 * np.pi * (k * cell % length) / length) * np.sqrt(2 / length))
        else:
            rows.append(
                np.sin(2 * np.pi * ((length - k) * cell % length) / length) * np.sqrt(2 / length)
            )
    return np.stack(rows)


def strip_basis(cells):
    place = np.arange(cells) - (cells - 1) / 2
    mode = 2 * np.arange(cells // 2) + 1
    angle = np.pi * mode[:, None] * place[None, :] / cells
    basis = np.concatenate([np.cos(angle), np.sin(angle)]) * np.sqrt(2 / cells)
    eig = 4 * np.sin(np.pi * mode / (2 * cells)) ** 2
    return basis, np.concatenate([eig, eig])


def strip_coupling(count, rows):
    basis = fourier_basis(count)
    turn = np.zeros((count, count))
    theta = 2 * np.pi * np.arange(count) / count
    for k in range(1, (count + 1) // 2):
        turn[k, count - k] = np.sin(theta[k])
        turn[count - k, k] = -np.sin(theta[k])
    wide = lambda matrix: np.kron(matrix, np.eye(rows))
    mixes = np.stack([wide(basis), wide(turn @ basis), wide(basis.T)])
    half_sine = np.sin(theta / 2) ** 2
    factors = np.stack([half_sine, 4 * (1 - half_sine)])
    return mixes, np.repeat(factors, rows, axis=1)[:, :, None]


def axis_weights(cells, first, count):
    table = np.zeros((len(cells), count))
    for row, cell in enumerate(cells):
        mark = 2 * cell - 1 + REF
        low = mark // (2 * REF)
        frac = (mark - 2 * REF * low) / (2 * REF)
        table[row, low - first] += 1 - frac
        if frac:
            table[row, low + 1 - first] += frac
    return table


PATCH = REG + 2
PATCH_X = REG + 2
PATCH_Y = REG + 4
PATCH_Z = REG + 2


def patch_tables():
    inner = np.arange(1, CELLS + 1)
    x_side = axis_weights(np.concatenate([inner, [0, CELLS + 1]]), 0, PATCH_X)
    x_table = np.zeros((CELLS + 8, 16))
    x_table[: CELLS + 2, :PATCH_X] = x_side
    y_cells = np.arange(1 - EDGE, CELLS + EDGE + 1)
    y_side = axis_weights(y_cells, -1, PATCH_Y)
    y_out = axis_weights(np.array([-EDGE, CELLS + EDGE + 1]), -1, PATCH_Y)
    z_side = axis_weights(np.arange(CELLS + 2), 0, PATCH_Z)
    z_edge = np.zeros((CELLS, PATCH_Z))
    z_edge[0] = z_side[0]
    z_edge[-1] = z_side[-1]
    y_edge = np.zeros((LAYERS, PATCH_Y))
    y_edge[0] = y_out[0]
    y_edge[-1] = y_out[1]

    def both(ys, zs):
        return np.einsum("jb,kc->bcjk", ys, zs).reshape(PATCH_Y * PATCH_Z, WIDE)

    table = np.zeros((128, 3 * WIDE))
    table[: PATCH_Y * PATCH_Z] = np.concatenate(
        [both(y_side, z_side[1:-1]), both(y_side, z_edge), both(y_edge, z_side[1:-1])], axis=1
    )
    return x_table.astype(np.float32), table.astype(np.float32)


def decay(delta):
    return 1.0 / (1.0 + 0.5 * delta + jnp.sqrt(delta + 0.25 * delta * delta))


def power(value, exponent):
    result = None
    while exponent:
        if exponent & 1:
            result = value if result is None else result * value
        exponent >>= 1
        if exponent:
            value = value * value
    return result


def halves(value):
    high = value.astype(jnp.bfloat16)
    return high, (value - high.astype(F32)).astype(jnp.bfloat16)


def thirds(value):
    high = value.astype(jnp.bfloat16)
    rest = value - high.astype(F32)
    middle = rest.astype(jnp.bfloat16)
    return high, middle, (rest - middle.astype(F32)).astype(jnp.bfloat16)


def owner_shift(place_second):
    return place_second // 2 * 2 + 2


LANES = 128
BLOCK = 16


def grid_kernel(
    sizes,
    anchor_ref,
    root_hbm,
    eig_b_ref,
    eig_ref,
    own_ref,
    vec_ref,
    basis_ref,
    mix_ref,
    angle_ref,
    strip_ref,
    unstrip_ref,
    wave_ref,
    density_ref,
    out_hbm,
    arrived_ref,
    low_ref,
    high_ref,
    edge_ref,
    f_ref,
    out_ref,
    pair,
    forward,
    patches,
    cut,
    lines,
    sent,
    got,
    answer,
    back,
    mom_one,
    mom_two,
    part,
    table,
    factor,
    weight,
    in_sem,
    out_sem,
    send_one,
    recv_one,
    send_two,
    recv_two,
    send_line,
    recv_line,
    send_back,
    recv_back,
    self_sem,
    send_face,
    recv_face,
    send_patch,
    recv_patch,
):
    count_first, count_second = sizes
    devices = count_first * count_second
    rows, strip, wave = f_ref.shape
    tiles = wave // LANES
    groups = strip // 8
    half = strip // 2
    middle = rows // 2
    fold = 4
    chunk = got.shape[1]
    width = lines.shape[0]
    mesh = pl.DeviceIdType.MESH
    place_first = lax.axis_index("px")
    place_second = lax.axis_index("py")
    me = place_first * count_second + place_second
    own_tile = lax.rem(
        place_first + 2 * count_second * count_first - owner_shift(place_second), count_first
    )
    is_owner = own_tile < tiles
    barrier = pltpu.get_barrier_semaphore()

    def greet(step, carry):
        other = lax.rem(me + step, devices)
        pl.semaphore_signal(
            barrier,
            inc=1,
            device_id=(other // count_second, lax.rem(other, count_second)),
            device_id_type=mesh,
        )
        return carry

    lax.fori_loop(1, devices, greet, 0)
    lane_of = lambda t: slice(t * LANES, (t + 1) * LANES)

    def load(n):
        piece = pl.ds(n * BLOCK, BLOCK)
        return pltpu.make_async_copy(root_hbm.at[piece], f_ref.at[piece], in_sem.at[n])

    def store(n):
        return pltpu.make_async_copy(
            out_ref.at[pl.ds(n * BLOCK + 1, BLOCK)],
            out_hbm.at[pl.ds(n * BLOCK, BLOCK)],
            out_sem.at[n],
        )

    blocks = rows // BLOCK
    for n in range(blocks):
        load(n).start()
    dot = lambda a, b: jnp.dot(a, b, preferred_element_type=F32)
    forward[...] = jnp.zeros_like(forward)
    for t in range(tiles):
        forward[t, :wave, :LANES] = basis_ref[0, :, lane_of(t)]
        forward[t, wave:, :LANES] = basis_ref[0, :, lane_of(t)]
        forward[t, :wave, LANES:] = basis_ref[1, :, lane_of(t)]

    window = [slice(8 * g, 8 * g + 8) for g in range(groups)]
    even_groups = [g for g in range(groups) if 8 * g < half]
    odd_groups = [g for g in range(groups) if 8 * g + 8 > half]
    zeros = tuple(jnp.zeros((8, LANES), F32) for _ in range(groups))

    r_all = decay(eig_b_ref[...] + eig_ref[...])
    scale_all = -r_all / ((1.0 - r_all) * (1.0 + r_all))
    ratio_all = power(r_all, rows)
    weight[0] = r_all
    weight[1] = scale_all
    weight[2] = 2.0 * vec_ref[0] * scale_all
    weight[3] = -2.0 * vec_ref[1] * scale_all
    weight[4] = ratio_all
    weight[5] = 1.0 / (1.0 - power(ratio_all, count_first))

    def weights(which, t):
        return tuple(weight[which, window[g], lane_of(t)] for g in range(groups))

    def row_of(ref, i, t):
        return tuple(ref[i, window[g], lane_of(t)] for g in range(groups))

    def step_on(r, state, f):
        return tuple(r[g] * state[g] + f[g] for g in range(groups))

    def both_ways(start, stop, body, carry):
        def folded(n, carry):
            for k in range(fold):
                i = start + n * fold + k
                carry = body(i, rows - 1 - i, carry)
            return carry

        return lax.fori_loop(0, (stop - start) // fold, folded, carry)

    def store_moments(buffer, t, up, down):
        for g in range(groups):
            buffer[t, 0, 0, window[g], :] = up[g]
            buffer[t, 0, 1, window[g], :] = down[g]

    def shares(buffer, send, recv, t):
        return [
            pltpu.make_async_remote_copy(
                src_ref=buffer.at[t, 0],
                dst_ref=buffer.at[t, d],
                send_sem=send.at[t, d],
                recv_sem=recv.at[t, d],
                device_id=(lax.rem(place_first + d, count_first), place_second),
                device_id_type=mesh,
            )
            for d in range(1, count_first)
        ]

    def carries(buffer, t):
        ratio, norm = weights(4, t), weights(5, t)
        up, down = [], []
        for g in range(groups):
            total = buffer[t, 0, 0, window[g], :]
            for d in range(count_first - 1, 0, -1):
                total = ratio[g] * total + buffer[t, d, 0, window[g], :]
            up.append(total * norm[g])
            total = buffer[t, 0, 1, window[g], :]
            for d in range(1, count_first):
                total = ratio[g] * total + buffer[t, d, 1, window[g], :]
            down.append(total * norm[g])
        return tuple(up), tuple(down)

    first = []
    for t in range(tiles):
        r = weights(0, t)

        def transform(n, carry):
            piece = pl.ds(n * BLOCK, BLOCK)
            if t == 0:
                load(n).wait()
                high, low = halves(f_ref[piece].reshape(BLOCK * strip, wave))
                pair[n, :, :wave] = high
                pair[n, :, wave:] = low
            both = dot(pair[n], forward[t])
            value = both[:, :LANES] + both[:, LANES:]
            for m in range(0, BLOCK, 2):
                sides = [value[(m + q) * strip : (m + q + 1) * strip] for q in range(2)]
                high, low = halves(jnp.concatenate(sides, axis=1))
                stack = jnp.concatenate([high, high, low], axis=0)
                result = dot(strip_ref[...], stack)
                for q in range(2):
                    f_ref[n * BLOCK + m + q, :, lane_of(t)] = result[:, lane_of(q)]
            return carry

        lax.fori_loop(0, blocks, transform, 0)

        def moments(i, j, carry):
            up, down, total = carry
            f = row_of(f_ref, i, t)
            up = step_on(r, up, f)
            down = step_on(r, down, row_of(f_ref, j, t))
            if t == 0:
                total = tuple(total[g] + f[g] for g in range(groups))
            return up, down, total

        up, down, total = both_ways(0, rows, moments, (zeros, zeros, zeros if t == 0 else ()))
        store_moments(mom_one, t, up, down)
        if t == 0:
            whole = jnp.concatenate(total, axis=0)
            pl.semaphore_wait(barrier, devices - 1)
        first.append(shares(mom_one, send_one, recv_one, t))
        for copy in first[t]:
            copy.start()

    face = low_ref.shape[2]
    inner = density_ref.shape[2]
    faces = [
        pltpu.make_async_remote_copy(
            src_ref=density_ref.at[:, :, pl.ds(start, face)],
            dst_ref=target,
            send_sem=send_face.at[n],
            recv_sem=recv_face.at[n],
            device_id=(place_first, lax.rem(place_second + step, count_second)),
            device_id_type=mesh,
        )
        for n, (start, target, step) in enumerate(
            ((inner - face, low_ref, 1), (0, high_ref, count_second - 1))
        )
    ]

    def line_copy(t, k):
        return pltpu.make_async_remote_copy(
            src_ref=sent.at[t, pl.ds(k * chunk, chunk)],
            dst_ref=got.at[me],
            send_sem=send_line.at[t, k],
            recv_sem=recv_line.at[me],
            device_id=(lax.rem(owner_shift(k) + t, count_first), k),
            device_id_type=mesh,
        )

    def line_from(d):
        return pltpu.make_async_remote_copy(
            src_ref=sent.at[0, pl.ds(0, chunk)],
            dst_ref=got.at[d],
            send_sem=self_sem.at[1],
            recv_sem=recv_line.at[d],
            device_id=(d // count_second, lax.rem(d, count_second)),
            device_id_type=mesh,
        )

    def back_copy(d):
        return pltpu.make_async_remote_copy(
            src_ref=answer.at[d],
            dst_ref=back.at[own_tile, pl.ds(place_second * chunk, chunk)],
            send_sem=send_back.at[d],
            recv_sem=recv_back.at[own_tile, place_second],
            device_id=(d // count_second, lax.rem(d, count_second)),
            device_id_type=mesh,
        )

    def back_from(t, k):
        return pltpu.make_async_remote_copy(
            src_ref=answer.at[0],
            dst_ref=back.at[t, pl.ds(k * chunk, chunk)],
            send_sem=self_sem.at[1],
            recv_sem=recv_back.at[t, k],
            device_id=(lax.rem(owner_shift(k) + t, count_first), k),
            device_id_type=mesh,
        )

    def over_devices(action):
        def body(d, carry):
            @pl.when(d != me)
            def _():
                action(d)

            return carry

        lax.fori_loop(0, devices, body, 0)

    def over_owners(t, action):
        def body(k, carry):
            @pl.when((k != place_second) | (own_tile != t))
            def _():
                action(t, k)

            return carry

        lax.fori_loop(0, count_second, body, 0)

    def weighed(values, members, state):
        total = None
        for g in members:
            term = values[g] * state[g]
            total = term if total is None else total + term
        return total

    for t in range(tiles):
        r, even, odd = weights(0, t), weights(2, t), weights(3, t)
        for copy in first[t]:
            copy.wait()
        state = carries(mom_one, t)

        def lines_of(add):
            def body(i, j, carry):
                up, down = carry
                up = step_on(r, up, row_of(f_ref, i, t))
                down = tuple(r[g] * down[g] for g in range(groups))
                for n, (values, members) in enumerate(((even, even_groups), (odd, odd_groups))):
                    one = weighed(values, members, up)
                    two = weighed(values, members, down)
                    part[n, i] = part[n, i] + one if add else one
                    part[n, j] = part[n, j] + two if add else two
                f = row_of(f_ref, j, t)
                return up, tuple(down[g] + f[g] for g in range(groups))

            return body

        state = both_ways(0, middle, lines_of(False), state)
        both_ways(middle, rows, lines_of(True), state)
        lines[:rows, :] = jnp.sum(part[0], axis=1)
        lines[rows : 2 * rows, :] = jnp.sum(part[1], axis=1)
        lines[2 * rows :, :] = jnp.zeros((width - 2 * rows, LANES), F32)
        if t == 0:
            for n in range(2):
                lines[2 * rows + n : 2 * rows + n + 1, :] = jnp.sum(
                    vec_ref[2 + n] * whole, axis=0, keepdims=True
                )
        sent[t] = lines[...].T
        over_owners(t, lambda t, k: line_copy(t, k).start())
    for copy in faces:
        copy.start()

    @pl.when(is_owner)
    def _():
        own = pltpu.make_async_copy(
            sent.at[own_tile, pl.ds(place_second * chunk, chunk)], got.at[me], self_sem.at[0]
        )
        own.start()
        table[...] = jnp.zeros_like(table)
        for i in range(count_first):
            for n in range(2):
                block = basis_ref[n, i * rows : (i + 1) * rows, :]
                table[n, i, :rows, :wave] = block
                table[n, i, rows : 2 * rows, wave:] = block
                for place, row in enumerate((rows * (i + 1) % wave, (rows * i - 1) % wave)):
                    line = basis_ref[n, row : row + 1, :]
                    table[n, i, 2 * rows + 2 + place : 2 * rows + 3 + place, :wave] = line
                    table[n, i, 2 * rows + 4 + place : 2 * rows + 5 + place, wave:] = line
        start = own_tile * LANES + place_second * chunk
        own_eig = jnp.concatenate([own_ref[pl.ds(start, chunk), :]] * count_second, axis=0)
        lam = own_eig + eig_ref[...]
        sinh = jnp.sqrt(lam + 0.25 * lam * lam)
        flat = lam <= 0.0
        far = power(decay(lam), strip)
        tanh = (1.0 - far) / (1.0 + far)
        green = jnp.where(flat, strip / 4.0, tanh / jnp.where(flat, 1.0, 2.0 * sinh))
        square = tanh * tanh
        half_sine = angle_ref[0]
        det = half_sine * (1.0 - square) + square
        zero = flat & (half_sine <= 0.0)
        inverse = jnp.where(zero, 0.0, 1.0 / jnp.where(zero, 1.0, det))
        gain = angle_ref[1] * green * inverse
        factor[0] = gain * (2.0 + 0.5 * lam)
        factor[1] = jnp.where(zero, 2.0 / strip, gain * (0.5 * lam))
        factor[2] = inverse
        factor[3] = jnp.where(zero, 1.0, 0.0)
        over_devices(lambda d: line_from(d).wait_recv())
        own.wait()
        modes = None
        for i in range(count_first):
            piece = got[i * count_second : (i + 1) * count_second]
            high, low = halves(piece.reshape(count_second * chunk, width))
            term = dot(high, table[0, i]) + dot(high, table[1, i]) + dot(low, table[0, i])
            modes = term if modes is None else modes + term

        def mixed(which, value):
            high, low = halves(value)
            stack = jnp.concatenate([high, high, low], axis=0)
            return dot(mix_ref[which], stack)

        straight = mixed(0, modes)
        turned = mixed(1, modes)
        s, t = straight[:, :wave], straight[:, wave:]
        s_turned, t_turned = turned[:, :wave], turned[:, wave:]
        sums = jnp.sum(got[...], axis=0)
        lane = lax.broadcasted_iota(jnp.int32, sums.shape, 1)
        sigma = jnp.sum(jnp.where(lane == 2 * rows, sums, 0.0), axis=1, keepdims=True)
        lever = jnp.sum(jnp.where(lane == 2 * rows + 1, sums, 0.0), axis=1, keepdims=True)
        k = np.arange(strip)
        bow = 0.5 * (k * k - (strip - 1) * k) - strip / 4
        mean = jnp.where(own_eig[:chunk] <= 0.0, sigma, 0.0) * (1.0 / (wave * wave))
        gauge = lever - mean * float(wave * count_second * bow.sum())
        gauge = gauge * float(1.0 / (bow[0] * np.sqrt(wave * count_second)))
        tall = lambda value: jnp.concatenate([value] * count_second, axis=0)
        mean, gauge = tall(mean), tall(gauge)
        new_s = factor[0] * s - t_turned * factor[2] + factor[3] * gauge
        new_t = factor[1] * t - s_turned * factor[2]
        solved = mixed(2, jnp.concatenate([new_s, new_t], axis=1))
        high, low = halves(solved)
        wide = lax.broadcasted_iota(jnp.int32, (count_second * chunk, width), 1)
        across = lambda a, b: lax.dot_general(
            a, b, (((1,), (1,)), ((), ())), preferred_element_type=F32
        )
        for i in range(count_first):
            piece = across(high, table[0, i]) + across(high, table[1, i]) + across(low, table[0, i])
            piece = jnp.where(wide == 2 * rows, mean, piece)
            answer[i * count_second : (i + 1) * count_second] = piece.reshape(
                count_second, chunk, width
            )
        over_devices(lambda d: back_copy(d).start())
        kept = pltpu.make_async_copy(
            answer.at[me], back.at[own_tile, pl.ds(place_second * chunk, chunk)], self_sem.at[0]
        )
        kept.start()
        kept.wait()

    second = []
    edge_ref[...] = jnp.zeros_like(edge_ref)
    for t in range(tiles):
        over_owners(t, lambda t, k: back_from(t, k).wait_recv())
        lines[...] = back[t].T
        after = 2 * rows + 2
        for place, sign in ((0, -1.0), (7, 1.0)):
            mixed_lines = 0.5 * (lines[:rows, :] + sign * lines[rows : 2 * rows, :])
            edge_ref[1 : rows + 1, place, lane_of(t)] = mixed_lines
            ends = 0.5 * (lines[after : after + 2, :] + sign * lines[after + 2 : after + 4, :])
            edge_ref[rows + 1, place : place + 1, lane_of(t)] = ends[0:1]
            edge_ref[0, place : place + 1, lane_of(t)] = ends[1:2]
        r = weights(0, t)
        if t == 0:
            mean_term = vec_ref[2] * lines[2 * rows : 2 * rows + 1, :]
            mean_term = tuple(mean_term[window[g]] for g in range(groups))
        wide_vec = [
            jnp.broadcast_to(vec_ref[n], (strip, LANES)) for n in range(2)
        ]

        def fresh(i):
            f = list(row_of(f_ref, i, t))
            line_s = lines[pl.ds(i, 1), :]
            line_t = lines[pl.ds(rows + i, 1), :]
            for g in range(groups):
                if t == 0:
                    f[g] = f[g] - mean_term[g]
                if g in even_groups:
                    f[g] = f[g] - wide_vec[0][window[g]] * line_s
                if g in odd_groups:
                    f[g] = f[g] - wide_vec[1][window[g]] * line_t
                f_ref[i, window[g], lane_of(t)] = f[g]
            return tuple(f)

        def renewed(make):
            def body(i, j, carry):
                up, down = carry
                one = fresh(i) if make else row_of(f_ref, i, t)
                two = fresh(j) if make else row_of(f_ref, j, t)
                return step_on(r, up, one), step_on(r, down, two)

            return body

        state = both_ways(0, middle, renewed(True), (zeros, zeros))
        up, down = both_ways(middle, rows, renewed(False), state)
        store_moments(mom_two, t, up, down)
        second.append(shares(mom_two, send_two, recv_two, t))
        for copy in second[t]:
            copy.start()

    for t in range(tiles):
        r, scale = weights(0, t), weights(1, t)
        for copy in second[t]:
            copy.wait()
        carry_up, carry_down = carries(mom_two, t)

        def put(i, value, add):
            for g in range(groups):
                if add:
                    out_ref[i + 1, window[g], lane_of(t)] = (
                        out_ref[i + 1, window[g], lane_of(t)] + value[g]
                    ) * scale[g]
                else:
                    out_ref[i + 1, window[g], lane_of(t)] = value[g]

        def last(add):
            def body(i, j, carry):
                up, down = carry
                up = step_on(r, up, row_of(f_ref, i, t))
                down = tuple(r[g] * down[g] for g in range(groups))
                put(i, up, add)
                put(j, down, add)
                f = row_of(f_ref, j, t)
                return up, tuple(down[g] + f[g] for g in range(groups))

            return body

        state = both_ways(0, middle, last(False), (carry_up, carry_down))
        up, down = both_ways(middle, rows, last(True), state)
        for g in range(groups):
            out_ref[rows + 1, window[g], lane_of(t)] = (r[g] * up[g] + carry_down[g]) * scale[g]
            out_ref[0, window[g], lane_of(t)] = (carry_up[g] + r[g] * down[g]) * scale[g]

    tall = strip + 8
    tall_row = lax.broadcasted_iota(jnp.int32, (24, tall), 0)
    tall_column = lax.broadcasted_iota(jnp.int32, (24, tall), 1)
    cell = lax.broadcasted_iota(jnp.int32, (wave, LANES), 0)
    spot = lax.broadcasted_iota(jnp.int32, (wave, LANES), 1)
    lane = lax.broadcasted_iota(jnp.int32, (16, LANES), 1)
    cut[...] = jnp.zeros_like(cut)

    def patch(t, carry):
        slot = (place_first * count_second + t) * count_second + lax.rem(
            place_second - t + count_second, count_second
        )
        x = jnp.clip(anchor_ref[0, slot] - place_first * rows, 0, rows - REG)
        y = jnp.clip(anchor_ref[1, slot] - place_second * strip, 0, strip - REG) // 8
        origin = jnp.clip(anchor_ref[2, slot], 0, wave - REG) - 1 + spot
        origin = jnp.where(origin < 0, origin + wave, origin)
        origin = jnp.where(origin >= wave, origin - wave, origin)
        select = jnp.where(cell == origin, 1.0, 0.0).astype(jnp.bfloat16)
        wave_high = dot(wave_ref[0], select).astype(jnp.bfloat16)
        wave_low = dot(wave_ref[1], select).astype(jnp.bfloat16)
        table_top = jnp.concatenate([wave_high, wave_low], axis=1)
        table_low = jnp.concatenate([wave_high, jnp.zeros_like(wave_low)], axis=1)
        wanted = tall_row + 8 * y - 8
        wanted = jnp.where(wanted < 0, wanted + tall, wanted)
        pick = jnp.where(tall_column == wanted, 1.0, 0.0).astype(jnp.bfloat16)
        mix = dot(pick, unstrip_ref[...]).astype(jnp.bfloat16)
        halo_row = jnp.where(wanted[:, :1] >= strip, 1.0, 0.0)
        values = []
        for i in range(PATCH):
            high, low = halves(out_ref[x + i])
            value = dot(mix, jnp.concatenate([high, high, low], axis=0))
            halo = jnp.concatenate([edge_ref[x + i]] * 3, axis=0)
            values.append(value + halo * halo_row)
        high, low = halves(jnp.concatenate(values, axis=0))
        both = dot(high, table_top) + dot(low, table_low)
        both = both[:, :LANES] + both[:, LANES:]
        for i in range(PATCH):
            cut[i] = both[24 * i : 24 * i + 24]
        total = jnp.zeros(lane.shape, F32)
        for b in range(PATCH):
            line = jnp.where(lane < PATCH, cut[:, 7 + b, :], 0.0)
            total = total + (pltpu.roll(line, PATCH * b, 1) if b else line)
        patches[t + 1] = total
        return carry

    lax.fori_loop(0, count_second, patch, 0)
    patches[0] = patches[count_second]
    patches[count_second + 1] = patches[1]
    own = pltpu.make_async_copy(
        patches.at[pl.ds(place_second, 3)], arrived_ref.at[0], self_sem.at[0]
    )
    own.start()
    moves = []
    for d in range(1, count_second):
        target = lax.rem(place_second + d, count_second)
        moves.append(
            pltpu.make_async_remote_copy(
                src_ref=patches.at[pl.ds(target, 3)],
                dst_ref=arrived_ref.at[count_second - d],
                send_sem=send_patch.at[d],
                recv_sem=recv_patch.at[d],
                device_id=(place_first, target),
                device_id_type=mesh,
            )
        )
    for copy in moves:
        copy.start()
    unstrip = unstrip_ref[:strip, :]

    def restore(n, carry):
        for m in range(BLOCK):
            row = n * BLOCK + m + 1
            high, low = halves(out_ref[row])
            out_ref[row] = dot(unstrip, jnp.concatenate([high, high, low], axis=0))
        store(n).start()
        return carry

    lax.fori_loop(0, blocks, restore, 0)
    for t in range(tiles):
        over_owners(t, lambda t, k: line_copy(t, k).wait_send())

    @pl.when(is_owner)
    def _():
        over_devices(lambda d: back_copy(d).wait_send())

    for copy in faces + moves + [own]:
        copy.wait()
    for n in range(blocks):
        store(n).wait()


def grid_values_kernel(u_ref, wave_ref, out_ref):
    planes, strip, wave = u_ref.shape
    high, low = halves(u_ref[...].reshape(planes * strip, wave))
    pair = jnp.concatenate([high, low], axis=1)
    for t in range(wave // LANES):
        lanes = slice(t * LANES, (t + 1) * LANES)
        both = jnp.dot(pair, wave_ref[t], preferred_element_type=F32)
        value = both[:, :LANES] + both[:, LANES:]
        out_ref[:, :, lanes] = value.reshape(planes, strip, LANES)


def subgrid_kernel(
    count_ref,
    near_ref,
    patch_ref,
    xt_ref,
    yz_ref,
    mid_ref,
    low_ref,
    high_ref,
    vel_ref,
    pot_ref,
    kick_ref,
    plane_ref,
):
    device = lax.axis_index("px") * lax.axis_size("py") + lax.axis_index("py")
    place = pl.program_id(0)
    slot = device * pl.num_programs(0) + place
    below = near_ref[0, slot]
    above = near_ref[1, slot]
    live = place < count_ref[device]
    has_below = below >= 0
    has_above = above >= 0
    back_below = near_ref[1, jnp.maximum(below, 0)] >= 0
    back_above = near_ref[0, jnp.maximum(above, 0)] >= 0

    @pl.when(place == 0)
    def _():
        column = lax.broadcasted_iota(jnp.int32, (16, LANES), 1)
        count = patch_ref.shape[0]
        stack = []
        for s in range(count):
            own = pltpu.roll(patch_ref[s, 1], PATCH, 1)
            under = pltpu.roll(patch_ref[(s - 1) % count, 0], LANES - (REG - 1) * PATCH, 1)
            over = pltpu.roll(patch_ref[(s + 1) % count, 2], (PATCH - 1) * PATCH, 1)
            patch = jnp.where(
                column < PATCH, under, jnp.where(column < (PATCH + 1) * PATCH, own, over)
            )
            stack.append(jnp.where(column < (PATCH + 2) * PATCH, patch, 0.0))
        total = None
        for piece in thirds(jnp.concatenate(stack, axis=0)):
            term = jnp.dot(piece, yz_ref[...], preferred_element_type=F32)
            total = term if total is None else total + term
        plane_ref[...] = total.reshape(plane_ref.shape)

    pieces = jnp.concatenate(thirds(plane_ref[place]), axis=0)
    coarse = jnp.dot(xt_ref[...], pieces, preferred_element_type=F32)
    start = coarse[:CELLS, :WIDE]
    x_low = coarse[CELLS : CELLS + 1, :WIDE]
    x_high = coarse[CELLS + 1 : CELLS + 2, :WIDE]
    z_edge = coarse[:CELLS, WIDE : 2 * WIDE]
    y_edge = coarse[:CELLS, 2 * WIDE :]
    shape = (CELLS, WIDE)
    row = lax.broadcasted_iota(jnp.int32, shape, 0)
    lane = lax.broadcasted_iota(jnp.int32, shape, 1)
    third = lane % CELLS
    side = EDGE * CELLS
    end = WIDE - side
    y_above = jnp.where(lane >= WIDE - CELLS, y_edge, pltpu.roll(start, WIDE - CELLS, 1))
    y_below = jnp.where(lane < CELLS, y_edge, pltpu.roll(start, CELLS, 1))
    cut_above = (lane >= WIDE - CELLS) | (
        (lane >= side - CELLS) & (lane < side) & jnp.logical_not(back_below)
    )
    cut_below = (lane < CELLS) | (
        (lane >= end) & (lane < end + CELLS) & jnp.logical_not(back_above)
    )
    fixed = ((lane < side) & jnp.logical_not(has_below)) | (
        (lane >= end) & jnp.logical_not(has_above)
    )
    rho = jnp.concatenate([low_ref[0], mid_ref[0], high_ref[0]], axis=1) * (1.0 / (REF * REF))

    def beside(v):
        return (
            (
                jnp.where(row == 0, x_low, pltpu.roll(v, 1, 0)),
                jnp.where(row == CELLS - 1, x_high, pltpu.roll(v, CELLS - 1, 0)),
            ),
            (
                jnp.where(cut_below, y_below, pltpu.roll(v, CELLS, 1)),
                jnp.where(cut_above, y_above, pltpu.roll(v, WIDE - CELLS, 1)),
            ),
            (
                jnp.where(third == 0, z_edge, pltpu.roll(v, 1, 1)),
                jnp.where(third == CELLS - 1, z_edge, pltpu.roll(v, WIDE - 1, 1)),
            ),
        )

    v = start
    for _ in range(SWEEPS):
        first, second, last = beside(v)
        total = first[1] + first[0] + second[1] + second[0] + last[1] + last[0]
        new = (total + (v - rho)) * (RELAXATION / 6.0)
        v = jnp.where(fixed, v, new)
    pot_ref[0] = jnp.where(live, v[:, side:end], 0.0)
    for q, (below, above) in enumerate(beside(v)):
        slope = (above[:, side:end] - below[:, side:end]) * (REF / 2.0)
        kick_ref[q, 0] = jnp.where(live, vel_ref[q, 0] - slope, 0.0)


def poisson(root_density, density, slot_anchor):
    count_first = lax.axis_size("px")
    count_second = lax.axis_size("py")
    devices = count_first * count_second
    rows, strip, wave = root_density.shape
    tiles = wave // LANES
    chunk = LANES // count_second
    width = -(-(2 * rows + 6) // 128) * 128
    basis = fourier_basis(wave)
    strip_table, strip_eig = strip_basis(strip)
    eig = 4.0 * np.sin(np.pi / wave * np.arange(wave)) ** 2
    mixes, angles = strip_coupling(count_second, chunk)
    cell = np.arange(strip)
    bow = 0.5 * (cell * cell - (strip - 1) * cell) - strip / 4
    lower = cell < strip // 2
    edge = strip_table[:, 0]
    vectors = np.stack(
        [
            np.where(lower, edge, 0.0),
            np.where(lower, 0.0, edge),
            strip_table.sum(1),
            strip_table @ bow,
        ]
    )[:, :, None]
    mix_high, mix_low = halves(jnp.asarray(mixes, F32))
    wave_halves = jnp.stack(halves(jnp.asarray(basis, F32)))
    high, low = halves(jnp.asarray(strip_table, F32))
    strip_wide = jnp.concatenate([high, low, high], axis=1)
    extended = np.zeros((strip + 8, strip))
    extended[:strip] = strip_table.T
    extended[strip] = -strip_table[:, 0]
    extended[-1] = -strip_table[:, -1]
    high, low = halves(jnp.asarray(extended, F32))
    unstrip_wide = jnp.concatenate([high, low, high], axis=1)
    moment = pltpu.VMEM((tiles, count_first, 2, strip, LANES), F32)
    dma = pltpu.SemaphoreType.DMA
    face = jax.ShapeDtypeStruct(density.shape[:2] + (EDGE * CELLS,), F32)
    vmem = pl.BlockSpec(memory_space=pltpu.VMEM)
    hbm = pl.BlockSpec(memory_space=pl.ANY)
    uy, arrived, low_density, high_density = pl.pallas_call(
        lambda *refs: grid_kernel((count_first, count_second), *refs),
        in_specs=[pl.BlockSpec(memory_space=pltpu.SMEM), hbm] + [vmem] * 10 + [hbm],
        out_specs=[hbm, vmem, hbm, hbm],
        out_shape=[
            jax.ShapeDtypeStruct((rows, strip, wave), F32),
            jax.ShapeDtypeStruct((count_second, 3, 16, LANES), F32),
            face,
            face,
        ],
        scratch_shapes=[
            pltpu.VMEM((rows + 2, 8, wave), F32),
            pltpu.VMEM((rows, strip, wave), F32),
            pltpu.VMEM((rows + 2, strip, wave), F32),
            pltpu.VMEM((rows // BLOCK, BLOCK * strip, 2 * wave), jnp.bfloat16),
            pltpu.VMEM((tiles, 2 * wave, 2 * LANES), jnp.bfloat16),
            pltpu.VMEM((count_second + 2, 16, LANES), F32),
            pltpu.VMEM((16, 24, LANES), F32),
            pltpu.VMEM((width, LANES), F32),
            pltpu.VMEM((tiles, LANES, width), F32),
            pltpu.VMEM((devices, chunk, width), F32),
            pltpu.VMEM((devices, chunk, width), F32),
            pltpu.VMEM((tiles, LANES, width), F32),
            moment,
            moment,
            pltpu.VMEM((2, rows, 8, LANES), F32),
            pltpu.VMEM((2, count_first, width, 2 * wave), jnp.bfloat16),
            pltpu.VMEM((4, count_second * chunk, wave), F32),
            pltpu.VMEM((6, strip, wave), F32),
            dma((rows // BLOCK,)),
            dma((rows // BLOCK,)),
            dma((tiles, count_first)),
            dma((tiles, count_first)),
            dma((tiles, count_first)),
            dma((tiles, count_first)),
            dma((tiles, count_second)),
            dma((devices,)),
            dma((devices,)),
            dma((tiles, count_second)),
            dma((2,)),
            dma((2,)),
            dma((2,)),
            dma((count_second,)),
            dma((count_second,)),
        ],
        compiler_params=pltpu.CompilerParams(
            collective_id=1, has_side_effects=True, vmem_limit_bytes=60 * 1024 * 1024
        ),
    )(
        slot_anchor,
        root_density,
        jnp.asarray(strip_eig[:, None], F32),
        jnp.asarray(eig[None, :], F32),
        jnp.asarray(eig[:, None], F32),
        jnp.asarray(vectors, F32),
        jnp.stack(halves(jnp.asarray(basis.T, F32))),
        jnp.concatenate([mix_high, mix_low, mix_high], axis=2),
        jnp.asarray(angles, F32),
        strip_wide,
        unstrip_wide,
        wave_halves,
        density,
    )
    step = 8
    high = wave_halves[0].reshape(wave, tiles, LANES)
    low = wave_halves[1].reshape(wave, tiles, LANES)
    top = jnp.concatenate([high, low], axis=2)
    bottom = jnp.concatenate([high, jnp.zeros_like(low)], axis=2)
    inverse = jnp.concatenate([top, bottom], axis=0).transpose(1, 0, 2)
    block = pl.BlockSpec((step, strip, wave), lambda n: (n, 0, 0))
    coarse = pl.pallas_call(
        grid_values_kernel,
        grid=(rows // step,),
        in_specs=[block, pl.BlockSpec(inverse.shape, lambda n: (0, 0, 0))],
        out_specs=block,
        out_shape=jax.ShapeDtypeStruct((rows, strip, wave), F32),
        compiler_params=pltpu.CompilerParams(vmem_limit_bytes=60 * 1024 * 1024),
    )(uy, inverse)
    return coarse, arrived, low_density, high_density


def local(root_density, subgrid_density, velocity, slot_anchor, slot_count, neighbour):
    per_device = subgrid_density.shape[0]
    side = EDGE * CELLS
    inner = CELLS * CELLS
    coarse_potential, patches, low_density, high_density = poisson(
        root_density, subgrid_density, slot_anchor
    )
    x_table, yz_table = patch_tables()
    smem = pl.BlockSpec(memory_space=pltpu.SMEM)
    slot_spec = lambda width: pl.BlockSpec((1, CELLS, width), lambda s: (s, 0, 0))
    vel_spec = pl.BlockSpec((3, 1, CELLS, inner), lambda s: (0, s, 0, 0))
    x_table = jnp.asarray(np.tile(x_table, (1, 3)), jnp.bfloat16)
    yz_table = jnp.asarray(yz_table, jnp.bfloat16)
    potential, kicked = pl.pallas_call(
        subgrid_kernel,
        grid=(per_device,),
        in_specs=[
            smem,
            smem,
            pl.BlockSpec(patches.shape, lambda s: (0, 0, 0, 0)),
            pl.BlockSpec(x_table.shape, lambda s: (0, 0)),
            pl.BlockSpec(yz_table.shape, lambda s: (0, 0)),
            slot_spec(inner),
            slot_spec(side),
            slot_spec(side),
            vel_spec,
        ],
        out_specs=[slot_spec(inner), vel_spec],
        out_shape=[
            jax.ShapeDtypeStruct(subgrid_density.shape, F32),
            jax.ShapeDtypeStruct(velocity.shape, F32),
        ],
        scratch_shapes=[pltpu.VMEM((per_device, 16, 3 * WIDE), F32)],
        compiler_params=pltpu.CompilerParams(
            dimension_semantics=("arbitrary",), vmem_limit_bytes=60 * 1024 * 1024
        ),
    )(
        slot_count,
        neighbour,
        patches,
        x_table,
        yz_table,
        subgrid_density,
        low_density,
        high_density,
        velocity,
    )
    return (coarse_potential, potential, kicked)


def solution(mesh):
    return jax.shard_map(
        local,
        mesh=mesh,
        in_specs=(
            P("px", "py", None),
            P(("px", "py"), None, None),
            P(None, ("px", "py"), None, None),
            P(),
            P(),
            P(),
        ),
        out_specs=(
            P("px", "py", None),
            P(("px", "py"), None, None),
            P(None, ("px", "py"), None, None),
        ),
        check_vma=False,
    )
```

```python
import jax
import jax.numpy as jnp
import numpy as np
from jax import lax
from jax.experimental import pallas as pl
from jax.experimental.pallas import tpu as pltpu
from jax.sharding import PartitionSpec as P

NR = 384
REG = 8
REF = 4
SWEEPS = 4
CELLS = REG * REF
EDGE = SWEEPS
LAYERS = CELLS + 2 * EDGE
WIDE = LAYERS * CELLS
RELAXATION = 6.0 / 7.0
LANES = 128
F32 = jnp.float32


def fourier_basis(length):
    cell = np.arange(length)
    rows = []
    for k in range(length):
        if k in (0, length // 2):
            rows.append(np.cos(2 * np.pi * (k * cell % length) / length) / np.sqrt(length))
        elif k < length // 2:
            rows.append(np.cos(2 * np.pi * (k * cell % length) / length) * np.sqrt(2 / length))
        else:
            rows.append(
                np.sin(2 * np.pi * ((length - k) * cell % length) / length) * np.sqrt(2 / length)
            )
    return np.stack(rows)


def strip_basis(cells):
    place = np.arange(cells) - (cells - 1) / 2
    mode = 2 * np.arange(cells // 2) + 1
    angle = np.pi * mode[:, None] * place[None, :] / cells
    basis = np.concatenate([np.cos(angle), np.sin(angle)]) * np.sqrt(2 / cells)
    eig = 4 * np.sin(np.pi * mode / (2 * cells)) ** 2
    return basis, np.concatenate([eig, eig])


def strip_coupling(count, rows):
    basis = fourier_basis(count)
    turn = np.zeros((count, count))
    theta = 2 * np.pi * np.arange(count) / count
    for k in range(1, (count + 1) // 2):
        turn[k, count - k] = np.sin(theta[k])
        turn[count - k, k] = -np.sin(theta[k])
    wide = lambda matrix: np.kron(matrix, np.eye(rows))
    mixes = np.stack([wide(basis), wide(turn @ basis), wide(basis.T)])
    half_sine = np.sin(theta / 2) ** 2
    factors = np.stack([half_sine, 4 * (1 - half_sine)])
    return mixes, np.repeat(factors, rows, axis=1)[:, :, None]


def axis_weights(cells, first, count):
    table = np.zeros((len(cells), count))
    for row, cell in enumerate(cells):
        mark = 2 * cell - 1 + REF
        low = mark // (2 * REF)
        frac = (mark - 2 * REF * low) / (2 * REF)
        table[row, low - first] += 1 - frac
        if frac:
            table[row, low + 1 - first] += frac
    return table


PATCH = REG + 2
PATCH_X = REG + 2
PATCH_Y = REG + 4
PATCH_Z = REG + 2


def patch_tables():
    inner = np.arange(1, CELLS + 1)
    x_side = axis_weights(np.concatenate([inner, [0, CELLS + 1]]), 0, PATCH_X)
    x_table = np.zeros((CELLS + 8, 16))
    x_table[: CELLS + 2, :PATCH_X] = x_side
    y_cells = np.arange(1 - EDGE, CELLS + EDGE + 1)
    y_side = axis_weights(y_cells, -1, PATCH_Y)
    y_out = axis_weights(np.array([-EDGE, CELLS + EDGE + 1]), -1, PATCH_Y)
    z_side = axis_weights(np.arange(CELLS + 2), 0, PATCH_Z)
    z_edge = np.zeros((CELLS, PATCH_Z))
    z_edge[0] = z_side[0]
    z_edge[-1] = z_side[-1]
    y_edge = np.zeros((LAYERS, PATCH_Y))
    y_edge[0] = y_out[0]
    y_edge[-1] = y_out[1]

    def both(ys, zs):
        return np.einsum("jb,kc->bcjk", ys, zs).reshape(PATCH_Y * PATCH_Z, WIDE)

    ends = both(y_edge, z_side[1:-1])
    table = np.zeros((LANES, 2 * WIDE + 2 * LANES))
    table[: PATCH_Y * PATCH_Z] = np.concatenate(
        [
            both(y_side, z_side[1:-1]),
            both(y_side, z_edge),
            ends[:, :LANES],
            ends[:, -LANES:],
        ],
        axis=1,
    )
    return x_table.astype(np.float32), table.astype(np.float32)


def decay(delta):
    return 1.0 / (1.0 + 0.5 * delta + jnp.sqrt(delta + 0.25 * delta * delta))


def power(value, exponent):
    result = None
    while exponent:
        if exponent & 1:
            result = value if result is None else result * value
        exponent >>= 1
        if exponent:
            value = value * value
    return result


def halves(value):
    high = value.astype(jnp.bfloat16)
    return high, (value - high.astype(F32)).astype(jnp.bfloat16)


def thirds(value):
    high = value.astype(jnp.bfloat16)
    rest = value - high.astype(F32)
    middle = rest.astype(jnp.bfloat16)
    return high, middle, (rest - middle.astype(F32)).astype(jnp.bfloat16)


def owner_shift(place_second):
    return place_second // 2 * 2 + 2


BLOCK = 16


def grid_kernel(
    sizes,
    anchor_ref,
    root_hbm,
    eig_b_ref,
    eig_ref,
    own_ref,
    vec_ref,
    basis_ref,
    mix_ref,
    angle_ref,
    strip_ref,
    unstrip_ref,
    wave_ref,
    density_ref,
    out_hbm,
    arrived_ref,
    low_ref,
    high_ref,
    edge_ref,
    f_ref,
    out_ref,
    pair,
    forward,
    patches,
    cut,
    lines,
    sent,
    got,
    answer,
    back,
    mom_one,
    mom_two,
    part,
    table,
    factor,
    weight,
    in_sem,
    out_sem,
    send_one,
    recv_one,
    send_two,
    recv_two,
    send_line,
    recv_line,
    send_back,
    recv_back,
    self_sem,
    send_face,
    recv_face,
    send_patch,
    recv_patch,
):
    count_first, count_second = sizes
    devices = count_first * count_second
    rows, strip, wave = f_ref.shape
    tiles = wave // LANES
    groups = strip // 8
    half = strip // 2
    middle = rows // 2
    fold = 4
    chunk = got.shape[1]
    width = lines.shape[0]
    mesh = pl.DeviceIdType.MESH
    place_first = lax.axis_index("px")
    place_second = lax.axis_index("py")
    me = place_first * count_second + place_second
    own_tile = lax.rem(
        place_first + 2 * count_second * count_first - owner_shift(place_second), count_first
    )
    is_owner = own_tile < tiles
    barrier = pltpu.get_barrier_semaphore()

    def greet(step, carry):
        other = lax.rem(me + step, devices)
        pl.semaphore_signal(
            barrier,
            inc=1,
            device_id=(other // count_second, lax.rem(other, count_second)),
            device_id_type=mesh,
        )
        return carry

    lax.fori_loop(1, devices, greet, 0)
    lane_of = lambda t: slice(t * LANES, (t + 1) * LANES)

    def load(n):
        piece = pl.ds(n * BLOCK, BLOCK)
        return pltpu.make_async_copy(root_hbm.at[piece], f_ref.at[piece], in_sem.at[n])

    def store(n):
        return pltpu.make_async_copy(
            out_ref.at[pl.ds(n * BLOCK + 1, BLOCK)],
            out_hbm.at[pl.ds(n * BLOCK, BLOCK)],
            out_sem.at[n],
        )

    blocks = rows // BLOCK
    for n in range(blocks):
        load(n).start()
    dot = lambda a, b: jnp.dot(a, b, preferred_element_type=F32)
    forward[...] = jnp.zeros_like(forward)
    for t in range(tiles):
        forward[t, :wave, :LANES] = basis_ref[0, :, lane_of(t)]
        forward[t, wave:, :LANES] = basis_ref[0, :, lane_of(t)]
        forward[t, :wave, LANES:] = basis_ref[1, :, lane_of(t)]

    window = [slice(8 * g, 8 * g + 8) for g in range(groups)]
    even_groups = [g for g in range(groups) if 8 * g < half]
    odd_groups = [g for g in range(groups) if 8 * g + 8 > half]
    zeros = tuple(jnp.zeros((8, LANES), F32) for _ in range(groups))

    r_all = decay(eig_b_ref[...] + eig_ref[...])
    scale_all = -r_all / ((1.0 - r_all) * (1.0 + r_all))
    ratio_all = power(r_all, rows)
    weight[0] = r_all
    weight[1] = scale_all
    weight[2] = 2.0 * vec_ref[0] * scale_all
    weight[3] = -2.0 * vec_ref[1] * scale_all
    weight[4] = ratio_all
    weight[5] = 1.0 / (1.0 - power(ratio_all, count_first))

    def weights(which, t):
        return tuple(weight[which, window[g], lane_of(t)] for g in range(groups))

    def row_of(ref, i, t):
        return tuple(ref[i, window[g], lane_of(t)] for g in range(groups))

    def step_on(r, state, f):
        return tuple(r[g] * state[g] + f[g] for g in range(groups))

    def both_ways(start, stop, body, carry):
        def folded(n, carry):
            for k in range(fold):
                i = start + n * fold + k
                carry = body(i, rows - 1 - i, carry)
            return carry

        return lax.fori_loop(0, (stop - start) // fold, folded, carry)

    def store_moments(buffer, t, up, down):
        for g in range(groups):
            buffer[t, 0, 0, window[g], :] = up[g]
            buffer[t, 0, 1, window[g], :] = down[g]

    def shares(buffer, send, recv, t):
        return [
            pltpu.make_async_remote_copy(
                src_ref=buffer.at[t, 0],
                dst_ref=buffer.at[t, d],
                send_sem=send.at[t, d],
                recv_sem=recv.at[t, d],
                device_id=(lax.rem(place_first + d, count_first), place_second),
                device_id_type=mesh,
            )
            for d in range(1, count_first)
        ]

    def carries(buffer, t):
        ratio, norm = weights(4, t), weights(5, t)
        up, down = [], []
        for g in range(groups):
            total = buffer[t, 0, 0, window[g], :]
            for d in range(count_first - 1, 0, -1):
                total = ratio[g] * total + buffer[t, d, 0, window[g], :]
            up.append(total * norm[g])
            total = buffer[t, 0, 1, window[g], :]
            for d in range(1, count_first):
                total = ratio[g] * total + buffer[t, d, 1, window[g], :]
            down.append(total * norm[g])
        return tuple(up), tuple(down)

    first = []
    for t in range(tiles):
        r = weights(0, t)

        def transform(n, carry):
            piece = pl.ds(n * BLOCK, BLOCK)
            if t == 0:
                load(n).wait()
                high, low = halves(f_ref[piece].reshape(BLOCK * strip, wave))
                pair[n, :, :wave] = high
                pair[n, :, wave:] = low
            both = dot(pair[n], forward[t])
            value = both[:, :LANES] + both[:, LANES:]
            for m in range(0, BLOCK, 2):
                sides = [value[(m + q) * strip : (m + q + 1) * strip] for q in range(2)]
                high, low = halves(jnp.concatenate(sides, axis=1))
                stack = jnp.concatenate([high, high, low], axis=0)
                result = dot(strip_ref[...], stack)
                for q in range(2):
                    f_ref[n * BLOCK + m + q, :, lane_of(t)] = result[:, lane_of(q)]
            return carry

        lax.fori_loop(0, blocks, transform, 0)

        def moments(i, j, carry):
            up, down, total = carry
            f = row_of(f_ref, i, t)
            up = step_on(r, up, f)
            down = step_on(r, down, row_of(f_ref, j, t))
            if t == 0:
                total = tuple(total[g] + f[g] for g in range(groups))
            return up, down, total

        up, down, total = both_ways(0, rows, moments, (zeros, zeros, zeros if t == 0 else ()))
        store_moments(mom_one, t, up, down)
        if t == 0:
            whole = jnp.concatenate(total, axis=0)
            pl.semaphore_wait(barrier, devices - 1)
        first.append(shares(mom_one, send_one, recv_one, t))
        for copy in first[t]:
            copy.start()

    face = low_ref.shape[2]
    inner = density_ref.shape[2]
    faces = [
        pltpu.make_async_remote_copy(
            src_ref=density_ref.at[:, :, pl.ds(start, face)],
            dst_ref=target,
            send_sem=send_face.at[n],
            recv_sem=recv_face.at[n],
            device_id=(place_first, lax.rem(place_second + step, count_second)),
            device_id_type=mesh,
        )
        for n, (start, target, step) in enumerate(
            ((inner - face, low_ref, 1), (0, high_ref, count_second - 1))
        )
    ]

    def line_copy(t, k):
        return pltpu.make_async_remote_copy(
            src_ref=sent.at[t, pl.ds(k * chunk, chunk)],
            dst_ref=got.at[me],
            send_sem=send_line.at[t, k],
            recv_sem=recv_line.at[me],
            device_id=(lax.rem(owner_shift(k) + t, count_first), k),
            device_id_type=mesh,
        )

    def line_from(d):
        return pltpu.make_async_remote_copy(
            src_ref=sent.at[0, pl.ds(0, chunk)],
            dst_ref=got.at[d],
            send_sem=self_sem.at[1],
            recv_sem=recv_line.at[d],
            device_id=(d // count_second, lax.rem(d, count_second)),
            device_id_type=mesh,
        )

    def back_copy(d):
        return pltpu.make_async_remote_copy(
            src_ref=answer.at[d],
            dst_ref=back.at[own_tile, pl.ds(place_second * chunk, chunk)],
            send_sem=send_back.at[d],
            recv_sem=recv_back.at[own_tile, place_second],
            device_id=(d // count_second, lax.rem(d, count_second)),
            device_id_type=mesh,
        )

    def back_from(t, k):
        return pltpu.make_async_remote_copy(
            src_ref=answer.at[0],
            dst_ref=back.at[t, pl.ds(k * chunk, chunk)],
            send_sem=self_sem.at[1],
            recv_sem=recv_back.at[t, k],
            device_id=(lax.rem(owner_shift(k) + t, count_first), k),
            device_id_type=mesh,
        )

    def over_devices(action):
        def body(d, carry):
            @pl.when(d != me)
            def _():
                action(d)

            return carry

        lax.fori_loop(0, devices, body, 0)

    def over_owners(t, action):
        def body(k, carry):
            @pl.when((k != place_second) | (own_tile != t))
            def _():
                action(t, k)

            return carry

        lax.fori_loop(0, count_second, body, 0)

    def weighed(values, members, state):
        total = None
        for g in members:
            term = values[g] * state[g]
            total = term if total is None else total + term
        return total

    for t in range(tiles):
        r, even, odd = weights(0, t), weights(2, t), weights(3, t)
        for copy in first[t]:
            copy.wait()
        state = carries(mom_one, t)

        def lines_of(add):
            def body(i, j, carry):
                up, down = carry
                up = step_on(r, up, row_of(f_ref, i, t))
                down = tuple(r[g] * down[g] for g in range(groups))
                for n, (values, members) in enumerate(((even, even_groups), (odd, odd_groups))):
                    one = weighed(values, members, up)
                    two = weighed(values, members, down)
                    part[n, i] = part[n, i] + one if add else one
                    part[n, j] = part[n, j] + two if add else two
                f = row_of(f_ref, j, t)
                return up, tuple(down[g] + f[g] for g in range(groups))

            return body

        state = both_ways(0, middle, lines_of(False), state)
        both_ways(middle, rows, lines_of(True), state)
        lines[:rows, :] = jnp.sum(part[0], axis=1)
        lines[rows : 2 * rows, :] = jnp.sum(part[1], axis=1)
        lines[2 * rows :, :] = jnp.zeros((width - 2 * rows, LANES), F32)
        if t == 0:
            for n in range(2):
                lines[2 * rows + n : 2 * rows + n + 1, :] = jnp.sum(
                    vec_ref[2 + n] * whole, axis=0, keepdims=True
                )
        sent[t] = lines[...].T
        over_owners(t, lambda t, k: line_copy(t, k).start())
    for copy in faces:
        copy.start()

    @pl.when(is_owner)
    def _():
        own = pltpu.make_async_copy(
            sent.at[own_tile, pl.ds(place_second * chunk, chunk)], got.at[me], self_sem.at[0]
        )
        own.start()
        table[...] = jnp.zeros_like(table)
        for i in range(count_first):
            for n in range(2):
                block = basis_ref[n, i * rows : (i + 1) * rows, :]
                table[n, i, :rows, :wave] = block
                table[n, i, rows : 2 * rows, wave:] = block
                for place, row in enumerate((rows * (i + 1) % wave, (rows * i - 1) % wave)):
                    line = basis_ref[n, row : row + 1, :]
                    table[n, i, 2 * rows + 2 + place : 2 * rows + 3 + place, :wave] = line
                    table[n, i, 2 * rows + 4 + place : 2 * rows + 5 + place, wave:] = line
        start = own_tile * LANES + place_second * chunk
        own_eig = jnp.concatenate([own_ref[pl.ds(start, chunk), :]] * count_second, axis=0)
        lam = own_eig + eig_ref[...]
        sinh = jnp.sqrt(lam + 0.25 * lam * lam)
        flat = lam <= 0.0
        far = power(decay(lam), strip)
        tanh = (1.0 - far) / (1.0 + far)
        green = jnp.where(flat, strip / 4.0, tanh / jnp.where(flat, 1.0, 2.0 * sinh))
        square = tanh * tanh
        half_sine = angle_ref[0]
        det = half_sine * (1.0 - square) + square
        zero = flat & (half_sine <= 0.0)
        inverse = jnp.where(zero, 0.0, 1.0 / jnp.where(zero, 1.0, det))
        gain = angle_ref[1] * green * inverse
        factor[0] = gain * (2.0 + 0.5 * lam)
        factor[1] = jnp.where(zero, 2.0 / strip, gain * (0.5 * lam))
        factor[2] = inverse
        factor[3] = jnp.where(zero, 1.0, 0.0)
        over_devices(lambda d: line_from(d).wait_recv())
        own.wait()
        modes = None
        for i in range(count_first):
            piece = got[i * count_second : (i + 1) * count_second]
            high, low = halves(piece.reshape(count_second * chunk, width))
            term = dot(high, table[0, i]) + dot(high, table[1, i]) + dot(low, table[0, i])
            modes = term if modes is None else modes + term

        def mixed(which, value):
            high, low = halves(value)
            stack = jnp.concatenate([high, high, low], axis=0)
            return dot(mix_ref[which], stack)

        straight = mixed(0, modes)
        turned = mixed(1, modes)
        s, t = straight[:, :wave], straight[:, wave:]
        s_turned, t_turned = turned[:, :wave], turned[:, wave:]
        sums = jnp.sum(got[...], axis=0)
        lane = lax.broadcasted_iota(jnp.int32, sums.shape, 1)
        sigma = jnp.sum(jnp.where(lane == 2 * rows, sums, 0.0), axis=1, keepdims=True)
        lever = jnp.sum(jnp.where(lane == 2 * rows + 1, sums, 0.0), axis=1, keepdims=True)
        k = np.arange(strip)
        bow = 0.5 * (k * k - (strip - 1) * k) - strip / 4
        mean = jnp.where(own_eig[:chunk] <= 0.0, sigma, 0.0) * (1.0 / (wave * wave))
        gauge = lever - mean * float(wave * count_second * bow.sum())
        gauge = gauge * float(1.0 / (bow[0] * np.sqrt(wave * count_second)))
        tall = lambda value: jnp.concatenate([value] * count_second, axis=0)
        mean, gauge = tall(mean), tall(gauge)
        new_s = factor[0] * s - t_turned * factor[2] + factor[3] * gauge
        new_t = factor[1] * t - s_turned * factor[2]
        solved = mixed(2, jnp.concatenate([new_s, new_t], axis=1))
        high, low = halves(solved)
        wide = lax.broadcasted_iota(jnp.int32, (count_second * chunk, width), 1)
        across = lambda a, b: lax.dot_general(
            a, b, (((1,), (1,)), ((), ())), preferred_element_type=F32
        )
        for i in range(count_first):
            piece = across(high, table[0, i]) + across(high, table[1, i]) + across(low, table[0, i])
            piece = jnp.where(wide == 2 * rows, mean, piece)
            answer[i * count_second : (i + 1) * count_second] = piece.reshape(
                count_second, chunk, width
            )
        over_devices(lambda d: back_copy(d).start())
        kept = pltpu.make_async_copy(
            answer.at[me], back.at[own_tile, pl.ds(place_second * chunk, chunk)], self_sem.at[0]
        )
        kept.start()
        kept.wait()

    second = []
    edge_ref[...] = jnp.zeros_like(edge_ref)
    for t in range(tiles):
        over_owners(t, lambda t, k: back_from(t, k).wait_recv())
        lines[...] = back[t].T
        after = 2 * rows + 2
        for place, sign in ((0, -1.0), (7, 1.0)):
            mixed_lines = 0.5 * (lines[:rows, :] + sign * lines[rows : 2 * rows, :])
            edge_ref[1 : rows + 1, place, lane_of(t)] = mixed_lines
            ends = 0.5 * (lines[after : after + 2, :] + sign * lines[after + 2 : after + 4, :])
            edge_ref[rows + 1, place : place + 1, lane_of(t)] = ends[0:1]
            edge_ref[0, place : place + 1, lane_of(t)] = ends[1:2]
        r = weights(0, t)
        if t == 0:
            mean_term = vec_ref[2] * lines[2 * rows : 2 * rows + 1, :]
            mean_term = tuple(mean_term[window[g]] for g in range(groups))
        wide_vec = [
            jnp.broadcast_to(vec_ref[n], (strip, LANES)) for n in range(2)
        ]

        def fresh(i):
            f = list(row_of(f_ref, i, t))
            line_s = lines[pl.ds(i, 1), :]
            line_t = lines[pl.ds(rows + i, 1), :]
            for g in range(groups):
                if t == 0:
                    f[g] = f[g] - mean_term[g]
                if g in even_groups:
                    f[g] = f[g] - wide_vec[0][window[g]] * line_s
                if g in odd_groups:
                    f[g] = f[g] - wide_vec[1][window[g]] * line_t
                f_ref[i, window[g], lane_of(t)] = f[g]
            return tuple(f)

        def renewed(make):
            def body(i, j, carry):
                up, down = carry
                one = fresh(i) if make else row_of(f_ref, i, t)
                two = fresh(j) if make else row_of(f_ref, j, t)
                return step_on(r, up, one), step_on(r, down, two)

            return body

        state = both_ways(0, middle, renewed(True), (zeros, zeros))
        up, down = both_ways(middle, rows, renewed(False), state)
        store_moments(mom_two, t, up, down)
        second.append(shares(mom_two, send_two, recv_two, t))
        for copy in second[t]:
            copy.start()

    for t in range(tiles):
        r, scale = weights(0, t), weights(1, t)
        for copy in second[t]:
            copy.wait()
        carry_up, carry_down = carries(mom_two, t)

        def put(i, value, add):
            for g in range(groups):
                if add:
                    out_ref[i + 1, window[g], lane_of(t)] = (
                        out_ref[i + 1, window[g], lane_of(t)] + value[g]
                    ) * scale[g]
                else:
                    out_ref[i + 1, window[g], lane_of(t)] = value[g]

        def last(add):
            def body(i, j, carry):
                up, down = carry
                up = step_on(r, up, row_of(f_ref, i, t))
                down = tuple(r[g] * down[g] for g in range(groups))
                put(i, up, add)
                put(j, down, add)
                f = row_of(f_ref, j, t)
                return up, tuple(down[g] + f[g] for g in range(groups))

            return body

        state = both_ways(0, middle, last(False), (carry_up, carry_down))
        up, down = both_ways(middle, rows, last(True), state)
        for g in range(groups):
            out_ref[rows + 1, window[g], lane_of(t)] = (r[g] * up[g] + carry_down[g]) * scale[g]
            out_ref[0, window[g], lane_of(t)] = (carry_up[g] + r[g] * down[g]) * scale[g]

    tall = strip + 8
    tall_row = lax.broadcasted_iota(jnp.int32, (24, tall), 0)
    tall_column = lax.broadcasted_iota(jnp.int32, (24, tall), 1)
    cell = lax.broadcasted_iota(jnp.int32, (wave, LANES), 0)
    spot = lax.broadcasted_iota(jnp.int32, (wave, LANES), 1)
    lane = lax.broadcasted_iota(jnp.int32, (16, LANES), 1)
    cut[...] = jnp.zeros_like(cut)

    def patch(t, carry):
        slot = (place_first * count_second + t) * count_second + lax.rem(
            place_second - t + count_second, count_second
        )
        x = jnp.clip(anchor_ref[0, slot] - place_first * rows, 0, rows - REG)
        y = jnp.clip(anchor_ref[1, slot] - place_second * strip, 0, strip - REG) // 8
        origin = jnp.clip(anchor_ref[2, slot], 0, wave - REG) - 1 + spot
        origin = jnp.where(origin < 0, origin + wave, origin)
        origin = jnp.where(origin >= wave, origin - wave, origin)
        select = jnp.where(cell == origin, 1.0, 0.0).astype(jnp.bfloat16)
        wave_high = dot(wave_ref[0], select).astype(jnp.bfloat16)
        wave_low = dot(wave_ref[1], select).astype(jnp.bfloat16)
        table_top = jnp.concatenate([wave_high, wave_low], axis=1)
        table_low = jnp.concatenate([wave_high, jnp.zeros_like(wave_low)], axis=1)
        wanted = tall_row + 8 * y - 8
        wanted = jnp.where(wanted < 0, wanted + tall, wanted)
        pick = jnp.where(tall_column == wanted, 1.0, 0.0).astype(jnp.bfloat16)
        mix = dot(pick, unstrip_ref[...]).astype(jnp.bfloat16)
        halo_row = jnp.where(wanted[:, :1] >= strip, 1.0, 0.0)
        values = []
        for i in range(PATCH):
            high, low = halves(out_ref[x + i])
            value = dot(mix, jnp.concatenate([high, high, low], axis=0))
            halo = jnp.concatenate([edge_ref[x + i]] * 3, axis=0)
            values.append(value + halo * halo_row)
        high, low = halves(jnp.concatenate(values, axis=0))
        both = dot(high, table_top) + dot(low, table_low)
        both = both[:, :LANES] + both[:, LANES:]
        for i in range(PATCH):
            cut[i] = both[24 * i : 24 * i + 24]
        total = jnp.zeros(lane.shape, F32)
        for b in range(PATCH):
            line = jnp.where(lane < PATCH, cut[:, 7 + b, :], 0.0)
            total = total + (pltpu.roll(line, PATCH * b, 1) if b else line)
        patches[t + 1] = total
        return carry

    lax.fori_loop(0, count_second, patch, 0)
    patches[0] = patches[count_second]
    patches[count_second + 1] = patches[1]
    own = pltpu.make_async_copy(
        patches.at[pl.ds(place_second, 3)], arrived_ref.at[0], self_sem.at[0]
    )
    own.start()
    moves = []
    for d in range(1, count_second):
        target = lax.rem(place_second + d, count_second)
        moves.append(
            pltpu.make_async_remote_copy(
                src_ref=patches.at[pl.ds(target, 3)],
                dst_ref=arrived_ref.at[count_second - d],
                send_sem=send_patch.at[d],
                recv_sem=recv_patch.at[d],
                device_id=(place_first, target),
                device_id_type=mesh,
            )
        )
    for copy in moves:
        copy.start()
    unstrip = unstrip_ref[:strip, :]

    def restore(n, carry):
        for m in range(BLOCK):
            row = n * BLOCK + m + 1
            high, low = halves(out_ref[row])
            out_ref[row] = dot(unstrip, jnp.concatenate([high, high, low], axis=0))
        store(n).start()
        return carry

    lax.fori_loop(0, blocks, restore, 0)
    for t in range(tiles):
        over_owners(t, lambda t, k: line_copy(t, k).wait_send())

    @pl.when(is_owner)
    def _():
        over_devices(lambda d: back_copy(d).wait_send())

    for copy in faces + moves + [own]:
        copy.wait()
    for n in range(blocks):
        store(n).wait()


def subgrid_kernel(
    count_ref,
    near_ref,
    patch_ref,
    xt_ref,
    yz_ref,
    mid_ref,
    low_ref,
    high_ref,
    vel_ref,
    u_ref,
    wave_ref,
    pot_ref,
    kick_ref,
    grid_ref,
    plane_ref,
    coarse_ref,
    iterate,
    steady,
    pair,
):
    device = lax.axis_index("px") * lax.axis_size("py") + lax.axis_index("py")
    place = pl.program_id(0)
    slot = device * pl.num_programs(0) + place
    below = near_ref[0, slot]
    above = near_ref[1, slot]
    live = place < count_ref[device]
    has_below = below >= 0
    has_above = above >= 0
    back_below = near_ref[1, jnp.maximum(below, 0)] >= 0
    back_above = near_ref[0, jnp.maximum(above, 0)] >= 0
    tiles = WIDE // LANES
    lanes = lambda g: slice(g * LANES, (g + 1) * LANES)
    planes, strip, wave = u_ref.shape
    dot = lambda a, b: jnp.dot(a, b, preferred_element_type=F32)

    @pl.when(place == 0)
    def _():
        column = lax.broadcasted_iota(jnp.int32, (16, LANES), 1)
        count = patch_ref.shape[0]
        stack = []
        for s in range(count):
            own = pltpu.roll(patch_ref[s, 1], PATCH, 1)
            under = pltpu.roll(patch_ref[(s - 1) % count, 0], LANES - (REG - 1) * PATCH, 1)
            over = pltpu.roll(patch_ref[(s + 1) % count, 2], (PATCH - 1) * PATCH, 1)
            patch = jnp.where(
                column < PATCH, under, jnp.where(column < (PATCH + 1) * PATCH, own, over)
            )
            stack.append(jnp.where(column < (PATCH + 2) * PATCH, patch, 0.0))
        total = None
        for piece in thirds(jnp.concatenate(stack, axis=0)):
            term = dot(piece, yz_ref[...])
            total = term if total is None else total + term
        plane_ref[...] = total.reshape(plane_ref.shape)

    coarse_ref[...] = dot(xt_ref[...], jnp.concatenate(thirds(plane_ref[place]), axis=0))
    high, low = halves(u_ref[...].reshape(planes * strip, wave))
    pair[:, :wave] = high
    pair[:, wave:] = low

    def restore(t):
        both = dot(pair[...], wave_ref[t])
        value = both[:, :LANES] + both[:, LANES:]
        grid_ref[:, :, lanes(t)] = value.reshape(planes, strip, LANES)

    lane = lax.broadcasted_iota(jnp.int32, (CELLS, LANES), 1)
    first = lane % CELLS == 0
    final = lane % CELLS == CELLS - 1
    front = lane < CELLS
    rear = lane >= LANES - CELLS
    body = slice(8, 8 + CELLS)
    behind = slice(7, 7 + CELLS)
    ahead = slice(9, 9 + CELLS)

    for g in range(tiles):
        start = coarse_ref[:CELLS, lanes(g)]
        iterate[0, g, body] = start
        for n in range(2):
            iterate[n, g, 7:8] = coarse_ref[CELLS : CELLS + 1, lanes(g)]
            iterate[n, g, 8 + CELLS : 9 + CELLS] = coarse_ref[CELLS + 1 : CELLS + 2, lanes(g)]
        if g == 0:
            rho = low_ref[0]
        elif g == tiles - 1:
            rho = high_ref[0]
        else:
            rho = mid_ref[0, :, lanes(g - 1)]
        steady[g] = coarse_ref[:CELLS, lanes(tiles + g)] - rho * (1.0 / (REF * REF))

    def turn(value, amount):
        return pltpu.roll(value, amount % LANES, 1)

    edge_low = coarse_ref[:CELLS, lanes(2 * tiles)]
    edge_high = coarse_ref[:CELLS, lanes(2 * tiles + 1)]
    held_above = jnp.where(back_below, 0.0, turn(coarse_ref[:CELLS, lanes(1)], -CELLS))
    held_below = jnp.where(back_above, 0.0, turn(coarse_ref[:CELLS, lanes(tiles - 2)], CELLS))

    def second_sides(source, g):
        value = source[g]
        down = turn(value, CELLS)
        up = turn(value, -CELLS)
        if g == 0:
            lower = edge_low
        else:
            lower = turn(source[g - 1], CELLS)
            if g == tiles - 1:
                lower = jnp.where(back_above, lower, held_below)
        if g == tiles - 1:
            upper = edge_high
        else:
            upper = turn(source[g + 1], -CELLS)
            if g == 0:
                upper = jnp.where(back_below, upper, held_above)
        return jnp.where(front, lower, down), jnp.where(rear, upper, up)

    for n in range(SWEEPS):
        if n < wave // LANES:
            restore(n)
        now, later = n % 2, (n + 1) % 2
        source = {}
        for g in range(tiles):
            for k in (g, g + 1):
                if k < tiles and k not in source:
                    source[k] = iterate[now, k, body]
            value = source[g]
            total = iterate[now, g, behind] + iterate[now, g, ahead]
            lower, upper = second_sides(source, g)
            total = total + (lower + upper)
            total = total + jnp.where(first, 0.0, turn(value, 1))
            total = total + jnp.where(final, 0.0, turn(value, -1))
            new = (total + (value + steady[g])) * (RELAXATION / 6.0)
            if g == 0:
                new = jnp.where(has_below, new, value)
            if g == tiles - 1:
                new = jnp.where(has_above, new, value)
            iterate[later, g, body] = new
    for n in range(SWEEPS, wave // LANES):
        restore(n)

    now = SWEEPS % 2
    source = {g: iterate[now, g, body] for g in range(3)}
    for g in range(1, tiles - 1):
        source[g + 1] = iterate[now, g + 1, body]
        value = source[g]
        lower, upper = second_sides(source, g)
        edge = coarse_ref[:CELLS, lanes(tiles + g)]
        slopes = (
            iterate[now, g, ahead] - iterate[now, g, behind],
            upper - lower,
            jnp.where(final, edge, turn(value, -1)) - jnp.where(first, edge, turn(value, 1)),
        )
        pot_ref[0, :, lanes(g - 1)] = jnp.where(live, value, 0.0)
        for q, slope in enumerate(slopes):
            moved = vel_ref[q, 0, :, lanes(g - 1)] - slope * (REF / 2.0)
            kick_ref[q, 0, :, lanes(g - 1)] = jnp.where(live, moved, 0.0)


def poisson(root_density, density, slot_anchor):
    count_first = lax.axis_size("px")
    count_second = lax.axis_size("py")
    devices = count_first * count_second
    rows, strip, wave = root_density.shape
    tiles = wave // LANES
    chunk = LANES // count_second
    width = -(-(2 * rows + 6) // 128) * 128
    basis = fourier_basis(wave)
    strip_table, strip_eig = strip_basis(strip)
    eig = 4.0 * np.sin(np.pi / wave * np.arange(wave)) ** 2
    mixes, angles = strip_coupling(count_second, chunk)
    cell = np.arange(strip)
    bow = 0.5 * (cell * cell - (strip - 1) * cell) - strip / 4
    lower = cell < strip // 2
    edge = strip_table[:, 0]
    vectors = np.stack(
        [
            np.where(lower, edge, 0.0),
            np.where(lower, 0.0, edge),
            strip_table.sum(1),
            strip_table @ bow,
        ]
    )[:, :, None]
    mix_high, mix_low = halves(jnp.asarray(mixes, F32))
    wave_halves = jnp.stack(halves(jnp.asarray(basis, F32)))
    high, low = halves(jnp.asarray(strip_table, F32))
    strip_wide = jnp.concatenate([high, low, high], axis=1)
    extended = np.zeros((strip + 8, strip))
    extended[:strip] = strip_table.T
    extended[strip] = -strip_table[:, 0]
    extended[-1] = -strip_table[:, -1]
    high, low = halves(jnp.asarray(extended, F32))
    unstrip_wide = jnp.concatenate([high, low, high], axis=1)
    moment = pltpu.VMEM((tiles, count_first, 2, strip, LANES), F32)
    dma = pltpu.SemaphoreType.DMA
    face = jax.ShapeDtypeStruct(density.shape[:2] + (EDGE * CELLS,), F32)
    vmem = pl.BlockSpec(memory_space=pltpu.VMEM)
    hbm = pl.BlockSpec(memory_space=pl.ANY)
    uy, arrived, low_density, high_density = pl.pallas_call(
        lambda *refs: grid_kernel((count_first, count_second), *refs),
        in_specs=[pl.BlockSpec(memory_space=pltpu.SMEM), hbm] + [vmem] * 10 + [hbm],
        out_specs=[hbm, vmem, hbm, hbm],
        out_shape=[
            jax.ShapeDtypeStruct((rows, strip, wave), F32),
            jax.ShapeDtypeStruct((count_second, 3, 16, LANES), F32),
            face,
            face,
        ],
        scratch_shapes=[
            pltpu.VMEM((rows + 2, 8, wave), F32),
            pltpu.VMEM((rows, strip, wave), F32),
            pltpu.VMEM((rows + 2, strip, wave), F32),
            pltpu.VMEM((rows // BLOCK, BLOCK * strip, 2 * wave), jnp.bfloat16),
            pltpu.VMEM((tiles, 2 * wave, 2 * LANES), jnp.bfloat16),
            pltpu.VMEM((count_second + 2, 16, LANES), F32),
            pltpu.VMEM((16, 24, LANES), F32),
            pltpu.VMEM((width, LANES), F32),
            pltpu.VMEM((tiles, LANES, width), F32),
            pltpu.VMEM((devices, chunk, width), F32),
            pltpu.VMEM((devices, chunk, width), F32),
            pltpu.VMEM((tiles, LANES, width), F32),
            moment,
            moment,
            pltpu.VMEM((2, rows, 8, LANES), F32),
            pltpu.VMEM((2, count_first, width, 2 * wave), jnp.bfloat16),
            pltpu.VMEM((4, count_second * chunk, wave), F32),
            pltpu.VMEM((6, strip, wave), F32),
            dma((rows // BLOCK,)),
            dma((rows // BLOCK,)),
            dma((tiles, count_first)),
            dma((tiles, count_first)),
            dma((tiles, count_first)),
            dma((tiles, count_first)),
            dma((tiles, count_second)),
            dma((devices,)),
            dma((devices,)),
            dma((tiles, count_second)),
            dma((2,)),
            dma((2,)),
            dma((2,)),
            dma((count_second,)),
            dma((count_second,)),
        ],
        compiler_params=pltpu.CompilerParams(
            collective_id=1, has_side_effects=True, vmem_limit_bytes=60 * 1024 * 1024
        ),
    )(
        slot_anchor,
        root_density,
        jnp.asarray(strip_eig[:, None], F32),
        jnp.asarray(eig[None, :], F32),
        jnp.asarray(eig[:, None], F32),
        jnp.asarray(vectors, F32),
        jnp.stack(halves(jnp.asarray(basis.T, F32))),
        jnp.concatenate([mix_high, mix_low, mix_high], axis=2),
        jnp.asarray(angles, F32),
        strip_wide,
        unstrip_wide,
        wave_halves,
        density,
    )
    high = wave_halves[0].reshape(wave, tiles, LANES)
    low = wave_halves[1].reshape(wave, tiles, LANES)
    top = jnp.concatenate([high, low], axis=2)
    bottom = jnp.concatenate([high, jnp.zeros_like(low)], axis=2)
    inverse = jnp.concatenate([top, bottom], axis=0).transpose(1, 0, 2)
    return uy, inverse, arrived, low_density, high_density


def local(root_density, subgrid_density, velocity, slot_anchor, slot_count, neighbour):
    per_device = subgrid_density.shape[0]
    side = EDGE * CELLS
    inner = CELLS * CELLS
    uy, inverse, patches, low_density, high_density = poisson(
        root_density, subgrid_density, slot_anchor
    )
    x_table, yz_table = patch_tables()
    smem = pl.BlockSpec(memory_space=pltpu.SMEM)
    slot_spec = lambda width: pl.BlockSpec((1, CELLS, width), lambda s: (s, 0, 0))
    vel_spec = pl.BlockSpec((3, 1, CELLS, inner), lambda s: (0, s, 0, 0))
    x_table = jnp.asarray(np.tile(x_table, (1, 3)), jnp.bfloat16)
    yz_table = jnp.asarray(yz_table, jnp.bfloat16)
    columns = yz_table.shape[1]
    planes, strip, wave = uy.shape
    planes //= per_device
    grid_spec = pl.BlockSpec((planes, strip, wave), lambda s: (s, 0, 0))
    potential, kicked, coarse_potential = pl.pallas_call(
        subgrid_kernel,
        grid=(per_device,),
        in_specs=[
            smem,
            smem,
            pl.BlockSpec(patches.shape, lambda s: (0, 0, 0, 0)),
            pl.BlockSpec(x_table.shape, lambda s: (0, 0)),
            pl.BlockSpec(yz_table.shape, lambda s: (0, 0)),
            slot_spec(inner),
            slot_spec(side),
            slot_spec(side),
            vel_spec,
            grid_spec,
            pl.BlockSpec(inverse.shape, lambda s: (0, 0, 0)),
        ],
        out_specs=[slot_spec(inner), vel_spec, grid_spec],
        out_shape=[
            jax.ShapeDtypeStruct(subgrid_density.shape, F32),
            jax.ShapeDtypeStruct(velocity.shape, F32),
            jax.ShapeDtypeStruct(uy.shape, F32),
        ],
        scratch_shapes=[
            pltpu.VMEM((per_device, 16, columns), F32),
            pltpu.VMEM((CELLS + 8, columns), F32),
            pltpu.VMEM((2, WIDE // LANES, CELLS + 16, LANES), F32),
            pltpu.VMEM((WIDE // LANES, CELLS, LANES), F32),
            pltpu.VMEM((planes * strip, 2 * wave), jnp.bfloat16),
        ],
        compiler_params=pltpu.CompilerParams(
            dimension_semantics=("arbitrary",), vmem_limit_bytes=60 * 1024 * 1024
        ),
    )(
        slot_count,
        neighbour,
        patches,
        x_table,
        yz_table,
        subgrid_density,
        low_density,
        high_density,
        velocity,
        uy,
        inverse,
    )
    return (coarse_potential, potential, kicked)


def solution(mesh):
    return jax.shard_map(
        local,
        mesh=mesh,
        in_specs=(
            P("px", "py", None),
            P(("px", "py"), None, None),
            P(None, ("px", "py"), None, None),
            P(),
            P(),
            P(),
        ),
        out_specs=(
            P("px", "py", None),
            P(("px", "py"), None, None),
            P(None, ("px", "py"), None, None),
        ),
        check_vma=False,
    )
```

```python
import jax
import jax.numpy as jnp
import numpy as np
from jax import lax
from jax.experimental import pallas as pl
from jax.experimental.pallas import tpu as pltpu
from jax.sharding import PartitionSpec as P

NR = 384
REG = 8
REF = 4
SWEEPS = 4
CELLS = REG * REF
EDGE = SWEEPS
LAYERS = CELLS + 2 * EDGE
WIDE = LAYERS * CELLS
RELAXATION = 6.0 / 7.0
LANES = 128
F32 = jnp.float32


def fourier_basis(length):
    cell = np.arange(length)
    rows = []
    for k in range(length):
        if k in (0, length // 2):
            rows.append(np.cos(2 * np.pi * (k * cell % length) / length) / np.sqrt(length))
        elif k < length // 2:
            rows.append(np.cos(2 * np.pi * (k * cell % length) / length) * np.sqrt(2 / length))
        else:
            rows.append(
                np.sin(2 * np.pi * ((length - k) * cell % length) / length) * np.sqrt(2 / length)
            )
    return np.stack(rows)


def strip_basis(cells):
    place = np.arange(cells) - (cells - 1) / 2
    mode = 2 * np.arange(cells // 2) + 1
    angle = np.pi * mode[:, None] * place[None, :] / cells
    basis = np.concatenate([np.cos(angle), np.sin(angle)]) * np.sqrt(2 / cells)
    eig = 4 * np.sin(np.pi * mode / (2 * cells)) ** 2
    return basis, np.concatenate([eig, eig])


def strip_coupling(count, rows):
    basis = fourier_basis(count)
    turn = np.zeros((count, count))
    theta = 2 * np.pi * np.arange(count) / count
    for k in range(1, (count + 1) // 2):
        turn[k, count - k] = np.sin(theta[k])
        turn[count - k, k] = -np.sin(theta[k])
    wide = lambda matrix: np.kron(matrix, np.eye(rows))
    mixes = np.stack([wide(basis), wide(turn @ basis), wide(basis.T)])
    half_sine = np.sin(theta / 2) ** 2
    factors = np.stack([half_sine, 4 * (1 - half_sine)])
    return mixes, np.repeat(factors, rows, axis=1)[:, :, None]


def axis_weights(cells, first, count):
    table = np.zeros((len(cells), count))
    for row, cell in enumerate(cells):
        mark = 2 * cell - 1 + REF
        low = mark // (2 * REF)
        frac = (mark - 2 * REF * low) / (2 * REF)
        table[row, low - first] += 1 - frac
        if frac:
            table[row, low + 1 - first] += frac
    return table


PATCH = REG + 2
PATCH_X = REG + 2
PATCH_Y = REG + 4
PATCH_Z = REG + 2


def patch_tables():
    inner = np.arange(1, CELLS + 1)
    x_side = axis_weights(np.concatenate([inner, [0, CELLS + 1]]), 0, PATCH_X)
    x_table = np.zeros((CELLS + 8, 16))
    x_table[: CELLS + 2, :PATCH_X] = x_side
    y_cells = np.arange(1 - EDGE, CELLS + EDGE + 1)
    y_side = axis_weights(y_cells, -1, PATCH_Y)
    y_out = axis_weights(np.array([-EDGE, CELLS + EDGE + 1]), -1, PATCH_Y)
    z_side = axis_weights(np.arange(CELLS + 2), 0, PATCH_Z)
    z_edge = np.zeros((CELLS, PATCH_Z))
    z_edge[0] = z_side[0]
    z_edge[-1] = z_side[-1]
    y_edge = np.zeros((LAYERS, PATCH_Y))
    y_edge[0] = y_out[0]
    y_edge[-1] = y_out[1]

    def both(ys, zs):
        return np.einsum("jb,kc->bcjk", ys, zs).reshape(PATCH_Y * PATCH_Z, WIDE)

    ends = both(y_edge, z_side[1:-1])
    table = np.zeros((LANES, 2 * WIDE + 2 * LANES))
    table[: PATCH_Y * PATCH_Z] = np.concatenate(
        [
            both(y_side, z_side[1:-1]),
            both(y_side, z_edge),
            ends[:, :LANES],
            ends[:, -LANES:],
        ],
        axis=1,
    )
    return x_table.astype(np.float32), table.astype(np.float32)


def decay(delta):
    return 1.0 / (1.0 + 0.5 * delta + jnp.sqrt(delta + 0.25 * delta * delta))


def power(value, exponent):
    result = None
    while exponent:
        if exponent & 1:
            result = value if result is None else result * value
        exponent >>= 1
        if exponent:
            value = value * value
    return result


def halves(value):
    high = value.astype(jnp.bfloat16)
    return high, (value - high.astype(F32)).astype(jnp.bfloat16)


def thirds(value):
    high = value.astype(jnp.bfloat16)
    rest = value - high.astype(F32)
    middle = rest.astype(jnp.bfloat16)
    return high, middle, (rest - middle.astype(F32)).astype(jnp.bfloat16)


def owner_shift(place_second):
    return place_second // 2 * 2 + 2


BLOCKS = 6


def grid_kernel(
    sizes,
    anchor_ref,
    root_hbm,
    eig_b_ref,
    eig_ref,
    own_ref,
    vec_ref,
    basis_ref,
    mix_ref,
    angle_ref,
    strip_ref,
    unstrip_ref,
    wave_ref,
    density_ref,
    out_hbm,
    arrived_ref,
    low_ref,
    high_ref,
    edge_ref,
    f_ref,
    out_ref,
    pair,
    forward,
    patches,
    cut,
    windows,
    strip_mix,
    halo_rows,
    lines,
    sent,
    got,
    answer,
    back,
    mom_one,
    mom_two,
    part,
    table,
    factor,
    weight,
    in_sem,
    out_sem,
    send_one,
    recv_one,
    send_two,
    recv_two,
    send_line,
    recv_line,
    send_back,
    recv_back,
    self_sem,
    send_face,
    recv_face,
    send_patch,
    recv_patch,
):
    count_first, count_second = sizes
    devices = count_first * count_second
    rows, strip, wave = f_ref.shape
    tiles = wave // LANES
    groups = strip // 8
    half = strip // 2
    middle = rows // 2
    fold = 4
    chunk = got.shape[1]
    width = lines.shape[0]
    mesh = pl.DeviceIdType.MESH
    place_first = lax.axis_index("px")
    place_second = lax.axis_index("py")
    me = place_first * count_second + place_second
    own_tile = lax.rem(
        place_first + 2 * count_second * count_first - owner_shift(place_second), count_first
    )
    is_owner = own_tile < tiles
    barrier = pltpu.get_barrier_semaphore()

    lane_of = lambda t: slice(t * LANES, (t + 1) * LANES)

    block = rows // BLOCKS

    def load(n):
        piece = pl.ds(n * block, block)
        return pltpu.make_async_copy(root_hbm.at[piece], f_ref.at[piece], in_sem.at[n])

    def store(n):
        return pltpu.make_async_copy(
            out_ref.at[pl.ds(n * block + 1, block)],
            out_hbm.at[pl.ds(n * block, block)],
            out_sem.at[n],
        )

    for n in range(BLOCKS):
        load(n).start()
    def greet(step, carry):
        other = lax.rem(me + step, devices)
        pl.semaphore_signal(
            barrier,
            inc=1,
            device_id=(other // count_second, lax.rem(other, count_second)),
            device_id_type=mesh,
        )
        return carry

    lax.fori_loop(1, devices, greet, 0)
    dot = lambda a, b: jnp.dot(a, b, preferred_element_type=F32)
    forward[...] = jnp.zeros_like(forward)
    for t in range(tiles):
        forward[t, :wave, :LANES] = basis_ref[0, :, lane_of(t)]
        forward[t, wave:, :LANES] = basis_ref[0, :, lane_of(t)]
        forward[t, :wave, LANES:] = basis_ref[1, :, lane_of(t)]

    window = [slice(8 * g, 8 * g + 8) for g in range(groups)]
    even_groups = [g for g in range(groups) if 8 * g < half]
    odd_groups = [g for g in range(groups) if 8 * g + 8 > half]
    zeros = tuple(jnp.zeros((8, LANES), F32) for _ in range(groups))

    r_all = decay(eig_b_ref[...] + eig_ref[...])
    scale_all = -r_all / ((1.0 - r_all) * (1.0 + r_all))
    ratio_all = power(r_all, rows)
    weight[0] = r_all
    weight[1] = scale_all
    weight[2] = 2.0 * vec_ref[0] * scale_all
    weight[3] = -2.0 * vec_ref[1] * scale_all
    weight[4] = ratio_all
    weight[5] = 1.0 / (1.0 - power(ratio_all, count_first))

    def weights(which, t):
        return tuple(weight[which, window[g], lane_of(t)] for g in range(groups))

    def row_of(ref, i, t):
        return tuple(ref[i, window[g], lane_of(t)] for g in range(groups))

    def step_on(r, state, f):
        return tuple(r[g] * state[g] + f[g] for g in range(groups))

    def both_ways(start, stop, body, carry):
        def folded(n, carry):
            for k in range(fold):
                i = start + n * fold + k
                carry = body(i, rows - 1 - i, carry)
            return carry

        return lax.fori_loop(0, (stop - start) // fold, folded, carry)

    def store_moments(buffer, t, up, down):
        for g in range(groups):
            buffer[t, 0, 0, window[g], :] = up[g]
            buffer[t, 0, 1, window[g], :] = down[g]

    def shares(buffer, send, recv, t):
        return [
            pltpu.make_async_remote_copy(
                src_ref=buffer.at[t, 0],
                dst_ref=buffer.at[t, d],
                send_sem=send.at[t, d],
                recv_sem=recv.at[t, d],
                device_id=(lax.rem(place_first + d, count_first), place_second),
                device_id_type=mesh,
            )
            for d in range(1, count_first)
        ]

    def carries(buffer, t):
        ratio, norm = weights(4, t), weights(5, t)
        up, down = [], []
        for g in range(groups):
            total = buffer[t, 0, 0, window[g], :]
            for d in range(count_first - 1, 0, -1):
                total = ratio[g] * total + buffer[t, d, 0, window[g], :]
            up.append(total * norm[g])
            total = buffer[t, 0, 1, window[g], :]
            for d in range(1, count_first):
                total = ratio[g] * total + buffer[t, d, 1, window[g], :]
            down.append(total * norm[g])
        return tuple(up), tuple(down)

    first = []
    whole = []

    def open_tile(t):
        r = weights(0, t)
        span = (2 if t == 0 else 3) * block

        def transform(n, carry):
            piece = pl.ds(n * span, span)
            spread = pl.ds(pl.multiple_of(n * span * strip, 8), span * strip)
            if t == 0:
                for m in range(span // block):
                    load(n * (span // block) + m).wait()
                high, low = halves(f_ref[piece].reshape(span * strip, wave))
                pair[spread, :wave] = high
                pair[spread, wave:] = low
            both = dot(pair[spread], forward[t])
            value = both[:, :LANES] + both[:, LANES:]
            for m in range(0, span, 2):
                sides = [value[(m + q) * strip : (m + q + 1) * strip] for q in range(2)]
                high, low = halves(jnp.concatenate(sides, axis=1))
                stack = jnp.concatenate([high, high, low], axis=0)
                result = dot(strip_ref[...], stack)
                for q in range(2):
                    f_ref[n * span + m + q, :, lane_of(t)] = result[:, lane_of(q)]
            return carry

        lax.fori_loop(0, rows // span, transform, 0)

        def moments(i, j, carry):
            up, down, total = carry
            f = row_of(f_ref, i, t)
            up = step_on(r, up, f)
            down = step_on(r, down, row_of(f_ref, j, t))
            if t == 0:
                total = tuple(total[g] + f[g] for g in range(groups))
            return up, down, total

        up, down, total = both_ways(0, rows, moments, (zeros, zeros, zeros if t == 0 else ()))
        store_moments(mom_one, t, up, down)
        if t == 0:
            whole.append(jnp.concatenate(total, axis=0))
            pl.semaphore_wait(barrier, devices - 1)
        first.append(shares(mom_one, send_one, recv_one, t))
        for copy in first[t]:
            copy.start()

    face = low_ref.shape[2]
    inner = density_ref.shape[2]
    faces = [
        pltpu.make_async_remote_copy(
            src_ref=density_ref.at[:, :, pl.ds(start, face)],
            dst_ref=target,
            send_sem=send_face.at[n],
            recv_sem=recv_face.at[n],
            device_id=(place_first, lax.rem(place_second + step, count_second)),
            device_id_type=mesh,
        )
        for n, (start, target, step) in enumerate(
            ((inner - face, low_ref, 1), (0, high_ref, count_second - 1))
        )
    ]

    def line_copy(t, k):
        return pltpu.make_async_remote_copy(
            src_ref=sent.at[t, pl.ds(k * chunk, chunk)],
            dst_ref=got.at[me],
            send_sem=send_line.at[t, k],
            recv_sem=recv_line.at[me],
            device_id=(lax.rem(owner_shift(k) + t, count_first), k),
            device_id_type=mesh,
        )

    def line_from(d):
        return pltpu.make_async_remote_copy(
            src_ref=sent.at[0, pl.ds(0, chunk)],
            dst_ref=got.at[d],
            send_sem=self_sem.at[1],
            recv_sem=recv_line.at[d],
            device_id=(d // count_second, lax.rem(d, count_second)),
            device_id_type=mesh,
        )

    def back_copy(d):
        return pltpu.make_async_remote_copy(
            src_ref=answer.at[d],
            dst_ref=back.at[own_tile, pl.ds(place_second * chunk, chunk)],
            send_sem=send_back.at[d],
            recv_sem=recv_back.at[own_tile, place_second],
            device_id=(d // count_second, lax.rem(d, count_second)),
            device_id_type=mesh,
        )

    def back_from(t, k):
        return pltpu.make_async_remote_copy(
            src_ref=answer.at[0],
            dst_ref=back.at[t, pl.ds(k * chunk, chunk)],
            send_sem=self_sem.at[1],
            recv_sem=recv_back.at[t, k],
            device_id=(lax.rem(owner_shift(k) + t, count_first), k),
            device_id_type=mesh,
        )

    def over_devices(action, part=None):
        def body(d, carry):
            @pl.when(d != me)
            def _():
                action(d)

            return carry

        start, stop = 0, devices
        if part is not None:
            start, stop = part * count_second, (part + 1) * count_second
        lax.fori_loop(start, stop, body, 0)

    def over_owners(t, action):
        def body(k, carry):
            @pl.when((k != place_second) | (own_tile != t))
            def _():
                action(t, k)

            return carry

        lax.fori_loop(0, count_second, body, 0)

    def weighed(values, members, state):
        total = None
        for g in members:
            term = values[g] * state[g]
            total = term if total is None else total + term
        return total

    def close_tile(t):
        r, even, odd = weights(0, t), weights(2, t), weights(3, t)
        for copy in first[t]:
            copy.wait()
        state = carries(mom_one, t)

        def lines_of(add):
            def body(i, j, carry):
                up, down = carry
                up = step_on(r, up, row_of(f_ref, i, t))
                down = tuple(r[g] * down[g] for g in range(groups))
                for n, (values, members) in enumerate(((even, even_groups), (odd, odd_groups))):
                    one = weighed(values, members, up)
                    two = weighed(values, members, down)
                    part[n, i] = part[n, i] + one if add else one
                    part[n, j] = part[n, j] + two if add else two
                f = row_of(f_ref, j, t)
                return up, tuple(down[g] + f[g] for g in range(groups))

            return body

        state = both_ways(0, middle, lines_of(False), state)
        both_ways(middle, rows, lines_of(True), state)
        lines[:rows, :] = jnp.sum(part[0], axis=1)
        lines[rows : 2 * rows, :] = jnp.sum(part[1], axis=1)
        lines[2 * rows :, :] = jnp.zeros((width - 2 * rows, LANES), F32)
        if t == 0:
            for n in range(2):
                lines[2 * rows + n : 2 * rows + n + 1, :] = jnp.sum(
                    vec_ref[2 + n] * whole[0], axis=0, keepdims=True
                )
        sent[t] = lines[...].T
        over_owners(t, lambda t, k: line_copy(t, k).start())

    for t in range(tiles):
        open_tile(t)
        if t > 0 and t < tiles - 1:
            close_tile(t - 1)
    for t in range(max(tiles - 2, 0), tiles):
        close_tile(t)
    for copy in faces:
        copy.start()

    @pl.when(is_owner)
    def _():
        own = pltpu.make_async_copy(
            sent.at[own_tile, pl.ds(place_second * chunk, chunk)], got.at[me], self_sem.at[0]
        )
        own.start()
        table[...] = jnp.zeros_like(table)
        for i in range(count_first):
            for n in range(2):
                block = basis_ref[n, i * rows : (i + 1) * rows, :]
                table[n, i, :rows, :wave] = block
                table[n, i, rows : 2 * rows, wave:] = block
                for place, row in enumerate((rows * (i + 1) % wave, (rows * i - 1) % wave)):
                    line = basis_ref[n, row : row + 1, :]
                    table[n, i, 2 * rows + 2 + place : 2 * rows + 3 + place, :wave] = line
                    table[n, i, 2 * rows + 4 + place : 2 * rows + 5 + place, wave:] = line
        start = own_tile * LANES + place_second * chunk
        own_eig = jnp.concatenate([own_ref[pl.ds(start, chunk), :]] * count_second, axis=0)
        lam = own_eig + eig_ref[...]
        sinh = jnp.sqrt(lam + 0.25 * lam * lam)
        flat = lam <= 0.0
        far = power(decay(lam), strip)
        tanh = (1.0 - far) / (1.0 + far)
        green = jnp.where(flat, strip / 4.0, tanh / jnp.where(flat, 1.0, 2.0 * sinh))
        square = tanh * tanh
        half_sine = angle_ref[0]
        det = half_sine * (1.0 - square) + square
        zero = flat & (half_sine <= 0.0)
        inverse = jnp.where(zero, 0.0, 1.0 / jnp.where(zero, 1.0, det))
        gain = angle_ref[1] * green * inverse
        factor[0] = gain * (2.0 + 0.5 * lam)
        factor[1] = jnp.where(zero, 2.0 / strip, gain * (0.5 * lam))
        factor[2] = inverse
        factor[3] = jnp.where(zero, 1.0, 0.0)
        modes = None
        own.wait()
        for i in range(count_first):
            over_devices(lambda d: line_from(d).wait_recv(), i)
            piece = got[i * count_second : (i + 1) * count_second]
            high, low = halves(piece.reshape(count_second * chunk, width))
            term = dot(high, table[0, i]) + dot(high, table[1, i]) + dot(low, table[0, i])
            modes = term if modes is None else modes + term

        def mixed(which, value):
            high, low = halves(value)
            stack = jnp.concatenate([high, high, low], axis=0)
            return dot(mix_ref[which], stack)

        straight = mixed(0, modes)
        turned = mixed(1, modes)
        s, t = straight[:, :wave], straight[:, wave:]
        s_turned, t_turned = turned[:, :wave], turned[:, wave:]
        sums = jnp.sum(got[...], axis=0)
        lane = lax.broadcasted_iota(jnp.int32, sums.shape, 1)
        sigma = jnp.sum(jnp.where(lane == 2 * rows, sums, 0.0), axis=1, keepdims=True)
        lever = jnp.sum(jnp.where(lane == 2 * rows + 1, sums, 0.0), axis=1, keepdims=True)
        k = np.arange(strip)
        bow = 0.5 * (k * k - (strip - 1) * k) - strip / 4
        mean = jnp.where(own_eig[:chunk] <= 0.0, sigma, 0.0) * (1.0 / (wave * wave))
        gauge = lever - mean * float(wave * count_second * bow.sum())
        gauge = gauge * float(1.0 / (bow[0] * np.sqrt(wave * count_second)))
        tall = lambda value: jnp.concatenate([value] * count_second, axis=0)
        mean, gauge = tall(mean), tall(gauge)
        new_s = factor[0] * s - t_turned * factor[2] + factor[3] * gauge
        new_t = factor[1] * t - s_turned * factor[2]
        solved = mixed(2, jnp.concatenate([new_s, new_t], axis=1))
        high, low = halves(solved)
        wide = lax.broadcasted_iota(jnp.int32, (count_second * chunk, width), 1)
        across = lambda a, b: lax.dot_general(
            a, b, (((1,), (1,)), ((), ())), preferred_element_type=F32
        )
        for i in range(count_first):
            piece = across(high, table[0, i]) + across(high, table[1, i]) + across(low, table[0, i])
            piece = jnp.where(wide == 2 * rows, mean, piece)
            answer[i * count_second : (i + 1) * count_second] = piece.reshape(
                count_second, chunk, width
            )
            over_devices(lambda d: back_copy(d).start(), i)
        kept = pltpu.make_async_copy(
            answer.at[me], back.at[own_tile, pl.ds(place_second * chunk, chunk)], self_sem.at[0]
        )
        kept.start()
        kept.wait()

    tall = strip + 8
    tall_row = lax.broadcasted_iota(jnp.int32, (24, tall), 0)
    tall_column = lax.broadcasted_iota(jnp.int32, (24, tall), 1)
    cell = lax.broadcasted_iota(jnp.int32, (wave, LANES), 0)
    spot = lax.broadcasted_iota(jnp.int32, (wave, LANES), 1)
    lane = lax.broadcasted_iota(jnp.int32, (16, LANES), 1)
    cut[...] = jnp.zeros_like(cut)


    def corner(t):
        slot = (place_first * count_second + t) * count_second + lax.rem(
            place_second - t + count_second, count_second
        )
        x = jnp.clip(anchor_ref[0, slot] - place_first * rows, 0, rows - REG)
        return x, slot

    def prepare(t, carry):
        _, slot = corner(t)
        y = jnp.clip(anchor_ref[1, slot] - place_second * strip, 0, strip - REG) // 8
        origin = jnp.clip(anchor_ref[2, slot], 0, wave - REG) - 1 + spot
        origin = jnp.where(origin < 0, origin + wave, origin)
        origin = jnp.where(origin >= wave, origin - wave, origin)
        select = jnp.where(cell == origin, 1.0, 0.0).astype(jnp.bfloat16)
        wave_high = dot(wave_ref[0], select).astype(jnp.bfloat16)
        windows[t, :wave, :LANES] = wave_high
        windows[t, wave:, :LANES] = wave_high
        windows[t, :wave, LANES:] = dot(wave_ref[1], select).astype(jnp.bfloat16)
        windows[t, wave:, LANES:] = jnp.zeros((wave, LANES), jnp.bfloat16)
        wanted = tall_row + 8 * y - 8
        wanted = jnp.where(wanted < 0, wanted + tall, wanted)
        pick = jnp.where(tall_column == wanted, 1.0, 0.0).astype(jnp.bfloat16)
        strip_mix[t] = dot(pick, unstrip_ref[...]).astype(jnp.bfloat16)
        halo_rows[t] = jnp.broadcast_to(
            jnp.where(wanted[:, :1] >= strip, 1.0, 0.0), halo_rows.shape[1:]
        )
        return carry

    lax.fori_loop(0, count_second, prepare, 0)
    second = []
    edge_ref[...] = jnp.zeros_like(edge_ref)
    for t in range(tiles):
        over_owners(t, lambda t, k: back_from(t, k).wait_recv())
        lines[...] = back[t].T
        after = 2 * rows + 2
        for place, sign in ((0, -1.0), (7, 1.0)):
            mixed_lines = 0.5 * (lines[:rows, :] + sign * lines[rows : 2 * rows, :])
            edge_ref[1 : rows + 1, place, lane_of(t)] = mixed_lines
            ends = 0.5 * (lines[after : after + 2, :] + sign * lines[after + 2 : after + 4, :])
            edge_ref[rows + 1, place : place + 1, lane_of(t)] = ends[0:1]
            edge_ref[0, place : place + 1, lane_of(t)] = ends[1:2]
        r = weights(0, t)
        if t == 0:
            mean_term = vec_ref[2] * lines[2 * rows : 2 * rows + 1, :]
            mean_term = tuple(mean_term[window[g]] for g in range(groups))
        wide_vec = [
            jnp.broadcast_to(vec_ref[n], (strip, LANES)) for n in range(2)
        ]

        def fresh(i):
            f = list(row_of(f_ref, i, t))
            line_s = lines[pl.ds(i, 1), :]
            line_t = lines[pl.ds(rows + i, 1), :]
            for g in range(groups):
                if t == 0:
                    f[g] = f[g] - mean_term[g]
                if g in even_groups:
                    f[g] = f[g] - wide_vec[0][window[g]] * line_s
                if g in odd_groups:
                    f[g] = f[g] - wide_vec[1][window[g]] * line_t
                f_ref[i, window[g], lane_of(t)] = f[g]
            return tuple(f)

        def renewed(make):
            def body(i, j, carry):
                up, down = carry
                one = fresh(i) if make else row_of(f_ref, i, t)
                two = fresh(j) if make else row_of(f_ref, j, t)
                return step_on(r, up, one), step_on(r, down, two)

            return body

        state = both_ways(0, middle, renewed(True), (zeros, zeros))
        up, down = both_ways(middle, rows, renewed(False), state)
        store_moments(mom_two, t, up, down)
        second.append(shares(mom_two, send_two, recv_two, t))
        for copy in second[t]:
            copy.start()

    for t in range(tiles):
        r, scale = weights(0, t), weights(1, t)
        for copy in second[t]:
            copy.wait()
        carry_up, carry_down = carries(mom_two, t)

        def put(i, value, add):
            for g in range(groups):
                if add:
                    out_ref[i + 1, window[g], lane_of(t)] = (
                        out_ref[i + 1, window[g], lane_of(t)] + value[g]
                    ) * scale[g]
                else:
                    out_ref[i + 1, window[g], lane_of(t)] = value[g]

        def last(add):
            def body(i, j, carry):
                up, down = carry
                up = step_on(r, up, row_of(f_ref, i, t))
                down = tuple(r[g] * down[g] for g in range(groups))
                put(i, up, add)
                put(j, down, add)
                f = row_of(f_ref, j, t)
                return up, tuple(down[g] + f[g] for g in range(groups))

            return body

        state = both_ways(0, middle, last(False), (carry_up, carry_down))
        up, down = both_ways(middle, rows, last(True), state)
        for g in range(groups):
            out_ref[rows + 1, window[g], lane_of(t)] = (r[g] * up[g] + carry_down[g]) * scale[g]
            out_ref[0, window[g], lane_of(t)] = (carry_up[g] + r[g] * down[g]) * scale[g]

    def patch(t):
        x, _ = corner(t)
        mix, halo_row = strip_mix[t], halo_rows[t]
        values = []
        for i in range(PATCH):
            high, low = halves(out_ref[x + i])
            value = dot(mix, jnp.concatenate([high, high, low], axis=0))
            halo = jnp.concatenate([edge_ref[x + i]] * 3, axis=0)
            values.append(value + halo * halo_row[:, :1])
        high, low = halves(jnp.concatenate(values, axis=0))
        both = dot(jnp.concatenate([high, low], axis=1), windows[t])
        both = both[:, :LANES] + both[:, LANES:]
        for i in range(PATCH):
            cut[t, i] = both[24 * i : 24 * i + 24]
        total = jnp.zeros(lane.shape, F32)
        for b in range(PATCH):
            line = jnp.where(lane < PATCH, cut[t, :, 7 + b, :], 0.0)
            total = total + (pltpu.roll(line, PATCH * b, 1) if b else line)
        return total

    def patch_pair(n, carry):
        totals = [patch(2 * n + q) for q in range(2)]
        for q in range(2):
            patches[2 * n + q + 1] = totals[q]
        return carry

    lax.fori_loop(0, count_second // 2, patch_pair, 0)
    patches[0] = patches[count_second]
    patches[count_second + 1] = patches[1]
    own = pltpu.make_async_copy(
        patches.at[pl.ds(place_second, 3)], arrived_ref.at[0], self_sem.at[0]
    )
    own.start()
    moves = []
    for d in range(1, count_second):
        target = lax.rem(place_second + d, count_second)
        moves.append(
            pltpu.make_async_remote_copy(
                src_ref=patches.at[pl.ds(target, 3)],
                dst_ref=arrived_ref.at[count_second - d],
                send_sem=send_patch.at[d],
                recv_sem=recv_patch.at[d],
                device_id=(place_first, target),
                device_id_type=mesh,
            )
        )
    for copy in moves:
        copy.start()
    unstrip = unstrip_ref[:strip, :]

    def restore(n, carry):
        for m in range(block):
            row = n * block + m + 1
            high, low = halves(out_ref[row])
            out_ref[row] = dot(unstrip, jnp.concatenate([high, high, low], axis=0))
        store(n).start()
        return carry

    lax.fori_loop(0, BLOCKS, restore, 0)
    for t in range(tiles):
        over_owners(t, lambda t, k: line_copy(t, k).wait_send())

    @pl.when(is_owner)
    def _():
        over_devices(lambda d: back_copy(d).wait_send())

    for copy in faces + moves + [own]:
        copy.wait()
    for n in range(BLOCKS):
        store(n).wait()


def subgrid_kernel(
    count_ref,
    near_ref,
    patch_ref,
    xt_ref,
    yz_ref,
    mid_ref,
    low_ref,
    high_ref,
    vel_ref,
    u_ref,
    wave_ref,
    pot_ref,
    kick_ref,
    grid_ref,
    plane_ref,
    coarse_ref,
    iterate,
    steady,
    pair,
):
    device = lax.axis_index("px") * lax.axis_size("py") + lax.axis_index("py")
    place = pl.program_id(0)
    slot = device * pl.num_programs(0) + place
    below = near_ref[0, slot]
    above = near_ref[1, slot]
    live = place < count_ref[device]
    has_below = below >= 0
    has_above = above >= 0
    back_below = near_ref[1, jnp.maximum(below, 0)] >= 0
    back_above = near_ref[0, jnp.maximum(above, 0)] >= 0
    tiles = WIDE // LANES
    lanes = lambda g: slice(g * LANES, (g + 1) * LANES)
    planes, strip, wave = u_ref.shape
    dot = lambda a, b: jnp.dot(a, b, preferred_element_type=F32)

    @pl.when(place == 0)
    def _():
        column = lax.broadcasted_iota(jnp.int32, (16, LANES), 1)
        count = patch_ref.shape[0]
        stack = []
        for s in range(count):
            own = pltpu.roll(patch_ref[s, 1], PATCH, 1)
            under = pltpu.roll(patch_ref[(s - 1) % count, 0], LANES - (REG - 1) * PATCH, 1)
            over = pltpu.roll(patch_ref[(s + 1) % count, 2], (PATCH - 1) * PATCH, 1)
            patch = jnp.where(
                column < PATCH, under, jnp.where(column < (PATCH + 1) * PATCH, own, over)
            )
            stack.append(jnp.where(column < (PATCH + 2) * PATCH, patch, 0.0))
        total = None
        for piece in thirds(jnp.concatenate(stack, axis=0)):
            term = dot(piece, yz_ref[...])
            total = term if total is None else total + term
        plane_ref[...] = total.reshape(plane_ref.shape)

    coarse_ref[...] = dot(xt_ref[...], jnp.concatenate(thirds(plane_ref[place]), axis=0))
    high, low = halves(u_ref[...].reshape(planes * strip, wave))
    pair[:, :wave] = high
    pair[:, wave:] = low

    def restore(t):
        both = dot(pair[...], wave_ref[t])
        value = both[:, :LANES] + both[:, LANES:]
        grid_ref[:, :, lanes(t)] = value.reshape(planes, strip, LANES)

    lane = lax.broadcasted_iota(jnp.int32, (CELLS, LANES), 1)
    first = lane % CELLS == 0
    final = lane % CELLS == CELLS - 1
    front = lane < CELLS
    rear = lane >= LANES - CELLS
    body = slice(8, 8 + CELLS)
    behind = slice(7, 7 + CELLS)
    ahead = slice(9, 9 + CELLS)

    for g in range(tiles):
        start = coarse_ref[:CELLS, lanes(g)]
        iterate[0, g, body] = start
        for n in range(2):
            iterate[n, g, 7:8] = coarse_ref[CELLS : CELLS + 1, lanes(g)]
            iterate[n, g, 8 + CELLS : 9 + CELLS] = coarse_ref[CELLS + 1 : CELLS + 2, lanes(g)]
        if g == 0:
            rho = low_ref[0]
        elif g == tiles - 1:
            rho = high_ref[0]
        else:
            rho = mid_ref[0, :, lanes(g - 1)]
        steady[g] = coarse_ref[:CELLS, lanes(tiles + g)] - rho * (1.0 / (REF * REF))

    def turn(value, amount):
        return pltpu.roll(value, amount % LANES, 1)

    edge_low = coarse_ref[:CELLS, lanes(2 * tiles)]
    edge_high = coarse_ref[:CELLS, lanes(2 * tiles + 1)]
    held_above = jnp.where(back_below, 0.0, turn(coarse_ref[:CELLS, lanes(1)], -CELLS))
    held_below = jnp.where(back_above, 0.0, turn(coarse_ref[:CELLS, lanes(tiles - 2)], CELLS))

    def second_sides(source, g):
        value = source[g]
        down = turn(value, CELLS)
        up = turn(value, -CELLS)
        if g == 0:
            lower = edge_low
        else:
            lower = turn(source[g - 1], CELLS)
            if g == tiles - 1:
                lower = jnp.where(back_above, lower, held_below)
        if g == tiles - 1:
            upper = edge_high
        else:
            upper = turn(source[g + 1], -CELLS)
            if g == 0:
                upper = jnp.where(back_below, upper, held_above)
        return jnp.where(front, lower, down), jnp.where(rear, upper, up)

    for n in range(SWEEPS):
        if n < wave // LANES:
            restore(n)
        now, later = n % 2, (n + 1) % 2
        source = {}
        for g in range(tiles):
            for k in (g, g + 1):
                if k < tiles and k not in source:
                    source[k] = iterate[now, k, body]
            value = source[g]
            total = iterate[now, g, behind] + iterate[now, g, ahead]
            lower, upper = second_sides(source, g)
            total = total + (lower + upper)
            total = total + jnp.where(first, 0.0, turn(value, 1))
            total = total + jnp.where(final, 0.0, turn(value, -1))
            new = (total + (value + steady[g])) * (RELAXATION / 6.0)
            if g == 0:
                new = jnp.where(has_below, new, value)
            if g == tiles - 1:
                new = jnp.where(has_above, new, value)
            iterate[later, g, body] = new
    for n in range(SWEEPS, wave // LANES):
        restore(n)

    now = SWEEPS % 2
    source = {g: iterate[now, g, body] for g in range(3)}
    for g in range(1, tiles - 1):
        source[g + 1] = iterate[now, g + 1, body]
        value = source[g]
        lower, upper = second_sides(source, g)
        edge = coarse_ref[:CELLS, lanes(tiles + g)]
        slopes = (
            iterate[now, g, ahead] - iterate[now, g, behind],
            upper - lower,
            jnp.where(final, edge, turn(value, -1)) - jnp.where(first, edge, turn(value, 1)),
        )
        pot_ref[0, :, lanes(g - 1)] = jnp.where(live, value, 0.0)
        for q, slope in enumerate(slopes):
            moved = vel_ref[q, 0, :, lanes(g - 1)] - slope * (REF / 2.0)
            kick_ref[q, 0, :, lanes(g - 1)] = jnp.where(live, moved, 0.0)


def poisson(root_density, density, slot_anchor):
    count_first = lax.axis_size("px")
    count_second = lax.axis_size("py")
    devices = count_first * count_second
    rows, strip, wave = root_density.shape
    tiles = wave // LANES
    chunk = LANES // count_second
    width = -(-(2 * rows + 6) // 128) * 128
    basis = fourier_basis(wave)
    strip_table, strip_eig = strip_basis(strip)
    eig = 4.0 * np.sin(np.pi / wave * np.arange(wave)) ** 2
    mixes, angles = strip_coupling(count_second, chunk)
    cell = np.arange(strip)
    bow = 0.5 * (cell * cell - (strip - 1) * cell) - strip / 4
    lower = cell < strip // 2
    edge = strip_table[:, 0]
    vectors = np.stack(
        [
            np.where(lower, edge, 0.0),
            np.where(lower, 0.0, edge),
            strip_table.sum(1),
            strip_table @ bow,
        ]
    )[:, :, None]
    mix_high, mix_low = halves(jnp.asarray(mixes, F32))
    wave_halves = jnp.stack(halves(jnp.asarray(basis, F32)))
    high, low = halves(jnp.asarray(strip_table, F32))
    strip_wide = jnp.concatenate([high, low, high], axis=1)
    extended = np.zeros((strip + 8, strip))
    extended[:strip] = strip_table.T
    extended[strip] = -strip_table[:, 0]
    extended[-1] = -strip_table[:, -1]
    high, low = halves(jnp.asarray(extended, F32))
    unstrip_wide = jnp.concatenate([high, low, high], axis=1)
    moment = pltpu.VMEM((tiles, count_first, 2, strip, LANES), F32)
    dma = pltpu.SemaphoreType.DMA
    face = jax.ShapeDtypeStruct(density.shape[:2] + (EDGE * CELLS,), F32)
    vmem = pl.BlockSpec(memory_space=pltpu.VMEM)
    hbm = pl.BlockSpec(memory_space=pl.ANY)
    uy, arrived, low_density, high_density = pl.pallas_call(
        lambda *refs: grid_kernel((count_first, count_second), *refs),
        in_specs=[pl.BlockSpec(memory_space=pltpu.SMEM), hbm] + [vmem] * 10 + [hbm],
        out_specs=[hbm, vmem, hbm, hbm],
        out_shape=[
            jax.ShapeDtypeStruct((rows, strip, wave), F32),
            jax.ShapeDtypeStruct((count_second, 3, 16, LANES), F32),
            face,
            face,
        ],
        scratch_shapes=[
            pltpu.VMEM((rows + 2, 8, wave), F32),
            pltpu.VMEM((rows, strip, wave), F32),
            pltpu.VMEM((rows + 2, strip, wave), F32),
            pltpu.VMEM((rows * strip, 2 * wave), jnp.bfloat16),
            pltpu.VMEM((tiles, 2 * wave, 2 * LANES), jnp.bfloat16),
            pltpu.VMEM((count_second + 2, 16, LANES), F32),
            pltpu.VMEM((count_second, 16, 24, LANES), F32),
            pltpu.VMEM((count_second, 2 * wave, 2 * LANES), jnp.bfloat16),
            pltpu.VMEM((count_second, 24, 3 * strip), jnp.bfloat16),
            pltpu.VMEM((count_second, 24, LANES), F32),
            pltpu.VMEM((width, LANES), F32),
            pltpu.VMEM((tiles, LANES, width), F32),
            pltpu.VMEM((devices, chunk, width), F32),
            pltpu.VMEM((devices, chunk, width), F32),
            pltpu.VMEM((tiles, LANES, width), F32),
            moment,
            moment,
            pltpu.VMEM((2, rows, 8, LANES), F32),
            pltpu.VMEM((2, count_first, width, 2 * wave), jnp.bfloat16),
            pltpu.VMEM((4, count_second * chunk, wave), F32),
            pltpu.VMEM((6, strip, wave), F32),
            dma((BLOCKS,)),
            dma((BLOCKS,)),
            dma((tiles, count_first)),
            dma((tiles, count_first)),
            dma((tiles, count_first)),
            dma((tiles, count_first)),
            dma((tiles, count_second)),
            dma((devices,)),
            dma((devices,)),
            dma((tiles, count_second)),
            dma((2,)),
            dma((2,)),
            dma((2,)),
            dma((count_second,)),
            dma((count_second,)),
        ],
        compiler_params=pltpu.CompilerParams(
            collective_id=1, has_side_effects=True, vmem_limit_bytes=60 * 1024 * 1024
        ),
    )(
        slot_anchor,
        root_density,
        jnp.asarray(strip_eig[:, None], F32),
        jnp.asarray(eig[None, :], F32),
        jnp.asarray(eig[:, None], F32),
        jnp.asarray(vectors, F32),
        jnp.stack(halves(jnp.asarray(basis.T, F32))),
        jnp.concatenate([mix_high, mix_low, mix_high], axis=2),
        jnp.asarray(angles, F32),
        strip_wide,
        unstrip_wide,
        wave_halves,
        density,
    )
    high = wave_halves[0].reshape(wave, tiles, LANES)
    low = wave_halves[1].reshape(wave, tiles, LANES)
    top = jnp.concatenate([high, low], axis=2)
    bottom = jnp.concatenate([high, jnp.zeros_like(low)], axis=2)
    inverse = jnp.concatenate([top, bottom], axis=0).transpose(1, 0, 2)
    return uy, inverse, arrived, low_density, high_density


def local(root_density, subgrid_density, velocity, slot_anchor, slot_count, neighbour):
    per_device = subgrid_density.shape[0]
    side = EDGE * CELLS
    inner = CELLS * CELLS
    uy, inverse, patches, low_density, high_density = poisson(
        root_density, subgrid_density, slot_anchor
    )
    x_table, yz_table = patch_tables()
    smem = pl.BlockSpec(memory_space=pltpu.SMEM)
    slot_spec = lambda width: pl.BlockSpec((1, CELLS, width), lambda s: (s, 0, 0))
    vel_spec = pl.BlockSpec((3, 1, CELLS, inner), lambda s: (0, s, 0, 0))
    x_table = jnp.asarray(np.tile(x_table, (1, 3)), jnp.bfloat16)
    yz_table = jnp.asarray(yz_table, jnp.bfloat16)
    columns = yz_table.shape[1]
    planes, strip, wave = uy.shape
    planes //= per_device
    grid_spec = pl.BlockSpec((planes, strip, wave), lambda s: (s, 0, 0))
    potential, kicked, coarse_potential = pl.pallas_call(
        subgrid_kernel,
        grid=(per_device,),
        in_specs=[
            smem,
            smem,
            pl.BlockSpec(patches.shape, lambda s: (0, 0, 0, 0)),
            pl.BlockSpec(x_table.shape, lambda s: (0, 0)),
            pl.BlockSpec(yz_table.shape, lambda s: (0, 0)),
            slot_spec(inner),
            slot_spec(side),
            slot_spec(side),
            vel_spec,
            grid_spec,
            pl.BlockSpec(inverse.shape, lambda s: (0, 0, 0)),
        ],
        out_specs=[slot_spec(inner), vel_spec, grid_spec],
        out_shape=[
            jax.ShapeDtypeStruct(subgrid_density.shape, F32),
            jax.ShapeDtypeStruct(velocity.shape, F32),
            jax.ShapeDtypeStruct(uy.shape, F32),
        ],
        scratch_shapes=[
            pltpu.VMEM((per_device, 16, columns), F32),
            pltpu.VMEM((CELLS + 8, columns), F32),
            pltpu.VMEM((2, WIDE // LANES, CELLS + 16, LANES), F32),
            pltpu.VMEM((WIDE // LANES, CELLS, LANES), F32),
            pltpu.VMEM((planes * strip, 2 * wave), jnp.bfloat16),
        ],
        compiler_params=pltpu.CompilerParams(
            dimension_semantics=("arbitrary",), vmem_limit_bytes=60 * 1024 * 1024
        ),
    )(
        slot_count,
        neighbour,
        patches,
        x_table,
        yz_table,
        subgrid_density,
        low_density,
        high_density,
        velocity,
        uy,
        inverse,
    )
    return (coarse_potential, potential, kicked)


def solution(mesh):
    return jax.shard_map(
        local,
        mesh=mesh,
        in_specs=(
            P("px", "py", None),
            P(("px", "py"), None, None),
            P(None, ("px", "py"), None, None),
            P(),
            P(),
            P(),
        ),
        out_specs=(
            P("px", "py", None),
            P(("px", "py"), None, None),
            P(None, ("px", "py"), None, None),
        ),
        check_vma=False,
    )
```

```python
import jax
import jax.numpy as jnp
import numpy as np
from jax import lax
from jax.experimental import pallas as pl
from jax.experimental.pallas import tpu as pltpu
from jax.sharding import PartitionSpec as P

NR = 384
REG = 8
REF = 4
SWEEPS = 4
CELLS = REG * REF
EDGE = SWEEPS
LAYERS = CELLS + 2 * EDGE
WIDE = LAYERS * CELLS
RELAXATION = 6.0 / 7.0
LANES = 128
F32 = jnp.float32


def fourier_basis(length):
    cell = np.arange(length)
    rows = []
    for k in range(length):
        if k in (0, length // 2):
            rows.append(np.cos(2 * np.pi * (k * cell % length) / length) / np.sqrt(length))
        elif k < length // 2:
            rows.append(np.cos(2 * np.pi * (k * cell % length) / length) * np.sqrt(2 / length))
        else:
            rows.append(
                np.sin(2 * np.pi * ((length - k) * cell % length) / length) * np.sqrt(2 / length)
            )
    return np.stack(rows)


def strip_basis(cells):
    place = np.arange(cells) - (cells - 1) / 2
    mode = 2 * np.arange(cells // 2) + 1
    angle = np.pi * mode[:, None] * place[None, :] / cells
    basis = np.concatenate([np.cos(angle), np.sin(angle)]) * np.sqrt(2 / cells)
    eig = 4 * np.sin(np.pi * mode / (2 * cells)) ** 2
    return basis, np.concatenate([eig, eig])


def strip_coupling(count, rows):
    basis = fourier_basis(count)
    turn = np.zeros((count, count))
    theta = 2 * np.pi * np.arange(count) / count
    for k in range(1, (count + 1) // 2):
        turn[k, count - k] = np.sin(theta[k])
        turn[count - k, k] = -np.sin(theta[k])
    wide = lambda matrix: np.kron(matrix, np.eye(rows))
    mixes = np.stack([wide(basis), wide(turn @ basis), wide(basis.T)])
    half_sine = np.sin(theta / 2) ** 2
    factors = np.stack([half_sine, 4 * (1 - half_sine)])
    return mixes, np.repeat(factors, rows, axis=1)[:, :, None]


def axis_weights(cells, first, count):
    table = np.zeros((len(cells), count))
    for row, cell in enumerate(cells):
        mark = 2 * cell - 1 + REF
        low = mark // (2 * REF)
        frac = (mark - 2 * REF * low) / (2 * REF)
        table[row, low - first] += 1 - frac
        if frac:
            table[row, low + 1 - first] += frac
    return table


PATCH = REG + 2
PATCH_X = REG + 2
PATCH_Y = REG + 4
PATCH_Z = REG + 2


def patch_tables():
    inner = np.arange(1, CELLS + 1)
    x_side = axis_weights(np.concatenate([inner, [0, CELLS + 1]]), 0, PATCH_X)
    x_table = np.zeros((CELLS + 8, 16))
    x_table[: CELLS + 2, :PATCH_X] = x_side
    y_cells = np.arange(1 - EDGE, CELLS + EDGE + 1)
    y_side = axis_weights(y_cells, -1, PATCH_Y)
    y_out = axis_weights(np.array([-EDGE, CELLS + EDGE + 1]), -1, PATCH_Y)
    z_side = axis_weights(np.arange(CELLS + 2), 0, PATCH_Z)
    z_edge = np.zeros((CELLS, PATCH_Z))
    z_edge[0] = z_side[0]
    z_edge[-1] = z_side[-1]
    y_edge = np.zeros((LAYERS, PATCH_Y))
    y_edge[0] = y_out[0]
    y_edge[-1] = y_out[1]

    def both(ys, zs):
        return np.einsum("jb,kc->bcjk", ys, zs).reshape(PATCH_Y * PATCH_Z, WIDE)

    ends = both(y_edge, z_side[1:-1])
    table = np.zeros((LANES, 2 * WIDE + 2 * LANES))
    table[: PATCH_Y * PATCH_Z] = np.concatenate(
        [
            both(y_side, z_side[1:-1]),
            both(y_side, z_edge),
            ends[:, :LANES],
            ends[:, -LANES:],
        ],
        axis=1,
    )
    return x_table.astype(np.float32), table.astype(np.float32)


def decay(delta):
    return 1.0 / (1.0 + 0.5 * delta + jnp.sqrt(delta + 0.25 * delta * delta))


def power(value, exponent):
    result = None
    while exponent:
        if exponent & 1:
            result = value if result is None else result * value
        exponent >>= 1
        if exponent:
            value = value * value
    return result


def halves(value):
    high = value.astype(jnp.bfloat16)
    return high, (value - high.astype(F32)).astype(jnp.bfloat16)


def thirds(value):
    high = value.astype(jnp.bfloat16)
    rest = value - high.astype(F32)
    middle = rest.astype(jnp.bfloat16)
    return high, middle, (rest - middle.astype(F32)).astype(jnp.bfloat16)


def owner_shift(place_second):
    return place_second // 2 * 2 + 2


BLOCKS = 6


def grid_kernel(
    sizes,
    anchor_ref,
    root_hbm,
    eig_b_ref,
    eig_ref,
    own_ref,
    vec_ref,
    basis_ref,
    mix_ref,
    angle_ref,
    strip_ref,
    unstrip_ref,
    wave_ref,
    density_ref,
    out_hbm,
    arrived_ref,
    low_ref,
    high_ref,
    edge_ref,
    f_ref,
    out_ref,
    pair,
    forward,
    patches,
    cut,
    windows,
    strip_mix,
    halo_rows,
    lines,
    sent,
    got,
    answer,
    back,
    mom_one,
    mom_two,
    part,
    table,
    factor,
    weight,
    in_sem,
    out_sem,
    send_one,
    recv_one,
    send_two,
    recv_two,
    send_line,
    recv_line,
    send_back,
    recv_back,
    self_sem,
    send_face,
    recv_face,
    send_patch,
    recv_patch,
):
    count_first, count_second = sizes
    devices = count_first * count_second
    rows, strip, wave = f_ref.shape
    tiles = wave // LANES
    groups = strip // 8
    half = strip // 2
    middle = rows // 2
    fold = 4
    chunk = got.shape[1]
    width = lines.shape[0]
    mesh = pl.DeviceIdType.MESH
    place_first = lax.axis_index("px")
    place_second = lax.axis_index("py")
    me = place_first * count_second + place_second
    own_tile = lax.rem(
        place_first + 2 * count_second * count_first - owner_shift(place_second), count_first
    )
    is_owner = own_tile < tiles
    barrier = pltpu.get_barrier_semaphore()

    lane_of = lambda t: slice(t * LANES, (t + 1) * LANES)

    block = rows // BLOCKS

    def load(n):
        piece = pl.ds(n * block, block)
        return pltpu.make_async_copy(root_hbm.at[piece], f_ref.at[piece], in_sem.at[n])

    def store(n):
        return pltpu.make_async_copy(
            out_ref.at[pl.ds(n * block + 1, block)],
            out_hbm.at[pl.ds(n * block, block)],
            out_sem.at[n],
        )

    for n in range(BLOCKS):
        load(n).start()
    def greet(step, carry):
        other = lax.rem(me + step, devices)
        pl.semaphore_signal(
            barrier,
            inc=1,
            device_id=(other // count_second, lax.rem(other, count_second)),
            device_id_type=mesh,
        )
        return carry

    lax.fori_loop(1, devices, greet, 0)
    dot = lambda a, b: jnp.dot(a, b, preferred_element_type=F32)
    forward[...] = jnp.zeros_like(forward)
    for t in range(tiles):
        forward[t, :wave, :LANES] = basis_ref[0, :, lane_of(t)]
        forward[t, wave:, :LANES] = basis_ref[0, :, lane_of(t)]
        forward[t, :wave, LANES:] = basis_ref[1, :, lane_of(t)]

    window = [slice(8 * g, 8 * g + 8) for g in range(groups)]
    even_groups = [g for g in range(groups) if 8 * g < half]
    odd_groups = [g for g in range(groups) if 8 * g + 8 > half]
    zeros = tuple(jnp.zeros((8, LANES), F32) for _ in range(groups))

    r_all = decay(eig_b_ref[...] + eig_ref[...])
    scale_all = -r_all / ((1.0 - r_all) * (1.0 + r_all))
    ratio_all = power(r_all, rows)
    weight[0] = r_all
    weight[1] = scale_all
    weight[2] = 2.0 * vec_ref[0] * scale_all
    weight[3] = -2.0 * vec_ref[1] * scale_all
    weight[4] = ratio_all
    weight[5] = 1.0 / (1.0 - power(ratio_all, count_first))

    def weights(which, t):
        return tuple(weight[which, window[g], lane_of(t)] for g in range(groups))

    def row_of(ref, i, t):
        return tuple(ref[i, window[g], lane_of(t)] for g in range(groups))

    def step_on(r, state, f):
        return tuple(r[g] * state[g] + f[g] for g in range(groups))

    def both_ways(start, stop, body, carry):
        def folded(n, carry):
            for k in range(fold):
                i = start + n * fold + k
                carry = body(i, rows - 1 - i, carry)
            return carry

        return lax.fori_loop(0, (stop - start) // fold, folded, carry)

    def store_moments(buffer, t, up, down):
        for g in range(groups):
            buffer[t, 0, 0, window[g], :] = up[g]
            buffer[t, 0, 1, window[g], :] = down[g]

    def shares(buffer, send, recv, t):
        return [
            pltpu.make_async_remote_copy(
                src_ref=buffer.at[t, 0],
                dst_ref=buffer.at[t, d],
                send_sem=send.at[t, d],
                recv_sem=recv.at[t, d],
                device_id=(lax.rem(place_first + d, count_first), place_second),
                device_id_type=mesh,
            )
            for d in range(1, count_first)
        ]

    def carries(buffer, t):
        ratio, norm = weights(4, t), weights(5, t)
        up, down = [], []
        for g in range(groups):
            total = buffer[t, 0, 0, window[g], :]
            for d in range(count_first - 1, 0, -1):
                total = ratio[g] * total + buffer[t, d, 0, window[g], :]
            up.append(total * norm[g])
            total = buffer[t, 0, 1, window[g], :]
            for d in range(1, count_first):
                total = ratio[g] * total + buffer[t, d, 1, window[g], :]
            down.append(total * norm[g])
        return tuple(up), tuple(down)

    face = low_ref.shape[2]
    inner = density_ref.shape[2]
    faces = [
        pltpu.make_async_remote_copy(
            src_ref=density_ref.at[:, :, pl.ds(start, face)],
            dst_ref=target,
            send_sem=send_face.at[n],
            recv_sem=recv_face.at[n],
            device_id=(place_first, lax.rem(place_second + step, count_second)),
            device_id_type=mesh,
        )
        for n, (start, target, step) in enumerate(
            ((inner - face, low_ref, 1), (0, high_ref, count_second - 1))
        )
    ]

    tall = strip + 8
    tall_row = lax.broadcasted_iota(jnp.int32, (24, tall), 0)
    tall_column = lax.broadcasted_iota(jnp.int32, (24, tall), 1)
    cell = lax.broadcasted_iota(jnp.int32, (wave, LANES), 0)
    spot = lax.broadcasted_iota(jnp.int32, (wave, LANES), 1)
    lane = lax.broadcasted_iota(jnp.int32, (16, LANES), 1)
    cut[...] = jnp.zeros_like(cut)


    def corner(t):
        slot = (place_first * count_second + t) * count_second + lax.rem(
            place_second - t + count_second, count_second
        )
        x = jnp.clip(anchor_ref[0, slot] - place_first * rows, 0, rows - REG)
        return x, slot

    def prepare(t, carry):
        _, slot = corner(t)
        y = jnp.clip(anchor_ref[1, slot] - place_second * strip, 0, strip - REG) // 8
        origin = jnp.clip(anchor_ref[2, slot], 0, wave - REG) - 1 + spot
        origin = jnp.where(origin < 0, origin + wave, origin)
        origin = jnp.where(origin >= wave, origin - wave, origin)
        select = jnp.where(cell == origin, 1.0, 0.0).astype(jnp.bfloat16)
        wave_high = dot(wave_ref[0], select).astype(jnp.bfloat16)
        windows[t, :wave, :LANES] = wave_high
        windows[t, wave:, :LANES] = wave_high
        windows[t, :wave, LANES:] = dot(wave_ref[1], select).astype(jnp.bfloat16)
        windows[t, wave:, LANES:] = jnp.zeros((wave, LANES), jnp.bfloat16)
        wanted = tall_row + 8 * y - 8
        wanted = jnp.where(wanted < 0, wanted + tall, wanted)
        pick = jnp.where(tall_column == wanted, 1.0, 0.0).astype(jnp.bfloat16)
        strip_mix[t] = dot(pick, unstrip_ref[...]).astype(jnp.bfloat16)
        halo_rows[t] = jnp.broadcast_to(
            jnp.where(wanted[:, :1] >= strip, 1.0, 0.0), halo_rows.shape[1:]
        )
        return carry

    lax.fori_loop(0, count_second, prepare, 0)
    @pl.when(is_owner)
    def _():
        table[...] = jnp.zeros_like(table)
        for i in range(count_first):
            for n in range(2):
                block = basis_ref[n, i * rows : (i + 1) * rows, :]
                table[n, i, :rows, :wave] = block
                table[n, i, rows : 2 * rows, wave:] = block
                for place, row in enumerate((rows * (i + 1) % wave, (rows * i - 1) % wave)):
                    line = basis_ref[n, row : row + 1, :]
                    table[n, i, 2 * rows + 2 + place : 2 * rows + 3 + place, :wave] = line
                    table[n, i, 2 * rows + 4 + place : 2 * rows + 5 + place, wave:] = line
        start = own_tile * LANES + place_second * chunk
        own_eig = jnp.concatenate([own_ref[pl.ds(start, chunk), :]] * count_second, axis=0)
        lam = own_eig + eig_ref[...]
        sinh = jnp.sqrt(lam + 0.25 * lam * lam)
        flat = lam <= 0.0
        far = power(decay(lam), strip)
        tanh = (1.0 - far) / (1.0 + far)
        green = jnp.where(flat, strip / 4.0, tanh / jnp.where(flat, 1.0, 2.0 * sinh))
        square = tanh * tanh
        half_sine = angle_ref[0]
        det = half_sine * (1.0 - square) + square
        zero = flat & (half_sine <= 0.0)
        inverse = jnp.where(zero, 0.0, 1.0 / jnp.where(zero, 1.0, det))
        gain = angle_ref[1] * green * inverse
        factor[0] = gain * (2.0 + 0.5 * lam)
        factor[1] = jnp.where(zero, 2.0 / strip, gain * (0.5 * lam))
        factor[2] = inverse
        factor[3] = jnp.where(zero, 1.0, 0.0)

    first = []
    whole = []

    def open_tile(t):
        r = weights(0, t)
        span = (2 if t == 0 else 3) * block

        def transform(n, carry):
            piece = pl.ds(n * span, span)
            spread = pl.ds(pl.multiple_of(n * span * strip, 8), span * strip)
            if t == 0:
                for m in range(span // block):
                    load(n * (span // block) + m).wait()
                high, low = halves(f_ref[piece].reshape(span * strip, wave))
                pair[spread, :wave] = high
                pair[spread, wave:] = low
            both = dot(pair[spread], forward[t])
            value = both[:, :LANES] + both[:, LANES:]
            for m in range(0, span, 2):
                sides = [value[(m + q) * strip : (m + q + 1) * strip] for q in range(2)]
                high, low = halves(jnp.concatenate(sides, axis=1))
                stack = jnp.concatenate([high, high, low], axis=0)
                result = dot(strip_ref[...], stack)
                for q in range(2):
                    f_ref[n * span + m + q, :, lane_of(t)] = result[:, lane_of(q)]
            return carry

        lax.fori_loop(0, rows // span, transform, 0)

        def moments(i, j, carry):
            up, down, total = carry
            f = row_of(f_ref, i, t)
            up = step_on(r, up, f)
            down = step_on(r, down, row_of(f_ref, j, t))
            if t == 0:
                total = tuple(total[g] + f[g] for g in range(groups))
            return up, down, total

        up, down, total = both_ways(0, rows, moments, (zeros, zeros, zeros if t == 0 else ()))
        store_moments(mom_one, t, up, down)
        if t == 0:
            whole.append(jnp.concatenate(total, axis=0))
            pl.semaphore_wait(barrier, devices - 1)
        first.append(shares(mom_one, send_one, recv_one, t))
        for copy in first[t] + (faces if t == 0 else []):
            copy.start()

    def line_copy(t, k):
        return pltpu.make_async_remote_copy(
            src_ref=sent.at[t, pl.ds(k * chunk, chunk)],
            dst_ref=got.at[me],
            send_sem=send_line.at[t, k],
            recv_sem=recv_line.at[me],
            device_id=(lax.rem(owner_shift(k) + t, count_first), k),
            device_id_type=mesh,
        )

    def line_from(d):
        return pltpu.make_async_remote_copy(
            src_ref=sent.at[0, pl.ds(0, chunk)],
            dst_ref=got.at[d],
            send_sem=self_sem.at[1],
            recv_sem=recv_line.at[d],
            device_id=(d // count_second, lax.rem(d, count_second)),
            device_id_type=mesh,
        )

    def back_copy(d):
        return pltpu.make_async_remote_copy(
            src_ref=answer.at[d],
            dst_ref=back.at[own_tile, pl.ds(place_second * chunk, chunk)],
            send_sem=send_back.at[d],
            recv_sem=recv_back.at[own_tile, place_second],
            device_id=(d // count_second, lax.rem(d, count_second)),
            device_id_type=mesh,
        )

    def back_from(t, k):
        return pltpu.make_async_remote_copy(
            src_ref=answer.at[0],
            dst_ref=back.at[t, pl.ds(k * chunk, chunk)],
            send_sem=self_sem.at[1],
            recv_sem=recv_back.at[t, k],
            device_id=(lax.rem(owner_shift(k) + t, count_first), k),
            device_id_type=mesh,
        )

    def over_devices(action, part=None):
        def body(d, carry):
            @pl.when(d != me)
            def _():
                action(d)

            return carry

        start, stop = 0, devices
        if part is not None:
            start, stop = part * count_second, (part + 1) * count_second
        lax.fori_loop(start, stop, body, 0)

    def over_owners(t, action):
        def body(k, carry):
            @pl.when((k != place_second) | (own_tile != t))
            def _():
                action(t, k)

            return carry

        lax.fori_loop(0, count_second, body, 0)

    def weighed(values, members, state):
        total = None
        for g in members:
            term = values[g] * state[g]
            total = term if total is None else total + term
        return total

    def close_tile(t):
        r, even, odd = weights(0, t), weights(2, t), weights(3, t)
        for copy in first[t]:
            copy.wait()
        state = carries(mom_one, t)

        def lines_of(add):
            def body(i, j, carry):
                up, down = carry
                up = step_on(r, up, row_of(f_ref, i, t))
                down = tuple(r[g] * down[g] for g in range(groups))
                for n, (values, members) in enumerate(((even, even_groups), (odd, odd_groups))):
                    one = weighed(values, members, up)
                    two = weighed(values, members, down)
                    part[n, i] = part[n, i] + one if add else one
                    part[n, j] = part[n, j] + two if add else two
                f = row_of(f_ref, j, t)
                return up, tuple(down[g] + f[g] for g in range(groups))

            return body

        state = both_ways(0, middle, lines_of(False), state)
        both_ways(middle, rows, lines_of(True), state)
        lines[:rows, :] = jnp.sum(part[0], axis=1)
        lines[rows : 2 * rows, :] = jnp.sum(part[1], axis=1)
        lines[2 * rows :, :] = jnp.zeros((width - 2 * rows, LANES), F32)
        if t == 0:
            for n in range(2):
                lines[2 * rows + n : 2 * rows + n + 1, :] = jnp.sum(
                    vec_ref[2 + n] * whole[0], axis=0, keepdims=True
                )
        sent[t] = lines[...].T
        over_owners(t, lambda t, k: line_copy(t, k).start())

    for t in range(tiles):
        open_tile(t)
        if t > 0 and t < tiles - 1:
            close_tile(t - 1)
    for t in range(max(tiles - 2, 0), tiles):
        close_tile(t)
    @pl.when(is_owner)
    def _():
        own = pltpu.make_async_copy(
            sent.at[own_tile, pl.ds(place_second * chunk, chunk)], got.at[me], self_sem.at[0]
        )
        own.start()
        modes = None
        own.wait()
        for i in range(count_first):
            over_devices(lambda d: line_from(d).wait_recv(), i)
            piece = got[i * count_second : (i + 1) * count_second]
            high, low = halves(piece.reshape(count_second * chunk, width))
            term = dot(high, table[0, i]) + dot(high, table[1, i]) + dot(low, table[0, i])
            modes = term if modes is None else modes + term

        def mixed(which, value):
            high, low = halves(value)
            stack = jnp.concatenate([high, high, low], axis=0)
            return dot(mix_ref[which], stack)

        straight = mixed(0, modes)
        turned = mixed(1, modes)
        s, t = straight[:, :wave], straight[:, wave:]
        s_turned, t_turned = turned[:, :wave], turned[:, wave:]
        sums = jnp.sum(got[...], axis=0)
        lane = lax.broadcasted_iota(jnp.int32, sums.shape, 1)
        sigma = jnp.sum(jnp.where(lane == 2 * rows, sums, 0.0), axis=1, keepdims=True)
        lever = jnp.sum(jnp.where(lane == 2 * rows + 1, sums, 0.0), axis=1, keepdims=True)
        k = np.arange(strip)
        bow = 0.5 * (k * k - (strip - 1) * k) - strip / 4
        first_eig = own_ref[pl.ds(own_tile * LANES + place_second * chunk, chunk), :]
        mean = jnp.where(first_eig <= 0.0, sigma, 0.0) * (1.0 / (wave * wave))
        gauge = lever - mean * float(wave * count_second * bow.sum())
        gauge = gauge * float(1.0 / (bow[0] * np.sqrt(wave * count_second)))
        tall = lambda value: jnp.concatenate([value] * count_second, axis=0)
        mean, gauge = tall(mean), tall(gauge)
        new_s = factor[0] * s - t_turned * factor[2] + factor[3] * gauge
        new_t = factor[1] * t - s_turned * factor[2]
        solved = mixed(2, jnp.concatenate([new_s, new_t], axis=1))
        high, low = halves(solved)
        wide = lax.broadcasted_iota(jnp.int32, (count_second * chunk, width), 1)
        across = lambda a, b: lax.dot_general(
            a, b, (((1,), (1,)), ((), ())), preferred_element_type=F32
        )
        for i in range(count_first):
            piece = across(high, table[0, i]) + across(high, table[1, i]) + across(low, table[0, i])
            piece = jnp.where(wide == 2 * rows, mean, piece)
            answer[i * count_second : (i + 1) * count_second] = piece.reshape(
                count_second, chunk, width
            )
            over_devices(lambda d: back_copy(d).start(), i)
        kept = pltpu.make_async_copy(
            answer.at[me], back.at[own_tile, pl.ds(place_second * chunk, chunk)], self_sem.at[0]
        )
        kept.start()
        kept.wait()

    second = []
    edge_ref[...] = jnp.zeros_like(edge_ref)
    for t in range(tiles):
        over_owners(t, lambda t, k: back_from(t, k).wait_recv())
        lines[...] = back[t].T
        after = 2 * rows + 2
        for place, sign in ((0, -1.0), (7, 1.0)):
            mixed_lines = 0.5 * (lines[:rows, :] + sign * lines[rows : 2 * rows, :])
            edge_ref[1 : rows + 1, place, lane_of(t)] = mixed_lines
            ends = 0.5 * (lines[after : after + 2, :] + sign * lines[after + 2 : after + 4, :])
            edge_ref[rows + 1, place : place + 1, lane_of(t)] = ends[0:1]
            edge_ref[0, place : place + 1, lane_of(t)] = ends[1:2]
        r = weights(0, t)
        if t == 0:
            mean_term = vec_ref[2] * lines[2 * rows : 2 * rows + 1, :]
            mean_term = tuple(mean_term[window[g]] for g in range(groups))
        wide_vec = [
            jnp.broadcast_to(vec_ref[n], (strip, LANES)) for n in range(2)
        ]

        def fresh(i):
            f = list(row_of(f_ref, i, t))
            line_s = lines[pl.ds(i, 1), :]
            line_t = lines[pl.ds(rows + i, 1), :]
            for g in range(groups):
                if t == 0:
                    f[g] = f[g] - mean_term[g]
                if g in even_groups:
                    f[g] = f[g] - wide_vec[0][window[g]] * line_s
                if g in odd_groups:
                    f[g] = f[g] - wide_vec[1][window[g]] * line_t
                f_ref[i, window[g], lane_of(t)] = f[g]
            return tuple(f)

        def renewed(make):
            def body(i, j, carry):
                up, down = carry
                one = fresh(i) if make else row_of(f_ref, i, t)
                two = fresh(j) if make else row_of(f_ref, j, t)
                return step_on(r, up, one), step_on(r, down, two)

            return body

        state = both_ways(0, middle, renewed(True), (zeros, zeros))
        up, down = both_ways(middle, rows, renewed(False), state)
        store_moments(mom_two, t, up, down)
        second.append(shares(mom_two, send_two, recv_two, t))
        for copy in second[t]:
            copy.start()

    for t in range(tiles):
        r, scale = weights(0, t), weights(1, t)
        for copy in second[t]:
            copy.wait()
        carry_up, carry_down = carries(mom_two, t)

        def put(i, value, add):
            for g in range(groups):
                if add:
                    out_ref[i + 1, window[g], lane_of(t)] = (
                        out_ref[i + 1, window[g], lane_of(t)] + value[g]
                    ) * scale[g]
                else:
                    out_ref[i + 1, window[g], lane_of(t)] = value[g]

        def last(add):
            def body(i, j, carry):
                up, down = carry
                up = step_on(r, up, row_of(f_ref, i, t))
                down = tuple(r[g] * down[g] for g in range(groups))
                put(i, up, add)
                put(j, down, add)
                f = row_of(f_ref, j, t)
                return up, tuple(down[g] + f[g] for g in range(groups))

            return body

        state = both_ways(0, middle, last(False), (carry_up, carry_down))
        up, down = both_ways(middle, rows, last(True), state)
        for g in range(groups):
            out_ref[rows + 1, window[g], lane_of(t)] = (r[g] * up[g] + carry_down[g]) * scale[g]
            out_ref[0, window[g], lane_of(t)] = (carry_up[g] + r[g] * down[g]) * scale[g]

    def patch(t):
        x, _ = corner(t)
        mix, halo_row = strip_mix[t], halo_rows[t]
        values = []
        for i in range(PATCH):
            high, low = halves(out_ref[x + i])
            value = dot(mix, jnp.concatenate([high, high, low], axis=0))
            halo = jnp.concatenate([edge_ref[x + i]] * 3, axis=0)
            values.append(value + halo * halo_row[:, :1])
        high, low = halves(jnp.concatenate(values, axis=0))
        both = dot(jnp.concatenate([high, low], axis=1), windows[t])
        both = both[:, :LANES] + both[:, LANES:]
        for i in range(PATCH):
            cut[t, i] = both[24 * i : 24 * i + 24]
        total = jnp.zeros(lane.shape, F32)
        for b in range(PATCH):
            line = jnp.where(lane < PATCH, cut[t, :, 7 + b, :], 0.0)
            total = total + (pltpu.roll(line, PATCH * b, 1) if b else line)
        return total

    def patch_pair(n, carry):
        totals = [patch(2 * n + q) for q in range(2)]
        for q in range(2):
            patches[2 * n + q + 1] = totals[q]
        return carry

    lax.fori_loop(0, count_second // 2, patch_pair, 0)
    patches[0] = patches[count_second]
    patches[count_second + 1] = patches[1]
    own = pltpu.make_async_copy(
        patches.at[pl.ds(place_second, 3)], arrived_ref.at[0], self_sem.at[0]
    )
    own.start()
    moves = []
    for d in range(1, count_second):
        target = lax.rem(place_second + d, count_second)
        moves.append(
            pltpu.make_async_remote_copy(
                src_ref=patches.at[pl.ds(target, 3)],
                dst_ref=arrived_ref.at[count_second - d],
                send_sem=send_patch.at[d],
                recv_sem=recv_patch.at[d],
                device_id=(place_first, target),
                device_id_type=mesh,
            )
        )
    for copy in moves:
        copy.start()
    unstrip = unstrip_ref[:strip, :]

    def restore(n, carry):
        for m in range(block):
            row = n * block + m + 1
            high, low = halves(out_ref[row])
            out_ref[row] = dot(unstrip, jnp.concatenate([high, high, low], axis=0))
        store(n).start()
        return carry

    lax.fori_loop(0, BLOCKS, restore, 0)
    for t in range(tiles):
        over_owners(t, lambda t, k: line_copy(t, k).wait_send())

    @pl.when(is_owner)
    def _():
        over_devices(lambda d: back_copy(d).wait_send())

    for copy in faces + moves + [own]:
        copy.wait()
    for n in range(BLOCKS):
        store(n).wait()


def subgrid_kernel(
    count_ref,
    near_ref,
    patch_ref,
    xt_ref,
    yz_ref,
    mid_ref,
    low_ref,
    high_ref,
    vel_ref,
    u_ref,
    wave_ref,
    pot_ref,
    kick_ref,
    grid_ref,
    plane_ref,
    coarse_ref,
    iterate,
    steady,
    pair,
):
    device = lax.axis_index("px") * lax.axis_size("py") + lax.axis_index("py")
    place = pl.program_id(0)
    slot = device * pl.num_programs(0) + place
    below = near_ref[0, slot]
    above = near_ref[1, slot]
    live = place < count_ref[device]
    has_below = below >= 0
    has_above = above >= 0
    back_below = near_ref[1, jnp.maximum(below, 0)] >= 0
    back_above = near_ref[0, jnp.maximum(above, 0)] >= 0
    tiles = WIDE // LANES
    lanes = lambda g: slice(g * LANES, (g + 1) * LANES)
    planes, strip, wave = u_ref.shape
    dot = lambda a, b: jnp.dot(a, b, preferred_element_type=F32)

    @pl.when(place == 0)
    def _():
        column = lax.broadcasted_iota(jnp.int32, (16, LANES), 1)
        count = patch_ref.shape[0]
        stack = []
        for s in range(count):
            own = pltpu.roll(patch_ref[s, 1], PATCH, 1)
            under = pltpu.roll(patch_ref[(s - 1) % count, 0], LANES - (REG - 1) * PATCH, 1)
            over = pltpu.roll(patch_ref[(s + 1) % count, 2], (PATCH - 1) * PATCH, 1)
            patch = jnp.where(
                column < PATCH, under, jnp.where(column < (PATCH + 1) * PATCH, own, over)
            )
            stack.append(jnp.where(column < (PATCH + 2) * PATCH, patch, 0.0))
        total = None
        for piece in thirds(jnp.concatenate(stack, axis=0)):
            term = dot(piece, yz_ref[...])
            total = term if total is None else total + term
        plane_ref[...] = total.reshape(plane_ref.shape)

    coarse_ref[...] = dot(xt_ref[...], jnp.concatenate(thirds(plane_ref[place]), axis=0))
    high, low = halves(u_ref[...].reshape(planes * strip, wave))
    pair[:, :wave] = high
    pair[:, wave:] = low

    def restore(t):
        both = dot(pair[...], wave_ref[t])
        value = both[:, :LANES] + both[:, LANES:]
        grid_ref[:, :, lanes(t)] = value.reshape(planes, strip, LANES)

    lane = lax.broadcasted_iota(jnp.int32, (CELLS, LANES), 1)
    first = lane % CELLS == 0
    final = lane % CELLS == CELLS - 1
    front = lane < CELLS
    rear = lane >= LANES - CELLS
    body = slice(8, 8 + CELLS)
    behind = slice(7, 7 + CELLS)
    ahead = slice(9, 9 + CELLS)

    for g in range(tiles):
        start = coarse_ref[:CELLS, lanes(g)]
        iterate[0, g, body] = start
        for n in range(2):
            iterate[n, g, 7:8] = coarse_ref[CELLS : CELLS + 1, lanes(g)]
            iterate[n, g, 8 + CELLS : 9 + CELLS] = coarse_ref[CELLS + 1 : CELLS + 2, lanes(g)]
        if g == 0:
            rho = low_ref[0]
        elif g == tiles - 1:
            rho = high_ref[0]
        else:
            rho = mid_ref[0, :, lanes(g - 1)]
        steady[g] = coarse_ref[:CELLS, lanes(tiles + g)] - rho * (1.0 / (REF * REF))

    def turn(value, amount):
        return pltpu.roll(value, amount % LANES, 1)

    edge_low = coarse_ref[:CELLS, lanes(2 * tiles)]
    edge_high = coarse_ref[:CELLS, lanes(2 * tiles + 1)]
    held_above = jnp.where(back_below, 0.0, turn(coarse_ref[:CELLS, lanes(1)], -CELLS))
    held_below = jnp.where(back_above, 0.0, turn(coarse_ref[:CELLS, lanes(tiles - 2)], CELLS))

    def second_sides(source, g):
        value = source[g]
        down = turn(value, CELLS)
        up = turn(value, -CELLS)
        if g == 0:
            lower = edge_low
        else:
            lower = turn(source[g - 1], CELLS)
            if g == tiles - 1:
                lower = jnp.where(back_above, lower, held_below)
        if g == tiles - 1:
            upper = edge_high
        else:
            upper = turn(source[g + 1], -CELLS)
            if g == 0:
                upper = jnp.where(back_below, upper, held_above)
        return jnp.where(front, lower, down), jnp.where(rear, upper, up)

    for n in range(SWEEPS):
        if n < wave // LANES:
            restore(n)
        now, later = n % 2, (n + 1) % 2
        source = {}
        for g in range(tiles):
            for k in (g, g + 1):
                if k < tiles and k not in source:
                    source[k] = iterate[now, k, body]
            value = source[g]
            total = iterate[now, g, behind] + iterate[now, g, ahead]
            lower, upper = second_sides(source, g)
            total = total + (lower + upper)
            total = total + jnp.where(first, 0.0, turn(value, 1))
            total = total + jnp.where(final, 0.0, turn(value, -1))
            new = (total + (value + steady[g])) * (RELAXATION / 6.0)
            if g == 0:
                new = jnp.where(has_below, new, value)
            if g == tiles - 1:
                new = jnp.where(has_above, new, value)
            iterate[later, g, body] = new
    for n in range(SWEEPS, wave // LANES):
        restore(n)

    now = SWEEPS % 2
    source = {g: iterate[now, g, body] for g in range(3)}
    for g in range(1, tiles - 1):
        source[g + 1] = iterate[now, g + 1, body]
        value = source[g]
        lower, upper = second_sides(source, g)
        edge = coarse_ref[:CELLS, lanes(tiles + g)]
        slopes = (
            iterate[now, g, ahead] - iterate[now, g, behind],
            upper - lower,
            jnp.where(final, edge, turn(value, -1)) - jnp.where(first, edge, turn(value, 1)),
        )
        pot_ref[0, :, lanes(g - 1)] = jnp.where(live, value, 0.0)
        for q, slope in enumerate(slopes):
            moved = vel_ref[q, 0, :, lanes(g - 1)] - slope * (REF / 2.0)
            kick_ref[q, 0, :, lanes(g - 1)] = jnp.where(live, moved, 0.0)


def poisson(root_density, density, slot_anchor):
    count_first = lax.axis_size("px")
    count_second = lax.axis_size("py")
    devices = count_first * count_second
    rows, strip, wave = root_density.shape
    tiles = wave // LANES
    chunk = LANES // count_second
    width = -(-(2 * rows + 6) // 128) * 128
    basis = fourier_basis(wave)
    strip_table, strip_eig = strip_basis(strip)
    eig = 4.0 * np.sin(np.pi / wave * np.arange(wave)) ** 2
    mixes, angles = strip_coupling(count_second, chunk)
    cell = np.arange(strip)
    bow = 0.5 * (cell * cell - (strip - 1) * cell) - strip / 4
    lower = cell < strip // 2
    edge = strip_table[:, 0]
    vectors = np.stack(
        [
            np.where(lower, edge, 0.0),
            np.where(lower, 0.0, edge),
            strip_table.sum(1),
            strip_table @ bow,
        ]
    )[:, :, None]
    mix_high, mix_low = halves(jnp.asarray(mixes, F32))
    wave_halves = jnp.stack(halves(jnp.asarray(basis, F32)))
    high, low = halves(jnp.asarray(strip_table, F32))
    strip_wide = jnp.concatenate([high, low, high], axis=1)
    extended = np.zeros((strip + 8, strip))
    extended[:strip] = strip_table.T
    extended[strip] = -strip_table[:, 0]
    extended[-1] = -strip_table[:, -1]
    high, low = halves(jnp.asarray(extended, F32))
    unstrip_wide = jnp.concatenate([high, low, high], axis=1)
    moment = pltpu.VMEM((tiles, count_first, 2, strip, LANES), F32)
    dma = pltpu.SemaphoreType.DMA
    face = jax.ShapeDtypeStruct(density.shape[:2] + (EDGE * CELLS,), F32)
    vmem = pl.BlockSpec(memory_space=pltpu.VMEM)
    hbm = pl.BlockSpec(memory_space=pl.ANY)
    uy, arrived, low_density, high_density = pl.pallas_call(
        lambda *refs: grid_kernel((count_first, count_second), *refs),
        in_specs=[pl.BlockSpec(memory_space=pltpu.SMEM), hbm] + [vmem] * 10 + [hbm],
        out_specs=[hbm, vmem, hbm, hbm],
        out_shape=[
            jax.ShapeDtypeStruct((rows, strip, wave), F32),
            jax.ShapeDtypeStruct((count_second, 3, 16, LANES), F32),
            face,
            face,
        ],
        scratch_shapes=[
            pltpu.VMEM((rows + 2, 8, wave), F32),
            pltpu.VMEM((rows, strip, wave), F32),
            pltpu.VMEM((rows + 2, strip, wave), F32),
            pltpu.VMEM((rows * strip, 2 * wave), jnp.bfloat16),
            pltpu.VMEM((tiles, 2 * wave, 2 * LANES), jnp.bfloat16),
            pltpu.VMEM((count_second + 2, 16, LANES), F32),
            pltpu.VMEM((count_second, 16, 24, LANES), F32),
            pltpu.VMEM((count_second, 2 * wave, 2 * LANES), jnp.bfloat16),
            pltpu.VMEM((count_second, 24, 3 * strip), jnp.bfloat16),
            pltpu.VMEM((count_second, 24, LANES), F32),
            pltpu.VMEM((width, LANES), F32),
            pltpu.VMEM((tiles, LANES, width), F32),
            pltpu.VMEM((devices, chunk, width), F32),
            pltpu.VMEM((devices, chunk, width), F32),
            pltpu.VMEM((tiles, LANES, width), F32),
            moment,
            moment,
            pltpu.VMEM((2, rows, 8, LANES), F32),
            pltpu.VMEM((2, count_first, width, 2 * wave), jnp.bfloat16),
            pltpu.VMEM((4, count_second * chunk, wave), F32),
            pltpu.VMEM((6, strip, wave), F32),
            dma((BLOCKS,)),
            dma((BLOCKS,)),
            dma((tiles, count_first)),
            dma((tiles, count_first)),
            dma((tiles, count_first)),
            dma((tiles, count_first)),
            dma((tiles, count_second)),
            dma((devices,)),
            dma((devices,)),
            dma((tiles, count_second)),
            dma((2,)),
            dma((2,)),
            dma((2,)),
            dma((count_second,)),
            dma((count_second,)),
        ],
        compiler_params=pltpu.CompilerParams(
            collective_id=1, has_side_effects=True, vmem_limit_bytes=60 * 1024 * 1024
        ),
    )(
        slot_anchor,
        root_density,
        jnp.asarray(strip_eig[:, None], F32),
        jnp.asarray(eig[None, :], F32),
        jnp.asarray(eig[:, None], F32),
        jnp.asarray(vectors, F32),
        jnp.stack(halves(jnp.asarray(basis.T, F32))),
        jnp.concatenate([mix_high, mix_low, mix_high], axis=2),
        jnp.asarray(angles, F32),
        strip_wide,
        unstrip_wide,
        wave_halves,
        density,
    )
    high = wave_halves[0].reshape(wave, tiles, LANES)
    low = wave_halves[1].reshape(wave, tiles, LANES)
    top = jnp.concatenate([high, low], axis=2)
    bottom = jnp.concatenate([high, jnp.zeros_like(low)], axis=2)
    inverse = jnp.concatenate([top, bottom], axis=0).transpose(1, 0, 2)
    return uy, inverse, arrived, low_density, high_density


def local(root_density, subgrid_density, velocity, slot_anchor, slot_count, neighbour):
    per_device = subgrid_density.shape[0]
    side = EDGE * CELLS
    inner = CELLS * CELLS
    uy, inverse, patches, low_density, high_density = poisson(
        root_density, subgrid_density, slot_anchor
    )
    x_table, yz_table = patch_tables()
    smem = pl.BlockSpec(memory_space=pltpu.SMEM)
    slot_spec = lambda width: pl.BlockSpec((1, CELLS, width), lambda s: (s, 0, 0))
    vel_spec = pl.BlockSpec((3, 1, CELLS, inner), lambda s: (0, s, 0, 0))
    x_table = jnp.asarray(np.tile(x_table, (1, 3)), jnp.bfloat16)
    yz_table = jnp.asarray(yz_table, jnp.bfloat16)
    columns = yz_table.shape[1]
    planes, strip, wave = uy.shape
    planes //= per_device
    grid_spec = pl.BlockSpec((planes, strip, wave), lambda s: (s, 0, 0))
    potential, kicked, coarse_potential = pl.pallas_call(
        subgrid_kernel,
        grid=(per_device,),
        in_specs=[
            smem,
            smem,
            pl.BlockSpec(patches.shape, lambda s: (0, 0, 0, 0)),
            pl.BlockSpec(x_table.shape, lambda s: (0, 0)),
            pl.BlockSpec(yz_table.shape, lambda s: (0, 0)),
            slot_spec(inner),
            slot_spec(side),
            slot_spec(side),
            vel_spec,
            grid_spec,
            pl.BlockSpec(inverse.shape, lambda s: (0, 0, 0)),
        ],
        out_specs=[slot_spec(inner), vel_spec, grid_spec],
        out_shape=[
            jax.ShapeDtypeStruct(subgrid_density.shape, F32),
            jax.ShapeDtypeStruct(velocity.shape, F32),
            jax.ShapeDtypeStruct(uy.shape, F32),
        ],
        scratch_shapes=[
            pltpu.VMEM((per_device, 16, columns), F32),
            pltpu.VMEM((CELLS + 8, columns), F32),
            pltpu.VMEM((2, WIDE // LANES, CELLS + 16, LANES), F32),
            pltpu.VMEM((WIDE // LANES, CELLS, LANES), F32),
            pltpu.VMEM((planes * strip, 2 * wave), jnp.bfloat16),
        ],
        compiler_params=pltpu.CompilerParams(
            dimension_semantics=("arbitrary",), vmem_limit_bytes=60 * 1024 * 1024
        ),
    )(
        slot_count,
        neighbour,
        patches,
        x_table,
        yz_table,
        subgrid_density,
        low_density,
        high_density,
        velocity,
        uy,
        inverse,
    )
    return (coarse_potential, potential, kicked)


def solution(mesh):
    return jax.shard_map(
        local,
        mesh=mesh,
        in_specs=(
            P("px", "py", None),
            P(("px", "py"), None, None),
            P(None, ("px", "py"), None, None),
            P(),
            P(),
            P(),
        ),
        out_specs=(
            P("px", "py", None),
            P(("px", "py"), None, None),
            P(None, ("px", "py"), None, None),
        ),
        check_vma=False,
    )
```

```python
import jax
import jax.numpy as jnp
import numpy as np
from jax import lax
from jax.experimental import pallas as pl
from jax.experimental.pallas import tpu as pltpu
from jax.sharding import PartitionSpec as P

NR = 384
REG = 8
REF = 4
SWEEPS = 4
CELLS = REG * REF
EDGE = SWEEPS
LAYERS = CELLS + 2 * EDGE
WIDE = LAYERS * CELLS
RELAXATION = 6.0 / 7.0
LANES = 128
F32 = jnp.float32


def fourier_basis(length):
    cell = np.arange(length)
    rows = []
    for k in range(length):
        if k in (0, length // 2):
            rows.append(np.cos(2 * np.pi * (k * cell % length) / length) / np.sqrt(length))
        elif k < length // 2:
            rows.append(np.cos(2 * np.pi * (k * cell % length) / length) * np.sqrt(2 / length))
        else:
            rows.append(
                np.sin(2 * np.pi * ((length - k) * cell % length) / length) * np.sqrt(2 / length)
            )
    return np.stack(rows)


def strip_basis(cells):
    place = np.arange(cells) - (cells - 1) / 2
    mode = 2 * np.arange(cells // 2) + 1
    angle = np.pi * mode[:, None] * place[None, :] / cells
    basis = np.concatenate([np.cos(angle), np.sin(angle)]) * np.sqrt(2 / cells)
    eig = 4 * np.sin(np.pi * mode / (2 * cells)) ** 2
    return basis, np.concatenate([eig, eig])


def strip_coupling(count, rows):
    basis = fourier_basis(count)
    turn = np.zeros((count, count))
    theta = 2 * np.pi * np.arange(count) / count
    for k in range(1, (count + 1) // 2):
        turn[k, count - k] = np.sin(theta[k])
        turn[count - k, k] = -np.sin(theta[k])
    wide = lambda matrix: np.kron(matrix, np.eye(rows))
    mixes = np.stack([wide(basis), wide(turn @ basis), wide(basis.T)])
    half_sine = np.sin(theta / 2) ** 2
    factors = np.stack([half_sine, 4 * (1 - half_sine)])
    return mixes, np.repeat(factors, rows, axis=1)[:, :, None]


def axis_weights(cells, first, count):
    table = np.zeros((len(cells), count))
    for row, cell in enumerate(cells):
        mark = 2 * cell - 1 + REF
        low = mark // (2 * REF)
        frac = (mark - 2 * REF * low) / (2 * REF)
        table[row, low - first] += 1 - frac
        if frac:
            table[row, low + 1 - first] += frac
    return table


PATCH = REG + 2
PATCH_X = REG + 2
PATCH_Y = REG + 4
PATCH_Z = REG + 2


def patch_tables():
    inner = np.arange(1, CELLS + 1)
    x_side = axis_weights(np.concatenate([inner, [0, CELLS + 1]]), 0, PATCH_X)
    x_table = np.zeros((CELLS + 8, 16))
    x_table[: CELLS + 2, :PATCH_X] = x_side
    y_cells = np.arange(1 - EDGE, CELLS + EDGE + 1)
    y_side = axis_weights(y_cells, -1, PATCH_Y)
    y_out = axis_weights(np.array([-EDGE, CELLS + EDGE + 1]), -1, PATCH_Y)
    z_side = axis_weights(np.arange(CELLS + 2), 0, PATCH_Z)
    z_edge = np.zeros((CELLS, PATCH_Z))
    z_edge[0] = z_side[0]
    z_edge[-1] = z_side[-1]
    y_edge = np.zeros((LAYERS, PATCH_Y))
    y_edge[0] = y_out[0]
    y_edge[-1] = y_out[1]

    def both(ys, zs):
        return np.einsum("jb,kc->bcjk", ys, zs).reshape(PATCH_Y * PATCH_Z, WIDE)

    ends = both(y_edge, z_side[1:-1])
    table = np.zeros((LANES, 2 * WIDE + 2 * LANES))
    table[: PATCH_Y * PATCH_Z] = np.concatenate(
        [
            both(y_side, z_side[1:-1]),
            both(y_side, z_edge),
            ends[:, :LANES],
            ends[:, -LANES:],
        ],
        axis=1,
    )
    return x_table.astype(np.float32), table.astype(np.float32)


def decay(delta):
    return 1.0 / (1.0 + 0.5 * delta + jnp.sqrt(delta + 0.25 * delta * delta))


def power(value, exponent):
    result = None
    while exponent:
        if exponent & 1:
            result = value if result is None else result * value
        exponent >>= 1
        if exponent:
            value = value * value
    return result


def halves(value):
    high = value.astype(jnp.bfloat16)
    return high, (value - high.astype(F32)).astype(jnp.bfloat16)


def thirds(value):
    high = value.astype(jnp.bfloat16)
    rest = value - high.astype(F32)
    middle = rest.astype(jnp.bfloat16)
    return high, middle, (rest - middle.astype(F32)).astype(jnp.bfloat16)


def owner_shift(place_second):
    return place_second // 2 * 2 + 2


BLOCKS = 6


def grid_kernel(
    sizes,
    anchor_ref,
    root_hbm,
    eig_b_ref,
    eig_ref,
    own_ref,
    vec_ref,
    basis_ref,
    mix_ref,
    angle_ref,
    strip_ref,
    unstrip_ref,
    wave_ref,
    density_ref,
    out_hbm,
    arrived_ref,
    low_ref,
    high_ref,
    edge_ref,
    f_ref,
    out_ref,
    pair,
    forward,
    patches,
    cut,
    windows,
    strip_mix,
    halo_rows,
    lines,
    sent,
    got,
    answer,
    back,
    mom_one,
    mom_two,
    part,
    table,
    factor,
    weight,
    in_sem,
    out_sem,
    send_one,
    recv_one,
    send_two,
    recv_two,
    send_line,
    recv_line,
    send_back,
    recv_back,
    self_sem,
    send_face,
    recv_face,
    send_patch,
    recv_patch,
):
    count_first, count_second = sizes
    devices = count_first * count_second
    rows, strip, wave = f_ref.shape
    tiles = wave // LANES
    groups = strip // 8
    half = strip // 2
    middle = rows // 2
    fold = 4
    chunk = got.shape[1]
    width = lines.shape[0]
    mesh = pl.DeviceIdType.MESH
    place_first = lax.axis_index("px")
    place_second = lax.axis_index("py")
    me = place_first * count_second + place_second
    own_tile = lax.rem(
        place_first + 2 * count_second * count_first - owner_shift(place_second), count_first
    )
    is_owner = own_tile < tiles
    barrier = pltpu.get_barrier_semaphore()

    lane_of = lambda t: slice(t * LANES, (t + 1) * LANES)

    block = rows // BLOCKS

    def load(n):
        piece = pl.ds(n * block, block)
        return pltpu.make_async_copy(root_hbm.at[piece], f_ref.at[piece], in_sem.at[n])

    def store(n):
        return pltpu.make_async_copy(
            out_ref.at[pl.ds(n * block + 1, block)],
            out_hbm.at[pl.ds(n * block, block)],
            out_sem.at[n],
        )

    for n in range(BLOCKS):
        load(n).start()
    def greet(step, carry):
        other = lax.rem(me + step, devices)
        pl.semaphore_signal(
            barrier,
            inc=1,
            device_id=(other // count_second, lax.rem(other, count_second)),
            device_id_type=mesh,
        )
        return carry

    lax.fori_loop(1, devices, greet, 0)
    dot = lambda a, b: jnp.dot(a, b, preferred_element_type=F32)
    forward[...] = jnp.zeros_like(forward)
    for t in range(tiles):
        forward[t, :wave, :LANES] = basis_ref[0, :, lane_of(t)]
        forward[t, wave:, :LANES] = basis_ref[0, :, lane_of(t)]
        forward[t, :wave, LANES:] = basis_ref[1, :, lane_of(t)]

    window = [slice(8 * g, 8 * g + 8) for g in range(groups)]
    even_groups = [g for g in range(groups) if 8 * g < half]
    odd_groups = [g for g in range(groups) if 8 * g + 8 > half]
    zeros = tuple(jnp.zeros((8, LANES), F32) for _ in range(groups))

    r_all = decay(eig_b_ref[...] + eig_ref[...])
    scale_all = -r_all / ((1.0 - r_all) * (1.0 + r_all))
    ratio_all = power(r_all, rows)
    weight[0] = r_all
    weight[1] = scale_all
    weight[2] = 2.0 * vec_ref[0] * scale_all
    weight[3] = -2.0 * vec_ref[1] * scale_all
    weight[4] = ratio_all
    weight[5] = 1.0 / (1.0 - power(ratio_all, count_first))

    def weights(which, t):
        return tuple(weight[which, window[g], lane_of(t)] for g in range(groups))

    def row_of(ref, i, t):
        return tuple(ref[i, window[g], lane_of(t)] for g in range(groups))

    def step_on(r, state, f):
        return tuple(r[g] * state[g] + f[g] for g in range(groups))

    def both_ways(start, stop, body, carry):
        def folded(n, carry):
            for k in range(fold):
                i = start + n * fold + k
                carry = body(i, rows - 1 - i, carry)
            return carry

        return lax.fori_loop(0, (stop - start) // fold, folded, carry)

    def store_moments(buffer, t, up, down):
        for g in range(groups):
            buffer[t, 0, 0, window[g], :] = up[g]
            buffer[t, 0, 1, window[g], :] = down[g]

    def shares(buffer, send, recv, t):
        return [
            pltpu.make_async_remote_copy(
                src_ref=buffer.at[t, 0],
                dst_ref=buffer.at[t, d],
                send_sem=send.at[t, d],
                recv_sem=recv.at[t, d],
                device_id=(lax.rem(place_first + d, count_first), place_second),
                device_id_type=mesh,
            )
            for d in range(1, count_first)
        ]

    def carries(buffer, t):
        ratio, norm = weights(4, t), weights(5, t)
        up, down = [], []
        for g in range(groups):
            total = buffer[t, 0, 0, window[g], :]
            for d in range(count_first - 1, 0, -1):
                total = ratio[g] * total + buffer[t, d, 0, window[g], :]
            up.append(total * norm[g])
            total = buffer[t, 0, 1, window[g], :]
            for d in range(1, count_first):
                total = ratio[g] * total + buffer[t, d, 1, window[g], :]
            down.append(total * norm[g])
        return tuple(up), tuple(down)

    face = low_ref.shape[2]
    inner = density_ref.shape[2]
    faces = [
        pltpu.make_async_remote_copy(
            src_ref=density_ref.at[:, :, pl.ds(start, face)],
            dst_ref=target,
            send_sem=send_face.at[n],
            recv_sem=recv_face.at[n],
            device_id=(place_first, lax.rem(place_second + step, count_second)),
            device_id_type=mesh,
        )
        for n, (start, target, step) in enumerate(
            ((inner - face, low_ref, 1), (0, high_ref, count_second - 1))
        )
    ]

    tall = strip + 8
    tall_row = lax.broadcasted_iota(jnp.int32, (24, tall), 0)
    tall_column = lax.broadcasted_iota(jnp.int32, (24, tall), 1)
    cell = lax.broadcasted_iota(jnp.int32, (wave, LANES), 0)
    spot = lax.broadcasted_iota(jnp.int32, (wave, LANES), 1)
    lane = lax.broadcasted_iota(jnp.int32, (16, LANES), 1)
    cut[...] = jnp.zeros_like(cut)


    def corner(t):
        slot = (place_first * count_second + t) * count_second + lax.rem(
            place_second - t + count_second, count_second
        )
        x = jnp.clip(anchor_ref[0, slot] - place_first * rows, 0, rows - REG)
        return x, slot

    def prepare(t, carry):
        _, slot = corner(t)
        y = jnp.clip(anchor_ref[1, slot] - place_second * strip, 0, strip - REG) // 8
        origin = jnp.clip(anchor_ref[2, slot], 0, wave - REG) - 1 + spot
        origin = jnp.where(origin < 0, origin + wave, origin)
        origin = jnp.where(origin >= wave, origin - wave, origin)
        select = jnp.where(cell == origin, 1.0, 0.0).astype(jnp.bfloat16)
        wave_high = dot(wave_ref[0], select).astype(jnp.bfloat16)
        windows[t, :wave, :LANES] = wave_high
        windows[t, wave:, :LANES] = wave_high
        windows[t, :wave, LANES:] = dot(wave_ref[1], select).astype(jnp.bfloat16)
        windows[t, wave:, LANES:] = jnp.zeros((wave, LANES), jnp.bfloat16)
        wanted = tall_row + 8 * y - 8
        wanted = jnp.where(wanted < 0, wanted + tall, wanted)
        pick = jnp.where(tall_column == wanted, 1.0, 0.0).astype(jnp.bfloat16)
        strip_mix[t] = dot(pick, unstrip_ref[...]).astype(jnp.bfloat16)
        halo_rows[t] = jnp.broadcast_to(
            jnp.where(wanted[:, :1] >= strip, 1.0, 0.0), halo_rows.shape[1:]
        )
        return carry

    @pl.when(is_owner)
    def _():
        table[...] = jnp.zeros_like(table)
        for i in range(count_first):
            for n in range(2):
                block = basis_ref[n, i * rows : (i + 1) * rows, :]
                table[n, i, :rows, :wave] = block
                table[n, i, rows : 2 * rows, wave:] = block
                for place, row in enumerate((rows * (i + 1) % wave, (rows * i - 1) % wave)):
                    line = basis_ref[n, row : row + 1, :]
                    table[n, i, 2 * rows + 2 + place : 2 * rows + 3 + place, :wave] = line
                    table[n, i, 2 * rows + 4 + place : 2 * rows + 5 + place, wave:] = line
        start = own_tile * LANES + place_second * chunk
        own_eig = jnp.concatenate([own_ref[pl.ds(start, chunk), :]] * count_second, axis=0)
        lam = own_eig + eig_ref[...]
        sinh = jnp.sqrt(lam + 0.25 * lam * lam)
        flat = lam <= 0.0
        far = power(decay(lam), strip)
        tanh = (1.0 - far) / (1.0 + far)
        green = jnp.where(flat, strip / 4.0, tanh / jnp.where(flat, 1.0, 2.0 * sinh))
        square = tanh * tanh
        half_sine = angle_ref[0]
        det = half_sine * (1.0 - square) + square
        zero = flat & (half_sine <= 0.0)
        inverse = jnp.where(zero, 0.0, 1.0 / jnp.where(zero, 1.0, det))
        gain = angle_ref[1] * green * inverse
        factor[0] = gain * (2.0 + 0.5 * lam)
        factor[1] = jnp.where(zero, 2.0 / strip, gain * (0.5 * lam))
        factor[2] = inverse
        factor[3] = jnp.where(zero, 1.0, 0.0)

    first = []
    whole = []

    def open_tile(t):
        r = weights(0, t)
        span = (2 if t == 0 else 3) * block

        def transform(n, carry):
            piece = pl.ds(n * span, span)
            spread = pl.ds(pl.multiple_of(n * span * strip, 8), span * strip)
            if t == 0:
                for m in range(span // block):
                    load(n * (span // block) + m).wait()
                high, low = halves(f_ref[piece].reshape(span * strip, wave))
                pair[spread, :wave] = high
                pair[spread, wave:] = low
            both = dot(pair[spread], forward[t])
            value = both[:, :LANES] + both[:, LANES:]
            for m in range(0, span, 2):
                sides = [value[(m + q) * strip : (m + q + 1) * strip] for q in range(2)]
                high, low = halves(jnp.concatenate(sides, axis=1))
                stack = jnp.concatenate([high, high, low], axis=0)
                result = dot(strip_ref[...], stack)
                for q in range(2):
                    f_ref[n * span + m + q, :, lane_of(t)] = result[:, lane_of(q)]
            return carry

        lax.fori_loop(0, rows // span, transform, 0)

        def moments(i, j, carry):
            up, down, total = carry
            f = row_of(f_ref, i, t)
            up = step_on(r, up, f)
            down = step_on(r, down, row_of(f_ref, j, t))
            if t == 0:
                total = tuple(total[g] + f[g] for g in range(groups))
            return up, down, total

        up, down, total = both_ways(0, rows, moments, (zeros, zeros, zeros if t == 0 else ()))
        store_moments(mom_one, t, up, down)
        if t == 0:
            whole.append(jnp.concatenate(total, axis=0))
            pl.semaphore_wait(barrier, devices - 1)
        first.append(shares(mom_one, send_one, recv_one, t))
        for copy in first[t] + (faces if t == 0 else []):
            copy.start()

    def line_copy(t, k):
        return pltpu.make_async_remote_copy(
            src_ref=sent.at[t, pl.ds(k * chunk, chunk)],
            dst_ref=got.at[me],
            send_sem=send_line.at[t, k],
            recv_sem=recv_line.at[me],
            device_id=(lax.rem(owner_shift(k) + t, count_first), k),
            device_id_type=mesh,
        )

    def line_from(d):
        return pltpu.make_async_remote_copy(
            src_ref=sent.at[0, pl.ds(0, chunk)],
            dst_ref=got.at[d],
            send_sem=self_sem.at[1],
            recv_sem=recv_line.at[d],
            device_id=(d // count_second, lax.rem(d, count_second)),
            device_id_type=mesh,
        )

    def back_copy(d):
        return pltpu.make_async_remote_copy(
            src_ref=answer.at[d],
            dst_ref=back.at[own_tile, pl.ds(place_second * chunk, chunk)],
            send_sem=send_back.at[d],
            recv_sem=recv_back.at[own_tile, place_second],
            device_id=(d // count_second, lax.rem(d, count_second)),
            device_id_type=mesh,
        )

    def back_from(t, k):
        return pltpu.make_async_remote_copy(
            src_ref=answer.at[0],
            dst_ref=back.at[t, pl.ds(k * chunk, chunk)],
            send_sem=self_sem.at[1],
            recv_sem=recv_back.at[t, k],
            device_id=(lax.rem(owner_shift(k) + t, count_first), k),
            device_id_type=mesh,
        )

    def over_devices(action, part=None):
        def body(d, carry):
            @pl.when(d != me)
            def _():
                action(d)

            return carry

        start, stop = 0, devices
        if part is not None:
            start, stop = part * count_second, (part + 1) * count_second
        lax.fori_loop(start, stop, body, 0)

    def over_owners(t, action):
        def body(k, carry):
            @pl.when((k != place_second) | (own_tile != t))
            def _():
                action(t, k)

            return carry

        lax.fori_loop(0, count_second, body, 0)

    def weighed(values, members, state):
        total = None
        for g in members:
            term = values[g] * state[g]
            total = term if total is None else total + term
        return total

    def close_tile(t):
        r, even, odd = weights(0, t), weights(2, t), weights(3, t)
        for copy in first[t]:
            copy.wait()
        state = carries(mom_one, t)

        def lines_of(add):
            def body(i, j, carry):
                up, down = carry
                up = step_on(r, up, row_of(f_ref, i, t))
                down = tuple(r[g] * down[g] for g in range(groups))
                for n, (values, members) in enumerate(((even, even_groups), (odd, odd_groups))):
                    one = weighed(values, members, up)
                    two = weighed(values, members, down)
                    part[n, i] = part[n, i] + one if add else one
                    part[n, j] = part[n, j] + two if add else two
                f = row_of(f_ref, j, t)
                return up, tuple(down[g] + f[g] for g in range(groups))

            return body

        state = both_ways(0, middle, lines_of(False), state)
        both_ways(middle, rows, lines_of(True), state)
        lines[:rows, :] = jnp.sum(part[0], axis=1)
        lines[rows : 2 * rows, :] = jnp.sum(part[1], axis=1)
        lines[2 * rows :, :] = jnp.zeros((width - 2 * rows, LANES), F32)
        if t == 0:
            for n in range(2):
                lines[2 * rows + n : 2 * rows + n + 1, :] = jnp.sum(
                    vec_ref[2 + n] * whole[0], axis=0, keepdims=True
                )
        sent[t] = lines[...].T
        over_owners(t, lambda t, k: line_copy(t, k).start())

    for t in range(tiles):
        open_tile(t)
        if t > 0 and t < tiles - 1:
            close_tile(t - 1)
    for t in range(max(tiles - 2, 0), tiles):
        close_tile(t)
    @pl.when(is_owner)
    def _():
        own = pltpu.make_async_copy(
            sent.at[own_tile, pl.ds(place_second * chunk, chunk)], got.at[me], self_sem.at[0]
        )
        own.start()
        modes = None
        own.wait()
        for i in range(count_first):
            over_devices(lambda d: line_from(d).wait_recv(), i)
            piece = got[i * count_second : (i + 1) * count_second]
            high, low = halves(piece.reshape(count_second * chunk, width))
            term = dot(high, table[0, i]) + dot(high, table[1, i]) + dot(low, table[0, i])
            modes = term if modes is None else modes + term

        def mixed(which, value):
            high, low = halves(value)
            stack = jnp.concatenate([high, high, low], axis=0)
            return dot(mix_ref[which], stack)

        straight = mixed(0, modes)
        turned = mixed(1, modes)
        s, t = straight[:, :wave], straight[:, wave:]
        s_turned, t_turned = turned[:, :wave], turned[:, wave:]
        sums = jnp.sum(got[...], axis=0)
        lane = lax.broadcasted_iota(jnp.int32, sums.shape, 1)
        sigma = jnp.sum(jnp.where(lane == 2 * rows, sums, 0.0), axis=1, keepdims=True)
        lever = jnp.sum(jnp.where(lane == 2 * rows + 1, sums, 0.0), axis=1, keepdims=True)
        k = np.arange(strip)
        bow = 0.5 * (k * k - (strip - 1) * k) - strip / 4
        first_eig = own_ref[pl.ds(own_tile * LANES + place_second * chunk, chunk), :]
        mean = jnp.where(first_eig <= 0.0, sigma, 0.0) * (1.0 / (wave * wave))
        gauge = lever - mean * float(wave * count_second * bow.sum())
        gauge = gauge * float(1.0 / (bow[0] * np.sqrt(wave * count_second)))
        tall = lambda value: jnp.concatenate([value] * count_second, axis=0)
        mean, gauge = tall(mean), tall(gauge)
        new_s = factor[0] * s - t_turned * factor[2] + factor[3] * gauge
        new_t = factor[1] * t - s_turned * factor[2]
        solved = mixed(2, jnp.concatenate([new_s, new_t], axis=1))
        high, low = halves(solved)
        wide = lax.broadcasted_iota(jnp.int32, (count_second * chunk, width), 1)
        across = lambda a, b: lax.dot_general(
            a, b, (((1,), (1,)), ((), ())), preferred_element_type=F32
        )
        for i in range(count_first):
            piece = across(high, table[0, i]) + across(high, table[1, i]) + across(low, table[0, i])
            piece = jnp.where(wide == 2 * rows, mean, piece)
            answer[i * count_second : (i + 1) * count_second] = piece.reshape(
                count_second, chunk, width
            )
            over_devices(lambda d: back_copy(d).start(), i)
        kept = pltpu.make_async_copy(
            answer.at[me], back.at[own_tile, pl.ds(place_second * chunk, chunk)], self_sem.at[0]
        )
        kept.start()
        kept.wait()

    lax.fori_loop(0, count_second, prepare, 0)
    second = []
    edge_ref[...] = jnp.zeros_like(edge_ref)
    for t in range(tiles):
        over_owners(t, lambda t, k: back_from(t, k).wait_recv())
        lines[...] = back[t].T
        after = 2 * rows + 2
        for place, sign in ((0, -1.0), (7, 1.0)):
            mixed_lines = 0.5 * (lines[:rows, :] + sign * lines[rows : 2 * rows, :])
            edge_ref[1 : rows + 1, place, lane_of(t)] = mixed_lines
            ends = 0.5 * (lines[after : after + 2, :] + sign * lines[after + 2 : after + 4, :])
            edge_ref[rows + 1, place : place + 1, lane_of(t)] = ends[0:1]
            edge_ref[0, place : place + 1, lane_of(t)] = ends[1:2]
        r = weights(0, t)
        if t == 0:
            mean_term = vec_ref[2] * lines[2 * rows : 2 * rows + 1, :]
            mean_term = tuple(mean_term[window[g]] for g in range(groups))
        wide_vec = [
            jnp.broadcast_to(vec_ref[n], (strip, LANES)) for n in range(2)
        ]

        def fresh(i):
            f = list(row_of(f_ref, i, t))
            line_s = lines[pl.ds(i, 1), :]
            line_t = lines[pl.ds(rows + i, 1), :]
            for g in range(groups):
                if t == 0:
                    f[g] = f[g] - mean_term[g]
                if g in even_groups:
                    f[g] = f[g] - wide_vec[0][window[g]] * line_s
                if g in odd_groups:
                    f[g] = f[g] - wide_vec[1][window[g]] * line_t
                f_ref[i, window[g], lane_of(t)] = f[g]
            return tuple(f)

        def renewed(make):
            def body(i, j, carry):
                up, down = carry
                one = fresh(i) if make else row_of(f_ref, i, t)
                two = fresh(j) if make else row_of(f_ref, j, t)
                return step_on(r, up, one), step_on(r, down, two)

            return body

        state = both_ways(0, middle, renewed(True), (zeros, zeros))
        up, down = both_ways(middle, rows, renewed(False), state)
        store_moments(mom_two, t, up, down)
        second.append(shares(mom_two, send_two, recv_two, t))
        for copy in second[t]:
            copy.start()

    for t in range(tiles):
        r, scale = weights(0, t), weights(1, t)
        for copy in second[t]:
            copy.wait()
        carry_up, carry_down = carries(mom_two, t)

        def put(i, value, add):
            for g in range(groups):
                if add:
                    out_ref[i + 1, window[g], lane_of(t)] = (
                        out_ref[i + 1, window[g], lane_of(t)] + value[g]
                    ) * scale[g]
                else:
                    out_ref[i + 1, window[g], lane_of(t)] = value[g]

        def last(add):
            def body(i, j, carry):
                up, down = carry
                up = step_on(r, up, row_of(f_ref, i, t))
                down = tuple(r[g] * down[g] for g in range(groups))
                put(i, up, add)
                put(j, down, add)
                f = row_of(f_ref, j, t)
                return up, tuple(down[g] + f[g] for g in range(groups))

            return body

        state = both_ways(0, middle, last(False), (carry_up, carry_down))
        up, down = both_ways(middle, rows, last(True), state)
        for g in range(groups):
            out_ref[rows + 1, window[g], lane_of(t)] = (r[g] * up[g] + carry_down[g]) * scale[g]
            out_ref[0, window[g], lane_of(t)] = (carry_up[g] + r[g] * down[g]) * scale[g]

    def patch(t):
        x, _ = corner(t)
        mix, halo_row = strip_mix[t], halo_rows[t]
        values = []
        for i in range(PATCH):
            high, low = halves(out_ref[x + i])
            value = dot(mix, jnp.concatenate([high, high, low], axis=0))
            halo = jnp.concatenate([edge_ref[x + i]] * 3, axis=0)
            values.append(value + halo * halo_row[:, :1])
        high, low = halves(jnp.concatenate(values, axis=0))
        both = dot(jnp.concatenate([high, low], axis=1), windows[t])
        both = both[:, :LANES] + both[:, LANES:]
        for i in range(PATCH):
            cut[t, i] = both[24 * i : 24 * i + 24]
        total = jnp.zeros(lane.shape, F32)
        for b in range(PATCH):
            line = jnp.where(lane < PATCH, cut[t, :, 7 + b, :], 0.0)
            total = total + (pltpu.roll(line, PATCH * b, 1) if b else line)
        return total

    def patch_pair(n, carry):
        totals = [patch(2 * n + q) for q in range(2)]
        for q in range(2):
            patches[2 * n + q + 1] = totals[q]
        return carry

    lax.fori_loop(0, count_second // 2, patch_pair, 0)
    patches[0] = patches[count_second]
    patches[count_second + 1] = patches[1]
    own = pltpu.make_async_copy(
        patches.at[pl.ds(place_second, 3)], arrived_ref.at[0], self_sem.at[0]
    )
    own.start()
    moves = []
    for d in range(1, count_second):
        target = lax.rem(place_second + d, count_second)
        moves.append(
            pltpu.make_async_remote_copy(
                src_ref=patches.at[pl.ds(target, 3)],
                dst_ref=arrived_ref.at[count_second - d],
                send_sem=send_patch.at[d],
                recv_sem=recv_patch.at[d],
                device_id=(place_first, target),
                device_id_type=mesh,
            )
        )
    for copy in moves:
        copy.start()
    unstrip = unstrip_ref[:strip, :]

    def restore(n, carry):
        for m in range(block):
            row = n * block + m + 1
            high, low = halves(out_ref[row])
            out_ref[row] = dot(unstrip, jnp.concatenate([high, high, low], axis=0))
        store(n).start()
        return carry

    lax.fori_loop(0, BLOCKS, restore, 0)
    for t in range(tiles):
        over_owners(t, lambda t, k: line_copy(t, k).wait_send())

    @pl.when(is_owner)
    def _():
        over_devices(lambda d: back_copy(d).wait_send())

    for copy in faces + moves + [own]:
        copy.wait()
    for n in range(BLOCKS):
        store(n).wait()


def subgrid_kernel(
    count_ref,
    near_ref,
    patch_ref,
    xt_ref,
    yz_ref,
    mid_ref,
    low_ref,
    high_ref,
    vel_ref,
    u_ref,
    wave_ref,
    pot_ref,
    kick_ref,
    grid_ref,
    plane_ref,
    coarse_ref,
    iterate,
    steady,
    pair,
):
    device = lax.axis_index("px") * lax.axis_size("py") + lax.axis_index("py")
    place = pl.program_id(0)
    slot = device * pl.num_programs(0) + place
    below = near_ref[0, slot]
    above = near_ref[1, slot]
    live = place < count_ref[device]
    has_below = below >= 0
    has_above = above >= 0
    back_below = near_ref[1, jnp.maximum(below, 0)] >= 0
    back_above = near_ref[0, jnp.maximum(above, 0)] >= 0
    tiles = WIDE // LANES
    lanes = lambda g: slice(g * LANES, (g + 1) * LANES)
    planes, strip, wave = u_ref.shape
    dot = lambda a, b: jnp.dot(a, b, preferred_element_type=F32)

    @pl.when(place == 0)
    def _():
        column = lax.broadcasted_iota(jnp.int32, (16, LANES), 1)
        count = patch_ref.shape[0]
        stack = []
        for s in range(count):
            own = pltpu.roll(patch_ref[s, 1], PATCH, 1)
            under = pltpu.roll(patch_ref[(s - 1) % count, 0], LANES - (REG - 1) * PATCH, 1)
            over = pltpu.roll(patch_ref[(s + 1) % count, 2], (PATCH - 1) * PATCH, 1)
            patch = jnp.where(
                column < PATCH, under, jnp.where(column < (PATCH + 1) * PATCH, own, over)
            )
            stack.append(jnp.where(column < (PATCH + 2) * PATCH, patch, 0.0))
        total = None
        for piece in thirds(jnp.concatenate(stack, axis=0)):
            term = dot(piece, yz_ref[...])
            total = term if total is None else total + term
        plane_ref[...] = total.reshape(plane_ref.shape)

    coarse_ref[...] = dot(xt_ref[...], jnp.concatenate(thirds(plane_ref[place]), axis=0))
    high, low = halves(u_ref[...].reshape(planes * strip, wave))
    pair[:, :wave] = high
    pair[:, wave:] = low

    def restore(t):
        both = dot(pair[...], wave_ref[t])
        value = both[:, :LANES] + both[:, LANES:]
        grid_ref[:, :, lanes(t)] = value.reshape(planes, strip, LANES)

    lane = lax.broadcasted_iota(jnp.int32, (CELLS, LANES), 1)
    first = lane % CELLS == 0
    final = lane % CELLS == CELLS - 1
    front = lane < CELLS
    rear = lane >= LANES - CELLS
    body = slice(8, 8 + CELLS)
    behind = slice(7, 7 + CELLS)
    ahead = slice(9, 9 + CELLS)

    for g in range(tiles):
        start = coarse_ref[:CELLS, lanes(g)]
        iterate[0, g, body] = start
        for n in range(2):
            iterate[n, g, 7:8] = coarse_ref[CELLS : CELLS + 1, lanes(g)]
            iterate[n, g, 8 + CELLS : 9 + CELLS] = coarse_ref[CELLS + 1 : CELLS + 2, lanes(g)]
        if g == 0:
            rho = low_ref[0]
        elif g == tiles - 1:
            rho = high_ref[0]
        else:
            rho = mid_ref[0, :, lanes(g - 1)]
        steady[g] = coarse_ref[:CELLS, lanes(tiles + g)] - rho * (1.0 / (REF * REF))

    def turn(value, amount):
        return pltpu.roll(value, amount % LANES, 1)

    edge_low = coarse_ref[:CELLS, lanes(2 * tiles)]
    edge_high = coarse_ref[:CELLS, lanes(2 * tiles + 1)]
    held_above = jnp.where(back_below, 0.0, turn(coarse_ref[:CELLS, lanes(1)], -CELLS))
    held_below = jnp.where(back_above, 0.0, turn(coarse_ref[:CELLS, lanes(tiles - 2)], CELLS))

    def second_sides(source, g):
        value = source[g]
        down = turn(value, CELLS)
        up = turn(value, -CELLS)
        if g == 0:
            lower = edge_low
        else:
            lower = turn(source[g - 1], CELLS)
            if g == tiles - 1:
                lower = jnp.where(back_above, lower, held_below)
        if g == tiles - 1:
            upper = edge_high
        else:
            upper = turn(source[g + 1], -CELLS)
            if g == 0:
                upper = jnp.where(back_below, upper, held_above)
        return jnp.where(front, lower, down), jnp.where(rear, upper, up)

    for n in range(SWEEPS):
        if n < wave // LANES:
            restore(n)
        now, later = n % 2, (n + 1) % 2
        source = {}
        for g in range(tiles):
            for k in (g, g + 1):
                if k < tiles and k not in source:
                    source[k] = iterate[now, k, body]
            value = source[g]
            total = iterate[now, g, behind] + iterate[now, g, ahead]
            lower, upper = second_sides(source, g)
            total = total + (lower + upper)
            total = total + jnp.where(first, 0.0, turn(value, 1))
            total = total + jnp.where(final, 0.0, turn(value, -1))
            new = (total + (value + steady[g])) * (RELAXATION / 6.0)
            if g == 0:
                new = jnp.where(has_below, new, value)
            if g == tiles - 1:
                new = jnp.where(has_above, new, value)
            iterate[later, g, body] = new
    for n in range(SWEEPS, wave // LANES):
        restore(n)

    now = SWEEPS % 2
    source = {g: iterate[now, g, body] for g in range(3)}
    for g in range(1, tiles - 1):
        source[g + 1] = iterate[now, g + 1, body]
        value = source[g]
        lower, upper = second_sides(source, g)
        edge = coarse_ref[:CELLS, lanes(tiles + g)]
        slopes = (
            iterate[now, g, ahead] - iterate[now, g, behind],
            upper - lower,
            jnp.where(final, edge, turn(value, -1)) - jnp.where(first, edge, turn(value, 1)),
        )
        pot_ref[0, :, lanes(g - 1)] = jnp.where(live, value, 0.0)
        for q, slope in enumerate(slopes):
            moved = vel_ref[q, 0, :, lanes(g - 1)] - slope * (REF / 2.0)
            kick_ref[q, 0, :, lanes(g - 1)] = jnp.where(live, moved, 0.0)


def poisson(root_density, density, slot_anchor):
    count_first = lax.axis_size("px")
    count_second = lax.axis_size("py")
    devices = count_first * count_second
    rows, strip, wave = root_density.shape
    tiles = wave // LANES
    chunk = LANES // count_second
    width = -(-(2 * rows + 6) // 128) * 128
    basis = fourier_basis(wave)
    strip_table, strip_eig = strip_basis(strip)
    eig = 4.0 * np.sin(np.pi / wave * np.arange(wave)) ** 2
    mixes, angles = strip_coupling(count_second, chunk)
    cell = np.arange(strip)
    bow = 0.5 * (cell * cell - (strip - 1) * cell) - strip / 4
    lower = cell < strip // 2
    edge = strip_table[:, 0]
    vectors = np.stack(
        [
            np.where(lower, edge, 0.0),
            np.where(lower, 0.0, edge),
            strip_table.sum(1),
            strip_table @ bow,
        ]
    )[:, :, None]
    mix_high, mix_low = halves(jnp.asarray(mixes, F32))
    wave_halves = jnp.stack(halves(jnp.asarray(basis, F32)))
    high, low = halves(jnp.asarray(strip_table, F32))
    strip_wide = jnp.concatenate([high, low, high], axis=1)
    extended = np.zeros((strip + 8, strip))
    extended[:strip] = strip_table.T
    extended[strip] = -strip_table[:, 0]
    extended[-1] = -strip_table[:, -1]
    high, low = halves(jnp.asarray(extended, F32))
    unstrip_wide = jnp.concatenate([high, low, high], axis=1)
    moment = pltpu.VMEM((tiles, count_first, 2, strip, LANES), F32)
    dma = pltpu.SemaphoreType.DMA
    face = jax.ShapeDtypeStruct(density.shape[:2] + (EDGE * CELLS,), F32)
    vmem = pl.BlockSpec(memory_space=pltpu.VMEM)
    hbm = pl.BlockSpec(memory_space=pl.ANY)
    uy, arrived, low_density, high_density = pl.pallas_call(
        lambda *refs: grid_kernel((count_first, count_second), *refs),
        in_specs=[pl.BlockSpec(memory_space=pltpu.SMEM), hbm] + [vmem] * 10 + [hbm],
        out_specs=[hbm, vmem, hbm, hbm],
        out_shape=[
            jax.ShapeDtypeStruct((rows, strip, wave), F32),
            jax.ShapeDtypeStruct((count_second, 3, 16, LANES), F32),
            face,
            face,
        ],
        scratch_shapes=[
            pltpu.VMEM((rows + 2, 8, wave), F32),
            pltpu.VMEM((rows, strip, wave), F32),
            pltpu.VMEM((rows + 2, strip, wave), F32),
            pltpu.VMEM((rows * strip, 2 * wave), jnp.bfloat16),
            pltpu.VMEM((tiles, 2 * wave, 2 * LANES), jnp.bfloat16),
            pltpu.VMEM((count_second + 2, 16, LANES), F32),
            pltpu.VMEM((count_second, 16, 24, LANES), F32),
            pltpu.VMEM((count_second, 2 * wave, 2 * LANES), jnp.bfloat16),
            pltpu.VMEM((count_second, 24, 3 * strip), jnp.bfloat16),
            pltpu.VMEM((count_second, 24, LANES), F32),
            pltpu.VMEM((width, LANES), F32),
            pltpu.VMEM((tiles, LANES, width), F32),
            pltpu.VMEM((devices, chunk, width), F32),
            pltpu.VMEM((devices, chunk, width), F32),
            pltpu.VMEM((tiles, LANES, width), F32),
            moment,
            moment,
            pltpu.VMEM((2, rows, 8, LANES), F32),
            pltpu.VMEM((2, count_first, width, 2 * wave), jnp.bfloat16),
            pltpu.VMEM((4, count_second * chunk, wave), F32),
            pltpu.VMEM((6, strip, wave), F32),
            dma((BLOCKS,)),
            dma((BLOCKS,)),
            dma((tiles, count_first)),
            dma((tiles, count_first)),
            dma((tiles, count_first)),
            dma((tiles, count_first)),
            dma((tiles, count_second)),
            dma((devices,)),
            dma((devices,)),
            dma((tiles, count_second)),
            dma((2,)),
            dma((2,)),
            dma((2,)),
            dma((count_second,)),
            dma((count_second,)),
        ],
        compiler_params=pltpu.CompilerParams(
            collective_id=1, has_side_effects=True, vmem_limit_bytes=60 * 1024 * 1024
        ),
    )(
        slot_anchor,
        root_density,
        jnp.asarray(strip_eig[:, None], F32),
        jnp.asarray(eig[None, :], F32),
        jnp.asarray(eig[:, None], F32),
        jnp.asarray(vectors, F32),
        jnp.stack(halves(jnp.asarray(basis.T, F32))),
        jnp.concatenate([mix_high, mix_low, mix_high], axis=2),
        jnp.asarray(angles, F32),
        strip_wide,
        unstrip_wide,
        wave_halves,
        density,
    )
    high = wave_halves[0].reshape(wave, tiles, LANES)
    low = wave_halves[1].reshape(wave, tiles, LANES)
    top = jnp.concatenate([high, low], axis=2)
    bottom = jnp.concatenate([high, jnp.zeros_like(low)], axis=2)
    inverse = jnp.concatenate([top, bottom], axis=0).transpose(1, 0, 2)
    return uy, inverse, arrived, low_density, high_density


def local(root_density, subgrid_density, velocity, slot_anchor, slot_count, neighbour):
    per_device = subgrid_density.shape[0]
    side = EDGE * CELLS
    inner = CELLS * CELLS
    uy, inverse, patches, low_density, high_density = poisson(
        root_density, subgrid_density, slot_anchor
    )
    x_table, yz_table = patch_tables()
    smem = pl.BlockSpec(memory_space=pltpu.SMEM)
    slot_spec = lambda width: pl.BlockSpec((1, CELLS, width), lambda s: (s, 0, 0))
    vel_spec = pl.BlockSpec((3, 1, CELLS, inner), lambda s: (0, s, 0, 0))
    x_table = jnp.asarray(np.tile(x_table, (1, 3)), jnp.bfloat16)
    yz_table = jnp.asarray(yz_table, jnp.bfloat16)
    columns = yz_table.shape[1]
    planes, strip, wave = uy.shape
    planes //= per_device
    grid_spec = pl.BlockSpec((planes, strip, wave), lambda s: (s, 0, 0))
    potential, kicked, coarse_potential = pl.pallas_call(
        subgrid_kernel,
        grid=(per_device,),
        in_specs=[
            smem,
            smem,
            pl.BlockSpec(patches.shape, lambda s: (0, 0, 0, 0)),
            pl.BlockSpec(x_table.shape, lambda s: (0, 0)),
            pl.BlockSpec(yz_table.shape, lambda s: (0, 0)),
            slot_spec(inner),
            slot_spec(side),
            slot_spec(side),
            vel_spec,
            grid_spec,
            pl.BlockSpec(inverse.shape, lambda s: (0, 0, 0)),
        ],
        out_specs=[slot_spec(inner), vel_spec, grid_spec],
        out_shape=[
            jax.ShapeDtypeStruct(subgrid_density.shape, F32),
            jax.ShapeDtypeStruct(velocity.shape, F32),
            jax.ShapeDtypeStruct(uy.shape, F32),
        ],
        scratch_shapes=[
            pltpu.VMEM((per_device, 16, columns), F32),
            pltpu.VMEM((CELLS + 8, columns), F32),
            pltpu.VMEM((2, WIDE // LANES, CELLS + 16, LANES), F32),
            pltpu.VMEM((WIDE // LANES, CELLS, LANES), F32),
            pltpu.VMEM((planes * strip, 2 * wave), jnp.bfloat16),
        ],
        compiler_params=pltpu.CompilerParams(
            dimension_semantics=("arbitrary",), vmem_limit_bytes=60 * 1024 * 1024
        ),
    )(
        slot_count,
        neighbour,
        patches,
        x_table,
        yz_table,
        subgrid_density,
        low_density,
        high_density,
        velocity,
        uy,
        inverse,
    )
    return (coarse_potential, potential, kicked)


def solution(mesh):
    return jax.shard_map(
        local,
        mesh=mesh,
        in_specs=(
            P("px", "py", None),
            P(("px", "py"), None, None),
            P(None, ("px", "py"), None, None),
            P(),
            P(),
            P(),
        ),
        out_specs=(
            P("px", "py", None),
            P(("px", "py"), None, None),
            P(None, ("px", "py"), None, None),
        ),
        check_vma=False,
    )
```

```python
import jax
import jax.numpy as jnp
import numpy as np
from jax import lax
from jax.experimental import pallas as pl
from jax.experimental.pallas import tpu as pltpu
from jax.sharding import PartitionSpec as P

NR = 384
REG = 8
REF = 4
SWEEPS = 4
CELLS = REG * REF
EDGE = SWEEPS
LAYERS = CELLS + 2 * EDGE
WIDE = LAYERS * CELLS
RELAXATION = 6.0 / 7.0
LANES = 128
F32 = jnp.float32


def fourier_basis(length):
    cell = np.arange(length)
    rows = []
    for k in range(length):
        if k in (0, length // 2):
            rows.append(np.cos(2 * np.pi * (k * cell % length) / length) / np.sqrt(length))
        elif k < length // 2:
            rows.append(np.cos(2 * np.pi * (k * cell % length) / length) * np.sqrt(2 / length))
        else:
            rows.append(
                np.sin(2 * np.pi * ((length - k) * cell % length) / length) * np.sqrt(2 / length)
            )
    return np.stack(rows)


def strip_basis(cells):
    place = np.arange(cells) - (cells - 1) / 2
    mode = 2 * np.arange(cells // 2) + 1
    angle = np.pi * mode[:, None] * place[None, :] / cells
    basis = np.concatenate([np.cos(angle), np.sin(angle)]) * np.sqrt(2 / cells)
    eig = 4 * np.sin(np.pi * mode / (2 * cells)) ** 2
    return basis, np.concatenate([eig, eig])


def strip_coupling(count, rows):
    basis = fourier_basis(count)
    turn = np.zeros((count, count))
    theta = 2 * np.pi * np.arange(count) / count
    for k in range(1, (count + 1) // 2):
        turn[k, count - k] = np.sin(theta[k])
        turn[count - k, k] = -np.sin(theta[k])
    wide = lambda matrix: np.kron(matrix, np.eye(rows))
    mixes = np.stack([wide(basis), wide(turn @ basis), wide(basis.T)])
    half_sine = np.sin(theta / 2) ** 2
    factors = np.stack([half_sine, 4 * (1 - half_sine)])
    return mixes, np.repeat(factors, rows, axis=1)[:, :, None]


def axis_weights(cells, first, count):
    table = np.zeros((len(cells), count))
    for row, cell in enumerate(cells):
        mark = 2 * cell - 1 + REF
        low = mark // (2 * REF)
        frac = (mark - 2 * REF * low) / (2 * REF)
        table[row, low - first] += 1 - frac
        if frac:
            table[row, low + 1 - first] += frac
    return table


PATCH = REG + 2
PATCH_X = REG + 2
PATCH_Y = REG + 4
PATCH_Z = REG + 2


def patch_tables():
    inner = np.arange(1, CELLS + 1)
    x_side = axis_weights(np.concatenate([inner, [0, CELLS + 1]]), 0, PATCH_X)
    x_table = np.zeros((CELLS + 8, 16))
    x_table[: CELLS + 2, :PATCH_X] = x_side
    y_cells = np.arange(1 - EDGE, CELLS + EDGE + 1)
    y_side = axis_weights(y_cells, -1, PATCH_Y)
    y_out = axis_weights(np.array([-EDGE, CELLS + EDGE + 1]), -1, PATCH_Y)
    z_side = axis_weights(np.arange(CELLS + 2), 0, PATCH_Z)
    z_edge = np.zeros((CELLS, PATCH_Z))
    z_edge[0] = z_side[0]
    z_edge[-1] = z_side[-1]
    y_edge = np.zeros((LAYERS, PATCH_Y))
    y_edge[0] = y_out[0]
    y_edge[-1] = y_out[1]

    def both(ys, zs):
        return np.einsum("jb,kc->bcjk", ys, zs).reshape(PATCH_Y * PATCH_Z, WIDE)

    ends = both(y_edge, z_side[1:-1])
    table = np.zeros((LANES, 2 * WIDE + 2 * LANES))
    table[: PATCH_Y * PATCH_Z] = np.concatenate(
        [
            both(y_side, z_side[1:-1]),
            both(y_side, z_edge),
            ends[:, :LANES],
            ends[:, -LANES:],
        ],
        axis=1,
    )
    return x_table.astype(np.float32), table.astype(np.float32)


def decay(delta):
    return 1.0 / (1.0 + 0.5 * delta + jnp.sqrt(delta + 0.25 * delta * delta))


def power(value, exponent):
    result = None
    while exponent:
        if exponent & 1:
            result = value if result is None else result * value
        exponent >>= 1
        if exponent:
            value = value * value
    return result


def halves(value):
    high = value.astype(jnp.bfloat16)
    return high, (value - high.astype(F32)).astype(jnp.bfloat16)


def thirds(value):
    high = value.astype(jnp.bfloat16)
    rest = value - high.astype(F32)
    middle = rest.astype(jnp.bfloat16)
    return high, middle, (rest - middle.astype(F32)).astype(jnp.bfloat16)


def owner_shift(place_second):
    return place_second // 2 * 2 + 2


BLOCKS = 6


def grid_kernel(
    sizes,
    anchor_ref,
    root_hbm,
    eig_b_ref,
    eig_ref,
    own_ref,
    vec_ref,
    basis_ref,
    mix_ref,
    angle_ref,
    strip_ref,
    unstrip_ref,
    wave_ref,
    density_ref,
    out_hbm,
    arrived_ref,
    low_ref,
    high_ref,
    edge_ref,
    f_ref,
    out_ref,
    pair,
    forward,
    patches,
    cut,
    windows,
    strip_mix,
    halo_rows,
    lines,
    sent,
    got,
    answer,
    back,
    mom_one,
    mom_two,
    part,
    table,
    factor,
    weight,
    in_sem,
    out_sem,
    send_one,
    recv_one,
    send_two,
    recv_two,
    send_line,
    recv_line,
    send_back,
    recv_back,
    self_sem,
    send_face,
    recv_face,
    send_patch,
    recv_patch,
):
    count_first, count_second = sizes
    devices = count_first * count_second
    rows, strip, wave = f_ref.shape
    tiles = wave // LANES
    groups = strip // 8
    half = strip // 2
    middle = rows // 2
    fold = 4
    chunk = got.shape[1]
    width = lines.shape[0]
    mesh = pl.DeviceIdType.MESH
    place_first = lax.axis_index("px")
    place_second = lax.axis_index("py")
    me = place_first * count_second + place_second
    own_tile = lax.rem(
        place_first + 2 * count_second * count_first - owner_shift(place_second), count_first
    )
    is_owner = own_tile < tiles
    barrier = pltpu.get_barrier_semaphore()

    lane_of = lambda t: slice(t * LANES, (t + 1) * LANES)

    block = rows // BLOCKS

    def load(n):
        piece = pl.ds(n * block, block)
        return pltpu.make_async_copy(root_hbm.at[piece], f_ref.at[piece], in_sem.at[n])

    def store(n):
        return pltpu.make_async_copy(
            out_ref.at[pl.ds(n * block + 1, block)],
            out_hbm.at[pl.ds(n * block, block)],
            out_sem.at[n],
        )

    for n in range(BLOCKS):
        load(n).start()
    def greet(step, carry):
        other = lax.rem(me + step, devices)
        pl.semaphore_signal(
            barrier,
            inc=1,
            device_id=(other // count_second, lax.rem(other, count_second)),
            device_id_type=mesh,
        )
        return carry

    lax.fori_loop(1, devices, greet, 0)
    dot = lambda a, b: jnp.dot(a, b, preferred_element_type=F32)
    forward[...] = jnp.zeros_like(forward)
    for t in range(tiles):
        forward[t, :wave, :LANES] = basis_ref[0, :, lane_of(t)]
        forward[t, wave:, :LANES] = basis_ref[0, :, lane_of(t)]
        forward[t, :wave, LANES:] = basis_ref[1, :, lane_of(t)]

    window = [slice(8 * g, 8 * g + 8) for g in range(groups)]
    even_groups = [g for g in range(groups) if 8 * g < half]
    odd_groups = [g for g in range(groups) if 8 * g + 8 > half]
    zeros = tuple(jnp.zeros((8, LANES), F32) for _ in range(groups))

    r_all = decay(eig_b_ref[...] + eig_ref[...])
    scale_all = -r_all / ((1.0 - r_all) * (1.0 + r_all))
    ratio_all = power(r_all, rows)
    weight[0] = r_all
    weight[1] = scale_all
    weight[2] = 2.0 * vec_ref[0] * scale_all
    weight[3] = -2.0 * vec_ref[1] * scale_all
    weight[4] = ratio_all
    weight[5] = 1.0 / (1.0 - power(ratio_all, count_first))

    def weights(which, t):
        return tuple(weight[which, window[g], lane_of(t)] for g in range(groups))

    def row_of(ref, i, t):
        return tuple(ref[i, window[g], lane_of(t)] for g in range(groups))

    def step_on(r, state, f):
        return tuple(r[g] * state[g] + f[g] for g in range(groups))

    def both_ways(start, stop, body, carry):
        def folded(n, carry):
            for k in range(fold):
                i = start + n * fold + k
                carry = body(i, rows - 1 - i, carry)
            return carry

        return lax.fori_loop(0, (stop - start) // fold, folded, carry)

    def store_moments(buffer, t, up, down):
        for g in range(groups):
            buffer[t, 0, 0, window[g], :] = up[g]
            buffer[t, 0, 1, window[g], :] = down[g]

    def shares(buffer, send, recv, t):
        return [
            pltpu.make_async_remote_copy(
                src_ref=buffer.at[t, 0],
                dst_ref=buffer.at[t, d],
                send_sem=send.at[t, d],
                recv_sem=recv.at[t, d],
                device_id=(lax.rem(place_first + d, count_first), place_second),
                device_id_type=mesh,
            )
            for d in range(1, count_first)
        ]

    def carries(buffer, t):
        ratio, norm = weights(4, t), weights(5, t)
        up, down = [], []
        for g in range(groups):
            total = buffer[t, 0, 0, window[g], :]
            for d in range(count_first - 1, 0, -1):
                total = ratio[g] * total + buffer[t, d, 0, window[g], :]
            up.append(total * norm[g])
            total = buffer[t, 0, 1, window[g], :]
            for d in range(1, count_first):
                total = ratio[g] * total + buffer[t, d, 1, window[g], :]
            down.append(total * norm[g])
        return tuple(up), tuple(down)

    face = low_ref.shape[2]
    inner = density_ref.shape[2]
    faces = [
        pltpu.make_async_remote_copy(
            src_ref=density_ref.at[:, :, pl.ds(start, face)],
            dst_ref=target,
            send_sem=send_face.at[n],
            recv_sem=recv_face.at[n],
            device_id=(place_first, lax.rem(place_second + step, count_second)),
            device_id_type=mesh,
        )
        for n, (start, target, step) in enumerate(
            ((inner - face, low_ref, 1), (0, high_ref, count_second - 1))
        )
    ]

    tall = strip + 8
    tall_row = lax.broadcasted_iota(jnp.int32, (24, tall), 0)
    tall_column = lax.broadcasted_iota(jnp.int32, (24, tall), 1)
    cell = lax.broadcasted_iota(jnp.int32, (wave, LANES), 0)
    spot = lax.broadcasted_iota(jnp.int32, (wave, LANES), 1)
    lane = lax.broadcasted_iota(jnp.int32, (16, LANES), 1)
    cut[...] = jnp.zeros_like(cut)


    def corner(t):
        slot = (place_first * count_second + t) * count_second + lax.rem(
            place_second - t + count_second, count_second
        )
        x = jnp.clip(anchor_ref[0, slot] - place_first * rows, 0, rows - REG)
        return x, slot

    def prepare(t, carry):
        _, slot = corner(t)
        y = jnp.clip(anchor_ref[1, slot] - place_second * strip, 0, strip - REG) // 8
        origin = jnp.clip(anchor_ref[2, slot], 0, wave - REG) - 1 + spot
        origin = jnp.where(origin < 0, origin + wave, origin)
        origin = jnp.where(origin >= wave, origin - wave, origin)
        select = jnp.where(cell == origin, 1.0, 0.0).astype(jnp.bfloat16)
        wave_high = dot(wave_ref[0], select).astype(jnp.bfloat16)
        windows[t, :wave, :LANES] = wave_high
        windows[t, wave:, :LANES] = wave_high
        windows[t, :wave, LANES:] = dot(wave_ref[1], select).astype(jnp.bfloat16)
        windows[t, wave:, LANES:] = jnp.zeros((wave, LANES), jnp.bfloat16)
        wanted = tall_row + 8 * y - 8
        wanted = jnp.where(wanted < 0, wanted + tall, wanted)
        pick = jnp.where(tall_column == wanted, 1.0, 0.0).astype(jnp.bfloat16)
        strip_mix[t] = dot(pick, unstrip_ref[...]).astype(jnp.bfloat16)
        halo_rows[t] = jnp.broadcast_to(
            jnp.where(wanted[:, :1] >= strip, 1.0, 0.0), halo_rows.shape[1:]
        )
        return carry

    @pl.when(is_owner)
    def _():
        table[...] = jnp.zeros_like(table)
        for i in range(count_first):
            for n in range(2):
                block = basis_ref[n, i * rows : (i + 1) * rows, :]
                table[n, i, :rows, :wave] = block
                table[n, i, rows : 2 * rows, wave:] = block
                for place, row in enumerate((rows * (i + 1) % wave, (rows * i - 1) % wave)):
                    line = basis_ref[n, row : row + 1, :]
                    table[n, i, 2 * rows + 2 + place : 2 * rows + 3 + place, :wave] = line
                    table[n, i, 2 * rows + 4 + place : 2 * rows + 5 + place, wave:] = line
        start = own_tile * LANES + place_second * chunk
        own_eig = jnp.concatenate([own_ref[pl.ds(start, chunk), :]] * count_second, axis=0)
        lam = own_eig + eig_ref[...]
        sinh = jnp.sqrt(lam + 0.25 * lam * lam)
        flat = lam <= 0.0
        far = power(decay(lam), strip)
        tanh = (1.0 - far) / (1.0 + far)
        green = jnp.where(flat, strip / 4.0, tanh / jnp.where(flat, 1.0, 2.0 * sinh))
        square = tanh * tanh
        half_sine = angle_ref[0]
        det = half_sine * (1.0 - square) + square
        zero = flat & (half_sine <= 0.0)
        inverse = jnp.where(zero, 0.0, 1.0 / jnp.where(zero, 1.0, det))
        gain = angle_ref[1] * green * inverse
        factor[0] = gain * (2.0 + 0.5 * lam)
        factor[1] = jnp.where(zero, 2.0 / strip, gain * (0.5 * lam))
        factor[2] = inverse
        factor[3] = jnp.where(zero, 1.0, 0.0)

    def inside(condition, action):
        @pl.when(condition)
        def _():
            action()

    first = []
    whole = []

    def open_tile(t):
        r = weights(0, t)
        span = (2 if t == 0 else 3) * block

        def transform(n, carry):
            piece = pl.ds(n * span, span)
            spread = pl.ds(pl.multiple_of(n * span * strip, 8), span * strip)
            if t == 0:
                for m in range(span // block):
                    load(n * (span // block) + m).wait()
                high, low = halves(f_ref[piece].reshape(span * strip, wave))
                pair[spread, :wave] = high
                pair[spread, wave:] = low
            both = dot(pair[spread], forward[t])
            value = both[:, :LANES] + both[:, LANES:]
            for m in range(0, span, 2):
                sides = [value[(m + q) * strip : (m + q + 1) * strip] for q in range(2)]
                high, low = halves(jnp.concatenate(sides, axis=1))
                stack = jnp.concatenate([high, high, low], axis=0)
                result = dot(strip_ref[...], stack)
                for q in range(2):
                    f_ref[n * span + m + q, :, lane_of(t)] = result[:, lane_of(q)]
            return carry

        lax.fori_loop(0, rows // span, transform, 0)

        def moments(i, j, carry):
            up, down, total = carry
            f = row_of(f_ref, i, t)
            up = step_on(r, up, f)
            down = step_on(r, down, row_of(f_ref, j, t))
            if t == 0:
                total = tuple(total[g] + f[g] for g in range(groups))
            return up, down, total

        up, down, total = both_ways(0, rows, moments, (zeros, zeros, zeros if t == 0 else ()))
        store_moments(mom_one, t, up, down)
        if t == 0:
            whole.append(jnp.concatenate(total, axis=0))
            pl.semaphore_wait(barrier, devices - 1)
        first.append(shares(mom_one, send_one, recv_one, t))
        for copy in first[t]:
            copy.start()
        if t == 0:
            inside(place_second < count_second - 1, faces[0].start)
            inside(place_second > 0, faces[1].start)

    def line_copy(t, k):
        return pltpu.make_async_remote_copy(
            src_ref=sent.at[t, pl.ds(k * chunk, chunk)],
            dst_ref=got.at[me],
            send_sem=send_line.at[t, k],
            recv_sem=recv_line.at[me],
            device_id=(lax.rem(owner_shift(k) + t, count_first), k),
            device_id_type=mesh,
        )

    def line_from(d):
        return pltpu.make_async_remote_copy(
            src_ref=sent.at[0, pl.ds(0, chunk)],
            dst_ref=got.at[d],
            send_sem=self_sem.at[1],
            recv_sem=recv_line.at[d],
            device_id=(d // count_second, lax.rem(d, count_second)),
            device_id_type=mesh,
        )

    def back_copy(d):
        return pltpu.make_async_remote_copy(
            src_ref=answer.at[d],
            dst_ref=back.at[own_tile, pl.ds(place_second * chunk, chunk)],
            send_sem=send_back.at[d],
            recv_sem=recv_back.at[own_tile, place_second],
            device_id=(d // count_second, lax.rem(d, count_second)),
            device_id_type=mesh,
        )

    def back_from(t, k):
        return pltpu.make_async_remote_copy(
            src_ref=answer.at[0],
            dst_ref=back.at[t, pl.ds(k * chunk, chunk)],
            send_sem=self_sem.at[1],
            recv_sem=recv_back.at[t, k],
            device_id=(lax.rem(owner_shift(k) + t, count_first), k),
            device_id_type=mesh,
        )

    def over_devices(action, part=None):
        def body(d, carry):
            @pl.when(d != me)
            def _():
                action(d)

            return carry

        start, stop = 0, devices
        if part is not None:
            start, stop = part * count_second, (part + 1) * count_second
        lax.fori_loop(start, stop, body, 0)

    def over_owners(t, action):
        def body(k, carry):
            @pl.when((k != place_second) | (own_tile != t))
            def _():
                action(t, k)

            return carry

        lax.fori_loop(0, count_second, body, 0)

    def weighed(values, members, state):
        total = None
        for g in members:
            term = values[g] * state[g]
            total = term if total is None else total + term
        return total

    def close_tile(t):
        r, even, odd = weights(0, t), weights(2, t), weights(3, t)
        for copy in first[t]:
            copy.wait()
        state = carries(mom_one, t)

        def lines_of(add):
            def body(i, j, carry):
                up, down = carry
                up = step_on(r, up, row_of(f_ref, i, t))
                down = tuple(r[g] * down[g] for g in range(groups))
                for n, (values, members) in enumerate(((even, even_groups), (odd, odd_groups))):
                    one = weighed(values, members, up)
                    two = weighed(values, members, down)
                    part[n, i] = part[n, i] + one if add else one
                    part[n, j] = part[n, j] + two if add else two
                f = row_of(f_ref, j, t)
                return up, tuple(down[g] + f[g] for g in range(groups))

            return body

        state = both_ways(0, middle, lines_of(False), state)
        both_ways(middle, rows, lines_of(True), state)
        lines[:rows, :] = jnp.sum(part[0], axis=1)
        lines[rows : 2 * rows, :] = jnp.sum(part[1], axis=1)
        lines[2 * rows :, :] = jnp.zeros((width - 2 * rows, LANES), F32)
        if t == 0:
            for n in range(2):
                lines[2 * rows + n : 2 * rows + n + 1, :] = jnp.sum(
                    vec_ref[2 + n] * whole[0], axis=0, keepdims=True
                )
        sent[t] = lines[...].T
        over_owners(t, lambda t, k: line_copy(t, k).start())

    for t in range(tiles):
        open_tile(t)
        if t > 0 and t < tiles - 1:
            close_tile(t - 1)
    for t in range(max(tiles - 2, 0), tiles):
        close_tile(t)
    @pl.when(is_owner)
    def _():
        own = pltpu.make_async_copy(
            sent.at[own_tile, pl.ds(place_second * chunk, chunk)], got.at[me], self_sem.at[0]
        )
        own.start()
        modes = None
        own.wait()
        for i in range(count_first):
            over_devices(lambda d: line_from(d).wait_recv(), i)
            piece = got[i * count_second : (i + 1) * count_second]
            high, low = halves(piece.reshape(count_second * chunk, width))
            term = dot(high, table[0, i]) + dot(high, table[1, i]) + dot(low, table[0, i])
            modes = term if modes is None else modes + term

        def mixed(which, value):
            high, low = halves(value)
            stack = jnp.concatenate([high, high, low], axis=0)
            return dot(mix_ref[which], stack)

        straight = mixed(0, modes)
        turned = mixed(1, modes)
        s, t = straight[:, :wave], straight[:, wave:]
        s_turned, t_turned = turned[:, :wave], turned[:, wave:]
        sums = jnp.sum(got[...], axis=0)
        lane = lax.broadcasted_iota(jnp.int32, sums.shape, 1)
        sigma = jnp.sum(jnp.where(lane == 2 * rows, sums, 0.0), axis=1, keepdims=True)
        lever = jnp.sum(jnp.where(lane == 2 * rows + 1, sums, 0.0), axis=1, keepdims=True)
        k = np.arange(strip)
        bow = 0.5 * (k * k - (strip - 1) * k) - strip / 4
        first_eig = own_ref[pl.ds(own_tile * LANES + place_second * chunk, chunk), :]
        mean = jnp.where(first_eig <= 0.0, sigma, 0.0) * (1.0 / (wave * wave))
        gauge = lever - mean * float(wave * count_second * bow.sum())
        gauge = gauge * float(1.0 / (bow[0] * np.sqrt(wave * count_second)))
        tall = lambda value: jnp.concatenate([value] * count_second, axis=0)
        mean, gauge = tall(mean), tall(gauge)
        new_s = factor[0] * s - t_turned * factor[2] + factor[3] * gauge
        new_t = factor[1] * t - s_turned * factor[2]
        solved = mixed(2, jnp.concatenate([new_s, new_t], axis=1))
        high, low = halves(solved)
        wide = lax.broadcasted_iota(jnp.int32, (count_second * chunk, width), 1)
        across = lambda a, b: lax.dot_general(
            a, b, (((1,), (1,)), ((), ())), preferred_element_type=F32
        )
        for i in range(count_first):
            piece = across(high, table[0, i]) + across(high, table[1, i]) + across(low, table[0, i])
            piece = jnp.where(wide == 2 * rows, mean, piece)
            answer[i * count_second : (i + 1) * count_second] = piece.reshape(
                count_second, chunk, width
            )
            over_devices(lambda d: back_copy(d).start(), i)
        kept = pltpu.make_async_copy(
            answer.at[me], back.at[own_tile, pl.ds(place_second * chunk, chunk)], self_sem.at[0]
        )
        kept.start()
        kept.wait()

    lax.fori_loop(0, count_second, prepare, 0)
    second = []
    edge_ref[...] = jnp.zeros_like(edge_ref)
    for t in range(tiles):
        over_owners(t, lambda t, k: back_from(t, k).wait_recv())
        lines[...] = back[t].T
        after = 2 * rows + 2
        for place, sign in ((0, -1.0), (7, 1.0)):
            mixed_lines = 0.5 * (lines[:rows, :] + sign * lines[rows : 2 * rows, :])
            edge_ref[1 : rows + 1, place, lane_of(t)] = mixed_lines
            ends = 0.5 * (lines[after : after + 2, :] + sign * lines[after + 2 : after + 4, :])
            edge_ref[rows + 1, place : place + 1, lane_of(t)] = ends[0:1]
            edge_ref[0, place : place + 1, lane_of(t)] = ends[1:2]
        r = weights(0, t)
        if t == 0:
            mean_term = vec_ref[2] * lines[2 * rows : 2 * rows + 1, :]
            mean_term = tuple(mean_term[window[g]] for g in range(groups))
        wide_vec = [
            jnp.broadcast_to(vec_ref[n], (strip, LANES)) for n in range(2)
        ]

        def fresh(i):
            f = list(row_of(f_ref, i, t))
            line_s = lines[pl.ds(i, 1), :]
            line_t = lines[pl.ds(rows + i, 1), :]
            for g in range(groups):
                if t == 0:
                    f[g] = f[g] - mean_term[g]
                if g in even_groups:
                    f[g] = f[g] - wide_vec[0][window[g]] * line_s
                if g in odd_groups:
                    f[g] = f[g] - wide_vec[1][window[g]] * line_t
                f_ref[i, window[g], lane_of(t)] = f[g]
            return tuple(f)

        def renewed(make):
            def body(i, j, carry):
                up, down = carry
                one = fresh(i) if make else row_of(f_ref, i, t)
                two = fresh(j) if make else row_of(f_ref, j, t)
                return step_on(r, up, one), step_on(r, down, two)

            return body

        state = both_ways(0, middle, renewed(True), (zeros, zeros))
        up, down = both_ways(middle, rows, renewed(False), state)
        store_moments(mom_two, t, up, down)
        second.append(shares(mom_two, send_two, recv_two, t))
        for copy in second[t]:
            copy.start()

    for t in range(tiles):
        r, scale = weights(0, t), weights(1, t)
        for copy in second[t]:
            copy.wait()
        carry_up, carry_down = carries(mom_two, t)

        def put(i, value, add):
            for g in range(groups):
                if add:
                    out_ref[i + 1, window[g], lane_of(t)] = (
                        out_ref[i + 1, window[g], lane_of(t)] + value[g]
                    ) * scale[g]
                else:
                    out_ref[i + 1, window[g], lane_of(t)] = value[g]

        def last(add):
            def body(i, j, carry):
                up, down = carry
                up = step_on(r, up, row_of(f_ref, i, t))
                down = tuple(r[g] * down[g] for g in range(groups))
                put(i, up, add)
                put(j, down, add)
                f = row_of(f_ref, j, t)
                return up, tuple(down[g] + f[g] for g in range(groups))

            return body

        state = both_ways(0, middle, last(False), (carry_up, carry_down))
        up, down = both_ways(middle, rows, last(True), state)
        for g in range(groups):
            out_ref[rows + 1, window[g], lane_of(t)] = (r[g] * up[g] + carry_down[g]) * scale[g]
            out_ref[0, window[g], lane_of(t)] = (carry_up[g] + r[g] * down[g]) * scale[g]

    def patch(t):
        x, _ = corner(t)
        mix, halo_row = strip_mix[t], halo_rows[t]
        values = []
        for i in range(PATCH):
            high, low = halves(out_ref[x + i])
            value = dot(mix, jnp.concatenate([high, high, low], axis=0))
            halo = jnp.concatenate([edge_ref[x + i]] * 3, axis=0)
            values.append(value + halo * halo_row[:, :1])
        high, low = halves(jnp.concatenate(values, axis=0))
        both = dot(jnp.concatenate([high, low], axis=1), windows[t])
        both = both[:, :LANES] + both[:, LANES:]
        for i in range(PATCH):
            cut[t, i] = both[24 * i : 24 * i + 24]
        total = jnp.zeros(lane.shape, F32)
        for b in range(PATCH):
            line = jnp.where(lane < PATCH, cut[t, :, 7 + b, :], 0.0)
            total = total + (pltpu.roll(line, PATCH * b, 1) if b else line)
        return total

    def patch_group(n, carry):
        totals = [patch(4 * n + q) for q in range(4)]
        for q in range(4):
            patches[4 * n + q + 1] = totals[q]
        return carry

    lax.fori_loop(0, count_second // 4, patch_group, 0)
    patches[0] = patches[count_second]
    patches[count_second + 1] = patches[1]
    own = pltpu.make_async_copy(
        patches.at[pl.ds(place_second, 3)], arrived_ref.at[0], self_sem.at[0]
    )
    own.start()
    moves = []
    for d in range(1, count_second):
        target = lax.rem(place_second + d, count_second)
        moves.append(
            pltpu.make_async_remote_copy(
                src_ref=patches.at[pl.ds(target, 3)],
                dst_ref=arrived_ref.at[count_second - d],
                send_sem=send_patch.at[d],
                recv_sem=recv_patch.at[d],
                device_id=(place_first, target),
                device_id_type=mesh,
            )
        )
    for copy in moves:
        copy.start()
    unstrip = unstrip_ref[:strip, :]

    def restore(n, carry):
        for m in range(block):
            row = n * block + m + 1
            high, low = halves(out_ref[row])
            out_ref[row] = dot(unstrip, jnp.concatenate([high, high, low], axis=0))
        store(n).start()
        return carry

    lax.fori_loop(0, BLOCKS, restore, 0)
    for t in range(tiles):
        over_owners(t, lambda t, k: line_copy(t, k).wait_send())

    @pl.when(is_owner)
    def _():
        over_devices(lambda d: back_copy(d).wait_send())

    inside(place_second < count_second - 1, faces[0].wait_send)
    inside(place_second > 0, faces[0].wait_recv)
    inside(place_second > 0, faces[1].wait_send)
    inside(place_second < count_second - 1, faces[1].wait_recv)
    for copy in moves + [own]:
        copy.wait()
    for n in range(BLOCKS):
        store(n).wait()


def subgrid_kernel(
    count_ref,
    near_ref,
    patch_ref,
    xt_ref,
    yz_ref,
    mid_ref,
    low_ref,
    high_ref,
    vel_ref,
    u_ref,
    wave_ref,
    pot_ref,
    kick_ref,
    grid_ref,
    plane_ref,
    coarse_ref,
    iterate,
    steady,
    pair,
):
    device = lax.axis_index("px") * lax.axis_size("py") + lax.axis_index("py")
    place = pl.program_id(0)
    slot = device * pl.num_programs(0) + place
    below = near_ref[0, slot]
    above = near_ref[1, slot]
    live = place < count_ref[device]
    has_below = below >= 0
    has_above = above >= 0
    back_below = near_ref[1, jnp.maximum(below, 0)] >= 0
    back_above = near_ref[0, jnp.maximum(above, 0)] >= 0
    tiles = WIDE // LANES
    lanes = lambda g: slice(g * LANES, (g + 1) * LANES)
    planes, strip, wave = u_ref.shape
    dot = lambda a, b: jnp.dot(a, b, preferred_element_type=F32)

    @pl.when(place == 0)
    def _():
        column = lax.broadcasted_iota(jnp.int32, (16, LANES), 1)
        count = patch_ref.shape[0]
        stack = []
        for s in range(count):
            own = pltpu.roll(patch_ref[s, 1], PATCH, 1)
            under = pltpu.roll(patch_ref[(s - 1) % count, 0], LANES - (REG - 1) * PATCH, 1)
            over = pltpu.roll(patch_ref[(s + 1) % count, 2], (PATCH - 1) * PATCH, 1)
            patch = jnp.where(
                column < PATCH, under, jnp.where(column < (PATCH + 1) * PATCH, own, over)
            )
            stack.append(jnp.where(column < (PATCH + 2) * PATCH, patch, 0.0))
        total = None
        for piece in thirds(jnp.concatenate(stack, axis=0)):
            term = dot(piece, yz_ref[...])
            total = term if total is None else total + term
        plane_ref[...] = total.reshape(plane_ref.shape)

    coarse_ref[...] = dot(xt_ref[...], jnp.concatenate(thirds(plane_ref[place]), axis=0))
    high, low = halves(u_ref[...].reshape(planes * strip, wave))
    pair[:, :wave] = high
    pair[:, wave:] = low

    def restore(t):
        both = dot(pair[...], wave_ref[t])
        value = both[:, :LANES] + both[:, LANES:]
        grid_ref[:, :, lanes(t)] = value.reshape(planes, strip, LANES)

    lane = lax.broadcasted_iota(jnp.int32, (CELLS, LANES), 1)
    first = lane % CELLS == 0
    final = lane % CELLS == CELLS - 1
    front = lane < CELLS
    rear = lane >= LANES - CELLS
    body = slice(8, 8 + CELLS)
    behind = slice(7, 7 + CELLS)
    ahead = slice(9, 9 + CELLS)

    for g in range(tiles):
        start = coarse_ref[:CELLS, lanes(g)]
        iterate[0, g, body] = start
        for n in range(2):
            iterate[n, g, 7:8] = coarse_ref[CELLS : CELLS + 1, lanes(g)]
            iterate[n, g, 8 + CELLS : 9 + CELLS] = coarse_ref[CELLS + 1 : CELLS + 2, lanes(g)]
        if g == 0:
            rho = low_ref[0]
        elif g == tiles - 1:
            rho = high_ref[0]
        else:
            rho = mid_ref[0, :, lanes(g - 1)]
        steady[g] = coarse_ref[:CELLS, lanes(tiles + g)] - rho * (1.0 / (REF * REF))

    def turn(value, amount):
        return pltpu.roll(value, amount % LANES, 1)

    edge_low = coarse_ref[:CELLS, lanes(2 * tiles)]
    edge_high = coarse_ref[:CELLS, lanes(2 * tiles + 1)]
    held_above = jnp.where(back_below, 0.0, turn(coarse_ref[:CELLS, lanes(1)], -CELLS))
    held_below = jnp.where(back_above, 0.0, turn(coarse_ref[:CELLS, lanes(tiles - 2)], CELLS))

    def second_sides(source, g):
        value = source[g]
        down = turn(value, CELLS)
        up = turn(value, -CELLS)
        if g == 0:
            lower = edge_low
        else:
            lower = turn(source[g - 1], CELLS)
            if g == tiles - 1:
                lower = jnp.where(back_above, lower, held_below)
        if g == tiles - 1:
            upper = edge_high
        else:
            upper = turn(source[g + 1], -CELLS)
            if g == 0:
                upper = jnp.where(back_below, upper, held_above)
        return jnp.where(front, lower, down), jnp.where(rear, upper, up)

    for n in range(SWEEPS):
        if n < wave // LANES:
            restore(n)
        now, later = n % 2, (n + 1) % 2
        source = {}
        for g in range(tiles):
            for k in (g, g + 1):
                if k < tiles and k not in source:
                    source[k] = iterate[now, k, body]
            value = source[g]
            total = iterate[now, g, behind] + iterate[now, g, ahead]
            lower, upper = second_sides(source, g)
            total = total + (lower + upper)
            total = total + jnp.where(first, 0.0, turn(value, 1))
            total = total + jnp.where(final, 0.0, turn(value, -1))
            new = (total + (value + steady[g])) * (RELAXATION / 6.0)
            if g == 0:
                new = jnp.where(has_below, new, value)
            if g == tiles - 1:
                new = jnp.where(has_above, new, value)
            iterate[later, g, body] = new
    for n in range(SWEEPS, wave // LANES):
        restore(n)

    now = SWEEPS % 2
    source = {g: iterate[now, g, body] for g in range(3)}
    for g in range(1, tiles - 1):
        source[g + 1] = iterate[now, g + 1, body]
        value = source[g]
        lower, upper = second_sides(source, g)
        edge = coarse_ref[:CELLS, lanes(tiles + g)]
        slopes = (
            iterate[now, g, ahead] - iterate[now, g, behind],
            upper - lower,
            jnp.where(final, edge, turn(value, -1)) - jnp.where(first, edge, turn(value, 1)),
        )
        pot_ref[0, :, lanes(g - 1)] = jnp.where(live, value, 0.0)
        for q, slope in enumerate(slopes):
            moved = vel_ref[q, 0, :, lanes(g - 1)] - slope * (REF / 2.0)
            kick_ref[q, 0, :, lanes(g - 1)] = jnp.where(live, moved, 0.0)


def poisson(root_density, density, slot_anchor):
    count_first = lax.axis_size("px")
    count_second = lax.axis_size("py")
    devices = count_first * count_second
    rows, strip, wave = root_density.shape
    tiles = wave // LANES
    chunk = LANES // count_second
    width = -(-(2 * rows + 6) // 128) * 128
    basis = fourier_basis(wave)
    strip_table, strip_eig = strip_basis(strip)
    eig = 4.0 * np.sin(np.pi / wave * np.arange(wave)) ** 2
    mixes, angles = strip_coupling(count_second, chunk)
    cell = np.arange(strip)
    bow = 0.5 * (cell * cell - (strip - 1) * cell) - strip / 4
    lower = cell < strip // 2
    edge = strip_table[:, 0]
    vectors = np.stack(
        [
            np.where(lower, edge, 0.0),
            np.where(lower, 0.0, edge),
            strip_table.sum(1),
            strip_table @ bow,
        ]
    )[:, :, None]
    mix_high, mix_low = halves(jnp.asarray(mixes, F32))
    wave_halves = jnp.stack(halves(jnp.asarray(basis, F32)))
    high, low = halves(jnp.asarray(strip_table, F32))
    strip_wide = jnp.concatenate([high, low, high], axis=1)
    extended = np.zeros((strip + 8, strip))
    extended[:strip] = strip_table.T
    extended[strip] = -strip_table[:, 0]
    extended[-1] = -strip_table[:, -1]
    high, low = halves(jnp.asarray(extended, F32))
    unstrip_wide = jnp.concatenate([high, low, high], axis=1)
    moment = pltpu.VMEM((tiles, count_first, 2, strip, LANES), F32)
    dma = pltpu.SemaphoreType.DMA
    face = jax.ShapeDtypeStruct(density.shape[:2] + (EDGE * CELLS,), F32)
    vmem = pl.BlockSpec(memory_space=pltpu.VMEM)
    hbm = pl.BlockSpec(memory_space=pl.ANY)
    uy, arrived, low_density, high_density = pl.pallas_call(
        lambda *refs: grid_kernel((count_first, count_second), *refs),
        in_specs=[pl.BlockSpec(memory_space=pltpu.SMEM), hbm] + [vmem] * 10 + [hbm],
        out_specs=[hbm, vmem, hbm, hbm],
        out_shape=[
            jax.ShapeDtypeStruct((rows, strip, wave), F32),
            jax.ShapeDtypeStruct((count_second, 3, 16, LANES), F32),
            face,
            face,
        ],
        scratch_shapes=[
            pltpu.VMEM((rows + 2, 8, wave), F32),
            pltpu.VMEM((rows, strip, wave), F32),
            pltpu.VMEM((rows + 2, strip, wave), F32),
            pltpu.VMEM((rows * strip, 2 * wave), jnp.bfloat16),
            pltpu.VMEM((tiles, 2 * wave, 2 * LANES), jnp.bfloat16),
            pltpu.VMEM((count_second + 2, 16, LANES), F32),
            pltpu.VMEM((count_second, 16, 24, LANES), F32),
            pltpu.VMEM((count_second, 2 * wave, 2 * LANES), jnp.bfloat16),
            pltpu.VMEM((count_second, 24, 3 * strip), jnp.bfloat16),
            pltpu.VMEM((count_second, 24, LANES), F32),
            pltpu.VMEM((width, LANES), F32),
            pltpu.VMEM((tiles, LANES, width), F32),
            pltpu.VMEM((devices, chunk, width), F32),
            pltpu.VMEM((devices, chunk, width), F32),
            pltpu.VMEM((tiles, LANES, width), F32),
            moment,
            moment,
            pltpu.VMEM((2, rows, 8, LANES), F32),
            pltpu.VMEM((2, count_first, width, 2 * wave), jnp.bfloat16),
            pltpu.VMEM((4, count_second * chunk, wave), F32),
            pltpu.VMEM((6, strip, wave), F32),
            dma((BLOCKS,)),
            dma((BLOCKS,)),
            dma((tiles, count_first)),
            dma((tiles, count_first)),
            dma((tiles, count_first)),
            dma((tiles, count_first)),
            dma((tiles, count_second)),
            dma((devices,)),
            dma((devices,)),
            dma((tiles, count_second)),
            dma((2,)),
            dma((2,)),
            dma((2,)),
            dma((count_second,)),
            dma((count_second,)),
        ],
        compiler_params=pltpu.CompilerParams(
            collective_id=1, has_side_effects=True, vmem_limit_bytes=60 * 1024 * 1024
        ),
    )(
        slot_anchor,
        root_density,
        jnp.asarray(strip_eig[:, None], F32),
        jnp.asarray(eig[None, :], F32),
        jnp.asarray(eig[:, None], F32),
        jnp.asarray(vectors, F32),
        jnp.stack(halves(jnp.asarray(basis.T, F32))),
        jnp.concatenate([mix_high, mix_low, mix_high], axis=2),
        jnp.asarray(angles, F32),
        strip_wide,
        unstrip_wide,
        wave_halves,
        density,
    )
    high = wave_halves[0].reshape(wave, tiles, LANES)
    low = wave_halves[1].reshape(wave, tiles, LANES)
    top = jnp.concatenate([high, low], axis=2)
    bottom = jnp.concatenate([high, jnp.zeros_like(low)], axis=2)
    inverse = jnp.concatenate([top, bottom], axis=0).transpose(1, 0, 2)
    return uy, inverse, arrived, low_density, high_density


def local(root_density, subgrid_density, velocity, slot_anchor, slot_count, neighbour):
    per_device = subgrid_density.shape[0]
    side = EDGE * CELLS
    inner = CELLS * CELLS
    uy, inverse, patches, low_density, high_density = poisson(
        root_density, subgrid_density, slot_anchor
    )
    x_table, yz_table = patch_tables()
    smem = pl.BlockSpec(memory_space=pltpu.SMEM)
    slot_spec = lambda width: pl.BlockSpec((1, CELLS, width), lambda s: (s, 0, 0))
    vel_spec = pl.BlockSpec((3, 1, CELLS, inner), lambda s: (0, s, 0, 0))
    x_table = jnp.asarray(np.tile(x_table, (1, 3)), jnp.bfloat16)
    yz_table = jnp.asarray(yz_table, jnp.bfloat16)
    columns = yz_table.shape[1]
    planes, strip, wave = uy.shape
    planes //= per_device
    grid_spec = pl.BlockSpec((planes, strip, wave), lambda s: (s, 0, 0))
    potential, kicked, coarse_potential = pl.pallas_call(
        subgrid_kernel,
        grid=(per_device,),
        in_specs=[
            smem,
            smem,
            pl.BlockSpec(patches.shape, lambda s: (0, 0, 0, 0)),
            pl.BlockSpec(x_table.shape, lambda s: (0, 0)),
            pl.BlockSpec(yz_table.shape, lambda s: (0, 0)),
            slot_spec(inner),
            slot_spec(side),
            slot_spec(side),
            vel_spec,
            grid_spec,
            pl.BlockSpec(inverse.shape, lambda s: (0, 0, 0)),
        ],
        out_specs=[slot_spec(inner), vel_spec, grid_spec],
        out_shape=[
            jax.ShapeDtypeStruct(subgrid_density.shape, F32),
            jax.ShapeDtypeStruct(velocity.shape, F32),
            jax.ShapeDtypeStruct(uy.shape, F32),
        ],
        scratch_shapes=[
            pltpu.VMEM((per_device, 16, columns), F32),
            pltpu.VMEM((CELLS + 8, columns), F32),
            pltpu.VMEM((2, WIDE // LANES, CELLS + 16, LANES), F32),
            pltpu.VMEM((WIDE // LANES, CELLS, LANES), F32),
            pltpu.VMEM((planes * strip, 2 * wave), jnp.bfloat16),
        ],
        compiler_params=pltpu.CompilerParams(
            dimension_semantics=("arbitrary",), vmem_limit_bytes=60 * 1024 * 1024
        ),
    )(
        slot_count,
        neighbour,
        patches,
        x_table,
        yz_table,
        subgrid_density,
        low_density,
        high_density,
        velocity,
        uy,
        inverse,
    )
    return (coarse_potential, potential, kicked)


def solution(mesh):
    return jax.shard_map(
        local,
        mesh=mesh,
        in_specs=(
            P("px", "py", None),
            P(("px", "py"), None, None),
            P(None, ("px", "py"), None, None),
            P(),
            P(),
            P(),
        ),
        out_specs=(
            P("px", "py", None),
            P(("px", "py"), None, None),
            P(None, ("px", "py"), None, None),
        ),
        check_vma=False,
    )
```
